64 devices in a mesh: dp: 4 (over x, y), cp: 16 (over z, core).
Axes of the slice: x: 2, y: 2, z: 8, core: 2. Of those that a mesh axis runs over, the one named last changes fastest.
The devices are a block of a 4x4x8 slice.
Arguments:
- x_act: bfloat16 [4, 2048, 2048], P('dp', 'cp'), parts along dimension 0
- d_out: bfloat16 [4, 2048, 2048], P('dp', 'cp'), parts along dimension 0
- positions: int32 [4, 2048], P('dp', 'cp'), parts along dimension 0
- ln_gain: float32 [2048], replicated
- ln_bias: float32 [2048], replicated
- w_query: bfloat16 [2048, 32, 64], replicated
- w_key: bfloat16 [2048, 8, 64], replicated
- w_value: bfloat16 [2048, 8, 64], replicated
- w_out: bfloat16 [2048, 2048], replicated
Outputs:
- output 1: bfloat16 [4, 2048, 2048], P('dp', 'cp'), parts along dimension 0
- output 2: bfloat16 [4, 2048, 2048], P('dp', 'cp'), parts along dimension 0
- output 3: float32 [8192, 32, 64], P(('dp', 'cp')), parts along dimension 0
- output 4: float32 [8192, 8, 64], P(('dp', 'cp')), parts along dimension 0
- output 5: float32 [8192, 8, 64], P(('dp', 'cp')), parts along dimension 0
- output 6: float32 [8192, 2048], P(('dp', 'cp')), parts along dimension 0
- output 7: float32 [8192], P('dp'), parts along dimension 0
- output 8: float32 [8192], P('dp'), parts along dimension 0
There are 4 independent parts. The reference program is written for one: setup_inputs(seed, part) draws one part's arguments, and reference() takes and returns one part's arrays. A program takes and returns all parts, laid end to end along the dimension named above; an argument that names none is the same for every part.
All inputs are finite; a program needn't handle non-finite values.
Results may differ from the reference program's by a relative error of at most 0.00648291.
Values are sent between devices in bfloat16 or wider.
A program may use at most 768 MiB of HBM per device.

```python
import math
import jax
import jax.numpy as jnp
from jax import lax

BATCH = 1
SEQ = 2048
WIDTH = 2048
Q_HEADS = 32
KV_HEADS = 8
HEAD_DIM = 64
Q_TILE = 128
TOKEN_KINDS = 64
DOC_SPAN = 128
GROUPS = Q_HEADS // KV_HEADS
EPS = 1e-5
ROPE_BASE = 10000.0


def setup_inputs(seed: int = 0, part: int = 0) -> dict:
    part_keys = jax.random.split(jax.random.fold_in(jax.random.key(seed), part), 5)
    shared_keys = jax.random.split(jax.random.key(seed + 1), 6)
    tokens = jax.random.randint(part_keys[0], (BATCH, SEQ), 0, TOKEN_KINDS)
    token_table = jax.random.normal(part_keys[1], (TOKEN_KINDS, WIDTH), jnp.float32)
    noise_draw = jax.random.normal(part_keys[2], (BATCH, SEQ, WIDTH), jnp.float32)
    x_act = (token_table[tokens] + 0.5 * noise_draw).astype(jnp.bfloat16)
    d_out = jax.random.normal(part_keys[3], (BATCH, SEQ, WIDTH), jnp.float32).astype(jnp.bfloat16)
    doc_flags = jax.random.randint(part_keys[4], (BATCH, SEQ), 0, DOC_SPAN) == 0
    seq_index = jnp.arange(SEQ, dtype=jnp.int32)
    starts = jnp.where(doc_flags, seq_index[None, :], 0)
    positions = (seq_index[None, :] - lax.cummax(starts, axis=1)).astype(jnp.int32)
    fan_in = WIDTH ** -0.5
    w_query = jax.random.normal(shared_keys[0], (WIDTH, Q_HEADS, HEAD_DIM), jnp.float32) * fan_in
    key_noise = jax.random.normal(shared_keys[1], (WIDTH, KV_HEADS, HEAD_DIM), jnp.float32) * fan_in
    w_key = 0.8 * w_query[:, ::GROUPS, :] + 0.6 * key_noise
    w_value = jax.random.normal(shared_keys[2], (WIDTH, KV_HEADS, HEAD_DIM), jnp.float32) * fan_in
    w_out = jax.random.normal(shared_keys[3], (Q_HEADS * HEAD_DIM, WIDTH), jnp.float32) * (Q_HEADS * HEAD_DIM) ** -0.5
    ln_gain = 0.3 * jax.random.normal(shared_keys[4], (WIDTH,), jnp.float32)
    ln_bias = 0.3 * jax.random.normal(shared_keys[5], (WIDTH,), jnp.float32)
    return {'x_act': x_act, 'd_out': d_out, 'positions': positions, 'ln_gain': ln_gain, 'ln_bias': ln_bias, 'w_query': w_query.astype(jnp.bfloat16), 'w_key': w_key.astype(jnp.bfloat16), 'w_value': w_value.astype(jnp.bfloat16), 'w_out': w_out.astype(jnp.bfloat16)}


def norm_forward(x_act, ln_gain, ln_bias):
    x_f32 = x_act.astype(jnp.float32)
    centered = x_f32 - jnp.mean(x_f32, axis=-1, keepdims=True)
    inv_std = lax.rsqrt(jnp.mean(centered * centered, axis=-1, keepdims=True) + EPS)
    x_hat = centered * inv_std
    return (x_hat * (1.0 + ln_gain) + ln_bias).astype(jnp.bfloat16), x_hat, inv_std


def norm_backward(grad_h, x_hat, inv_std, ln_gain):
    grad_hat = grad_h * (1.0 + ln_gain)
    mean_one = jnp.mean(grad_hat, axis=-1, keepdims=True)
    mean_two = jnp.mean(grad_hat * x_hat, axis=-1, keepdims=True)
    return inv_std * (grad_hat - mean_one - x_hat * mean_two)


def rope_tables(positions):
    quarter = HEAD_DIM // 4
    freq_tab = jnp.exp(jnp.arange(quarter, dtype=jnp.float32) * (-2.0 * math.log(ROPE_BASE) / (HEAD_DIM // 2)))
    angles = positions.astype(jnp.float32)[..., None] * freq_tab
    return jnp.cos(angles)[..., None, :], jnp.sin(angles)[..., None, :]


def rope_rotate(values, cos_tab, sin_tab):
    quarter = cos_tab.shape[-1]
    first_half = values[..., :quarter]
    second_half = values[..., quarter:2 * quarter]
    return jnp.concatenate([first_half * cos_tab - second_half * sin_tab, second_half * cos_tab + first_half * sin_tab, values[..., 2 * quarter:]], axis=-1)


def tile_probs(q_tile, key_f, q_first):
    scores = jnp.einsum('bqkgd,blkd->bkgql', q_tile, key_f) * (HEAD_DIM ** -0.5)
    q_index = q_first + jnp.arange(Q_TILE)
    k_index = jnp.arange(SEQ)
    scores = jnp.where(k_index[None, :] <= q_index[:, None], scores, -1e30)
    shifted = jnp.exp(scores - jnp.max(scores, axis=-1, keepdims=True))
    return shifted / jnp.sum(shifted, axis=-1, keepdims=True)


def attention_forward(q_grouped, key_f, value_f):
    def one_tile(tile_idx):
        q_first = tile_idx * Q_TILE
        q_tile = lax.dynamic_slice_in_dim(q_grouped, q_first, Q_TILE, axis=1)
        tile_prob = tile_probs(q_tile, key_f, q_first)
        prob_bf16 = tile_prob.astype(jnp.bfloat16).astype(jnp.float32)
        return jnp.einsum('bkgql,blkd->bqkgd', prob_bf16, value_f).astype(jnp.bfloat16)
    out_tiles = lax.map(one_tile, jnp.arange(SEQ // Q_TILE))
    return jnp.moveaxis(out_tiles, 0, 1).reshape(BATCH * SEQ, Q_HEADS * HEAD_DIM)


def attention_backward(q_grouped, key_f, value_f, grad_attn):
    def one_tile(acc_pair, tile_idx):
        grad_k, grad_v = acc_pair
        q_first = tile_idx * Q_TILE
        q_tile = lax.dynamic_slice_in_dim(q_grouped, q_first, Q_TILE, axis=1)
        ga_tile = lax.dynamic_slice_in_dim(grad_attn, q_first, Q_TILE, axis=1)
        tile_prob = tile_probs(q_tile, key_f, q_first)
        grad_prob = jnp.einsum('bqkgd,blkd->bkgql', ga_tile, value_f)
        row_dot = jnp.sum(tile_prob * grad_prob, axis=-1, keepdims=True)
        grad_score = (tile_prob * (grad_prob - row_dot) * (HEAD_DIM ** -0.5)).astype(jnp.bfloat16).astype(jnp.float32)
        grad_q = jnp.einsum('bkgql,blkd->bqkgd', grad_score, key_f)
        grad_k = grad_k + jnp.einsum('bkgql,bqkgd->blkd', grad_score, q_tile)
        prob_bf16 = tile_prob.astype(jnp.bfloat16).astype(jnp.float32)
        grad_v = grad_v + jnp.einsum('bkgql,bqkgd->blkd', prob_bf16, ga_tile)
        return (grad_k, grad_v), grad_q
    zero_acc = jnp.zeros((BATCH, SEQ, KV_HEADS, HEAD_DIM), jnp.float32)
    (grad_k, grad_v), q_tiles = lax.scan(one_tile, (zero_acc, zero_acc), jnp.arange(SEQ // Q_TILE))
    grad_q = jnp.moveaxis(q_tiles, 0, 1).reshape(BATCH, SEQ, Q_HEADS, HEAD_DIM)
    return grad_q, grad_k, grad_v


def reference(x_act, d_out, positions, ln_gain, ln_bias, w_query, w_key, w_value, w_out):
    n_tokens = BATCH * SEQ
    wq_flat = w_query.reshape(WIDTH, Q_HEADS * HEAD_DIM)
    wk_flat = w_key.reshape(WIDTH, KV_HEADS * HEAD_DIM)
    wv_flat = w_value.reshape(WIDTH, KV_HEADS * HEAD_DIM)
    normed, x_hat, inv_std = norm_forward(x_act, ln_gain, ln_bias)
    flat_h = normed.reshape(n_tokens, WIDTH)
    cos_tab, sin_tab = rope_tables(positions)
    q_act = rope_rotate(jnp.dot(flat_h, wq_flat, preferred_element_type=jnp.float32).reshape(BATCH, SEQ, Q_HEADS, HEAD_DIM), cos_tab, sin_tab).astype(jnp.bfloat16)
    k_act = rope_rotate(jnp.dot(flat_h, wk_flat, preferred_element_type=jnp.float32).reshape(BATCH, SEQ, KV_HEADS, HEAD_DIM), cos_tab, sin_tab).astype(jnp.bfloat16)
    v_act = jnp.dot(flat_h, wv_flat, preferred_element_type=jnp.float32).astype(jnp.bfloat16).reshape(BATCH, SEQ, KV_HEADS, HEAD_DIM)
    q_grouped = q_act.reshape(BATCH, SEQ, KV_HEADS, GROUPS, HEAD_DIM).astype(jnp.float32)
    key_f = k_act.astype(jnp.float32)
    value_f = v_act.astype(jnp.float32)
    attn_act = attention_forward(q_grouped, key_f, value_f)
    block_out = (x_act.astype(jnp.float32) + jnp.dot(attn_act, w_out, preferred_element_type=jnp.float32).reshape(BATCH, SEQ, WIDTH)).astype(jnp.bfloat16)
    grad_flat = d_out.reshape(n_tokens, WIDTH)
    grad_wo = jnp.dot(attn_act.T, grad_flat, preferred_element_type=jnp.float32)
    grad_attn = jnp.dot(grad_flat, w_out.T, preferred_element_type=jnp.float32).astype(jnp.bfloat16)
    grad_q, grad_k, grad_v = attention_backward(q_grouped, key_f, value_f, grad_attn.reshape(BATCH, SEQ, KV_HEADS, GROUPS, HEAD_DIM).astype(jnp.float32))
    grad_q_pre = rope_rotate(grad_q, cos_tab, -sin_tab).astype(jnp.bfloat16).reshape(n_tokens, Q_HEADS * HEAD_DIM)
    grad_k_pre = rope_rotate(grad_k, cos_tab, -sin_tab).astype(jnp.bfloat16).reshape(n_tokens, KV_HEADS * HEAD_DIM)
    grad_v_pre = grad_v.astype(jnp.bfloat16).reshape(n_tokens, KV_HEADS * HEAD_DIM)
    grad_h = (jnp.dot(grad_q_pre, wq_flat.T, preferred_element_type=jnp.float32) + jnp.dot(grad_k_pre, wk_flat.T, preferred_element_type=jnp.float32) + jnp.dot(grad_v_pre, wv_flat.T, preferred_element_type=jnp.float32)).reshape(BATCH, SEQ, WIDTH)
    grad_wq = jnp.dot(flat_h.T, grad_q_pre, preferred_element_type=jnp.float32).reshape(WIDTH, Q_HEADS, HEAD_DIM)
    grad_wk = jnp.dot(flat_h.T, grad_k_pre, preferred_element_type=jnp.float32).reshape(WIDTH, KV_HEADS, HEAD_DIM)
    grad_wv = jnp.dot(flat_h.T, grad_v_pre, preferred_element_type=jnp.float32).reshape(WIDTH, KV_HEADS, HEAD_DIM)
    grad_x = (d_out.astype(jnp.float32) + norm_backward(grad_h, x_hat, inv_std, ln_gain)).astype(jnp.bfloat16)
    grad_gain = jnp.sum(grad_h * x_hat, axis=(0, 1))
    grad_bias = jnp.sum(grad_h, axis=(0, 1))
    return (block_out, grad_x, grad_wq, grad_wk, grad_wv, grad_wo, grad_gain, grad_bias)
```

```python
import functools
import math

import jax
import jax.numpy as jnp
from jax import lax
from jax.experimental import pallas as pl
from jax.experimental.pallas import tpu as pltpu
from jax.sharding import PartitionSpec as P

EPS = 1e-5
ROPE_BASE = 10000.0
MESH = pl.DeviceIdType.MESH
BF = jnp.bfloat16
F32 = jnp.float32


def dot(lhs, rhs):
    return jnp.dot(lhs, rhs, preferred_element_type=F32)


def block_kernel(
    n_dev, hd, kv_w,
    x_hbm, dy_hbm, pos_ref, gain_ref, bias_ref, wq_hbm, wk_hbm, wv_hbm, wo_hbm,
    out_hbm, gx_hbm, gw_hbm, gwo_hbm, gg_hbm,
    hb, dyb, wt, wi_raw, wi, woi_raw, woi, pos_all, trig,
    qt, kvt, kv, bmat, bmat_t, sbuf, dpbuf, pds, dkv, dkvt, kv_rv, kv_mine,
    dwo, dwt, at_st, dqt_st, at_rv, dt_rv, a_nat, d_nat, x_v, dy_own, xhat, stat, dh, out_v, gg_st, gg_rv, gg_out,
    in_sem, wo_sem, w_sem, out_sem, loc_sem,
    hzs, hzr, hds, hdr, yzs, yzr, yds, ydr,
    pos_s, pos_r, a_s, a_r, q_s, q_r, x_s, x_r, kv_s, kv_r, w_s, w_r, wk_s, wk_r, g_s, g_r,
):
    tok, width = x_v.shape
    n_chip = n_dev // 2
    half = tok // 2
    me = lax.axis_index('cp')
    chip = me // 2
    core = me % 2
    right = 2 * ((chip + 1) % n_chip) + core
    left = 2 * ((chip + n_chip - 1) % n_chip) + core
    mate = 2 * chip + 1 - core
    q_rows = wq_hbm.shape[0]
    hw = 2 * hd
    quarter = hd // 4

    def remote(src, dst, send, recv, target):
        return pltpu.make_async_remote_copy(src_ref=src, dst_ref=dst, send_sem=send, recv_sem=recv, device_id={'cp': target}, device_id_type=MESH)

    def local(src, dst, sem):
        return pltpu.make_async_copy(src, dst, sem)

    load_x = local(x_hbm, x_v, in_sem.at[0])
    load_x.start()
    own_rows = pl.multiple_of(me * hw, hw)
    kv_rows = pl.multiple_of(chip * hd, hd)
    loads = [
        local(wq_hbm.at[pl.ds(own_rows, hw)], wi_raw.at[pl.ds(0, hw)], in_sem.at[1]),
        local(wk_hbm.at[pl.ds(kv_rows, hd)], wi_raw.at[pl.ds(hw, hd)], in_sem.at[2]),
        local(wv_hbm.at[pl.ds(kv_rows, hd)], wi_raw.at[pl.ds(hw + hd, hd)], in_sem.at[3]),
        local(wo_hbm.at[pl.ds(own_rows, hw)], woi_raw, in_sem.at[4]),
        local(dy_hbm, dyb.at[me], in_sem.at[5]),
        local(dy_hbm, dy_own, in_sem.at[6]),
    ]
    for item in loads:
        item.start()
    barrier = pltpu.get_barrier_semaphore()
    for step in range(1, n_dev):
        pl.semaphore_signal(barrier, inc=1, device_id={'cp': (me + step) % n_dev}, device_id_type=MESH)
    weight_loads = [
        local(wq_hbm, wt.at[pl.ds(0, q_rows)], w_sem.at[0]),
        local(wk_hbm, wt.at[pl.ds(q_rows, kv_w)], w_sem.at[1]),
        local(wv_hbm, wt.at[pl.ds(q_rows + kv_w, kv_w)], w_sem.at[2]),
    ]
    for item in weight_loads:
        item.start()

    load_x.wait()
    gain_one = 1.0 + gain_ref[...]
    x_f = x_v[...].astype(F32)
    centered = x_f - jnp.mean(x_f, axis=-1, keepdims=True)
    inv_std = lax.rsqrt(jnp.mean(centered * centered, axis=-1, keepdims=True) + EPS)
    x_hat = centered * inv_std
    xhat[...] = x_hat
    stat[...] = jnp.broadcast_to(inv_std, stat.shape)
    hb[me] = (x_hat * gain_one + bias_ref[...]).astype(BF)
    pos_all[me] = pos_ref[...]
    dkv[...] = jnp.zeros_like(dkv)
    dwo[...] = jnp.zeros_like(dwo)
    dwt[...] = jnp.zeros_like(dwt)
    bmat[...] = jnp.zeros_like(bmat)

    pl.semaphore_wait(barrier, n_dev - 1)

    def chunk(buf, slot, part):
        return buf.at[slot, pl.ds(pl.multiple_of(part * half, half), half)]

    def own_sends(buf, zs, zr, ds, dr):
        copies = []
        for part in range(2):
            piece = chunk(buf, me, part)
            copies.append(remote(piece, piece, zs.at[2 * part], zr.at[2 * part], right))
            copies.append(remote(piece, piece, zs.at[2 * part + 1], zr.at[2 * part + 1], left))
            copies.append(remote(piece, piece, ds.at[14 + part], dr.at[14 + part], mate))
        return copies

    def event_place(event, parity):
        step = event // 4 + 1
        turn = event % 4
        direction = turn % 2
        part = jnp.where(step < 4, turn // 2, turn)
        origin = jnp.where(direction == 0, chip + n_chip - step, chip + step) % n_chip
        return step, turn, direction, part, 2 * origin + parity

    def ring_event(buf, zs, zr, ds, dr, event):
        step, turn, direction, part, slot = event_place(event, core)
        piece = chunk(buf, slot, part)
        remote(piece, piece, zs.at[0], zr.at[event], right).wait_recv()
        onward = jnp.where(step < 3, event + 4, jnp.where(turn == 0, 12, 13))

        @pl.when((step < 3) | ((step == 3) & ((turn == 0) | (turn == 3))))
        def _():
            remote(piece, piece, zs.at[event + 4], zr.at[onward], jnp.where(direction == 0, right, left)).start()

        remote(piece, piece, ds.at[event], dr.at[event], mate).start()

    def ring_service(buf, zs, zr, ds, dr, k):
        @pl.when(k < 2)
        def _():
            ring_event(buf, zs, zr, ds, dr, 2 * k)
            ring_event(buf, zs, zr, ds, dr, 2 * k + 1)

        @pl.when((k >= 2) & (k < 12))
        def _():
            ring_event(buf, zs, zr, ds, dr, k + 2)

    def ring_slot(buf, ds, dr, k):
        turn = jnp.maximum(k - 2, 0)
        step = turn // 4 + 1
        way = turn % 4
        direction = way // 2
        other = jnp.where(k < 2, k, way % 2)
        origin = jnp.where(direction == 0, chip + n_chip - step, chip + step) % n_chip
        slot = 2 * jnp.where(k < 2, chip, origin) + jnp.where(other == 1, 1 - core, core)

        @pl.when(other == 1)
        def _():
            first = jnp.where(k < 2, 14, jnp.where(step < 4, 4 * (step - 1) + direction, 12))
            second = jnp.where(k < 2, 15, jnp.where(step < 4, 4 * (step - 1) + 2 + direction, 13))
            for part, event in ((0, first), (1, second)):
                piece = chunk(buf, slot, part)
                remote(piece, piece, ds.at[0], dr.at[event], mate).wait_recv()

        return slot

    h_sends = own_sends(hb, hzs, hzr, hds, hdr)
    for item in h_sends:
        item.start()
    pos_sends = [remote(pos_all.at[me], pos_all.at[me], pos_s.at[step], pos_r.at[step], (me + step) % n_dev) for step in range(1, n_dev)]
    for item in pos_sends:
        item.start()

    for item in loads:
        item.wait()
    for t in range(width // 128):
        cols = slice(128 * t, 128 * t + 128)
        wi[cols, 0:hw] = wi_raw[0:hw, cols].T
        wi[cols, hw:2 * hw] = wi_raw[hw:2 * hw, cols].T
        woi[cols, :] = woi_raw[:, cols].T

    freq = jnp.exp(lax.broadcasted_iota(jnp.int32, (quarter, tok), 0).astype(F32) * (-2.0 * math.log(ROPE_BASE) / (hd // 2)))

    def make_trig(slot):
        angle = pos_all[slot].astype(F32) * freq
        trig[slot, 0:quarter, :] = jnp.cos(angle)
        trig[slot, quarter:2 * quarter, :] = jnp.sin(angle)

    make_trig(me)
    for step in range(1, n_dev):
        source = (me + n_dev - step) % n_dev
        remote(pos_all.at[source], pos_all.at[source], pos_s.at[step], pos_r.at[step], me).wait_recv()
        make_trig(source)

    y_sends = own_sends(dyb, yzs, yzr, yds, ydr)

    @pl.loop(0, n_dev)
    def _(k):
        ring_service(hb, hzs, hzr, hds, hdr, k)

        @pl.when(k == 10)
        def _():
            for item in y_sends:
                item.start()

        slot = ring_slot(hb, hds, hdr, k)
        flat = dot(hb[slot], wi[...])
        q_f = flat[:, 0:hw].T
        kv_f = flat[:, hw:2 * hw].T
        cos_t = trig[slot, 0:quarter, :]
        sin_t = trig[slot, quarter:2 * quarter, :]

        def turned(val, base):
            u = val[base:base + quarter]
            w = val[base + quarter:base + 2 * quarter]
            return [u * cos_t - w * sin_t, w * cos_t + u * sin_t, val[base + 2 * quarter:base + hd]]

        for head in range(2):
            qt[slot, :, tok * head:tok * head + tok] = jnp.concatenate(turned(q_f, hd * head), axis=0).astype(BF)
        kv_rot = jnp.concatenate(turned(kv_f, 0) + [kv_f[hd:2 * hd]], axis=0).astype(BF)
        place = pl.ds(pl.multiple_of(slot * tok, tok), tok)
        kvt[:, place] = kv_rot
        kv[place, :] = kv_rot.T

    chunk_k = 2 * tok
    scale = hd ** -0.5

    @pl.loop(0, n_dev)
    def _(k):
        ring_service(dyb, yzs, yzr, yds, ydr, k)
        slot = ring_slot(dyb, yds, ydr, k)
        da = dot(dyb[slot], woi[...]).astype(BF)
        da_t = da.T
        bmat[0:hd, 0:2 * tok] = qt[slot]
        bmat[hd:2 * hd, 2 * tok:3 * tok] = da_t[0:hd]
        bmat[hd:2 * hd, 3 * tok:4 * tok] = da_t[hd:2 * hd]
        for t in range(4):
            bmat_t[tok * t:tok * t + tok, :] = bmat[:, tok * t:tok * t + tok].T
        n_chunks = slot // 2 + 1
        q_index = slot * tok + lax.broadcasted_iota(jnp.int32, (chunk_k, 2 * tok), 1) % tok
        k_row = lax.broadcasted_iota(jnp.int32, (chunk_k, 2 * tok), 0)

        def scores(c, top):
            rows = pl.ds(pl.multiple_of(c * chunk_k, chunk_k), chunk_k)
            both = dot(kv[rows, :], bmat[...])
            s = jnp.where(k_row + c * chunk_k <= q_index, both[:, 0:2 * tok] * scale, -1e30)
            sbuf[rows, :] = s
            dpbuf[rows, :] = both[:, 2 * tok:4 * tok]
            return jnp.maximum(top, jnp.max(s, axis=0, keepdims=True))

        top = lax.fori_loop(0, n_chunks, scores, jnp.full((1, 2 * tok), -3e38, F32))

        def exps(c, sums):
            rows = pl.ds(pl.multiple_of(c * chunk_k, chunk_k), chunk_k)
            p = jnp.exp(sbuf[rows, :] - top)
            sbuf[rows, :] = p
            return sums[0] + jnp.sum(p, axis=0, keepdims=True), sums[1] + jnp.sum(p * dpbuf[rows, :], axis=0, keepdims=True)

        zero_row = jnp.zeros((1, 2 * tok), F32)
        total, weighted = lax.fori_loop(0, n_chunks, exps, (zero_row, zero_row))
        inv = 1.0 / total
        row_dot = weighted * inv

        def grads(c, acc):
            rows = pl.ds(pl.multiple_of(c * chunk_k, chunk_k), chunk_k)
            p = sbuf[rows, :] * inv
            p_b = p.astype(BF)
            ds_b = (p * (dpbuf[rows, :] - row_dot) * scale).astype(BF)
            pds[:, 0:2 * tok] = ds_b
            pds[:, 2 * tok:4 * tok] = p_b
            dkv[rows, :] += dot(pds[...], bmat_t[...])
            return acc[0] + dot(kvt[hd:2 * hd, rows], p_b), acc[1] + dot(kvt[0:hd, rows], ds_b)

        zero_acc = jnp.zeros((hd, 2 * tok), F32)
        a_acc, dq_acc = lax.fori_loop(0, n_chunks, grads, (zero_acc, zero_acc))
        a_t = jnp.concatenate([a_acc[:, 0:tok], a_acc[:, tok:2 * tok]], axis=0).astype(BF)
        cos_t = trig[slot, 0:quarter, :]
        sin_t = trig[slot, quarter:2 * quarter, :]
        parts = []
        for head in range(2):
            u = dq_acc[0:quarter, tok * head:tok * head + tok]
            w = dq_acc[quarter:2 * quarter, tok * head:tok * head + tok]
            parts += [u * cos_t + w * sin_t, w * cos_t - u * sin_t, dq_acc[2 * quarter:hd, tok * head:tok * head + tok]]
        dq_t = jnp.concatenate(parts, axis=0).astype(BF)
        at_st[slot] = a_t
        dqt_st[slot] = dq_t

        @pl.when(slot == me)
        def _():
            at_rv[pl.ds(own_rows, hw), :] = a_t
            dt_rv[pl.ds(own_rows, hw), :] = dq_t

        @pl.when(slot != me)
        def _():
            remote(dqt_st.at[slot], dt_rv.at[pl.ds(own_rows, hw)], q_s.at[slot], q_r.at[me], slot).start()
            remote(at_st.at[slot], at_rv.at[pl.ds(own_rows, hw)], a_s.at[slot], a_r.at[me], slot).start()

        for t in range(width // 256):
            cols = slice(256 * t, 256 * t + 256)
            dwo[:, cols] += dot(a_t, dyb[slot, :, cols])
            dwt[0:hw, cols] += dot(dq_t, hb[slot, :, cols])

    for t in range(n_dev):
        dkvt[:, tok * t:tok * t + tok] = dkv[tok * t:tok * t + tok, :].T
    mine = pl.multiple_of(core * hd, hd)
    theirs = pl.multiple_of((1 - core) * hd, hd)
    swap = remote(dkvt.at[pl.ds(theirs, hd)], kv_rv, x_s, x_r, mate)
    swap.start()
    store_wo = local(dwo, gwo_hbm, out_sem.at[0])
    store_wo.start()

    def send_order():
        order = []
        for step in range(1, n_chip // 2 + 1):
            order += [step, n_chip - step] if 2 * step < n_chip else [step]
        return [(chip + step) % n_chip for step in order]

    targets = [mate] + [2 * far + c for far in send_order() for c in range(2)]

    swap.wait_recv()
    for t in range(n_dev):
        cols = slice(tok * t, tok * t + tok)
        g = dkvt[pl.ds(mine, hd), cols] + kv_rv[:, cols]
        cos_t = jnp.where(core == 0, trig[t, 0:quarter, :], 1.0)
        sin_t = jnp.where(core == 0, trig[t, quarter:2 * quarter, :], 0.0)
        u = g[0:quarter]
        w = g[quarter:2 * quarter]
        kv_mine[t] = jnp.concatenate([u * cos_t + w * sin_t, w * cos_t - u * sin_t, g[2 * quarter:hd]], axis=0).astype(BF)
    g_rows = pl.multiple_of(q_rows + core * kv_w + chip * hd, hd)
    dt_rv[pl.ds(g_rows, hd), :] = kv_mine[me]
    kv_sends = [remote(kv_mine.at[t], dt_rv.at[pl.ds(g_rows, hd)], kv_s.at[t], kv_r.at[me], t) for t in targets]
    for item in kv_sends:
        item.start()

    def block_cols(t):
        return pl.ds(pl.multiple_of(t * tok, tok), tok)

    w_own = local(dwt.at[pl.ds(0, hw), block_cols(me)], gw_hbm.at[pl.ds(own_rows, hw)], loc_sem.at[0])
    w_own.start()
    w_sends = [remote(dwt.at[pl.ds(0, hw), block_cols(t)], gw_hbm.at[pl.ds(own_rows, hw)], w_s.at[t], w_r.at[me], t) for t in targets]
    for item in w_sends:
        item.start()

    for t in range(width // 256):
        cols = slice(256 * t, 256 * t + 256)
        acc = jnp.zeros((hd, 256), F32)
        for s in range(0, n_dev):
            acc += dot(kv_mine[s], hb[s, :, cols])
        dwt[hw:hw + hd, cols] = acc
    wk_own = local(dwt.at[pl.ds(hw, hd), block_cols(me)], gw_hbm.at[pl.ds(g_rows, hd)], loc_sem.at[1])
    wk_own.start()

    def event_forwarded(event):
        return event < 8 or event in (8, 11)

    def finish_ring(buf, zs, zr, ds, dr):
        for item in own_sends(buf, zs, zr, ds, dr):
            item.wait_send()
        for event in range(14):
            _, _, direction, part, slot = event_place(event, core)
            piece = chunk(buf, slot, part)
            if event_forwarded(event):
                remote(piece, piece, zs.at[event + 4], zr.at[event], right).wait_send()
            remote(piece, piece, ds.at[event], dr.at[event], mate).wait_send()

    finish_ring(dyb, yzs, yzr, yds, ydr)
    wo_loads = [local(wo_hbm.at[pl.ds(tok * t, tok)], dyb.at[t], wo_sem.at[t]) for t in range(n_dev)]
    for item in wo_loads:
        item.start()

    for t in targets:
        rows = pl.ds(pl.multiple_of(t * hw, hw), hw)
        remote(at_st.at[0], at_rv.at[rows], a_s.at[t], a_r.at[t], t).wait_recv()
    for t in range(n_dev):
        a_nat[:, 128 * t:128 * t + 128] = at_rv[128 * t:128 * t + 128, :].T
    for item in wo_loads:
        item.wait()
    for t in range(width // 256):
        cols = slice(256 * t, 256 * t + 256)
        acc = x_v[:, cols].astype(F32)
        prod = jnp.zeros((tok, 256), F32)
        for s in range(n_dev):
            prod += dot(a_nat[:, 128 * s:128 * s + 128], dyb[s, :, cols])
        out_v[:, cols] = (acc + prod).astype(BF)
    store_out = local(out_v, out_hbm, out_sem.at[1])
    store_out.start()

    for item in weight_loads:
        item.wait()
    for t in targets:
        rows = pl.ds(pl.multiple_of(t * hw, hw), hw)
        remote(dqt_st.at[0], dt_rv.at[rows], q_s.at[t], q_r.at[t], t).wait_recv()
        rows = pl.ds(pl.multiple_of(q_rows + (t % 2) * kv_w + (t // 2) * hd, hd), hd)
        remote(kv_mine.at[0], dt_rv.at[rows], kv_s.at[t], kv_r.at[t], t).wait_recv()
    n_rows = q_rows + 2 * kv_w
    for t in range(n_rows // 128):
        d_nat[:, 128 * t:128 * t + 128] = dt_rv[128 * t:128 * t + 128, :].T

    for t in range(width // 256):
        cols = slice(256 * t, 256 * t + 256)
        acc = jnp.zeros((tok, 256), F32)
        for s in range(n_rows // 256):
            acc += dot(d_nat[:, 256 * s:256 * s + 256], wt[256 * s:256 * s + 256, cols])
        dh[:, cols] = acc
        gg_st[0:1, cols] = jnp.sum(acc * xhat[:, cols], axis=0, keepdims=True)
        gg_st[1:2, cols] = jnp.sum(acc, axis=0, keepdims=True)
    gg_rv[me] = gg_st[...]
    g_sends = [remote(gg_st, gg_rv.at[me], g_s.at[t], g_r.at[me], t) for t in targets]
    for item in g_sends:
        item.start()
    wk_sends = [remote(dwt.at[pl.ds(hw, hd), block_cols(t)], gw_hbm.at[pl.ds(g_rows, hd)], wk_s.at[t], wk_r.at[me], t) for t in targets]
    for item in wk_sends:
        item.start()

    grad_hat = dh[...] * gain_one
    x_hat = xhat[...]
    mean_one = jnp.mean(grad_hat, axis=-1, keepdims=True)
    mean_two = jnp.mean(grad_hat * x_hat, axis=-1, keepdims=True)
    store_out.wait()
    out_v[...] = (dy_own[...].astype(F32) + stat[:, 0:1] * (grad_hat - mean_one - x_hat * mean_two)).astype(BF)
    store_gx = local(out_v, gx_hbm, out_sem.at[2])
    store_gx.start()

    for t in targets:
        remote(gg_st, gg_rv.at[t], g_s.at[t], g_r.at[t], t).wait_recv()
    sums = gg_rv[0]
    for t in range(1, n_dev):
        sums = sums + gg_rv[t]
    gg_out[...] = sums
    store_gg = local(gg_out, gg_hbm, out_sem.at[3])
    store_gg.start()

    finish_ring(hb, hzs, hzr, hds, hdr)
    for item in pos_sends:
        item.wait_send()
    for t in targets:
        remote(at_st.at[0], at_rv.at[pl.ds(0, hw)], a_s.at[t], a_r.at[t], t).wait_send()
        remote(dqt_st.at[0], dt_rv.at[pl.ds(0, hw)], q_s.at[t], q_r.at[t], t).wait_send()
    swap.wait_send()
    for item in kv_sends + w_sends + g_sends + wk_sends:
        item.wait_send()
    for t in targets:
        rows = pl.ds(pl.multiple_of(t * hw, hw), hw)
        remote(dwt.at[pl.ds(0, hw), block_cols(t)], gw_hbm.at[rows], w_s.at[t], w_r.at[t], t).wait_recv()
        rows = pl.ds(pl.multiple_of(q_rows + (t % 2) * kv_w + (t // 2) * hd, hd), hd)
        remote(dwt.at[pl.ds(hw, hd), block_cols(t)], gw_hbm.at[rows], wk_s.at[t], wk_r.at[t], t).wait_recv()
    for item in (w_own, wk_own, store_wo, store_gx, store_gg):
        item.wait()


def solution(mesh):
    n_dev = mesh.shape['cp']

    def device_step(x_act, d_out, positions, ln_gain, ln_bias, w_query, w_key, w_value, w_out):
        tok, width = x_act.shape[1], x_act.shape[2]
        q_heads, hd = w_query.shape[1], w_query.shape[2]
        kv_heads = w_key.shape[1]
        q_w, kv_w = q_heads * hd, kv_heads * hd
        n_rows = q_w + 2 * kv_w
        seq = n_dev * tok
        hw = 2 * hd

        def flat_weight(w):
            return jnp.transpose(w, (1, 2, 0)).reshape(-1, width)

        hbm = pl.BlockSpec(memory_space=pltpu.HBM)
        vmem = pl.BlockSpec(memory_space=pltpu.VMEM)
        dma = pltpu.SemaphoreType.DMA
        scratch = [
            pltpu.VMEM((n_dev, tok, width), BF),
            pltpu.VMEM((n_dev, tok, width), BF),
            pltpu.VMEM((n_rows, width), BF),
            pltpu.VMEM((2 * hw, width), BF),
            pltpu.VMEM((width, 2 * hw), BF),
            pltpu.VMEM((hw, width), BF),
            pltpu.VMEM((width, hw), BF),
            pltpu.VMEM((n_dev, 1, tok), jnp.int32),
            pltpu.VMEM((n_dev, hd // 2, tok), F32),
            pltpu.VMEM((n_dev, hd, 2 * tok), BF),
            pltpu.VMEM((hw, seq), BF),
            pltpu.VMEM((seq, hw), BF),
            pltpu.VMEM((hw, 4 * tok), BF),
            pltpu.VMEM((4 * tok, hw), BF),
            pltpu.VMEM((seq, 2 * tok), F32),
            pltpu.VMEM((seq, 2 * tok), F32),
            pltpu.VMEM((2 * tok, 4 * tok), BF),
            pltpu.VMEM((seq, hw), F32),
            pltpu.VMEM((hw, seq), F32),
            pltpu.VMEM((hd, seq), F32),
            pltpu.VMEM((n_dev, hd, tok), BF),
            pltpu.VMEM((hw, width), F32),
            pltpu.VMEM((hw + hd, width), F32),
            pltpu.VMEM((n_dev, hw, tok), BF),
            pltpu.VMEM((n_dev, hw, tok), BF),
            pltpu.VMEM((q_w, tok), BF),
            pltpu.VMEM((n_rows, tok), BF),
            pltpu.VMEM((tok, q_w), BF),
            pltpu.VMEM((tok, n_rows), BF),
            pltpu.VMEM((tok, width), BF),
            pltpu.VMEM((tok, width), BF),
            pltpu.VMEM((tok, width), F32),
            pltpu.VMEM((tok, 128), F32),
            pltpu.VMEM((tok, width), F32),
            pltpu.VMEM((tok, width), BF),
            pltpu.VMEM((2, width), F32),
            pltpu.VMEM((n_dev, 2, width), F32),
            pltpu.VMEM((2, width), F32),
            dma((7,)), dma((n_dev,)), dma((3,)), dma((4,)), dma((2,)),
            dma((16,)), dma((14,)), dma((16,)), dma((16,)),
            dma((16,)), dma((14,)), dma((16,)), dma((16,)),
            dma((n_dev,)), dma((n_dev,)),
            dma((n_dev,)), dma((n_dev,)),
            dma((n_dev,)), dma((n_dev,)),
            dma, dma,
            dma((n_dev,)), dma((n_dev,)),
            dma((n_dev,)), dma((n_dev,)),
            dma((n_dev,)), dma((n_dev,)),
            dma((n_dev,)), dma((n_dev,)),
        ]
        out, gx, gw, gwo, gg = pl.pallas_call(
            functools.partial(block_kernel, n_dev, hd, kv_w),
            out_shape=(
                jax.ShapeDtypeStruct((tok, width), BF),
                jax.ShapeDtypeStruct((tok, width), BF),
                jax.ShapeDtypeStruct((n_rows, tok), F32),
                jax.ShapeDtypeStruct((hw, width), F32),
                jax.ShapeDtypeStruct((2, width), F32),
            ),
            in_specs=[hbm, hbm, vmem, vmem, vmem, hbm, hbm, hbm, hbm],
            out_specs=(hbm,) * 5,
            scratch_shapes=scratch,
            compiler_params=pltpu.CompilerParams(collective_id=0, has_side_effects=True, vmem_limit_bytes=67043328),
            name='attn_block',
        )(
            x_act.reshape(tok, width), d_out.reshape(tok, width), positions.reshape(1, tok),
            ln_gain.reshape(1, width), ln_bias.reshape(1, width),
            flat_weight(w_query), flat_weight(w_key), flat_weight(w_value), w_out,
        )

        def rows_out(block, heads):
            return jnp.transpose(block.reshape(heads, hd, tok), (2, 0, 1))

        return (
            out.reshape(1, tok, width), gx.reshape(1, tok, width),
            rows_out(gw[0:q_w], q_heads), rows_out(gw[q_w:q_w + kv_w], kv_heads), rows_out(gw[q_w + kv_w:], kv_heads),
            gwo, gg[0], gg[1],
        )

    return jax.shard_map(device_step, mesh=mesh, in_specs=(P('dp', 'cp', None), P('dp', 'cp', None), P('dp', 'cp'), P(None), P(None), P(None, None, None), P(None, None, None), P(None, None, None), P(None, None)), out_specs=(P('dp', 'cp', None), P('dp', 'cp', None), P(('dp', 'cp'), None, None), P(('dp', 'cp'), None, None), P(('dp', 'cp'), None, None), P(('dp', 'cp'), None), P('dp'), P('dp')), check_vma=False)
```

```python
import functools
import math

import jax
import jax.numpy as jnp
from jax import lax
from jax.experimental import pallas as pl
from jax.experimental.pallas import tpu as pltpu
from jax.sharding import PartitionSpec as P

EPS = 1e-5
ROPE_BASE = 10000.0
MESH = pl.DeviceIdType.MESH
BF = jnp.bfloat16
F32 = jnp.float32
EARLY = 4


def dot(lhs, rhs):
    return jnp.dot(lhs, rhs, preferred_element_type=F32)


def block_kernel(
    n_dev, hd, kv_w, early,
    x_hbm, dy_hbm, pos_ref, gain_ref, bias_ref, wq_hbm, wk_hbm, wv_hbm, wo_hbm,
    out_hbm, gx_hbm, gw_hbm, gwo_hbm, gg_hbm,
    hb, dyb, wt, wi_raw, wi, woi_raw, woi, pos_all, trig,
    qt, kvt, kv, bmat, bmat_t, sbuf, dpbuf, mbuf, adq, dkv, dkvt, kv_rv, kv_mine, kv_row,
    dwo, dwt, at_st, dqt_st, at_rv, dt_rv, a_nat, d_nat, x_v, dy_own, xhat, stat, dh, out_v, gg_st, gg_mx, gg_my, gg_rv, gg_out,
    in_sem, wo_sem, w_sem, out_sem, loc_sem,
    hzs, hzr, hds, hdr, yzs, yzr, yds, ydr,
    pos_s, pos_r, a_s, a_r, q_s, q_r, x_s, x_r, kv_s, kv_r, w_s, w_r, wk_s, wk_r, g_s, g_r,
):
    tok, width = x_v.shape
    n_chip = n_dev // 2
    half = tok // 2
    pair = 2 * tok
    me = lax.axis_index('cp')
    chip = me // 2
    core = me % 2
    right = 2 * ((chip + 1) % n_chip) + core
    left = 2 * ((chip + n_chip - 1) % n_chip) + core
    mate = 2 * chip + 1 - core
    q_rows = wq_hbm.shape[0]
    n_rows = q_rows + 2 * kv_w
    hw = 2 * hd
    quarter = hd // 4
    tile = 256

    def remote(src, dst, send, recv, target):
        return pltpu.make_async_remote_copy(src_ref=src, dst_ref=dst, send_sem=send, recv_sem=recv, device_id={'cp': target}, device_id_type=MESH)

    def local(src, dst, sem):
        return pltpu.make_async_copy(src, dst, sem)

    def part_of(i, size):
        return pl.ds(pl.multiple_of(i * size, size), size)

    load_x = local(x_hbm, x_v, in_sem.at[0])
    load_x.start()
    own_rows = part_of(me, hw)
    kv_rows = part_of(chip, hd)
    loads = [
        local(wq_hbm.at[own_rows], wi_raw.at[pl.ds(0, hw)], in_sem.at[1]),
        local(wk_hbm.at[kv_rows], wi_raw.at[pl.ds(hw, hd)], in_sem.at[2]),
        local(wv_hbm.at[kv_rows], wi_raw.at[pl.ds(hw + hd, hd)], in_sem.at[3]),
        local(wo_hbm.at[own_rows], woi_raw, in_sem.at[4]),
        local(dy_hbm, dyb.at[chip, part_of(core, tok)], in_sem.at[5]),
        local(dy_hbm, dy_own, in_sem.at[6]),
    ]
    for item in loads:
        item.start()
    barrier = pltpu.get_barrier_semaphore()
    for step in range(1, n_dev):
        pl.semaphore_signal(barrier, inc=1, device_id={'cp': (me + step) % n_dev}, device_id_type=MESH)

    load_x.wait()
    gain_one = 1.0 + gain_ref[...]
    x_f = x_v[...].astype(F32)
    centered = x_f - jnp.mean(x_f, axis=-1, keepdims=True)
    inv_std = lax.rsqrt(jnp.mean(centered * centered, axis=-1, keepdims=True) + EPS)
    x_hat = centered * inv_std
    hb[chip, part_of(core, tok), :] = (x_hat * gain_one + bias_ref[...]).astype(BF)
    xhat[...] = x_hat
    stat[...] = jnp.broadcast_to(inv_std, stat.shape)
    pos_all[me] = pos_ref[...]

    pl.semaphore_wait(barrier, n_dev - 1)

    def chunk(buf, origin, parity, part):
        return buf.at[origin, part_of(2 * parity + part, half)]

    def own_sends(buf, zs, zr, ds, dr):
        copies = []
        for part in range(2):
            piece = chunk(buf, chip, core, part)
            copies.append(remote(piece, piece, zs.at[2 * part], zr.at[2 * part], right))
            copies.append(remote(piece, piece, zs.at[2 * part + 1], zr.at[2 * part + 1], left))
            copies.append(remote(piece, piece, ds.at[14 + part], dr.at[14 + part], mate))
        return copies

    def event_place(event):
        step = event // 4 + 1
        turn = event % 4
        direction = turn % 2
        part = jnp.where(step < 4, turn // 2, turn)
        origin = jnp.where(direction == 0, chip + n_chip - step, chip + step) % n_chip
        return step, turn, direction, part, origin

    def ring_event(ring, event):
        buf, zs, zr, ds, dr = ring
        step, turn, direction, part, origin = event_place(event)
        piece = chunk(buf, origin, core, part)
        remote(piece, piece, zs.at[0], zr.at[event], right).wait_recv()
        onward = jnp.where(step < 3, event + 4, jnp.where(turn == 0, 12, 13))

        @pl.when((step < 3) | ((step == 3) & ((turn == 0) | (turn == 3))))
        def _():
            remote(piece, piece, zs.at[event + 4], zr.at[onward], jnp.where(direction == 0, right, left)).start()

        remote(piece, piece, ds.at[event], dr.at[event], mate).start()

    def ring_service(ring, event):
        @pl.when(event < 14)
        def _():
            ring_event(ring, event)

    def ring_origin(k):
        step = (k + 1) // 2
        return jnp.where(k % 2 == 1, chip + n_chip - step, chip + step) % n_chip

    def ring_mate(ring, k, origin):
        buf, zs, zr, ds, dr = ring
        step = (k + 1) // 2
        direction = (k + 1) % 2
        first = jnp.where(k == 0, 14, jnp.where(step < 4, 4 * (step - 1) + direction, 12))
        second = jnp.where(k == 0, 15, jnp.where(step < 4, 4 * (step - 1) + 2 + direction, 13))
        for part, event in ((0, first), (1, second)):
            piece = chunk(buf, origin, 1 - core, part)
            remote(piece, piece, ds.at[0], dr.at[event], mate).wait_recv()

    def finish_ring(ring):
        buf, zs, zr, ds, dr = ring
        for item in own_sends(buf, zs, zr, ds, dr):
            item.wait_send()
        for event in range(14):
            _, _, _, part, origin = event_place(event)
            piece = chunk(buf, origin, core, part)
            if event < 8 or event in (8, 11):
                remote(piece, piece, zs.at[event + 4], zr.at[event], right).wait_send()
            remote(piece, piece, ds.at[event], dr.at[event], mate).wait_send()

    h_ring = (hb, hzs, hzr, hds, hdr)
    y_ring = (dyb, yzs, yzr, yds, ydr)
    for item in own_sends(*h_ring):
        item.start()
    pos_sends = [remote(pos_all.at[me], pos_all.at[me], pos_s.at[step], pos_r.at[step], (me + step) % n_dev) for step in range(1, n_dev)]
    for item in pos_sends:
        item.start()
    weight_loads = [
        local(wq_hbm, wt.at[pl.ds(0, q_rows)], w_sem.at[0]),
        local(wk_hbm, wt.at[pl.ds(q_rows, kv_w)], w_sem.at[1]),
        local(wv_hbm, wt.at[pl.ds(q_rows + kv_w, kv_w)], w_sem.at[2]),
    ]
    for item in weight_loads:
        item.start()
    dkv[...] = jnp.zeros_like(dkv)
    dwo[...] = jnp.zeros_like(dwo)
    dwt[...] = jnp.zeros_like(dwt)
    bmat[...] = jnp.zeros_like(bmat)

    for item in loads:
        item.wait()
    for t in range(width // tok):
        cols = slice(tok * t, tok * t + tok)
        wi[cols, 0:hw] = wi_raw[0:hw, cols].T
        wi[cols, hw:2 * hw] = wi_raw[hw:2 * hw, cols].T
        woi[cols, :] = woi_raw[:, cols].T

    freq = jnp.exp(lax.broadcasted_iota(jnp.int32, (quarter, tok), 0).astype(F32) * (-2.0 * math.log(ROPE_BASE) / (hd // 2)))

    def make_trig(slot):
        angle = pos_all[slot].astype(F32) * freq
        trig[slot, 0:quarter, :] = jnp.cos(angle)
        trig[slot, quarter:2 * quarter, :] = jnp.sin(angle)

    make_trig(me)

    @pl.loop(1, n_dev)
    def _(step):
        source = (me + n_dev - step) % n_dev
        remote(pos_all.at[source], pos_all.at[source], pos_s.at[step], pos_r.at[step], me).wait_recv()
        make_trig(source)

    def turned(val, base, slot, back):
        cos_t = trig[slot, 0:quarter, :]
        sin_t = trig[slot, quarter:2 * quarter, :]
        u = val[base:base + quarter]
        w = val[base + quarter:base + 2 * quarter]
        rest = val[base + 2 * quarter:base + hd]
        if back:
            return [u * cos_t + w * sin_t, w * cos_t - u * sin_t, rest]
        return [u * cos_t - w * sin_t, w * cos_t + u * sin_t, rest]

    @pl.loop(0, n_chip)
    def _(k):
        ring_service(h_ring, 2 * k)
        ring_service(h_ring, 2 * k + 1)

        @pl.when(k == 5)
        def _():
            for item in own_sends(*y_ring):
                item.start()

        b = ring_origin(k)
        ring_mate(h_ring, k, b)
        flat = dot(hb[b], wi[...])
        for t in range(2):
            slot = 2 * b + t
            q_f = flat[tok * t:tok * t + tok, 0:hw].T
            kv_f = flat[tok * t:tok * t + tok, hw:2 * hw].T
            for head in range(2):
                qt[b, :, pair * t + tok * head:pair * t + tok * head + tok] = jnp.concatenate(turned(q_f, hd * head, slot, False), axis=0).astype(BF)
            kv_rot = jnp.concatenate(turned(kv_f, 0, slot, False) + [kv_f[hd:2 * hd]], axis=0).astype(BF)
            kvt[:, part_of(slot, tok)] = kv_rot
            kv[part_of(slot, tok), :] = kv_rot.T

    scale = hd ** -0.5
    cols_q = 2 * pair

    def send_a(slot):
        return remote(at_st.at[slot], at_rv.at[own_rows], a_s.at[slot], a_r.at[me], slot)

    @pl.loop(0, n_chip)
    def _(k):
        ring_service(y_ring, 2 * k)
        b = ring_origin(k)
        ring_mate(y_ring, k, b)
        da = dot(dyb[b], woi[...]).astype(BF)
        bmat[0:hd, 0:cols_q] = qt[b]
        for t in range(2):
            da_t = da[tok * t:tok * t + tok].T
            for head in range(2):
                lane = cols_q + pair * t + tok * head
                bmat[hd:2 * hd, lane:lane + tok] = da_t[hd * head:hd * head + hd]
        for t in range(2 * cols_q // tok):
            bmat_t[tok * t:tok * t + tok, :] = bmat[:, tok * t:tok * t + tok].T

        def both_of(c):
            rows = part_of(c, pair)
            both = dot(kv[rows, :], bmat[...])
            return rows, both[:, 0:cols_q] * scale, both[:, cols_q:2 * cols_q]

        lane = lax.broadcasted_iota(jnp.int32, (pair, cols_q), 1)
        seen = lax.broadcasted_iota(jnp.int32, (pair, cols_q), 0) <= (lane // pair) * tok + lane % tok
        rows, s, d_p = both_of(b)
        s = jnp.where(seen, s, -1e30)
        top = jnp.max(s, axis=0, keepdims=True)
        p = jnp.exp(s - top)
        sbuf[rows, :] = p
        dpbuf[rows, :] = d_p
        mbuf[b] = top

        def first_pass(c, state):
            old, total, weighted = state
            rows, s, d_p = both_of(c)
            new = jnp.maximum(old, jnp.max(s, axis=0, keepdims=True))
            p = jnp.exp(s - new)
            sbuf[rows, :] = p
            dpbuf[rows, :] = d_p
            mbuf[c] = new
            keep = jnp.exp(old - new)
            return new, total * keep + jnp.sum(p, axis=0, keepdims=True), weighted * keep + jnp.sum(p * d_p, axis=0, keepdims=True)

        top, total, weighted = lax.fori_loop(0, b, first_pass, (top, jnp.sum(p, axis=0, keepdims=True), jnp.sum(p * d_p, axis=0, keepdims=True)))
        inv = 1.0 / total
        row_dot = weighted * inv
        ring_service(y_ring, 2 * k + 1)
        adq[...] = jnp.zeros_like(adq)

        def second_pass(c, carry):
            rows = part_of(c, pair)
            p = sbuf[rows, :] * (jnp.exp(mbuf[c] - top) * inv)
            p_b = p.astype(BF)
            ds_b = (p * (dpbuf[rows, :] - row_dot) * scale).astype(BF)
            dkv[rows, :] += dot(ds_b, bmat_t[0:cols_q, :]) + dot(p_b, bmat_t[cols_q:2 * cols_q, :])
            adq[0:hd, :] += dot(kvt[0:hd, rows], ds_b)
            adq[hd:2 * hd, :] += dot(kvt[hd:2 * hd, rows], p_b)
            return carry

        lax.fori_loop(0, b + 1, second_pass, 0)
        a_pair = []
        dq_pair = []
        for t in range(2):
            slot = 2 * b + t
            lanes = [slice(pair * t + tok * head, pair * t + tok * head + tok) for head in range(2)]
            a_t = jnp.concatenate([adq[hd:2 * hd, lane] for lane in lanes], axis=0).astype(BF)
            parts = []
            for lane in lanes:
                parts += turned(adq[0:hd, lane], 0, slot, True)
            dq_t = jnp.concatenate(parts, axis=0).astype(BF)
            at_st[slot] = a_t
            dqt_st[slot] = dq_t
            a_pair.append(a_t)
            dq_pair.append(dq_t)

            @pl.when(slot == me)
            def _():
                at_rv[own_rows, :] = a_t
                dt_rv[own_rows, :] = dq_t

            @pl.when(slot != me)
            def _():
                remote(dqt_st.at[slot], dt_rv.at[own_rows], q_s.at[slot], q_r.at[me], slot).start()

            @pl.when((slot != me) & (k < early))
            def _():
                send_a(slot).start()

        a_pair = jnp.concatenate(a_pair, axis=1)
        dq_pair = jnp.concatenate(dq_pair, axis=1)
        for t in range(width // tile):
            cols = slice(tile * t, tile * t + tile)
            dwo[:, cols] += dot(a_pair, dyb[b, :, cols])
            dwt[0:hw, cols] += dot(dq_pair, hb[b, :, cols])

    for t in range(n_dev):
        dkvt[:, tok * t:tok * t + tok] = dkv[tok * t:tok * t + tok, :].T
    swap = remote(dkvt.at[part_of(1 - core, hd)], kv_rv, x_s, x_r, mate)
    swap.start()

    @pl.loop(early, n_chip)
    def _(k):
        b = ring_origin(k)
        for t in range(2):
            @pl.when(2 * b + t != me)
            def _():
                send_a(2 * b + t).start()

    store_wo = local(dwo, gwo_hbm, out_sem.at[0])
    store_wo.start()

    def order():
        steps = []
        for step in range(1, n_chip // 2 + 1):
            steps += [step, n_chip - step] if 2 * step < n_chip else [step]
        return [(chip + step) % n_chip for step in steps]

    far = order()
    targets = [mate] + [2 * c + p for c in far for p in range(2)]

    swap.wait_recv()
    mine = part_of(core, hd)
    g_rows = pl.ds(pl.multiple_of(q_rows + core * kv_w + chip * hd, hd), hd)
    for t in range(n_dev):
        cols = slice(tok * t, tok * t + tok)
        g = dkvt[mine, cols] + kv_rv[:, cols]
        cos_t = jnp.where(core == 0, trig[t, 0:quarter, :], 1.0)
        sin_t = jnp.where(core == 0, trig[t, quarter:2 * quarter, :], 0.0)
        u = g[0:quarter]
        w = g[quarter:2 * quarter]
        g_b = jnp.concatenate([u * cos_t + w * sin_t, w * cos_t - u * sin_t, g[2 * quarter:hd]], axis=0).astype(BF)
        kv_mine[t] = g_b
        kv_row[:, cols] = g_b
    dt_rv[g_rows, :] = kv_mine[me]
    kv_sends = [remote(kv_mine.at[t], dt_rv.at[g_rows], kv_s.at[t], kv_r.at[me], t) for t in targets]
    w_sends = [remote(dwt.at[pl.ds(0, hw), part_of(t, tok)], gw_hbm.at[own_rows], w_s.at[t], w_r.at[me], t) for t in targets]
    wk_sends = [remote(dwt.at[pl.ds(hw, hd), part_of(t, tok)], gw_hbm.at[g_rows], wk_s.at[t], wk_r.at[me], t) for t in targets]
    for item in kv_sends + w_sends:
        item.start()
    w_own = local(dwt.at[pl.ds(0, hw), part_of(me, tok)], gw_hbm.at[own_rows], loc_sem.at[0])
    w_own.start()

    for t in range(width // tile):
        cols = slice(tile * t, tile * t + tile)
        acc = jnp.zeros((hd, tile), F32)
        for s in range(n_chip):
            acc += dot(kv_row[:, pair * s:pair * s + pair], hb[s, :, cols])
        dwt[hw:hw + hd, cols] = acc
    wk_own = local(dwt.at[pl.ds(hw, hd), part_of(me, tok)], gw_hbm.at[g_rows], loc_sem.at[1])
    wk_own.start()

    finish_ring(y_ring)
    wo_loads = [local(wo_hbm.at[pl.ds(pair * t, pair)], dyb.at[t], wo_sem.at[t]) for t in range(n_chip)]
    for item in wo_loads:
        item.start()

    for t in targets:
        remote(at_st.at[0], at_rv.at[part_of(t, hw)], a_s.at[t], a_r.at[t], t).wait_recv()
    for t in range(q_rows // tok):
        a_nat[:, tok * t:tok * t + tok] = at_rv[tok * t:tok * t + tok, :].T
    for item in wo_loads:
        item.wait()
    for t in range(width // tile):
        cols = slice(tile * t, tile * t + tile)
        prod = jnp.zeros((tok, tile), F32)
        for s in range(n_chip):
            prod += dot(a_nat[:, pair * s:pair * s + pair], dyb[s, :, cols])
        out_v[:, cols] = (x_v[:, cols].astype(F32) + prod).astype(BF)
    store_out = local(out_v, out_hbm, out_sem.at[1])
    store_out.start()

    for item in weight_loads:
        item.wait()

    def kv_place(t):
        return pl.ds(pl.multiple_of(q_rows + (t % 2) * kv_w + (t // 2) * hd, hd), hd)

    for t in targets:
        remote(dqt_st.at[0], dt_rv.at[part_of(t, hw)], q_s.at[t], q_r.at[t], t).wait_recv()
        remote(kv_mine.at[0], dt_rv.at[kv_place(t)], kv_s.at[t], kv_r.at[t], t).wait_recv()
    for t in range(n_rows // tok):
        d_nat[:, tok * t:tok * t + tok] = dt_rv[tok * t:tok * t + tok, :].T

    for t in range(width // tile):
        cols = slice(tile * t, tile * t + tile)
        acc = jnp.zeros((tok, tile), F32)
        for s in range(n_rows // tile):
            acc += dot(d_nat[:, tile * s:tile * s + tile], wt[tile * s:tile * s + tile, cols])
        dh[:, cols] = acc
        gg_st[0, :, cols] = jnp.sum(acc * xhat[:, cols], axis=0, keepdims=True)
        gg_st[1, :, cols] = jnp.sum(acc, axis=0, keepdims=True)
    g_swap = remote(gg_st.at[1 - core], gg_mx, g_s.at[n_chip], g_r.at[n_chip], mate)
    g_swap.start()
    g_swap.wait_recv()
    gg_my[...] = jnp.where(core == 0, gg_st[0], gg_st[1]) + gg_mx[...]
    gg_rv[chip] = gg_my[...]
    g_sends = [remote(gg_my, gg_rv.at[chip], g_s.at[c], g_r.at[chip], 2 * c + core) for c in far]
    for item in g_sends + wk_sends:
        item.start()

    grad_hat = dh[...] * gain_one
    x_hat = xhat[...]
    mean_one = jnp.mean(grad_hat, axis=-1, keepdims=True)
    mean_two = jnp.mean(grad_hat * x_hat, axis=-1, keepdims=True)
    store_out.wait()
    out_v[...] = (dy_own[...].astype(F32) + stat[:, 0:1] * (grad_hat - mean_one - x_hat * mean_two)).astype(BF)
    store_gx = local(out_v, gx_hbm, out_sem.at[2])
    store_gx.start()

    for c in far:
        remote(gg_my, gg_rv.at[c], g_s.at[c], g_r.at[c], 2 * c + core).wait_recv()
    sums = gg_rv[0]
    for c in range(1, n_chip):
        sums = sums + gg_rv[c]
    gg_out[core] = sums
    g_swap_out = remote(gg_out.at[core], gg_out.at[core], g_s.at[n_chip + 1], g_r.at[n_chip + 1], mate)
    g_swap_out.start()
    remote(gg_out.at[core], gg_out.at[1 - core], g_s.at[n_chip + 1], g_r.at[n_chip + 1], mate).wait_recv()
    store_gg = local(gg_out, gg_hbm, out_sem.at[3])
    store_gg.start()

    finish_ring(h_ring)
    for item in pos_sends + [swap, g_swap, g_swap_out]:
        item.wait_send()
    for t in targets:
        remote(at_st.at[0], at_rv.at[pl.ds(0, hw)], a_s.at[t], a_r.at[t], t).wait_send()
        remote(dqt_st.at[0], dt_rv.at[pl.ds(0, hw)], q_s.at[t], q_r.at[t], t).wait_send()
    for item in kv_sends + w_sends + g_sends + wk_sends:
        item.wait_send()
    for t in targets:
        remote(dwt.at[pl.ds(0, hw), part_of(t, tok)], gw_hbm.at[part_of(t, hw)], w_s.at[t], w_r.at[t], t).wait_recv()
        remote(dwt.at[pl.ds(hw, hd), part_of(t, tok)], gw_hbm.at[kv_place(t)], wk_s.at[t], wk_r.at[t], t).wait_recv()
    for item in (w_own, wk_own, store_wo, store_gx, store_gg):
        item.wait()


def settle_kernel(q_rows, kv_w, out_i, gx_i, gw_i, gwo_i, gg_i, out_o, gx_o, gq_o, gk_o, gv_o, gwo_o, gain_o, bias_o, b_act, b_q, b_kv, b_o, b_gg, sem_in, sem_out, sem_gg):
    half_q = q_rows // 2
    half_o = gwo_i.shape[0] // 2
    moves = [(out_i, b_act.at[0], out_o), (gx_i, b_act.at[1], gx_o)]
    for t in range(2):
        moves.append((gw_i.at[pl.ds(half_q * t, half_q)], b_q.at[t], gq_o.at[pl.ds(half_q * t, half_q)]))
        moves.append((gwo_i.at[pl.ds(half_o * t, half_o)], b_o.at[t], gwo_o.at[pl.ds(half_o * t, half_o)]))
    moves.append((gw_i.at[pl.ds(q_rows, kv_w)], b_kv.at[0], gk_o))
    moves.append((gw_i.at[pl.ds(q_rows + kv_w, kv_w)], b_kv.at[1], gv_o))
    loads = [pltpu.make_async_copy(src, mid, sem_in.at[i]) for i, (src, mid, _) in enumerate(moves)]
    stores = [pltpu.make_async_copy(mid, dst, sem_out.at[i]) for i, (_, mid, dst) in enumerate(moves)]
    load_gg = pltpu.make_async_copy(gg_i, b_gg, sem_gg)
    load_gg.start()
    for item in loads:
        item.start()
    for load, store in zip(loads, stores):
        load.wait()
        store.start()
    load_gg.wait()
    gain_o[...] = b_gg[0, 0]
    bias_o[...] = b_gg[1, 0]
    for item in stores:
        item.wait()


def solution(mesh):
    n_dev = mesh.shape['cp']

    def device_step(x_act, d_out, positions, ln_gain, ln_bias, w_query, w_key, w_value, w_out):
        tok, width = x_act.shape[1], x_act.shape[2]
        q_heads, hd = w_query.shape[1], w_query.shape[2]
        kv_heads = w_key.shape[1]
        q_w, kv_w = q_heads * hd, kv_heads * hd
        n_rows = q_w + 2 * kv_w
        seq = n_dev * tok
        hw = 2 * hd

        def flat_weight(w):
            return jnp.transpose(w, (1, 2, 0)).reshape(-1, width)

        hbm = pl.BlockSpec(memory_space=pltpu.HBM)
        vmem = pl.BlockSpec(memory_space=pltpu.VMEM)
        dma = pltpu.SemaphoreType.DMA
        scratch = [
            pltpu.VMEM((n_dev // 2, 2 * tok, width), BF),
            pltpu.VMEM((n_dev // 2, 2 * tok, width), BF),
            pltpu.VMEM((n_rows, width), BF),
            pltpu.VMEM((2 * hw, width), BF),
            pltpu.VMEM((width, 2 * hw), BF),
            pltpu.VMEM((hw, width), BF),
            pltpu.VMEM((width, hw), BF),
            pltpu.VMEM((n_dev, 1, tok), jnp.int32),
            pltpu.VMEM((n_dev, hd // 2, tok), F32),
            pltpu.VMEM((n_dev // 2, hd, 4 * tok), BF),
            pltpu.VMEM((hw, seq), BF),
            pltpu.VMEM((seq, hw), BF),
            pltpu.VMEM((hw, 8 * tok), BF),
            pltpu.VMEM((8 * tok, hw), BF),
            pltpu.VMEM((seq, 4 * tok), F32),
            pltpu.VMEM((seq, 4 * tok), F32),
            pltpu.VMEM((n_dev // 2, 1, 4 * tok), F32),
            pltpu.VMEM((hw, 4 * tok), F32),
            pltpu.VMEM((seq, hw), F32),
            pltpu.VMEM((hw, seq), F32),
            pltpu.VMEM((hd, seq), F32),
            pltpu.VMEM((n_dev, hd, tok), BF),
            pltpu.VMEM((hd, seq), BF),
            pltpu.VMEM((hw, width), F32),
            pltpu.VMEM((hw + hd, width), F32),
            pltpu.VMEM((n_dev, hw, tok), BF),
            pltpu.VMEM((n_dev, hw, tok), BF),
            pltpu.VMEM((q_w, tok), BF),
            pltpu.VMEM((n_rows, tok), BF),
            pltpu.VMEM((tok, q_w), BF),
            pltpu.VMEM((tok, n_rows), BF),
            pltpu.VMEM((tok, width), BF),
            pltpu.VMEM((tok, width), BF),
            pltpu.VMEM((tok, width), F32),
            pltpu.VMEM((tok, 128), F32),
            pltpu.VMEM((tok, width), F32),
            pltpu.VMEM((tok, width), BF),
            pltpu.VMEM((2, 1, width), F32),
            pltpu.VMEM((1, width), F32),
            pltpu.VMEM((1, width), F32),
            pltpu.VMEM((n_dev // 2, 1, width), F32),
            pltpu.VMEM((2, 1, width), F32),
            dma((7,)), dma((n_dev,)), dma((3,)), dma((4,)), dma((2,)),
            dma((16,)), dma((14,)), dma((16,)), dma((16,)),
            dma((16,)), dma((14,)), dma((16,)), dma((16,)),
            dma((n_dev,)), dma((n_dev,)),
            dma((n_dev,)), dma((n_dev,)),
            dma((n_dev,)), dma((n_dev,)),
            dma, dma,
            dma((n_dev,)), dma((n_dev,)),
            dma((n_dev,)), dma((n_dev,)),
            dma((n_dev,)), dma((n_dev,)),
            dma((n_dev,)), dma((n_dev,)),
        ]
        out, gx, gw, gwo, gg = pl.pallas_call(
            functools.partial(block_kernel, n_dev, hd, kv_w, EARLY),
            out_shape=(
                jax.ShapeDtypeStruct((tok, width), BF),
                jax.ShapeDtypeStruct((tok, width), BF),
                jax.ShapeDtypeStruct((n_rows, tok), F32),
                jax.ShapeDtypeStruct((hw, width), F32),
                jax.ShapeDtypeStruct((2, 1, width), F32),
            ),
            in_specs=[hbm, hbm, vmem, vmem, vmem, hbm, hbm, hbm, hbm],
            out_specs=(hbm,) * 5,
            scratch_shapes=scratch,
            compiler_params=pltpu.CompilerParams(collective_id=0, has_side_effects=True, vmem_limit_bytes=67043328),
            name='attn_block',
        )(
            x_act.reshape(tok, width), d_out.reshape(tok, width), positions.reshape(1, tok),
            ln_gain.reshape(1, width), ln_bias.reshape(1, width),
            flat_weight(w_query), flat_weight(w_key), flat_weight(w_value), w_out,
        )

        out, gx, gq, gk, gv, gwo, gain, bias = pl.pallas_call(
            functools.partial(settle_kernel, q_w, kv_w),
            out_shape=(
                jax.ShapeDtypeStruct((tok, width), BF),
                jax.ShapeDtypeStruct((tok, width), BF),
                jax.ShapeDtypeStruct((q_w, tok), F32),
                jax.ShapeDtypeStruct((kv_w, tok), F32),
                jax.ShapeDtypeStruct((kv_w, tok), F32),
                jax.ShapeDtypeStruct((hw, width), F32),
                jax.ShapeDtypeStruct((width,), F32),
                jax.ShapeDtypeStruct((width,), F32),
            ),
            in_specs=[hbm] * 5,
            out_specs=(hbm,) * 6 + (vmem,) * 2,
            scratch_shapes=[
                pltpu.VMEM((2, tok, width), BF),
                pltpu.VMEM((2, q_w // 2, tok), F32),
                pltpu.VMEM((2, kv_w, tok), F32),
                pltpu.VMEM((2, hw // 2, width), F32),
                pltpu.VMEM((2, 1, width), F32),
                dma((8,)), dma((8,)), dma,
            ],
            name='settle',
        )(out, gx, gw, gwo, gg)

        def rows_out(block, heads):
            return jnp.transpose(block.reshape(heads, hd, tok), (2, 0, 1))

        return (
            out.reshape(1, tok, width), gx.reshape(1, tok, width),
            rows_out(gq, q_heads), rows_out(gk, kv_heads), rows_out(gv, kv_heads),
            gwo, gain, bias,
        )

    return jax.shard_map(device_step, mesh=mesh, in_specs=(P('dp', 'cp', None), P('dp', 'cp', None), P('dp', 'cp'), P(None), P(None), P(None, None, None), P(None, None, None), P(None, None, None), P(None, None)), out_specs=(P('dp', 'cp', None), P('dp', 'cp', None), P(('dp', 'cp'), None, None), P(('dp', 'cp'), None, None), P(('dp', 'cp'), None, None), P(('dp', 'cp'), None), P('dp'), P('dp')), check_vma=False)
```

```python
import functools
import math

import jax
import jax.numpy as jnp
from jax import lax
from jax.experimental import pallas as pl
from jax.experimental.pallas import tpu as pltpu
from jax.sharding import PartitionSpec as P

EPS = 1e-5
ROPE_BASE = 10000.0
MESH = pl.DeviceIdType.MESH
BF = jnp.bfloat16
F32 = jnp.float32
NEAR = 1


def dot(lhs, rhs):
    return jnp.dot(lhs, rhs, preferred_element_type=F32)


def dot_t(lhs, rhs):
    return lax.dot_general(lhs, rhs, (((1,), (1,)), ((), ())), preferred_element_type=F32)


def block_kernel(
    n_dev, hd, kv_w, near,
    x_hbm, dy_hbm, pos_hbm, gain_hbm, bias_hbm, wq_hbm, wk_hbm, wv_hbm, wo_hbm,
    out_hbm, gx_hbm, gw_hbm, gwo_hbm, gg_hbm,
    hb, dyb, wt, wi, woi, w_far, pos_all, trig,
    qt, kvt, kv, kvt_far, kv_far, bmat, bmat_t, sbuf, dpbuf, mbuf, adq, dkv, dkvt, kv_rv, kv_mine, kv_row,
    dwo, dwt, at_st, dqt_st, at_rv, dt_rv, a_nat, d_nat, x_v, dy_own, gb_v, stat, out_v, gg_st, gg_mx, gg_my, gg_rv, gg_out,
    in_sem, far_sem, wo_sem, w_sem, out_sem, loc_sem,
    hzs, hzr, hds, hdr, yzs, yzr, yds, ydr,
    pos_s, pos_r, a_s, a_r, q_s, q_r, x_s, x_r, kv_s, kv_r, w_s, w_r, wk_s, wk_r, g_s, g_r,
):
    tok, width = x_v.shape
    n_chip = n_dev // 2
    half = tok // 2
    pair = 2 * tok
    me = lax.axis_index('cp')
    chip = me // 2
    core = me % 2
    right = 2 * ((chip + 1) % n_chip) + core
    left = 2 * ((chip + n_chip - 1) % n_chip) + core
    mate = 2 * chip + 1 - core
    q_rows = wq_hbm.shape[0]
    n_rows = q_rows + 2 * kv_w
    hw = 2 * hd
    quarter = hd // 4
    tile = 256
    scale = hd ** -0.5
    cols_q = 2 * pair
    n_far = n_chip - 1 - 2 * near

    def remote(src, dst, send, recv, target):
        return pltpu.make_async_remote_copy(src_ref=src, dst_ref=dst, send_sem=send, recv_sem=recv, device_id={'cp': target}, device_id_type=MESH)

    def local(src, dst, sem):
        return pltpu.make_async_copy(src, dst, sem)

    def part_of(i, size):
        return pl.ds(pl.multiple_of(i * size, size), size)

    def ring_steps(k):
        step = (k + 1) // 2
        return step, k % 2

    def ring_origin(k):
        step, ahead = ring_steps(k)
        return jnp.where(ahead == 1, chip + n_chip - step, chip + step) % n_chip

    own = (chip, part_of(core, tok))
    first_loads = [
        local(x_hbm, x_v, in_sem.at[0]),
        local(gain_hbm, gb_v.at[0], in_sem.at[1]),
        local(bias_hbm, gb_v.at[1], in_sem.at[2]),
        local(pos_hbm, pos_all.at[me], in_sem.at[3]),
    ]
    for item in first_loads:
        item.start()
    barrier = pltpu.get_barrier_semaphore()
    for step in range(1, n_dev):
        pl.semaphore_signal(barrier, inc=1, device_id={'cp': (me + step) % n_dev}, device_id_type=MESH)
    own_rows = part_of(me, hw)
    kv_rows = part_of(chip, hd)
    loads = [
        local(wq_hbm.at[own_rows], wi.at[pl.ds(0, hw)], in_sem.at[4]),
        local(wk_hbm.at[kv_rows], wi.at[pl.ds(hw, hd)], in_sem.at[5]),
        local(wv_hbm.at[kv_rows], wi.at[pl.ds(hw + hd, hd)], in_sem.at[6]),
        local(wo_hbm.at[own_rows], woi, in_sem.at[7]),
        local(dy_hbm, dyb.at[own], in_sem.at[8]),
        local(dy_hbm, dy_own, in_sem.at[9]),
    ]
    for f in range(n_far):
        far_rows = part_of(ring_origin(2 * near + 1 + f), hd)
        loads.append(local(wk_hbm.at[far_rows], w_far.at[pl.ds(hw * f, hd)], far_sem.at[2 * f]))
        loads.append(local(wv_hbm.at[far_rows], w_far.at[pl.ds(hw * f + hd, hd)], far_sem.at[2 * f + 1]))
    for item in loads:
        item.start()

    for item in first_loads:
        item.wait()
    gain_one = 1.0 + gb_v[0]
    x_f = x_v[...].astype(F32)
    mean = jnp.mean(x_f, axis=-1, keepdims=True)
    centered = x_f - mean
    inv_std = lax.rsqrt(jnp.mean(centered * centered, axis=-1, keepdims=True) + EPS)
    hb[chip, part_of(core, tok), :] = (centered * inv_std * gain_one + gb_v[1]).astype(BF)
    stat[0] = jnp.broadcast_to(mean, (tok, 128))
    stat[1] = jnp.broadcast_to(inv_std, (tok, 128))

    pl.semaphore_wait(barrier, n_dev - 1)

    def chunk(buf, origin, parity, part):
        return buf.at[origin, part_of(2 * parity + part, half)]

    def own_sends(buf, zs, zr, ds, dr):
        copies = []
        for part in range(2):
            piece = chunk(buf, chip, core, part)
            copies.append(remote(piece, piece, zs.at[2 * part], zr.at[2 * part], right))
            copies.append(remote(piece, piece, zs.at[2 * part + 1], zr.at[2 * part + 1], left))
            copies.append(remote(piece, piece, ds.at[14 + part], dr.at[14 + part], mate))
        return copies

    def event_place(event):
        step = event // 4 + 1
        turn = event % 4
        direction = turn % 2
        part = jnp.where(step < 4, turn // 2, turn)
        origin = jnp.where(direction == 0, chip + n_chip - step, chip + step) % n_chip
        return step, turn, direction, part, origin

    def ring_event(ring, event):
        buf, zs, zr, ds, dr = ring
        step, turn, direction, part, origin = event_place(event)
        piece = chunk(buf, origin, core, part)
        remote(piece, piece, zs.at[0], zr.at[event], right).wait_recv()
        onward = jnp.where(step < 3, event + 4, jnp.where(turn == 0, 12, 13))

        @pl.when((step < 3) | ((step == 3) & ((turn == 0) | (turn == 3))))
        def _():
            remote(piece, piece, zs.at[event + 4], zr.at[onward], jnp.where(direction == 0, right, left)).start()

        remote(piece, piece, ds.at[event], dr.at[event], mate).start()

    def ring_service(ring, event):
        @pl.when(event < 14)
        def _():
            ring_event(ring, event)

    def ring_mate(ring, k, origin):
        buf, zs, zr, ds, dr = ring
        step, ahead = ring_steps(k)
        first = jnp.where(k == 0, 14, jnp.where(step < 4, 4 * (step - 1) + 1 - ahead, 12))
        second = jnp.where(k == 0, 15, jnp.where(step < 4, 4 * (step - 1) + 3 - ahead, 13))
        for part, event in ((0, first), (1, second)):
            piece = chunk(buf, origin, 1 - core, part)
            remote(piece, piece, ds.at[0], dr.at[event], mate).wait_recv()

    def finish_ring(ring):
        buf, zs, zr, ds, dr = ring
        for item in own_sends(*ring):
            item.wait_send()
        for event in range(14):
            _, _, _, part, origin = event_place(event)
            piece = chunk(buf, origin, core, part)
            if event < 8 or event in (8, 11):
                remote(piece, piece, zs.at[event + 4], zr.at[event], right).wait_send()
            remote(piece, piece, ds.at[event], dr.at[event], mate).wait_send()

    h_ring = (hb, hzs, hzr, hds, hdr)
    y_ring = (dyb, yzs, yzr, yds, ydr)
    for item in own_sends(*h_ring):
        item.start()
    pos_sends = [remote(pos_all.at[me], pos_all.at[me], pos_s.at[step], pos_r.at[step], (me + step) % n_dev) for step in range(1, n_dev)]
    for item in pos_sends:
        item.start()
    weight_loads = [
        local(wq_hbm, wt.at[pl.ds(0, q_rows)], w_sem.at[0]),
        local(wk_hbm, wt.at[pl.ds(q_rows, kv_w)], w_sem.at[1]),
        local(wv_hbm, wt.at[pl.ds(q_rows + kv_w, kv_w)], w_sem.at[2]),
    ]
    for item in weight_loads:
        item.start()
    dkv[...] = jnp.zeros_like(dkv)
    dwo[...] = jnp.zeros_like(dwo)
    dwt[...] = jnp.zeros_like(dwt)
    bmat[...] = jnp.zeros_like(bmat)

    freq = jnp.exp(lax.broadcasted_iota(jnp.int32, (quarter, tok), 0).astype(F32) * (-2.0 * math.log(ROPE_BASE) / (hd // 2)))

    def make_trig(slot):
        angle = pos_all[slot].astype(F32) * freq
        trig[slot // 2, 0:quarter, part_of(slot % 2, tok)] = jnp.cos(angle)
        trig[slot // 2, quarter:2 * quarter, part_of(slot % 2, tok)] = jnp.sin(angle)

    make_trig(me)

    @pl.loop(1, n_dev)
    def _(step):
        source = (me + n_dev - step) % n_dev
        remote(pos_all.at[source], pos_all.at[source], pos_s.at[step], pos_r.at[step], me).wait_recv()
        make_trig(source)

    for item in loads:
        item.wait()

    def turned(val, cos_t, sin_t):
        u = val[0:quarter]
        w = val[quarter:2 * quarter]
        return [u * cos_t - w * sin_t, w * cos_t + u * sin_t, val[2 * quarter:hd]]

    def keys_values(val, cos_t, sin_t):
        return jnp.concatenate(turned(val[0:hd], cos_t, sin_t) + [val[hd:hw]], axis=0).astype(BF)

    @pl.loop(0, n_chip)
    def _(k):
        ring_service(h_ring, 2 * k)
        ring_service(h_ring, 2 * k + 1)

        @pl.when(k == 5)
        def _():
            for item in own_sends(*y_ring):
                item.start()

        b = ring_origin(k)
        ring_mate(h_ring, k, b)
        place = part_of(b, pair)
        cos_t = trig[b, 0:quarter, :]
        sin_t = trig[b, quarter:2 * quarter, :]
        flat = dot_t(wi[...], hb[b])
        for head in range(2):
            q_rot = jnp.concatenate(turned(flat[hd * head:hd * head + hd], cos_t, sin_t), axis=0).astype(BF)
            for t in range(2):
                lane = pair * t + tok * head
                qt[b, :, lane:lane + tok] = q_rot[:, tok * t:tok * t + tok]
        kv_rot = keys_values(flat[hw:2 * hw], cos_t, sin_t)
        kvt[:, place] = kv_rot
        kv[place, :] = kv_rot.T

        @pl.when(b <= chip)
        def _():
            flat_far = dot_t(w_far[...], hb[b])
            for f in range(n_far):
                far_rot = keys_values(flat_far[hw * f:hw * f + hw], cos_t, sin_t)
                kvt_far[f, :, place] = far_rot
                kv_far[f, place, :] = far_rot.T

    def first_part(b, seen, kv_of):
        def both_of(c):
            rows = part_of(c, pair)
            both = dot(kv_of(rows), bmat[...])
            return rows, both[:, 0:cols_q] * scale, both[:, cols_q:2 * cols_q]

        rows, s, d_p = both_of(b)
        s = jnp.where(seen, s, -1e30)
        top = jnp.max(s, axis=0, keepdims=True)
        p = jnp.exp(s - top)
        sbuf[rows, :] = p
        dpbuf[rows, :] = d_p
        mbuf[b] = top

        def step(c, state):
            old, total, weighted = state
            rows, s, d_p = both_of(c)
            new = jnp.maximum(old, jnp.max(s, axis=0, keepdims=True))
            p = jnp.exp(s - new)
            sbuf[rows, :] = p
            dpbuf[rows, :] = d_p
            mbuf[c] = new
            keep = jnp.exp(old - new)
            return new, total * keep + jnp.sum(p, axis=0, keepdims=True), weighted * keep + jnp.sum(p * d_p, axis=0, keepdims=True)

        top, total, weighted = lax.fori_loop(0, b, step, (top, jnp.sum(p, axis=0, keepdims=True), jnp.sum(p * d_p, axis=0, keepdims=True)))
        inv = 1.0 / total
        return top, inv, weighted * inv

    def second_part(b, stats, kvt_of, with_keys):
        top, inv, row_dot = stats
        adq[...] = jnp.zeros_like(adq)

        def step(c, carry):
            rows = part_of(c, pair)
            p = sbuf[rows, :] * (jnp.exp(mbuf[c] - top) * inv)
            p_b = p.astype(BF)
            ds_b = (p * (dpbuf[rows, :] - row_dot) * scale).astype(BF)
            if with_keys:
                dkv[rows, :] += dot(ds_b, bmat_t[0:cols_q, :]) + dot(p_b, bmat_t[cols_q:2 * cols_q, :])
            adq[0:hd, :] += dot(kvt_of(slice(0, hd), rows), ds_b)
            adq[hd:hw, :] += dot(kvt_of(slice(hd, hw), rows), p_b)
            return carry

        lax.fori_loop(0, b + 1, step, 0)

    lane = lax.broadcasted_iota(jnp.int32, (pair, cols_q), 1)
    row = lax.broadcasted_iota(jnp.int32, (pair, cols_q), 0)

    @pl.loop(0, n_chip)
    def _(k):
        ring_service(y_ring, 2 * k)
        b = ring_origin(k)
        ring_mate(y_ring, k, b)
        da_t = dot_t(woi[...], dyb[b]).astype(BF)
        bmat[0:hd, 0:cols_q] = qt[b]
        for t in range(2):
            for head in range(2):
                at = cols_q + pair * t + tok * head
                bmat[hd:hw, at:at + tok] = da_t[hd * head:hd * head + hd, tok * t:tok * t + tok]
        for t in range(2 * cols_q // tok):
            bmat_t[tok * t:tok * t + tok, :] = bmat[:, tok * t:tok * t + tok].T
        stats = first_part(b, row <= (lane // pair) * tok + lane % tok, lambda rows: kv[rows, :])
        ring_service(y_ring, 2 * k + 1)
        second_part(b, stats, lambda part, rows: kvt[part, rows], True)
        a_pair = []
        dq_pair = []
        for t in range(2):
            slot = 2 * b + t
            lanes = [slice(pair * t + tok * head, pair * t + tok * head + tok) for head in range(2)]
            a_t = jnp.concatenate([adq[hd:hw, at] for at in lanes], axis=0).astype(BF)
            cos_t = trig[b, 0:quarter, tok * t:tok * t + tok]
            sin_t = trig[b, quarter:2 * quarter, tok * t:tok * t + tok]
            dq_t = jnp.concatenate([piece for at in lanes for piece in turned(adq[0:hd, at], cos_t, -sin_t)], axis=0).astype(BF)
            a_pair.append(a_t)
            dq_pair.append(dq_t)

            @pl.when(slot == me)
            def _():
                at_rv[own_rows, :] = a_t
                dt_rv[own_rows, :] = dq_t

            @pl.when((slot != me) & (k < 1 + 2 * near))
            def _():
                at_st[slot] = a_t
                dqt_st[slot] = dq_t
                remote(dqt_st.at[slot], dt_rv.at[own_rows], q_s.at[slot], q_r.at[me], slot).start()
                remote(at_st.at[slot], at_rv.at[own_rows], a_s.at[slot], a_r.at[me], slot).start()

        a_pair = jnp.concatenate(a_pair, axis=1)
        dq_pair = jnp.concatenate(dq_pair, axis=1)
        for t in range(width // tile):
            cols = slice(tile * t, tile * t + tile)
            dwo[:, cols] += dot(a_pair, dyb[b, :, cols])
            dwt[0:hw, cols] += dot(dq_pair, hb[b, :, cols])

    far = [ring_origin(k) for k in range(1, n_chip)]
    targets = [mate] + [2 * c + p for c in far for p in range(2)]
    near_targets = targets[0:1 + 4 * near]
    w_sends = [remote(dwt.at[pl.ds(0, hw), part_of(t, tok)], gw_hbm.at[own_rows], w_s.at[t], w_r.at[me], t) for t in targets]
    for item in w_sends:
        item.start()
    w_own = local(dwt.at[pl.ds(0, hw), part_of(me, tok)], gw_hbm.at[own_rows], loc_sem.at[0])
    w_own.start()

    for t in range(n_dev):
        dkvt[:, tok * t:tok * t + tok] = dkv[tok * t:tok * t + tok, :].T
    swap = remote(dkvt.at[part_of(1 - core, hd)], kv_rv, x_s, x_r, mate)
    swap.start()
    store_wo = local(dwo, gwo_hbm, out_sem.at[0])
    store_wo.start()

    finish_ring(y_ring)
    wo_loads = [local(wo_hbm.at[pl.ds(pair * t, pair)], dyb.at[t], wo_sem.at[t]) for t in range(n_chip)]
    for item in wo_loads:
        item.start()

    swap.wait_recv()
    mine = part_of(core, hd)
    g_rows = pl.ds(pl.multiple_of(q_rows + core * kv_w + chip * hd, hd), hd)
    for t in range(n_chip):
        cols = slice(pair * t, pair * t + pair)
        g = dkvt[mine, cols] + kv_rv[:, cols]
        cos_t = jnp.where(core == 0, trig[t, 0:quarter, :], 1.0)
        sin_t = jnp.where(core == 0, trig[t, quarter:2 * quarter, :], 0.0)
        g_b = jnp.concatenate(turned(g, cos_t, -sin_t), axis=0).astype(BF)
        kv_mine[2 * t] = g_b[:, 0:tok]
        kv_mine[2 * t + 1] = g_b[:, tok:pair]
        kv_row[:, cols] = g_b
    dt_rv[g_rows, :] = kv_mine[me]
    kv_sends = [remote(kv_mine.at[t], dt_rv.at[g_rows], kv_s.at[t], kv_r.at[me], t) for t in targets]
    for item in kv_sends:
        item.start()
    for t in range(width // tile):
        cols = slice(tile * t, tile * t + tile)
        acc = jnp.zeros((hd, tile), F32)
        for s in range(n_chip):
            acc += dot(kv_row[:, pair * s:pair * s + pair], hb[s, :, cols])
        dwt[hw:hw + hd, cols] = acc
    wk_own = local(dwt.at[pl.ds(hw, hd), part_of(me, tok)], gw_hbm.at[g_rows], loc_sem.at[1])
    wk_own.start()
    wk_sends = [remote(dwt.at[pl.ds(hw, hd), part_of(t, tok)], gw_hbm.at[g_rows], wk_s.at[t], wk_r.at[me], t) for t in targets]
    for item in wk_sends:
        item.start()

    for item in weight_loads + wo_loads:
        item.wait()

    @pl.loop(0, n_far)
    def _(f):
        c_far = ring_origin(2 * near + 1 + f)
        cos_t = trig[chip, 0:quarter, part_of(core, tok)]
        sin_t = trig[chip, quarter:2 * quarter, part_of(core, tok)]
        q_t = dot_t(wt[part_of(c_far, 2 * hw), :], hb[chip, part_of(core, tok), :])
        da_t = dot_t(dyb[c_far], dy_own[...]).astype(BF)
        for head in range(4):
            part = slice(hd * head, hd * head + hd)
            at = tok * head
            bmat[0:hd, at:at + tok] = jnp.concatenate(turned(q_t[part], cos_t, sin_t), axis=0).astype(BF)
            bmat[hd:hw, cols_q + at:cols_q + at + tok] = da_t[part]
        stats = first_part(chip, row <= core * tok + lane % tok, lambda rows: kv_far[f, rows, :])
        second_part(chip, stats, lambda part, rows: kvt_far[f, part, rows], False)
        for head in range(4):
            at = slice(tok * head, tok * head + tok)
            place = pl.ds(pl.multiple_of(c_far * 2 * hw + hd * head, hd), hd)
            at_rv[place, :] = adq[hd:hw, at].astype(BF)
            dt_rv[place, :] = jnp.concatenate(turned(adq[0:hd, at], cos_t, -sin_t), axis=0).astype(BF)

    for t in near_targets:
        remote(at_st.at[0], at_rv.at[part_of(t, hw)], a_s.at[t], a_r.at[t], t).wait_recv()
    for t in range(q_rows // tok):
        a_nat[:, tok * t:tok * t + tok] = at_rv[tok * t:tok * t + tok, :].T
    for t in range(width // tile):
        cols = slice(tile * t, tile * t + tile)
        prod = jnp.zeros((tok, tile), F32)
        for s in range(n_chip):
            prod += dot(a_nat[:, pair * s:pair * s + pair], dyb[s, :, cols])
        out_v[:, cols] = (x_v[:, cols].astype(F32) + prod).astype(BF)
    store_out = local(out_v, out_hbm, out_sem.at[1])
    store_out.start()

    def kv_place(t):
        return pl.ds(pl.multiple_of(q_rows + (t % 2) * kv_w + (t // 2) * hd, hd), hd)

    for t in near_targets:
        remote(dqt_st.at[0], dt_rv.at[part_of(t, hw)], q_s.at[t], q_r.at[t], t).wait_recv()
    for t in targets:
        remote(kv_mine.at[0], dt_rv.at[kv_place(t)], kv_s.at[t], kv_r.at[t], t).wait_recv()
    swap.wait_send()
    for t in range(n_rows // tok):
        d_nat[:, tok * t:tok * t + tok] = dt_rv[tok * t:tok * t + tok, :].T

    mean = stat[0, :, 0:1]
    inv_std = stat[1, :, 0:1]
    dh = dkvt
    for t in range(width // tile):
        cols = slice(tile * t, tile * t + tile)
        acc = jnp.zeros((tok, tile), F32)
        for s in range(n_rows // tile):
            acc += dot(d_nat[:, tile * s:tile * s + tile], wt[tile * s:tile * s + tile, cols])
        dh[:, cols] = acc
        gg_st[0, :, cols] = jnp.sum(acc * ((x_v[:, cols].astype(F32) - mean) * inv_std), axis=0, keepdims=True)
        gg_st[1, :, cols] = jnp.sum(acc, axis=0, keepdims=True)
    g_swap = remote(gg_st.at[1 - core], gg_mx, g_s.at[n_chip], g_r.at[n_chip], mate)
    g_swap.start()
    g_swap.wait_recv()
    gg_my[...] = jnp.where(core == 0, gg_st[0], gg_st[1]) + gg_mx[...]
    gg_rv[chip] = gg_my[...]
    g_sends = [remote(gg_my, gg_rv.at[chip], g_s.at[c], g_r.at[chip], 2 * c + core) for c in far]
    for item in g_sends:
        item.start()

    grad_hat = dh[...] * gain_one
    x_hat = (x_v[...].astype(F32) - mean) * inv_std
    mean_one = jnp.mean(grad_hat, axis=-1, keepdims=True)
    mean_two = jnp.mean(grad_hat * x_hat, axis=-1, keepdims=True)
    store_out.wait()
    out_v[...] = (dy_own[...].astype(F32) + inv_std * (grad_hat - mean_one - x_hat * mean_two)).astype(BF)
    store_gx = local(out_v, gx_hbm, out_sem.at[2])
    store_gx.start()

    for c in far:
        remote(gg_my, gg_rv.at[c], g_s.at[c], g_r.at[c], 2 * c + core).wait_recv()
    sums = gg_rv[0]
    for c in range(1, n_chip):
        sums = sums + gg_rv[c]
    gg_out[core] = sums
    g_swap_out = remote(gg_out.at[core], gg_out.at[core], g_s.at[n_chip + 1], g_r.at[n_chip + 1], mate)
    g_swap_out.start()
    remote(gg_out.at[core], gg_out.at[1 - core], g_s.at[n_chip + 1], g_r.at[n_chip + 1], mate).wait_recv()
    store_gg = local(gg_out, gg_hbm, out_sem.at[3])
    store_gg.start()

    finish_ring(h_ring)
    for item in pos_sends + [g_swap, g_swap_out]:
        item.wait_send()
    for t in near_targets:
        remote(at_st.at[0], at_rv.at[pl.ds(0, hw)], a_s.at[t], a_r.at[t], t).wait_send()
        remote(dqt_st.at[0], dt_rv.at[pl.ds(0, hw)], q_s.at[t], q_r.at[t], t).wait_send()
    for item in kv_sends + w_sends + g_sends + wk_sends:
        item.wait_send()
    for t in targets:
        remote(dwt.at[pl.ds(0, hw), part_of(t, tok)], gw_hbm.at[part_of(t, hw)], w_s.at[t], w_r.at[t], t).wait_recv()
        remote(dwt.at[pl.ds(hw, hd), part_of(t, tok)], gw_hbm.at[kv_place(t)], wk_s.at[t], wk_r.at[t], t).wait_recv()
    for item in (w_own, wk_own, store_wo, store_gx, store_gg):
        item.wait()


def settle_kernel(q_rows, kv_w, out_i, gx_i, gw_i, gwo_i, gg_i, out_o, gx_o, gq_o, gk_o, gv_o, gwo_o, gain_o, bias_o, b_act, b_q, b_kv, b_o, b_gg, sem_in, sem_out, sem_gg):
    half_q = q_rows // 2
    half_o = gwo_i.shape[0] // 2
    moves = [(out_i, b_act.at[0], out_o), (gx_i, b_act.at[1], gx_o)]
    for t in range(2):
        moves.append((gw_i.at[pl.ds(half_q * t, half_q)], b_q.at[t], gq_o.at[pl.ds(half_q * t, half_q)]))
        moves.append((gwo_i.at[pl.ds(half_o * t, half_o)], b_o.at[t], gwo_o.at[pl.ds(half_o * t, half_o)]))
    moves.append((gw_i.at[pl.ds(q_rows, kv_w)], b_kv.at[0], gk_o))
    moves.append((gw_i.at[pl.ds(q_rows + kv_w, kv_w)], b_kv.at[1], gv_o))
    loads = [pltpu.make_async_copy(src, mid, sem_in.at[i]) for i, (src, mid, _) in enumerate(moves)]
    stores = [pltpu.make_async_copy(mid, dst, sem_out.at[i]) for i, (_, mid, dst) in enumerate(moves)]
    load_gg = pltpu.make_async_copy(gg_i, b_gg, sem_gg)
    load_gg.start()
    for item in loads:
        item.start()
    for load, store in zip(loads, stores):
        load.wait()
        store.start()
    load_gg.wait()
    gain_o[...] = b_gg[0, 0]
    bias_o[...] = b_gg[1, 0]
    for item in stores:
        item.wait()


def solution(mesh):
    n_dev = mesh.shape['cp']

    def device_step(x_act, d_out, positions, ln_gain, ln_bias, w_query, w_key, w_value, w_out):
        tok, width = x_act.shape[1], x_act.shape[2]
        q_heads, hd = w_query.shape[1], w_query.shape[2]
        kv_heads = w_key.shape[1]
        q_w, kv_w = q_heads * hd, kv_heads * hd
        n_rows = q_w + 2 * kv_w
        seq = n_dev * tok
        hw = 2 * hd

        def flat_weight(w):
            return jnp.transpose(w, (1, 2, 0)).reshape(-1, width)

        hbm = pl.BlockSpec(memory_space=pltpu.HBM)
        vmem = pl.BlockSpec(memory_space=pltpu.VMEM)
        dma = pltpu.SemaphoreType.DMA
        n_chip = n_dev // 2
        n_far = n_chip - 1 - 2 * NEAR
        pair = 2 * tok
        scratch = [
            pltpu.VMEM((n_chip, pair, width), BF),
            pltpu.VMEM((n_chip, pair, width), BF),
            pltpu.VMEM((n_rows, width), BF),
            pltpu.VMEM((2 * hw, width), BF),
            pltpu.VMEM((hw, width), BF),
            pltpu.VMEM((n_far * hw, width), BF),
            pltpu.VMEM((n_dev, 1, tok), jnp.int32),
            pltpu.VMEM((n_chip, hd // 2, pair), F32),
            pltpu.VMEM((n_chip, hd, 2 * pair), BF),
            pltpu.VMEM((hw, seq), BF),
            pltpu.VMEM((seq, hw), BF),
            pltpu.VMEM((n_far, hw, seq), BF),
            pltpu.VMEM((n_far, seq, hw), BF),
            pltpu.VMEM((hw, 4 * pair), BF),
            pltpu.VMEM((4 * pair, hw), BF),
            pltpu.VMEM((seq, 2 * pair), F32),
            pltpu.VMEM((seq, 2 * pair), F32),
            pltpu.VMEM((n_chip, 1, 2 * pair), F32),
            pltpu.VMEM((hw, 2 * pair), F32),
            pltpu.VMEM((seq, hw), F32),
            pltpu.VMEM((hw, seq), F32),
            pltpu.VMEM((hd, seq), F32),
            pltpu.VMEM((n_dev, hd, tok), BF),
            pltpu.VMEM((hd, seq), BF),
            pltpu.VMEM((hw, width), F32),
            pltpu.VMEM((hw + hd, width), F32),
            pltpu.VMEM((n_dev, hw, tok), BF),
            pltpu.VMEM((n_dev, hw, tok), BF),
            pltpu.VMEM((q_w, tok), BF),
            pltpu.VMEM((n_rows, tok), BF),
            pltpu.VMEM((tok, q_w), BF),
            pltpu.VMEM((tok, n_rows), BF),
            pltpu.VMEM((tok, width), BF),
            pltpu.VMEM((tok, width), BF),
            pltpu.VMEM((2, 1, width), F32),
            pltpu.VMEM((2, tok, 128), F32),
            pltpu.VMEM((tok, width), BF),
            pltpu.VMEM((2, 1, width), F32),
            pltpu.VMEM((1, width), F32),
            pltpu.VMEM((1, width), F32),
            pltpu.VMEM((n_chip, 1, width), F32),
            pltpu.VMEM((2, 1, width), F32),
            dma((10,)), dma((2 * n_far,)), dma((n_chip,)), dma((3,)), dma((4,)), dma((2,)),
            dma((16,)), dma((14,)), dma((16,)), dma((16,)),
            dma((16,)), dma((14,)), dma((16,)), dma((16,)),
        ] + [dma((n_dev,))] * 6 + [dma] * 2 + [dma((n_dev,))] * 8
        out, gx, gw, gwo, gg = pl.pallas_call(
            functools.partial(block_kernel, n_dev, hd, kv_w, NEAR),
            out_shape=(
                jax.ShapeDtypeStruct((tok, width), BF),
                jax.ShapeDtypeStruct((tok, width), BF),
                jax.ShapeDtypeStruct((n_rows, tok), F32),
                jax.ShapeDtypeStruct((hw, width), F32),
                jax.ShapeDtypeStruct((2, 1, width), F32),
            ),
            in_specs=[hbm] * 9,
            out_specs=(hbm,) * 5,
            scratch_shapes=scratch,
            compiler_params=pltpu.CompilerParams(collective_id=0, has_side_effects=True, vmem_limit_bytes=67043328),
            name='attn_block',
        )(
            x_act.reshape(tok, width), d_out.reshape(tok, width), positions.reshape(1, tok),
            ln_gain.reshape(1, width), ln_bias.reshape(1, width),
            flat_weight(w_query), flat_weight(w_key), flat_weight(w_value), w_out,
        )

        out, gx, gq, gk, gv, gwo, gain, bias = pl.pallas_call(
            functools.partial(settle_kernel, q_w, kv_w),
            out_shape=(
                jax.ShapeDtypeStruct((tok, width), BF),
                jax.ShapeDtypeStruct((tok, width), BF),
                jax.ShapeDtypeStruct((q_w, tok), F32),
                jax.ShapeDtypeStruct((kv_w, tok), F32),
                jax.ShapeDtypeStruct((kv_w, tok), F32),
                jax.ShapeDtypeStruct((hw, width), F32),
                jax.ShapeDtypeStruct((width,), F32),
                jax.ShapeDtypeStruct((width,), F32),
            ),
            in_specs=[hbm] * 5,
            out_specs=(hbm,) * 6 + (vmem,) * 2,
            scratch_shapes=[
                pltpu.VMEM((2, tok, width), BF),
                pltpu.VMEM((2, q_w // 2, tok), F32),
                pltpu.VMEM((2, kv_w, tok), F32),
                pltpu.VMEM((2, hw // 2, width), F32),
                pltpu.VMEM((2, 1, width), F32),
                dma((8,)), dma((8,)), dma,
            ],
            name='settle',
        )(out, gx, gw, gwo, gg)

        def rows_out(block, heads):
            return jnp.transpose(block.reshape(heads, hd, tok), (2, 0, 1))

        return (
            out.reshape(1, tok, width), gx.reshape(1, tok, width),
            rows_out(gq, q_heads), rows_out(gk, kv_heads), rows_out(gv, kv_heads),
            gwo, gain, bias,
        )

    return jax.shard_map(device_step, mesh=mesh, in_specs=(P('dp', 'cp', None), P('dp', 'cp', None), P('dp', 'cp'), P(None), P(None), P(None, None, None), P(None, None, None), P(None, None, None), P(None, None)), out_specs=(P('dp', 'cp', None), P('dp', 'cp', None), P(('dp', 'cp'), None, None), P(('dp', 'cp'), None, None), P(('dp', 'cp'), None, None), P(('dp', 'cp'), None), P('dp'), P('dp')), check_vma=False)
```

```python
import functools
import math

import jax
import jax.numpy as jnp
from jax import lax
from jax.experimental import pallas as pl
from jax.experimental.pallas import tpu as pltpu
from jax.sharding import PartitionSpec as P

EPS = 1e-5
ROPE_BASE = 10000.0
MESH = pl.DeviceIdType.MESH
BF = jnp.bfloat16
F32 = jnp.float32
NEAR = 1
PARTS = 4


def dot(lhs, rhs):
    return jnp.dot(lhs, rhs, preferred_element_type=F32)


def dot_t(lhs, rhs):
    return lax.dot_general(lhs, rhs, (((1,), (1,)), ((), ())), preferred_element_type=F32)


def block_kernel(
    n_dev, hd, kv_w, near, parts,
    x_hbm, dy_hbm, pos_hbm, gain_hbm, bias_hbm, wq_hbm, wk_hbm, wv_hbm, wo_hbm,
    out_hbm, gx_hbm, gw_hbm, gwo_hbm, gg_hbm,
    hb, dyb, wt, wi, woi, w_far, pos_all, trig,
    qt, kvt, kv, kvt_far, kv_far, q_far, da_far, bmat, bmat_t, sbuf, dpbuf, mbuf, adq, dkv, dkvt, kv_rv, kv_mine, kv_row,
    dwo, dwt, at_st, dqt_st, at_rv, dt_rv, a_nat, d_nat, x_v, dy_own, gb_v, stat, out_v, gg_st, gg_mx, gg_my, gg_rv, gg_out,
    in_sem, far_sem, wo_sem, w_sem, out_sem, loc_sem,
    hzs, hzr, hds, hdr, yzs, yzr, yds, ydr,
    pos_s, pos_r, a_s, a_r, q_s, q_r, x_s, x_r, kv_s, kv_r, w_s, w_r, wk_s, wk_r, g_s, g_r,
):
    tok, width = x_v.shape
    n_chip = n_dev // 2
    pair = 2 * tok
    me = lax.axis_index('cp')
    chip = me // 2
    core = me % 2
    right = 2 * ((chip + 1) % n_chip) + core
    left = 2 * ((chip + n_chip - 1) % n_chip) + core
    mate = 2 * chip + 1 - core
    q_rows = wq_hbm.shape[0]
    n_rows = q_rows + 2 * kv_w
    hw = 2 * hd
    quarter = hd // 4
    tile = 256
    scale = hd ** -0.5
    cols_q = 2 * pair
    n_far = n_chip - 1 - 2 * near

    def remote(src, dst, send, recv, target):
        return pltpu.make_async_remote_copy(src_ref=src, dst_ref=dst, send_sem=send, recv_sem=recv, device_id={'cp': target}, device_id_type=MESH)

    def local(src, dst, sem):
        return pltpu.make_async_copy(src, dst, sem)

    def part_of(i, size):
        return pl.ds(pl.multiple_of(i * size, size), size)

    def ring_steps(k):
        step = (k + 1) // 2
        return step, k % 2

    def ring_origin(k):
        step, ahead = ring_steps(k)
        return jnp.where(ahead == 1, chip + n_chip - step, chip + step) % n_chip

    own = (chip, part_of(core, tok))
    first_loads = [
        local(x_hbm, x_v, in_sem.at[0]),
        local(gain_hbm, gb_v.at[0], in_sem.at[1]),
        local(bias_hbm, gb_v.at[1], in_sem.at[2]),
        local(pos_hbm, pos_all.at[me], in_sem.at[3]),
    ]
    for item in first_loads:
        item.start()
    barrier = pltpu.get_barrier_semaphore()
    for step in range(1, n_dev):
        pl.semaphore_signal(barrier, inc=1, device_id={'cp': (me + step) % n_dev}, device_id_type=MESH)
    own_rows = part_of(me, hw)
    kv_rows = part_of(chip, hd)
    loads = [
        local(wq_hbm.at[own_rows], wi.at[pl.ds(0, hw)], in_sem.at[4]),
        local(wk_hbm.at[kv_rows], wi.at[pl.ds(hw, hd)], in_sem.at[5]),
        local(wv_hbm.at[kv_rows], wi.at[pl.ds(hw + hd, hd)], in_sem.at[6]),
        local(wo_hbm.at[own_rows], woi, in_sem.at[7]),
        local(dy_hbm, dyb.at[own], in_sem.at[8]),
        local(dy_hbm, dy_own, in_sem.at[9]),
    ]
    for f in range(n_far):
        far_rows = part_of(ring_origin(2 * near + 1 + f), hd)
        loads.append(local(wk_hbm.at[far_rows], w_far.at[pl.ds(hw * f, hd)], far_sem.at[2 * f]))
        loads.append(local(wv_hbm.at[far_rows], w_far.at[pl.ds(hw * f + hd, hd)], far_sem.at[2 * f + 1]))
        far_wo = part_of(ring_origin(2 * near + 1 + f), 2 * hw)
        loads.append(local(wo_hbm.at[far_wo], wt.at[pl.ds(2 * hw * f, 2 * hw)], far_sem.at[2 * n_far + f]))
    for item in loads:
        item.start()

    for item in first_loads:
        item.wait()
    gain_one = 1.0 + gb_v[0]
    x_f = x_v[...].astype(F32)
    mean = jnp.mean(x_f, axis=-1, keepdims=True)
    centered = x_f - mean
    inv_std = lax.rsqrt(jnp.mean(centered * centered, axis=-1, keepdims=True) + EPS)
    hb[chip, part_of(core, tok), :] = (centered * inv_std * gain_one + gb_v[1]).astype(BF)
    stat[0] = jnp.broadcast_to(mean, (tok, 128))
    stat[1] = jnp.broadcast_to(inv_std, (tok, 128))

    pl.semaphore_wait(barrier, n_dev - 1)

    def chunk(buf, origin, parity, part):
        return buf.at[origin, part_of(parts * parity + part, tok // parts)]

    turns = 2 * parts

    def own_sends(buf, zs, zr, ds, dr):
        copies = []
        for part in range(parts):
            piece = chunk(buf, chip, core, part)
            copies.append(remote(piece, piece, zs.at[2 * part], zr.at[2 * part], right))
            copies.append(remote(piece, piece, zs.at[2 * part + 1], zr.at[2 * part + 1], left))
            copies.append(remote(piece, piece, ds.at[7 * parts + part], dr.at[7 * parts + part], mate))
        return copies

    def event_place(event):
        step = event // turns + 1
        turn = event % turns
        direction = turn % 2
        part = jnp.where(step < 4, turn // 2, turn // 2 + direction * (parts // 2))
        origin = jnp.where(direction == 0, chip + n_chip - step, chip + step) % n_chip
        return step, direction, part, origin

    def last_event(part, direction):
        return 6 * parts + 2 * (part - direction * (parts // 2)) + direction

    def ring_event(ring, event):
        buf, zs, zr, ds, dr = ring
        step, direction, part, origin = event_place(event)
        piece = chunk(buf, origin, core, part)
        remote(piece, piece, zs.at[0], zr.at[event], right).wait_recv()
        onward = jnp.where(step < 3, event + turns, last_event(part, direction))

        @pl.when((step < 3) | ((step == 3) & ((part >= parts // 2) == (direction == 1))))
        def _():
            remote(piece, piece, zs.at[event + turns], zr.at[onward], jnp.where(direction == 0, right, left)).start()

        remote(piece, piece, ds.at[event], dr.at[event], mate).start()

    def ring_service(ring, event):
        @pl.when(event < 7 * parts)
        def _():
            ring_event(ring, event)

    def ring_mate(ring, k, origin):
        buf, zs, zr, ds, dr = ring
        step, ahead = ring_steps(k)
        for part in range(parts):
            event = jnp.where(k == 0, 7 * parts + part, jnp.where(step < 4, turns * (step - 1) + 2 * part + 1 - ahead, last_event(part, part // (parts // 2))))
            piece = chunk(buf, origin, 1 - core, part)
            remote(piece, piece, ds.at[0], dr.at[event], mate).wait_recv()

    def finish_ring(ring):
        buf, zs, zr, ds, dr = ring
        for item in own_sends(*ring):
            item.wait_send()

        @pl.loop(0, 7 * parts)
        def _(event):
            step, direction, part, origin = event_place(event)
            piece = chunk(buf, origin, core, part)

            @pl.when((step < 3) | ((step == 3) & ((part >= parts // 2) == (direction == 1))))
            def _():
                remote(piece, piece, zs.at[event + turns], zr.at[event], right).wait_send()

            remote(piece, piece, ds.at[event], dr.at[event], mate).wait_send()

    h_ring = (hb, hzs, hzr, hds, hdr)
    y_ring = (dyb, yzs, yzr, yds, ydr)
    for item in own_sends(*h_ring):
        item.start()
    pos_sends = [remote(pos_all.at[me], pos_all.at[me], pos_s.at[step], pos_r.at[step], (me + step) % n_dev) for step in range(1, n_dev)]
    for item in pos_sends:
        item.start()
    weight_loads = [
        local(wq_hbm, wt.at[pl.ds(0, q_rows)], w_sem.at[0]),
        local(wk_hbm, wt.at[pl.ds(q_rows, kv_w)], w_sem.at[1]),
        local(wv_hbm, wt.at[pl.ds(q_rows + kv_w, kv_w)], w_sem.at[2]),
    ]
    dkv[...] = jnp.zeros_like(dkv)
    dwo[...] = jnp.zeros_like(dwo)
    dwt[...] = jnp.zeros_like(dwt)
    bmat[...] = jnp.zeros_like(bmat)

    freq = jnp.exp(lax.broadcasted_iota(jnp.int32, (quarter, tok), 0).astype(F32) * (-2.0 * math.log(ROPE_BASE) / (hd // 2)))

    def make_trig(slot):
        angle = pos_all[slot].astype(F32) * freq
        trig[slot // 2, 0:quarter, part_of(slot % 2, tok)] = jnp.cos(angle)
        trig[slot // 2, quarter:2 * quarter, part_of(slot % 2, tok)] = jnp.sin(angle)

    make_trig(me)

    @pl.loop(1, n_dev)
    def _(step):
        source = (me + n_dev - step) % n_dev
        remote(pos_all.at[source], pos_all.at[source], pos_s.at[step], pos_r.at[step], me).wait_recv()
        make_trig(source)

    for item in loads:
        item.wait()

    @pl.loop(0, n_far)
    def _(f):
        da_t = dot_t(wt[part_of(f, 2 * hw), :], dy_own[...]).astype(BF)
        for head in range(4):
            da_far[f, :, tok * head:tok * head + tok] = da_t[hd * head:hd * head + hd]

    for item in weight_loads:
        item.start()

    def turned(val, cos_t, sin_t):
        u = val[0:quarter]
        w = val[quarter:2 * quarter]
        return [u * cos_t - w * sin_t, w * cos_t + u * sin_t, val[2 * quarter:hd]]

    def eighth(val):
        return val.astype(BF) * jnp.asarray(scale, BF)

    def keys_values(val, cos_t, sin_t):
        return jnp.concatenate(turned(val[0:hd], cos_t, sin_t) + [val[hd:hw]], axis=0).astype(BF)

    @pl.loop(0, n_chip)
    def _(k):
        for turn in range(parts):
            ring_service(h_ring, parts * k + turn)

        @pl.when(k == 5)
        def _():
            for item in own_sends(*y_ring):
                item.start()

        @pl.when(k == 4)
        def _():
            for item in weight_loads:
                item.wait()

            @pl.loop(0, n_far)
            def _(f):
                cos_t = trig[chip, 0:quarter, part_of(core, tok)]
                sin_t = trig[chip, quarter:2 * quarter, part_of(core, tok)]
                q_t = dot_t(wt[part_of(ring_origin(2 * near + 1 + f), 2 * hw), :], hb[chip, part_of(core, tok), :])
                for head in range(4):
                    q_far[f, :, tok * head:tok * head + tok] = eighth(jnp.concatenate(turned(q_t[hd * head:hd * head + hd], cos_t, sin_t), axis=0))

        b = ring_origin(k)
        ring_mate(h_ring, k, b)
        place = part_of(b, pair)
        cos_t = trig[b, 0:quarter, :]
        sin_t = trig[b, quarter:2 * quarter, :]
        flat = dot_t(wi[...], hb[b])
        for head in range(2):
            q_rot = eighth(jnp.concatenate(turned(flat[hd * head:hd * head + hd], cos_t, sin_t), axis=0))
            for t in range(2):
                lane = pair * t + tok * head
                qt[b, :, lane:lane + tok] = q_rot[:, tok * t:tok * t + tok]
        kv_rot = keys_values(flat[hw:2 * hw], cos_t, sin_t)
        kvt[:, place] = kv_rot
        kv[place, :] = kv_rot.T

        @pl.when(b <= chip)
        def _():
            flat_far = dot_t(w_far[...], hb[b])
            for f in range(n_far):
                far_rot = keys_values(flat_far[hw * f:hw * f + hw], cos_t, sin_t)
                kvt_far[f, :, place] = far_rot
                kv_far[f, place, :] = far_rot.T

    groups = [slice(tile * g, tile * g + tile) for g in range(cols_q // tile)]

    def first_part(b, seen, kv_of):
        def scores(c, at):
            rows = part_of(c, pair)
            keys = kv_of(rows)
            s = dot(keys, bmat[:, at])
            d_p = dot(keys, bmat[:, cols_q + at.start:cols_q + at.stop])
            dpbuf[rows, at] = d_p
            return rows, s, d_p

        begin = []
        for at in groups:
            rows, s, d_p = scores(b, at)
            s = jnp.where(seen(at), s, -1e30)
            top = jnp.max(s, axis=0, keepdims=True)
            p = jnp.exp(s - top)
            sbuf[rows, at] = p
            mbuf[b, :, at] = top
            begin += [top, jnp.sum(p, axis=0, keepdims=True), jnp.sum(p * d_p, axis=0, keepdims=True)]

        def step(c, state):
            after = []
            for g, at in enumerate(groups):
                old, total, weighted = state[3 * g:3 * g + 3]
                rows, s, d_p = scores(c, at)
                new = jnp.maximum(old, jnp.max(s, axis=0, keepdims=True))
                p = jnp.exp(s - new)
                sbuf[rows, at] = p
                mbuf[c, :, at] = new
                keep = jnp.exp(old - new)
                after += [new, total * keep + jnp.sum(p, axis=0, keepdims=True), weighted * keep + jnp.sum(p * d_p, axis=0, keepdims=True)]
            return after

        state = lax.fori_loop(0, b, step, begin)
        stats = []
        for g in range(len(groups)):
            top, total, weighted = state[3 * g:3 * g + 3]
            inv = 1.0 / total
            stats.append((top, inv, weighted * inv))
        return stats

    def second_part(b, stats, kvt_of, with_keys):
        adq[...] = jnp.zeros_like(adq)

        def step(c, carry):
            rows = part_of(c, pair)
            grad = None
            for at, (top, inv, row_dot) in zip(groups, stats):
                p = sbuf[rows, at] * (jnp.exp(mbuf[c, :, at] - top) * inv)
                p_b = p.astype(BF)
                ds_b = (p * (dpbuf[rows, at] - row_dot)).astype(BF)
                adq[0:hd, at] += dot(kvt_of(slice(0, hd), rows), ds_b)
                adq[hd:hw, at] += dot(kvt_of(slice(hd, hw), rows), p_b)
                if with_keys:
                    more = dot(ds_b, bmat_t[at, :]) + dot(p_b, bmat_t[cols_q + at.start:cols_q + at.stop, :])
                    grad = more if grad is None else grad + more
            if with_keys:
                dkv[rows, :] += grad
            return carry

        lax.fori_loop(0, b + 1, step, 0)

    lane = lax.broadcasted_iota(jnp.int32, (pair, tile), 1)
    row = lax.broadcasted_iota(jnp.int32, (pair, tile), 0)

    @pl.loop(0, n_chip)
    def _(k):
        for turn in range(parts - 1):
            ring_service(y_ring, parts * k + turn)
        b = ring_origin(k)
        ring_mate(y_ring, k, b)
        da_t = dot_t(woi[...], dyb[b]).astype(BF)
        bmat[0:hd, 0:cols_q] = qt[b]
        for t in range(2):
            for head in range(2):
                at = cols_q + pair * t + tok * head
                bmat[hd:hw, at:at + tok] = da_t[hd * head:hd * head + hd, tok * t:tok * t + tok]
        for t in range(2 * cols_q // tok):
            bmat_t[tok * t:tok * t + tok, :] = bmat[:, tok * t:tok * t + tok].T
        stats = first_part(b, lambda at: row <= (at.start // pair) * tok + lane % tok, lambda rows: kv[rows, :])
        ring_service(y_ring, parts * k + parts - 1)
        second_part(b, stats, lambda part, rows: kvt[part, rows], True)
        a_pair = []
        dq_pair = []
        for t in range(2):
            slot = 2 * b + t
            lanes = [slice(pair * t + tok * head, pair * t + tok * head + tok) for head in range(2)]
            a_t = jnp.concatenate([adq[hd:hw, at] for at in lanes], axis=0).astype(BF)
            cos_t = trig[b, 0:quarter, tok * t:tok * t + tok]
            sin_t = trig[b, quarter:2 * quarter, tok * t:tok * t + tok]
            dq_t = jnp.concatenate([piece for at in lanes for piece in turned(adq[0:hd, at] * scale, cos_t, -sin_t)], axis=0).astype(BF)
            a_pair.append(a_t)
            dq_pair.append(dq_t)

            @pl.when(slot == me)
            def _():
                at_rv[own_rows, :] = a_t
                dt_rv[own_rows, :] = dq_t

            @pl.when((slot != me) & (k < 1 + 2 * near))
            def _():
                at_st[slot] = a_t
                dqt_st[slot] = dq_t
                remote(dqt_st.at[slot], dt_rv.at[own_rows], q_s.at[slot], q_r.at[me], slot).start()
                remote(at_st.at[slot], at_rv.at[own_rows], a_s.at[slot], a_r.at[me], slot).start()

        a_pair = jnp.concatenate(a_pair, axis=1)
        dq_pair = jnp.concatenate(dq_pair, axis=1)
        for t in range(width // tile):
            cols = slice(tile * t, tile * t + tile)
            dwo[:, cols] += dot(a_pair, dyb[b, :, cols])
            dwt[0:hw, cols] += dot(dq_pair, hb[b, :, cols])

    far = [ring_origin(k) for k in range(1, n_chip)]
    targets = [mate] + [2 * c + p for c in far for p in range(2)]
    near_targets = targets[0:1 + 4 * near]
    w_sends = [remote(dwt.at[pl.ds(0, hw), part_of(t, tok)], gw_hbm.at[own_rows], w_s.at[t], w_r.at[me], t) for t in targets]
    for item in w_sends:
        item.start()
    w_own = local(dwt.at[pl.ds(0, hw), part_of(me, tok)], gw_hbm.at[own_rows], loc_sem.at[0])
    w_own.start()

    for t in range(n_dev):
        dkvt[:, tok * t:tok * t + tok] = dkv[tok * t:tok * t + tok, :].T
    swap = remote(dkvt.at[part_of(1 - core, hd)], kv_rv, x_s, x_r, mate)
    swap.start()
    store_wo = local(dwo, gwo_hbm, out_sem.at[0])
    store_wo.start()

    finish_ring(y_ring)
    wo_loads = [local(wo_hbm.at[pl.ds(pair * t, pair)], dyb.at[t], wo_sem.at[t]) for t in range(n_chip)]
    for item in wo_loads:
        item.start()

    swap.wait_recv()
    mine = part_of(core, hd)
    g_rows = pl.ds(pl.multiple_of(q_rows + core * kv_w + chip * hd, hd), hd)
    for t in range(n_chip):
        cols = slice(pair * t, pair * t + pair)
        g = dkvt[mine, cols] + kv_rv[:, cols]
        cos_t = jnp.where(core == 0, trig[t, 0:quarter, :], 1.0)
        sin_t = jnp.where(core == 0, trig[t, quarter:2 * quarter, :], 0.0)
        g_b = jnp.concatenate(turned(g, cos_t, -sin_t), axis=0).astype(BF)
        kv_mine[2 * t] = g_b[:, 0:tok]
        kv_mine[2 * t + 1] = g_b[:, tok:pair]
        kv_row[:, cols] = g_b
    dt_rv[g_rows, :] = kv_mine[me]
    kv_sends = [remote(kv_mine.at[t], dt_rv.at[g_rows], kv_s.at[t], kv_r.at[me], t) for t in targets]
    for item in kv_sends:
        item.start()
    for t in range(width // tile):
        cols = slice(tile * t, tile * t + tile)
        acc = jnp.zeros((hd, tile), F32)
        for s in range(n_chip):
            acc += dot(kv_row[:, pair * s:pair * s + pair], hb[s, :, cols])
        dwt[hw:hw + hd, cols] = acc
    wk_own = local(dwt.at[pl.ds(hw, hd), part_of(me, tok)], gw_hbm.at[g_rows], loc_sem.at[1])
    wk_own.start()
    wk_sends = [remote(dwt.at[pl.ds(hw, hd), part_of(t, tok)], gw_hbm.at[g_rows], wk_s.at[t], wk_r.at[me], t) for t in targets]
    for item in wk_sends:
        item.start()

    @pl.loop(0, n_far)
    def _(f):
        c_far = ring_origin(2 * near + 1 + f)
        cos_t = trig[chip, 0:quarter, part_of(core, tok)]
        sin_t = trig[chip, quarter:2 * quarter, part_of(core, tok)]
        bmat[0:hd, 0:cols_q] = q_far[f]
        bmat[hd:hw, cols_q:2 * cols_q] = da_far[f]
        stats = first_part(chip, lambda at: row <= core * tok + lane % tok, lambda rows: kv_far[f, rows, :])
        second_part(chip, stats, lambda part, rows: kvt_far[f, part, rows], False)
        for head in range(4):
            at = slice(tok * head, tok * head + tok)
            place = pl.ds(pl.multiple_of(c_far * 2 * hw + hd * head, hd), hd)
            at_rv[place, :] = adq[hd:hw, at].astype(BF)
            dt_rv[place, :] = jnp.concatenate(turned(adq[0:hd, at] * scale, cos_t, -sin_t), axis=0).astype(BF)

    for t in near_targets:
        remote(at_st.at[0], at_rv.at[part_of(t, hw)], a_s.at[t], a_r.at[t], t).wait_recv()
    for item in wo_loads:
        item.wait()
    for t in range(q_rows // tok):
        a_nat[:, tok * t:tok * t + tok] = at_rv[tok * t:tok * t + tok, :].T
    for t in range(width // tile):
        cols = slice(tile * t, tile * t + tile)
        prod = jnp.zeros((tok, tile), F32)
        for s in range(n_chip):
            prod += dot(a_nat[:, pair * s:pair * s + pair], dyb[s, :, cols])
        out_v[:, cols] = (x_v[:, cols].astype(F32) + prod).astype(BF)
    store_out = local(out_v, out_hbm, out_sem.at[1])
    store_out.start()

    def kv_place(t):
        return pl.ds(pl.multiple_of(q_rows + (t % 2) * kv_w + (t // 2) * hd, hd), hd)

    for t in near_targets:
        remote(dqt_st.at[0], dt_rv.at[part_of(t, hw)], q_s.at[t], q_r.at[t], t).wait_recv()
    for t in targets:
        remote(kv_mine.at[0], dt_rv.at[kv_place(t)], kv_s.at[t], kv_r.at[t], t).wait_recv()
    swap.wait_send()
    for t in range(n_rows // tok):
        d_nat[:, tok * t:tok * t + tok] = dt_rv[tok * t:tok * t + tok, :].T

    mean = stat[0, :, 0:1]
    inv_std = stat[1, :, 0:1]
    dh = dkvt
    for t in range(width // tile):
        cols = slice(tile * t, tile * t + tile)
        acc = jnp.zeros((tok, tile), F32)
        for s in range(n_rows // tile):
            acc += dot(d_nat[:, tile * s:tile * s + tile], wt[tile * s:tile * s + tile, cols])
        dh[:, cols] = acc
        gg_st[0, :, cols] = jnp.sum(acc * ((x_v[:, cols].astype(F32) - mean) * inv_std), axis=0, keepdims=True)
        gg_st[1, :, cols] = jnp.sum(acc, axis=0, keepdims=True)
    g_swap = remote(gg_st.at[1 - core], gg_mx, g_s.at[n_chip], g_r.at[n_chip], mate)
    g_swap.start()
    g_swap.wait_recv()
    gg_my[...] = jnp.where(core == 0, gg_st[0], gg_st[1]) + gg_mx[...]
    gg_rv[chip] = gg_my[...]
    g_sends = [remote(gg_my, gg_rv.at[chip], g_s.at[c], g_r.at[chip], 2 * c + core) for c in far]
    for item in g_sends:
        item.start()

    grad_hat = dh[...] * gain_one
    x_hat = (x_v[...].astype(F32) - mean) * inv_std
    mean_one = jnp.mean(grad_hat, axis=-1, keepdims=True)
    mean_two = jnp.mean(grad_hat * x_hat, axis=-1, keepdims=True)
    store_out.wait()
    out_v[...] = (dy_own[...].astype(F32) + inv_std * (grad_hat - mean_one - x_hat * mean_two)).astype(BF)
    store_gx = local(out_v, gx_hbm, out_sem.at[2])
    store_gx.start()

    for c in far:
        remote(gg_my, gg_rv.at[c], g_s.at[c], g_r.at[c], 2 * c + core).wait_recv()
    sums = gg_rv[0]
    for c in range(1, n_chip):
        sums = sums + gg_rv[c]
    gg_out[core] = sums
    g_swap_out = remote(gg_out.at[core], gg_out.at[core], g_s.at[n_chip + 1], g_r.at[n_chip + 1], mate)
    g_swap_out.start()
    remote(gg_out.at[core], gg_out.at[1 - core], g_s.at[n_chip + 1], g_r.at[n_chip + 1], mate).wait_recv()
    store_gg = local(gg_out, gg_hbm, out_sem.at[3])
    store_gg.start()

    finish_ring(h_ring)
    for item in pos_sends + [g_swap, g_swap_out]:
        item.wait_send()
    for t in near_targets:
        remote(at_st.at[0], at_rv.at[pl.ds(0, hw)], a_s.at[t], a_r.at[t], t).wait_send()
        remote(dqt_st.at[0], dt_rv.at[pl.ds(0, hw)], q_s.at[t], q_r.at[t], t).wait_send()
    for item in kv_sends + w_sends + g_sends + wk_sends:
        item.wait_send()
    for t in targets:
        remote(dwt.at[pl.ds(0, hw), part_of(t, tok)], gw_hbm.at[part_of(t, hw)], w_s.at[t], w_r.at[t], t).wait_recv()
        remote(dwt.at[pl.ds(hw, hd), part_of(t, tok)], gw_hbm.at[kv_place(t)], wk_s.at[t], wk_r.at[t], t).wait_recv()
    for item in (w_own, wk_own, store_wo, store_gx, store_gg):
        item.wait()


def settle_kernel(q_rows, kv_w, out_i, gx_i, gw_i, gwo_i, gg_i, out_o, gx_o, gq_o, gk_o, gv_o, gwo_o, gain_o, bias_o, b_act, b_q, b_kv, b_o, b_gg, sem_in, sem_out, sem_gg):
    half_q = q_rows // 2
    half_o = gwo_i.shape[0] // 2
    moves = [(out_i, b_act.at[0], out_o), (gx_i, b_act.at[1], gx_o)]
    for t in range(2):
        moves.append((gw_i.at[pl.ds(half_q * t, half_q)], b_q.at[t], gq_o.at[pl.ds(half_q * t, half_q)]))
        moves.append((gwo_i.at[pl.ds(half_o * t, half_o)], b_o.at[t], gwo_o.at[pl.ds(half_o * t, half_o)]))
    moves.append((gw_i.at[pl.ds(q_rows, kv_w)], b_kv.at[0], gk_o))
    moves.append((gw_i.at[pl.ds(q_rows + kv_w, kv_w)], b_kv.at[1], gv_o))
    loads = [pltpu.make_async_copy(src, mid, sem_in.at[i]) for i, (src, mid, _) in enumerate(moves)]
    stores = [pltpu.make_async_copy(mid, dst, sem_out.at[i]) for i, (_, mid, dst) in enumerate(moves)]
    load_gg = pltpu.make_async_copy(gg_i, b_gg, sem_gg)
    load_gg.start()
    for item in loads:
        item.start()
    for load, store in zip(loads, stores):
        load.wait()
        store.start()
    load_gg.wait()
    gain_o[...] = b_gg[0, 0]
    bias_o[...] = b_gg[1, 0]
    for item in stores:
        item.wait()


def solution(mesh):
    n_dev = mesh.shape['cp']

    def device_step(x_act, d_out, positions, ln_gain, ln_bias, w_query, w_key, w_value, w_out):
        tok, width = x_act.shape[1], x_act.shape[2]
        q_heads, hd = w_query.shape[1], w_query.shape[2]
        kv_heads = w_key.shape[1]
        q_w, kv_w = q_heads * hd, kv_heads * hd
        n_rows = q_w + 2 * kv_w
        seq = n_dev * tok
        hw = 2 * hd

        def flat_weight(w):
            return jnp.transpose(w, (1, 2, 0)).reshape(-1, width)

        hbm = pl.BlockSpec(memory_space=pltpu.HBM)
        vmem = pl.BlockSpec(memory_space=pltpu.VMEM)
        dma = pltpu.SemaphoreType.DMA
        n_chip = n_dev // 2
        n_far = n_chip - 1 - 2 * NEAR
        pair = 2 * tok
        scratch = [
            pltpu.VMEM((n_chip, pair, width), BF),
            pltpu.VMEM((n_chip, pair, width), BF),
            pltpu.VMEM((n_rows, width), BF),
            pltpu.VMEM((2 * hw, width), BF),
            pltpu.VMEM((hw, width), BF),
            pltpu.VMEM((n_far * hw, width), BF),
            pltpu.VMEM((n_dev, 1, tok), jnp.int32),
            pltpu.VMEM((n_chip, hd // 2, pair), F32),
            pltpu.VMEM((n_chip, hd, 2 * pair), BF),
            pltpu.VMEM((hw, seq), BF),
            pltpu.VMEM((seq, hw), BF),
            pltpu.VMEM((n_far, hw, seq), BF),
            pltpu.VMEM((n_far, seq, hw), BF),
            pltpu.VMEM((n_far, hd, 2 * pair), BF),
            pltpu.VMEM((n_far, hd, 2 * pair), BF),
            pltpu.VMEM((hw, 4 * pair), BF),
            pltpu.VMEM((4 * pair, hw), BF),
            pltpu.VMEM((seq, 2 * pair), F32),
            pltpu.VMEM((seq, 2 * pair), F32),
            pltpu.VMEM((n_chip, 1, 2 * pair), F32),
            pltpu.VMEM((hw, 2 * pair), F32),
            pltpu.VMEM((seq, hw), F32),
            pltpu.VMEM((hw, seq), F32),
            pltpu.VMEM((hd, seq), F32),
            pltpu.VMEM((n_dev, hd, tok), BF),
            pltpu.VMEM((hd, seq), BF),
            pltpu.VMEM((hw, width), F32),
            pltpu.VMEM((hw + hd, width), F32),
            pltpu.VMEM((n_dev, hw, tok), BF),
            pltpu.VMEM((n_dev, hw, tok), BF),
            pltpu.VMEM((q_w, tok), BF),
            pltpu.VMEM((n_rows, tok), BF),
            pltpu.VMEM((tok, q_w), BF),
            pltpu.VMEM((tok, n_rows), BF),
            pltpu.VMEM((tok, width), BF),
            pltpu.VMEM((tok, width), BF),
            pltpu.VMEM((2, 1, width), F32),
            pltpu.VMEM((2, tok, 128), F32),
            pltpu.VMEM((tok, width), BF),
            pltpu.VMEM((2, 1, width), F32),
            pltpu.VMEM((1, width), F32),
            pltpu.VMEM((1, width), F32),
            pltpu.VMEM((n_chip, 1, width), F32),
            pltpu.VMEM((2, 1, width), F32),
            dma((10,)), dma((3 * n_far,)), dma((n_chip,)), dma((3,)), dma((4,)), dma((2,)),
        ] + [dma((9 * PARTS,)), dma((7 * PARTS,)), dma((8 * PARTS,)), dma((8 * PARTS,))] * 2 + [dma((n_dev,))] * 6 + [dma] * 2 + [dma((n_dev,))] * 8
        out, gx, gw, gwo, gg = pl.pallas_call(
            functools.partial(block_kernel, n_dev, hd, kv_w, NEAR, PARTS),
            out_shape=(
                jax.ShapeDtypeStruct((tok, width), BF),
                jax.ShapeDtypeStruct((tok, width), BF),
                jax.ShapeDtypeStruct((n_rows, tok), F32),
                jax.ShapeDtypeStruct((hw, width), F32),
                jax.ShapeDtypeStruct((2, 1, width), F32),
            ),
            in_specs=[hbm] * 9,
            out_specs=(hbm,) * 5,
            scratch_shapes=scratch,
            compiler_params=pltpu.CompilerParams(collective_id=0, has_side_effects=True, vmem_limit_bytes=67043328),
            name='attn_block',
        )(
            x_act.reshape(tok, width), d_out.reshape(tok, width), positions.reshape(1, tok),
            ln_gain.reshape(1, width), ln_bias.reshape(1, width),
            flat_weight(w_query), flat_weight(w_key), flat_weight(w_value), w_out,
        )

        out, gx, gq, gk, gv, gwo, gain, bias = pl.pallas_call(
            functools.partial(settle_kernel, q_w, kv_w),
            out_shape=(
                jax.ShapeDtypeStruct((tok, width), BF),
                jax.ShapeDtypeStruct((tok, width), BF),
                jax.ShapeDtypeStruct((q_w, tok), F32),
                jax.ShapeDtypeStruct((kv_w, tok), F32),
                jax.ShapeDtypeStruct((kv_w, tok), F32),
                jax.ShapeDtypeStruct((hw, width), F32),
                jax.ShapeDtypeStruct((width,), F32),
                jax.ShapeDtypeStruct((width,), F32),
            ),
            in_specs=[hbm] * 5,
            out_specs=(hbm,) * 6 + (vmem,) * 2,
            scratch_shapes=[
                pltpu.VMEM((2, tok, width), BF),
                pltpu.VMEM((2, q_w // 2, tok), F32),
                pltpu.VMEM((2, kv_w, tok), F32),
                pltpu.VMEM((2, hw // 2, width), F32),
                pltpu.VMEM((2, 1, width), F32),
                dma((8,)), dma((8,)), dma,
            ],
            name='settle',
        )(out, gx, gw, gwo, gg)

        def rows_out(block, heads):
            return jnp.transpose(block.reshape(heads, hd, tok), (2, 0, 1))

        return (
            out.reshape(1, tok, width), gx.reshape(1, tok, width),
            rows_out(gq, q_heads), rows_out(gk, kv_heads), rows_out(gv, kv_heads),
            gwo, gain, bias,
        )

    return jax.shard_map(device_step, mesh=mesh, in_specs=(P('dp', 'cp', None), P('dp', 'cp', None), P('dp', 'cp'), P(None), P(None), P(None, None, None), P(None, None, None), P(None, None, None), P(None, None)), out_specs=(P('dp', 'cp', None), P('dp', 'cp', None), P(('dp', 'cp'), None, None), P(('dp', 'cp'), None, None), P(('dp', 'cp'), None, None), P(('dp', 'cp'), None), P('dp'), P('dp')), check_vma=False)
```

```python
import functools
import math

import jax
import jax.numpy as jnp
from jax import lax
from jax.experimental import pallas as pl
from jax.experimental.pallas import tpu as pltpu
from jax.sharding import PartitionSpec as P

EPS = 1e-5
ROPE_BASE = 10000.0
MESH = pl.DeviceIdType.MESH
BF = jnp.bfloat16
F32 = jnp.float32
NEAR = 1
PARTS = 4


def dot(lhs, rhs):
    return jnp.dot(lhs, rhs, preferred_element_type=F32)


def dot_t(lhs, rhs):
    return lax.dot_general(lhs, rhs, (((1,), (1,)), ((), ())), preferred_element_type=F32)


def block_kernel(
    n_dev, hd, kv_w, near, parts,
    x_hbm, dy_hbm, pos_hbm, gain_hbm, bias_hbm, wq_hbm, wk_hbm, wv_hbm, wo_hbm,
    out_hbm, gx_hbm, gw_hbm, gwo_hbm, gg_hbm,
    hb, dyb, wt, wi, woi, w_far, pos_all, trig,
    qt, kvt, kv, kvt_far, kv_far, q_far, da_far, bmat, sbuf, dpbuf, mbuf, adq, dkvt, kv_rv, kv_mine, kv_row,
    dwo, dwt, at_st, dqt_st, at_rv, dt_rv, a_nat, d_nat, x_v, dy_own, gb_v, stat, out_v, gg_st, gg_mx, gg_my, gg_rv, gg_out,
    in_sem, far_sem, wo_sem, w_sem, out_sem, loc_sem,
    hzs, hzr, hds, hdr, yzs, yzr, yds, ydr,
    pos_s, pos_r, a_s, a_r, q_s, q_r, x_s, x_r, kv_s, kv_r, w_s, w_r, wk_s, wk_r, g_s, g_r,
):
    tok, width = x_v.shape
    n_chip = n_dev // 2
    pair = 2 * tok
    me = lax.axis_index('cp')
    chip = me // 2
    core = me % 2
    right = 2 * ((chip + 1) % n_chip) + core
    left = 2 * ((chip + n_chip - 1) % n_chip) + core
    mate = 2 * chip + 1 - core
    q_rows = wq_hbm.shape[0]
    n_rows = q_rows + 2 * kv_w
    hw = 2 * hd
    quarter = hd // 4
    tile = 256
    scale = hd ** -0.5
    cols_q = 2 * pair
    n_far = n_chip - 1 - 2 * near

    def remote(src, dst, send, recv, target):
        return pltpu.make_async_remote_copy(src_ref=src, dst_ref=dst, send_sem=send, recv_sem=recv, device_id={'cp': target}, device_id_type=MESH)

    def local(src, dst, sem):
        return pltpu.make_async_copy(src, dst, sem)

    def part_of(i, size):
        return pl.ds(pl.multiple_of(i * size, size), size)

    def ring_steps(k):
        step = (k + 1) // 2
        return step, k % 2

    def ring_origin(k):
        step, ahead = ring_steps(k)
        return jnp.where(ahead == 1, chip + n_chip - step, chip + step) % n_chip

    own = (chip, part_of(core, tok))
    first_loads = [
        local(x_hbm, x_v, in_sem.at[0]),
        local(gain_hbm, gb_v.at[0], in_sem.at[1]),
        local(bias_hbm, gb_v.at[1], in_sem.at[2]),
        local(pos_hbm, pos_all.at[me], in_sem.at[3]),
    ]
    for item in first_loads:
        item.start()
    barrier = pltpu.get_barrier_semaphore()
    for step in range(1, n_dev):
        pl.semaphore_signal(barrier, inc=1, device_id={'cp': (me + step) % n_dev}, device_id_type=MESH)
    own_rows = part_of(me, hw)
    kv_rows = part_of(chip, hd)
    loads = [
        local(wq_hbm.at[own_rows], wi.at[pl.ds(0, hw)], in_sem.at[4]),
        local(wk_hbm.at[kv_rows], wi.at[pl.ds(hw, hd)], in_sem.at[5]),
        local(wv_hbm.at[kv_rows], wi.at[pl.ds(hw + hd, hd)], in_sem.at[6]),
        local(wo_hbm.at[own_rows], woi, in_sem.at[7]),
        local(dy_hbm, dyb.at[own], in_sem.at[8]),
        local(dy_hbm, dy_own, in_sem.at[9]),
    ]
    for f in range(n_far):
        far_rows = part_of(ring_origin(2 * near + 1 + f), hd)
        loads.append(local(wk_hbm.at[far_rows], w_far.at[pl.ds(hw * f, hd)], far_sem.at[2 * f]))
        loads.append(local(wv_hbm.at[far_rows], w_far.at[pl.ds(hw * f + hd, hd)], far_sem.at[2 * f + 1]))
        far_wo = part_of(ring_origin(2 * near + 1 + f), 2 * hw)
        loads.append(local(wo_hbm.at[far_wo], wt.at[pl.ds(2 * hw * f, 2 * hw)], far_sem.at[2 * n_far + f]))
    for item in loads:
        item.start()

    for item in first_loads:
        item.wait()
    gain_one = 1.0 + gb_v[0]
    x_f = x_v[...].astype(F32)
    mean = jnp.mean(x_f, axis=-1, keepdims=True)
    centered = x_f - mean
    inv_std = lax.rsqrt(jnp.mean(centered * centered, axis=-1, keepdims=True) + EPS)
    hb[chip, part_of(core, tok), :] = (centered * inv_std * gain_one + gb_v[1]).astype(BF)
    stat[0] = jnp.broadcast_to(mean, (tok, 128))
    stat[1] = jnp.broadcast_to(inv_std, (tok, 128))

    pl.semaphore_wait(barrier, n_dev - 1)

    def chunk(buf, origin, parity, part):
        return buf.at[origin, part_of(parts * parity + part, tok // parts)]

    turns = 2 * parts

    def own_sends(buf, zs, zr, ds, dr):
        copies = []
        for part in range(parts):
            piece = chunk(buf, chip, core, part)
            copies.append(remote(piece, piece, zs.at[2 * part], zr.at[2 * part], right))
            copies.append(remote(piece, piece, zs.at[2 * part + 1], zr.at[2 * part + 1], left))
            copies.append(remote(piece, piece, ds.at[7 * parts + part], dr.at[7 * parts + part], mate))
        return copies

    def event_place(event):
        step = event // turns + 1
        turn = event % turns
        direction = turn % 2
        part = jnp.where(step < 4, turn // 2, turn // 2 + direction * (parts // 2))
        origin = jnp.where(direction == 0, chip + n_chip - step, chip + step) % n_chip
        return step, direction, part, origin

    def last_event(part, direction):
        return 6 * parts + 2 * (part - direction * (parts // 2)) + direction

    def ring_event(ring, event):
        buf, zs, zr, ds, dr = ring
        step, direction, part, origin = event_place(event)
        piece = chunk(buf, origin, core, part)
        remote(piece, piece, zs.at[0], zr.at[event], right).wait_recv()
        onward = jnp.where(step < 3, event + turns, last_event(part, direction))

        @pl.when((step < 3) | ((step == 3) & ((part >= parts // 2) == (direction == 1))))
        def _():
            remote(piece, piece, zs.at[event + turns], zr.at[onward], jnp.where(direction == 0, right, left)).start()

        remote(piece, piece, ds.at[event], dr.at[event], mate).start()

    def ring_service(ring, event):
        @pl.when(event < 7 * parts)
        def _():
            ring_event(ring, event)

    def ring_mate(ring, k, origin):
        buf, zs, zr, ds, dr = ring
        step, ahead = ring_steps(k)
        for part in range(parts):
            event = jnp.where(k == 0, 7 * parts + part, jnp.where(step < 4, turns * (step - 1) + 2 * part + 1 - ahead, last_event(part, part // (parts // 2))))
            piece = chunk(buf, origin, 1 - core, part)
            remote(piece, piece, ds.at[0], dr.at[event], mate).wait_recv()

    def finish_ring(ring):
        buf, zs, zr, ds, dr = ring
        for item in own_sends(*ring):
            item.wait_send()

        @pl.loop(0, 7 * parts)
        def _(event):
            step, direction, part, origin = event_place(event)
            piece = chunk(buf, origin, core, part)

            @pl.when((step < 3) | ((step == 3) & ((part >= parts // 2) == (direction == 1))))
            def _():
                remote(piece, piece, zs.at[event + turns], zr.at[event], right).wait_send()

            remote(piece, piece, ds.at[event], dr.at[event], mate).wait_send()

    h_ring = (hb, hzs, hzr, hds, hdr)
    y_ring = (dyb, yzs, yzr, yds, ydr)
    for item in own_sends(*h_ring):
        item.start()
    pos_sends = [remote(pos_all.at[me], pos_all.at[me], pos_s.at[step], pos_r.at[step], (me + step) % n_dev) for step in range(1, n_dev)]
    for item in pos_sends:
        item.start()
    weight_loads = [
        local(wq_hbm, wt.at[pl.ds(0, q_rows)], w_sem.at[0]),
        local(wk_hbm, wt.at[pl.ds(q_rows, kv_w)], w_sem.at[1]),
        local(wv_hbm, wt.at[pl.ds(q_rows + kv_w, kv_w)], w_sem.at[2]),
    ]
    dkvt[...] = jnp.zeros_like(dkvt)
    dwo[...] = jnp.zeros_like(dwo)
    dwt[...] = jnp.zeros_like(dwt)
    bmat[...] = jnp.zeros_like(bmat)

    freq = jnp.exp(lax.broadcasted_iota(jnp.int32, (quarter, tok), 0).astype(F32) * (-2.0 * math.log(ROPE_BASE) / (hd // 2)))

    def make_trig(slot):
        angle = pos_all[slot].astype(F32) * freq
        trig[slot // 2, 0:quarter, part_of(slot % 2, tok)] = jnp.cos(angle)
        trig[slot // 2, quarter:2 * quarter, part_of(slot % 2, tok)] = jnp.sin(angle)

    make_trig(me)

    @pl.loop(1, n_dev)
    def _(step):
        source = (me + n_dev - step) % n_dev
        remote(pos_all.at[source], pos_all.at[source], pos_s.at[step], pos_r.at[step], me).wait_recv()
        make_trig(source)

    for item in loads:
        item.wait()

    @pl.loop(0, n_far)
    def _(f):
        da_t = dot_t(wt[part_of(f, 2 * hw), :], dy_own[...]).astype(BF)
        for head in range(4):
            da_far[f, :, tok * head:tok * head + tok] = da_t[hd * head:hd * head + hd]

    for item in weight_loads:
        item.start()

    def turned(val, cos_t, sin_t):
        u = val[0:quarter]
        w = val[quarter:2 * quarter]
        return [u * cos_t - w * sin_t, w * cos_t + u * sin_t, val[2 * quarter:hd]]

    def eighth(val):
        return val.astype(BF) * jnp.asarray(scale, BF)

    def keys_values(val, cos_t, sin_t):
        return jnp.concatenate(turned(val[0:hd], cos_t, sin_t) + [val[hd:hw]], axis=0).astype(BF)

    @pl.loop(0, n_chip)
    def _(k):
        for turn in range(parts):
            ring_service(h_ring, parts * k + turn)

        @pl.when(k == 5)
        def _():
            for item in own_sends(*y_ring):
                item.start()

        @pl.when(k == 4)
        def _():
            for item in weight_loads:
                item.wait()

            @pl.loop(0, n_far)
            def _(f):
                cos_t = trig[chip, 0:quarter, part_of(core, tok)]
                sin_t = trig[chip, quarter:2 * quarter, part_of(core, tok)]
                q_t = dot_t(wt[part_of(ring_origin(2 * near + 1 + f), 2 * hw), :], hb[chip, part_of(core, tok), :])
                for head in range(4):
                    q_far[f, :, tok * head:tok * head + tok] = eighth(jnp.concatenate(turned(q_t[hd * head:hd * head + hd], cos_t, sin_t), axis=0))

        b = ring_origin(k)
        ring_mate(h_ring, k, b)
        place = part_of(b, pair)
        cos_t = trig[b, 0:quarter, :]
        sin_t = trig[b, quarter:2 * quarter, :]
        flat = dot_t(wi[...], hb[b])
        for head in range(2):
            q_rot = eighth(jnp.concatenate(turned(flat[hd * head:hd * head + hd], cos_t, sin_t), axis=0))
            for t in range(2):
                lane = pair * t + tok * head
                qt[b, :, lane:lane + tok] = q_rot[:, tok * t:tok * t + tok]
        kv_rot = keys_values(flat[hw:2 * hw], cos_t, sin_t)
        kvt[:, place] = kv_rot
        kv[place, :] = kv_rot.T

        @pl.when(b <= chip)
        def _():
            flat_far = dot_t(w_far[...], hb[b])
            for f in range(n_far):
                far_rot = keys_values(flat_far[hw * f:hw * f + hw], cos_t, sin_t)
                kvt_far[f, :, place] = far_rot
                kv_far[f, place, :] = far_rot.T

    groups = [slice(tile * g, tile * g + tile) for g in range(cols_q // tile)]

    def first_part(b, seen, kv_of):
        def both_of(c):
            rows = part_of(c, pair)
            both = dot(kv_of(rows), bmat[...])
            return rows, both[:, 0:cols_q], both[:, cols_q:2 * cols_q]

        rows, s, d_p = both_of(b)
        s = jnp.where(seen, s, -1e30)
        top = jnp.max(s, axis=0, keepdims=True)
        p = jnp.exp(s - top)
        sbuf[rows, :] = p
        dpbuf[rows, :] = d_p
        mbuf[b] = top

        def step(c, state):
            old, total, weighted = state
            rows, s, d_p = both_of(c)
            new = jnp.maximum(old, jnp.max(s, axis=0, keepdims=True))
            p = jnp.exp(s - new)
            sbuf[rows, :] = p
            dpbuf[rows, :] = d_p
            mbuf[c] = new
            keep = jnp.exp(old - new)
            return new, total * keep + jnp.sum(p, axis=0, keepdims=True), weighted * keep + jnp.sum(p * d_p, axis=0, keepdims=True)

        top, total, weighted = lax.fori_loop(0, b, step, (top, jnp.sum(p, axis=0, keepdims=True), jnp.sum(p * d_p, axis=0, keepdims=True)))
        inv = 1.0 / total
        return top, inv, weighted * inv

    def second_part(b, stats, kvt_of, with_keys):
        top, inv, row_dot = stats
        adq[...] = jnp.zeros_like(adq)

        def step(c, carry):
            rows = part_of(c, pair)
            factor = jnp.exp(mbuf[c] - top) * inv
            d_k = d_v = None
            for at in groups:
                p = sbuf[rows, at] * factor[:, at]
                p_b = p.astype(BF)
                ds_b = (p * (dpbuf[rows, at] - row_dot[:, at])).astype(BF)
                adq[0:hd, at] += dot(kvt_of(slice(0, hd), rows), ds_b)
                adq[hd:hw, at] += dot(kvt_of(slice(hd, hw), rows), p_b)
                if with_keys:
                    more_k = dot_t(bmat[0:hd, at], ds_b)
                    more_v = dot_t(bmat[hd:hw, cols_q + at.start:cols_q + at.stop], p_b)
                    d_k = more_k if d_k is None else d_k + more_k
                    d_v = more_v if d_v is None else d_v + more_v
            if with_keys:
                dkvt[0:hd, rows] += d_k
                dkvt[hd:hw, rows] += d_v
            return carry

        lax.fori_loop(0, b + 1, step, 0)

    lane = lax.broadcasted_iota(jnp.int32, (pair, cols_q), 1)
    row = lax.broadcasted_iota(jnp.int32, (pair, cols_q), 0)

    @pl.loop(0, n_chip)
    def _(k):
        for turn in range(parts - 1):
            ring_service(y_ring, parts * k + turn)
        b = ring_origin(k)
        ring_mate(y_ring, k, b)
        da_t = dot_t(woi[...], dyb[b]).astype(BF)
        bmat[0:hd, 0:cols_q] = qt[b]
        for t in range(2):
            for head in range(2):
                at = cols_q + pair * t + tok * head
                bmat[hd:hw, at:at + tok] = da_t[hd * head:hd * head + hd, tok * t:tok * t + tok]
        stats = first_part(b, row <= (lane // pair) * tok + lane % tok, lambda rows: kv[rows, :])
        ring_service(y_ring, parts * k + parts - 1)
        second_part(b, stats, lambda part, rows: kvt[part, rows], True)
        a_pair = []
        dq_pair = []
        for t in range(2):
            slot = 2 * b + t
            lanes = [slice(pair * t + tok * head, pair * t + tok * head + tok) for head in range(2)]
            a_t = jnp.concatenate([adq[hd:hw, at] for at in lanes], axis=0).astype(BF)
            cos_t = trig[b, 0:quarter, tok * t:tok * t + tok]
            sin_t = trig[b, quarter:2 * quarter, tok * t:tok * t + tok]
            dq_t = jnp.concatenate([piece for at in lanes for piece in turned(adq[0:hd, at] * scale, cos_t, -sin_t)], axis=0).astype(BF)
            a_pair.append(a_t)
            dq_pair.append(dq_t)

            @pl.when(slot == me)
            def _():
                at_rv[own_rows, :] = a_t
                dt_rv[own_rows, :] = dq_t

            @pl.when((slot != me) & (k < 1 + 2 * near))
            def _():
                at_st[slot] = a_t
                dqt_st[slot] = dq_t
                remote(dqt_st.at[slot], dt_rv.at[own_rows], q_s.at[slot], q_r.at[me], slot).start()
                remote(at_st.at[slot], at_rv.at[own_rows], a_s.at[slot], a_r.at[me], slot).start()

        a_pair = jnp.concatenate(a_pair, axis=1)
        dq_pair = jnp.concatenate(dq_pair, axis=1)
        for t in range(width // tile):
            cols = slice(tile * t, tile * t + tile)
            dwo[:, cols] += dot(a_pair, dyb[b, :, cols])
            dwt[0:hw, cols] += dot(dq_pair, hb[b, :, cols])

    far = [ring_origin(k) for k in range(1, n_chip)]
    targets = [mate] + [2 * c + p for c in far for p in range(2)]
    near_targets = targets[0:1 + 4 * near]
    w_sends = [remote(dwt.at[pl.ds(0, hw), part_of(t, tok)], gw_hbm.at[own_rows], w_s.at[t], w_r.at[me], t) for t in targets]
    for item in w_sends:
        item.start()
    w_own = local(dwt.at[pl.ds(0, hw), part_of(me, tok)], gw_hbm.at[own_rows], loc_sem.at[0])
    w_own.start()

    swap = remote(dkvt.at[part_of(1 - core, hd)], kv_rv, x_s, x_r, mate)
    swap.start()
    store_wo = local(dwo, gwo_hbm, out_sem.at[0])
    store_wo.start()

    finish_ring(y_ring)
    wo_loads = [local(wo_hbm.at[pl.ds(pair * t, pair)], dyb.at[t], wo_sem.at[t]) for t in range(n_chip)]
    for item in wo_loads:
        item.start()

    swap.wait_recv()
    mine = part_of(core, hd)
    g_rows = pl.ds(pl.multiple_of(q_rows + core * kv_w + chip * hd, hd), hd)
    for t in range(n_chip):
        cols = slice(pair * t, pair * t + pair)
        g = dkvt[mine, cols] + kv_rv[:, cols]
        cos_t = jnp.where(core == 0, trig[t, 0:quarter, :], 1.0)
        sin_t = jnp.where(core == 0, trig[t, quarter:2 * quarter, :], 0.0)
        g_b = jnp.concatenate(turned(g, cos_t, -sin_t), axis=0).astype(BF)
        kv_mine[2 * t] = g_b[:, 0:tok]
        kv_mine[2 * t + 1] = g_b[:, tok:pair]
        kv_row[:, cols] = g_b
    dt_rv[g_rows, :] = kv_mine[me]
    kv_sends = [remote(kv_mine.at[t], dt_rv.at[g_rows], kv_s.at[t], kv_r.at[me], t) for t in targets]
    for item in kv_sends:
        item.start()
    for t in range(width // tile):
        cols = slice(tile * t, tile * t + tile)
        acc = jnp.zeros((hd, tile), F32)
        for s in range(n_chip):
            acc += dot(kv_row[:, pair * s:pair * s + pair], hb[s, :, cols])
        dwt[hw:hw + hd, cols] = acc
    wk_own = local(dwt.at[pl.ds(hw, hd), part_of(me, tok)], gw_hbm.at[g_rows], loc_sem.at[1])
    wk_own.start()
    wk_sends = [remote(dwt.at[pl.ds(hw, hd), part_of(t, tok)], gw_hbm.at[g_rows], wk_s.at[t], wk_r.at[me], t) for t in targets]
    for item in wk_sends:
        item.start()

    @pl.loop(0, n_far)
    def _(f):
        c_far = ring_origin(2 * near + 1 + f)
        cos_t = trig[chip, 0:quarter, part_of(core, tok)]
        sin_t = trig[chip, quarter:2 * quarter, part_of(core, tok)]
        bmat[0:hd, 0:cols_q] = q_far[f]
        bmat[hd:hw, cols_q:2 * cols_q] = da_far[f]
        stats = first_part(chip, row <= core * tok + lane % tok, lambda rows: kv_far[f, rows, :])
        second_part(chip, stats, lambda part, rows: kvt_far[f, part, rows], False)
        for head in range(4):
            at = slice(tok * head, tok * head + tok)
            place = pl.ds(pl.multiple_of(c_far * 2 * hw + hd * head, hd), hd)
            at_rv[place, :] = adq[hd:hw, at].astype(BF)
            dt_rv[place, :] = jnp.concatenate(turned(adq[0:hd, at] * scale, cos_t, -sin_t), axis=0).astype(BF)

    for t in near_targets:
        remote(at_st.at[0], at_rv.at[part_of(t, hw)], a_s.at[t], a_r.at[t], t).wait_recv()
    for item in wo_loads:
        item.wait()
    for t in range(q_rows // tok):
        a_nat[:, tok * t:tok * t + tok] = at_rv[tok * t:tok * t + tok, :].T
    for t in range(width // tile):
        cols = slice(tile * t, tile * t + tile)
        prod = jnp.zeros((tok, tile), F32)
        for s in range(n_chip):
            prod += dot(a_nat[:, pair * s:pair * s + pair], dyb[s, :, cols])
        out_v[:, cols] = (x_v[:, cols].astype(F32) + prod).astype(BF)
    store_out = local(out_v, out_hbm, out_sem.at[1])
    store_out.start()

    def kv_place(t):
        return pl.ds(pl.multiple_of(q_rows + (t % 2) * kv_w + (t // 2) * hd, hd), hd)

    for t in near_targets:
        remote(dqt_st.at[0], dt_rv.at[part_of(t, hw)], q_s.at[t], q_r.at[t], t).wait_recv()
    for t in targets:
        remote(kv_mine.at[0], dt_rv.at[kv_place(t)], kv_s.at[t], kv_r.at[t], t).wait_recv()
    swap.wait_send()
    for t in range(n_rows // tok):
        d_nat[:, tok * t:tok * t + tok] = dt_rv[tok * t:tok * t + tok, :].T

    mean = stat[0, :, 0:1]
    inv_std = stat[1, :, 0:1]
    dh = dkvt
    for t in range(width // tile):
        cols = slice(tile * t, tile * t + tile)
        acc = jnp.zeros((tok, tile), F32)
        for s in range(n_rows // tile):
            acc += dot(d_nat[:, tile * s:tile * s + tile], wt[tile * s:tile * s + tile, cols])
        dh[:, cols] = acc
        gg_st[0, :, cols] = jnp.sum(acc * ((x_v[:, cols].astype(F32) - mean) * inv_std), axis=0, keepdims=True)
        gg_st[1, :, cols] = jnp.sum(acc, axis=0, keepdims=True)
    g_swap = remote(gg_st.at[1 - core], gg_mx, g_s.at[n_chip], g_r.at[n_chip], mate)
    g_swap.start()
    g_swap.wait_recv()
    gg_my[...] = jnp.where(core == 0, gg_st[0], gg_st[1]) + gg_mx[...]
    gg_rv[chip] = gg_my[...]
    g_sends = [remote(gg_my, gg_rv.at[chip], g_s.at[c], g_r.at[chip], 2 * c + core) for c in far]
    for item in g_sends:
        item.start()

    grad_hat = dh[...] * gain_one
    x_hat = (x_v[...].astype(F32) - mean) * inv_std
    mean_one = jnp.mean(grad_hat, axis=-1, keepdims=True)
    mean_two = jnp.mean(grad_hat * x_hat, axis=-1, keepdims=True)
    store_out.wait()
    out_v[...] = (dy_own[...].astype(F32) + inv_std * (grad_hat - mean_one - x_hat * mean_two)).astype(BF)
    store_gx = local(out_v, gx_hbm, out_sem.at[2])
    store_gx.start()

    for c in far:
        remote(gg_my, gg_rv.at[c], g_s.at[c], g_r.at[c], 2 * c + core).wait_recv()
    sums = gg_rv[0]
    for c in range(1, n_chip):
        sums = sums + gg_rv[c]
    gg_out[core] = sums
    g_swap_out = remote(gg_out.at[core], gg_out.at[core], g_s.at[n_chip + 1], g_r.at[n_chip + 1], mate)
    g_swap_out.start()
    remote(gg_out.at[core], gg_out.at[1 - core], g_s.at[n_chip + 1], g_r.at[n_chip + 1], mate).wait_recv()
    store_gg = local(gg_out, gg_hbm, out_sem.at[3])
    store_gg.start()

    finish_ring(h_ring)
    for item in pos_sends + [g_swap, g_swap_out]:
        item.wait_send()
    for t in near_targets:
        remote(at_st.at[0], at_rv.at[pl.ds(0, hw)], a_s.at[t], a_r.at[t], t).wait_send()
        remote(dqt_st.at[0], dt_rv.at[pl.ds(0, hw)], q_s.at[t], q_r.at[t], t).wait_send()
    for item in kv_sends + w_sends + g_sends + wk_sends:
        item.wait_send()
    for t in targets:
        remote(dwt.at[pl.ds(0, hw), part_of(t, tok)], gw_hbm.at[part_of(t, hw)], w_s.at[t], w_r.at[t], t).wait_recv()
        remote(dwt.at[pl.ds(hw, hd), part_of(t, tok)], gw_hbm.at[kv_place(t)], wk_s.at[t], wk_r.at[t], t).wait_recv()
    for item in (w_own, wk_own, store_wo, store_gx, store_gg):
        item.wait()


def settle_kernel(q_rows, kv_w, out_i, gx_i, gw_i, gwo_i, gg_i, out_o, gx_o, gq_o, gk_o, gv_o, gwo_o, gain_o, bias_o, b_act, b_q, b_kv, b_o, b_gg, sem_in, sem_out, sem_gg):
    half_q = q_rows // 2
    half_o = gwo_i.shape[0] // 2
    moves = [(out_i, b_act.at[0], out_o), (gx_i, b_act.at[1], gx_o)]
    for t in range(2):
        moves.append((gw_i.at[pl.ds(half_q * t, half_q)], b_q.at[t], gq_o.at[pl.ds(half_q * t, half_q)]))
        moves.append((gwo_i.at[pl.ds(half_o * t, half_o)], b_o.at[t], gwo_o.at[pl.ds(half_o * t, half_o)]))
    moves.append((gw_i.at[pl.ds(q_rows, kv_w)], b_kv.at[0], gk_o))
    moves.append((gw_i.at[pl.ds(q_rows + kv_w, kv_w)], b_kv.at[1], gv_o))
    loads = [pltpu.make_async_copy(src, mid, sem_in.at[i]) for i, (src, mid, _) in enumerate(moves)]
    stores = [pltpu.make_async_copy(mid, dst, sem_out.at[i]) for i, (_, mid, dst) in enumerate(moves)]
    load_gg = pltpu.make_async_copy(gg_i, b_gg, sem_gg)
    load_gg.start()
    for item in loads:
        item.start()
    for load, store in zip(loads, stores):
        load.wait()
        store.start()
    load_gg.wait()
    gain_o[...] = b_gg[0, 0]
    bias_o[...] = b_gg[1, 0]
    for item in stores:
        item.wait()


def solution(mesh):
    n_dev = mesh.shape['cp']

    def device_step(x_act, d_out, positions, ln_gain, ln_bias, w_query, w_key, w_value, w_out):
        tok, width = x_act.shape[1], x_act.shape[2]
        q_heads, hd = w_query.shape[1], w_query.shape[2]
        kv_heads = w_key.shape[1]
        q_w, kv_w = q_heads * hd, kv_heads * hd
        n_rows = q_w + 2 * kv_w
        seq = n_dev * tok
        hw = 2 * hd

        def flat_weight(w):
            return jnp.transpose(w, (1, 2, 0)).reshape(-1, width)

        hbm = pl.BlockSpec(memory_space=pltpu.HBM)
        vmem = pl.BlockSpec(memory_space=pltpu.VMEM)
        dma = pltpu.SemaphoreType.DMA
        n_chip = n_dev // 2
        n_far = n_chip - 1 - 2 * NEAR
        pair = 2 * tok
        scratch = [
            pltpu.VMEM((n_chip, pair, width), BF),
            pltpu.VMEM((n_chip, pair, width), BF),
            pltpu.VMEM((n_rows, width), BF),
            pltpu.VMEM((2 * hw, width), BF),
            pltpu.VMEM((hw, width), BF),
            pltpu.VMEM((n_far * hw, width), BF),
            pltpu.VMEM((n_dev, 1, tok), jnp.int32),
            pltpu.VMEM((n_chip, hd // 2, pair), F32),
            pltpu.VMEM((n_chip, hd, 2 * pair), BF),
            pltpu.VMEM((hw, seq), BF),
            pltpu.VMEM((seq, hw), BF),
            pltpu.VMEM((n_far, hw, seq), BF),
            pltpu.VMEM((n_far, seq, hw), BF),
            pltpu.VMEM((n_far, hd, 2 * pair), BF),
            pltpu.VMEM((n_far, hd, 2 * pair), BF),
            pltpu.VMEM((hw, 4 * pair), BF),
            pltpu.VMEM((seq, 2 * pair), F32),
            pltpu.VMEM((seq, 2 * pair), F32),
            pltpu.VMEM((n_chip, 1, 2 * pair), F32),
            pltpu.VMEM((hw, 2 * pair), F32),
            pltpu.VMEM((hw, seq), F32),
            pltpu.VMEM((hd, seq), F32),
            pltpu.VMEM((n_dev, hd, tok), BF),
            pltpu.VMEM((hd, seq), BF),
            pltpu.VMEM((hw, width), F32),
            pltpu.VMEM((hw + hd, width), F32),
            pltpu.VMEM((n_dev, hw, tok), BF),
            pltpu.VMEM((n_dev, hw, tok), BF),
            pltpu.VMEM((q_w, tok), BF),
            pltpu.VMEM((n_rows, tok), BF),
            pltpu.VMEM((tok, q_w), BF),
            pltpu.VMEM((tok, n_rows), BF),
            pltpu.VMEM((tok, width), BF),
            pltpu.VMEM((tok, width), BF),
            pltpu.VMEM((2, 1, width), F32),
            pltpu.VMEM((2, tok, 128), F32),
            pltpu.VMEM((tok, width), BF),
            pltpu.VMEM((2, 1, width), F32),
            pltpu.VMEM((1, width), F32),
            pltpu.VMEM((1, width), F32),
            pltpu.VMEM((n_chip, 1, width), F32),
            pltpu.VMEM((2, 1, width), F32),
            dma((10,)), dma((3 * n_far,)), dma((n_chip,)), dma((3,)), dma((4,)), dma((2,)),
        ] + [dma((9 * PARTS,)), dma((7 * PARTS,)), dma((8 * PARTS,)), dma((8 * PARTS,))] * 2 + [dma((n_dev,))] * 6 + [dma] * 2 + [dma((n_dev,))] * 8
        out, gx, gw, gwo, gg = pl.pallas_call(
            functools.partial(block_kernel, n_dev, hd, kv_w, NEAR, PARTS),
            out_shape=(
                jax.ShapeDtypeStruct((tok, width), BF),
                jax.ShapeDtypeStruct((tok, width), BF),
                jax.ShapeDtypeStruct((n_rows, tok), F32),
                jax.ShapeDtypeStruct((hw, width), F32),
                jax.ShapeDtypeStruct((2, 1, width), F32),
            ),
            in_specs=[hbm] * 9,
            out_specs=(hbm,) * 5,
            scratch_shapes=scratch,
            compiler_params=pltpu.CompilerParams(collective_id=0, has_side_effects=True, vmem_limit_bytes=67043328),
            name='attn_block',
        )(
            x_act.reshape(tok, width), d_out.reshape(tok, width), positions.reshape(1, tok),
            ln_gain.reshape(1, width), ln_bias.reshape(1, width),
            flat_weight(w_query), flat_weight(w_key), flat_weight(w_value), w_out,
        )

        out, gx, gq, gk, gv, gwo, gain, bias = pl.pallas_call(
            functools.partial(settle_kernel, q_w, kv_w),
            out_shape=(
                jax.ShapeDtypeStruct((tok, width), BF),
                jax.ShapeDtypeStruct((tok, width), BF),
                jax.ShapeDtypeStruct((q_w, tok), F32),
                jax.ShapeDtypeStruct((kv_w, tok), F32),
                jax.ShapeDtypeStruct((kv_w, tok), F32),
                jax.ShapeDtypeStruct((hw, width), F32),
                jax.ShapeDtypeStruct((width,), F32),
                jax.ShapeDtypeStruct((width,), F32),
            ),
            in_specs=[hbm] * 5,
            out_specs=(hbm,) * 6 + (vmem,) * 2,
            scratch_shapes=[
                pltpu.VMEM((2, tok, width), BF),
                pltpu.VMEM((2, q_w // 2, tok), F32),
                pltpu.VMEM((2, kv_w, tok), F32),
                pltpu.VMEM((2, hw // 2, width), F32),
                pltpu.VMEM((2, 1, width), F32),
                dma((8,)), dma((8,)), dma,
            ],
            name='settle',
        )(out, gx, gw, gwo, gg)

        def rows_out(block, heads):
            return jnp.transpose(block.reshape(heads, hd, tok), (2, 0, 1))

        return (
            out.reshape(1, tok, width), gx.reshape(1, tok, width),
            rows_out(gq, q_heads), rows_out(gk, kv_heads), rows_out(gv, kv_heads),
            gwo, gain, bias,
        )

    return jax.shard_map(device_step, mesh=mesh, in_specs=(P('dp', 'cp', None), P('dp', 'cp', None), P('dp', 'cp'), P(None), P(None), P(None, None, None), P(None, None, None), P(None, None, None), P(None, None)), out_specs=(P('dp', 'cp', None), P('dp', 'cp', None), P(('dp', 'cp'), None, None), P(('dp', 'cp'), None, None), P(('dp', 'cp'), None, None), P(('dp', 'cp'), None), P('dp'), P('dp')), check_vma=False)
```

```python
import functools
import math

import jax
import jax.numpy as jnp
from jax import lax
from jax.experimental import pallas as pl
from jax.experimental.pallas import tpu as pltpu
from jax.sharding import PartitionSpec as P

EPS = 1e-5
ROPE_BASE = 10000.0
MESH = pl.DeviceIdType.MESH
BF = jnp.bfloat16
F32 = jnp.float32
NEAR = 1
PARTS = 4
FIRST = 2
HELD = 4


def dot(lhs, rhs):
    return jnp.dot(lhs, rhs, preferred_element_type=F32)


def dot_t(lhs, rhs):
    return lax.dot_general(lhs, rhs, (((1,), (1,)), ((), ())), preferred_element_type=F32)


def block_kernel(
    n_dev, hd, kv_w, near, parts,
    x_hbm, dy_hbm, pos_hbm, gain_hbm, bias_hbm, wq_hbm, wk_hbm, wv_hbm, wo_hbm,
    out_hbm, gx_hbm, gw_hbm, gwo_hbm, gg_hbm,
    hb, dyb, wt, wi, woi, w_far, pos_all, trig,
    qt, kvt, kv, kvt_far, kv_far, q_far, da_far, bmat, sbuf, dpbuf, mbuf, adq, dkvt, kv_rv, kv_mine, kv_row,
    dwo, dwt, at_st, dqt_st, at_rv, dt_rv, a_nat, d_nat, x_v, dy_own, gb_v, stat, out_v, gg_st, gg_mx, gg_my, gg_rv, gg_out,
    in_sem, far_sem, wo_sem, w_sem, out_sem, loc_sem,
    hzs, hzr, hds, hdr, yzs, yzr, yds, ydr,
    pos_s, pos_r, a_s, a_r, q_s, q_r, x_s, x_r, kv_s, kv_r, w_s, w_r, wk_s, wk_r, g_s, g_r,
):
    tok, width = x_v.shape
    n_chip = n_dev // 2
    pair = 2 * tok
    me = lax.axis_index('cp')
    chip = me // 2
    core = me % 2
    right = 2 * ((chip + 1) % n_chip) + core
    left = 2 * ((chip + n_chip - 1) % n_chip) + core
    mate = 2 * chip + 1 - core
    q_rows = wq_hbm.shape[0]
    n_rows = q_rows + 2 * kv_w
    hw = 2 * hd
    quarter = hd // 4
    tile = 256
    scale = hd ** -0.5
    cols_q = 2 * pair
    n_far = n_chip - 1 - 2 * near

    def remote(src, dst, send, recv, target):
        return pltpu.make_async_remote_copy(src_ref=src, dst_ref=dst, send_sem=send, recv_sem=recv, device_id={'cp': target}, device_id_type=MESH)

    def local(src, dst, sem):
        return pltpu.make_async_copy(src, dst, sem)

    def part_of(i, size):
        return pl.ds(pl.multiple_of(i * size, size), size)

    def ring_steps(k):
        step = (k + 1) // 2
        return step, k % 2

    def ring_origin(k):
        step, ahead = ring_steps(k)
        return jnp.where(ahead == 1, chip + n_chip - step, chip + step) % n_chip

    own = (chip, part_of(core, tok))
    first_loads = [
        local(x_hbm, x_v, in_sem.at[0]),
        local(gain_hbm, gb_v.at[0], in_sem.at[1]),
        local(bias_hbm, gb_v.at[1], in_sem.at[2]),
        local(pos_hbm, pos_all.at[me], in_sem.at[3]),
    ]
    for item in first_loads:
        item.start()
    barrier = pltpu.get_barrier_semaphore()
    for step in range(1, n_dev):
        pl.semaphore_signal(barrier, inc=1, device_id={'cp': (me + step) % n_dev}, device_id_type=MESH)
    own_rows = part_of(me, hw)
    kv_rows = part_of(chip, hd)
    loads = [
        local(wq_hbm.at[own_rows], wi.at[pl.ds(0, hw)], in_sem.at[4]),
        local(wk_hbm.at[kv_rows], wi.at[pl.ds(hw, hd)], in_sem.at[5]),
        local(wv_hbm.at[kv_rows], wi.at[pl.ds(hw + hd, hd)], in_sem.at[6]),
        local(wo_hbm.at[own_rows], woi, in_sem.at[7]),
        local(dy_hbm, dyb.at[own], in_sem.at[8]),
        local(dy_hbm, dy_own, in_sem.at[9]),
    ]
    far_loads = []
    for f in range(n_far):
        far_rows = part_of(ring_origin(2 * near + 1 + f), hd)
        loads.append(local(wk_hbm.at[far_rows], w_far.at[pl.ds(hw * f, hd)], far_sem.at[2 * f]))
        loads.append(local(wv_hbm.at[far_rows], w_far.at[pl.ds(hw * f + hd, hd)], far_sem.at[2 * f + 1]))
        far_wo = part_of(ring_origin(2 * near + 1 + f), 2 * hw)
        far_loads.append(local(wo_hbm.at[far_wo], wt.at[pl.ds(2 * hw * f, 2 * hw)], far_sem.at[2 * n_far + f]))
    for item in loads + far_loads:
        item.start()

    for item in first_loads:
        item.wait()
    gain_one = 1.0 + gb_v[0]
    block = 16

    @pl.loop(0, tok // block)
    def _(i):
        rows = part_of(i, block)
        x_f = x_v[rows, :].astype(F32)
        mean = jnp.mean(x_f, axis=-1, keepdims=True)
        centered = x_f - mean
        inv_std = lax.rsqrt(jnp.mean(centered * centered, axis=-1, keepdims=True) + EPS)
        hb[chip, part_of(core * (tok // block) + i, block), :] = (centered * inv_std * gain_one + gb_v[1]).astype(BF)
        stat[0, rows, :] = jnp.broadcast_to(mean, (block, 128))
        stat[1, rows, :] = jnp.broadcast_to(inv_std, (block, 128))

    pl.semaphore_wait(barrier, n_dev - 1)

    def chunk(buf, origin, parity, part):
        return buf.at[origin, part_of(parts * parity + part, tok // parts)]

    turns = 2 * parts

    def own_sends(buf, zs, zr, ds, dr):
        copies = []
        for part in range(parts):
            piece = chunk(buf, chip, core, part)
            copies.append(remote(piece, piece, zs.at[2 * part], zr.at[2 * part], right))
            copies.append(remote(piece, piece, zs.at[2 * part + 1], zr.at[2 * part + 1], left))
            copies.append(remote(piece, piece, ds.at[7 * parts + part], dr.at[7 * parts + part], mate))
        return copies

    def event_place(event):
        step = event // turns + 1
        turn = event % turns
        direction = turn % 2
        part = jnp.where(step < 4, turn // 2, turn // 2 + direction * (parts // 2))
        origin = jnp.where(direction == 0, chip + n_chip - step, chip + step) % n_chip
        return step, direction, part, origin

    def last_event(part, direction):
        return 6 * parts + 2 * (part - direction * (parts // 2)) + direction

    def ring_event(ring, event):
        buf, zs, zr, ds, dr = ring
        step, direction, part, origin = event_place(event)
        piece = chunk(buf, origin, core, part)
        remote(piece, piece, zs.at[0], zr.at[event], right).wait_recv()
        onward = jnp.where(step < 3, event + turns, last_event(part, direction))

        @pl.when((step < 3) | ((step == 3) & ((part >= parts // 2) == (direction == 1))))
        def _():
            remote(piece, piece, zs.at[event + turns], zr.at[onward], jnp.where(direction == 0, right, left)).start()

        remote(piece, piece, ds.at[event], dr.at[event], mate).start()

    def ring_service(ring, event):
        @pl.when(event < 7 * parts)
        def _():
            ring_event(ring, event)

    def ring_mate(ring, k, origin):
        buf, zs, zr, ds, dr = ring
        step, ahead = ring_steps(k)
        for part in range(parts):
            event = jnp.where(k == 0, 7 * parts + part, jnp.where(step < 4, turns * (step - 1) + 2 * part + 1 - ahead, last_event(part, part // (parts // 2))))
            piece = chunk(buf, origin, 1 - core, part)
            remote(piece, piece, ds.at[0], dr.at[event], mate).wait_recv()

    def finish_ring(ring):
        buf, zs, zr, ds, dr = ring
        for item in own_sends(*ring):
            item.wait_send()

        @pl.loop(0, 7 * parts)
        def _(event):
            step, direction, part, origin = event_place(event)
            piece = chunk(buf, origin, core, part)

            @pl.when((step < 3) | ((step == 3) & ((part >= parts // 2) == (direction == 1))))
            def _():
                remote(piece, piece, zs.at[event + turns], zr.at[event], right).wait_send()

            remote(piece, piece, ds.at[event], dr.at[event], mate).wait_send()

    h_ring = (hb, hzs, hzr, hds, hdr)
    y_ring = (dyb, yzs, yzr, yds, ydr)
    for item in own_sends(*h_ring):
        item.start()
    pos_sends = [remote(pos_all.at[me], pos_all.at[me], pos_s.at[step], pos_r.at[me], (me + step) % n_dev) for step in range(1, n_dev)]
    for item in pos_sends:
        item.start()
    weight_loads = [
        local(wq_hbm, wt.at[pl.ds(0, q_rows)], w_sem.at[0]),
        local(wk_hbm, wt.at[pl.ds(q_rows, kv_w)], w_sem.at[1]),
        local(wv_hbm, wt.at[pl.ds(q_rows + kv_w, kv_w)], w_sem.at[2]),
    ]
    dkvt[...] = jnp.zeros_like(dkvt)
    dwo[...] = jnp.zeros_like(dwo)
    dwt[...] = jnp.zeros_like(dwt)
    bmat[...] = jnp.zeros_like(bmat)

    freq = jnp.exp(lax.broadcasted_iota(jnp.int32, (quarter, tok), 0).astype(F32) * (-2.0 * math.log(ROPE_BASE) / (hd // 2)))

    def make_trig(b):
        for t in range(2):
            slot = 2 * b + t

            @pl.when(slot != me)
            def _():
                remote(pos_all.at[slot], pos_all.at[slot], pos_s.at[0], pos_r.at[slot], me).wait_recv()

            angle = pos_all[slot].astype(F32) * freq
            trig[b, 0:quarter, tok * t:tok * t + tok] = jnp.cos(angle)
            trig[b, quarter:2 * quarter, tok * t:tok * t + tok] = jnp.sin(angle)

    def turned(val, cos_t, sin_t):
        u = val[0:quarter]
        w = val[quarter:2 * quarter]
        return [u * cos_t - w * sin_t, w * cos_t + u * sin_t, val[2 * quarter:hd]]

    def eighth(val):
        return val.astype(BF) * jnp.asarray(scale, BF)

    def keys_values(val, cos_t, sin_t):
        return jnp.concatenate(turned(val[0:hd], cos_t, sin_t) + [val[hd:hw]], axis=0).astype(BF)

    @pl.loop(0, n_chip)
    def _(k):
        for turn in range(parts):
            ring_service(h_ring, parts * k + turn)

        @pl.when(k == 5)
        def _():
            for item in own_sends(*y_ring):
                item.start()

        @pl.when(k == 0)
        def _():
            for item in loads:
                item.wait()

        @pl.when(k == 2)
        def _():
            for item in far_loads:
                item.wait()

        @pl.when((k >= 2) & (k < 2 + n_far))
        def _():
            f = k - 2
            da_t = dot_t(wt[part_of(f, 2 * hw), :], dy_own[...]).astype(BF)
            for head in range(4):
                da_far[f, :, tok * head:tok * head + tok] = da_t[hd * head:hd * head + hd]

        @pl.when(k == 1 + n_far)
        def _():
            for item in weight_loads:
                item.start()

        b = ring_origin(k)
        ring_mate(h_ring, k, b)
        make_trig(b)
        place = part_of(b, pair)
        cos_t = trig[b, 0:quarter, :]
        sin_t = trig[b, quarter:2 * quarter, :]
        flat = dot_t(wi[...], hb[b])
        for head in range(2):
            q_rot = eighth(jnp.concatenate(turned(flat[hd * head:hd * head + hd], cos_t, sin_t), axis=0))
            for t in range(2):
                lane = pair * t + tok * head
                qt[b, :, lane:lane + tok] = q_rot[:, tok * t:tok * t + tok]
        kv_rot = keys_values(flat[hw:2 * hw], cos_t, sin_t)
        kvt[:, place] = kv_rot
        kv[place, :] = kv_rot.T

        @pl.when(b <= chip)
        def _():
            flat_far = dot_t(w_far[...], hb[b])
            for f in range(n_far):
                far_rot = keys_values(flat_far[hw * f:hw * f + hw], cos_t, sin_t)
                kvt_far[f, :, place] = far_rot
                kv_far[f, place, :] = far_rot.T

    groups = [slice(tile * g, tile * g + tile) for g in range(cols_q // tile)]

    def first_part(b, seen, kv_of):
        def both_of(c):
            rows = part_of(c, pair)
            both = dot(kv_of(rows), bmat[...])
            return rows, both[:, 0:cols_q], both[:, cols_q:2 * cols_q]

        rows, s, d_p = both_of(b)
        s = jnp.where(seen, s, -1e30)
        top = jnp.max(s, axis=0, keepdims=True)
        p = jnp.exp(s - top)
        sbuf[rows, :] = p
        dpbuf[rows, :] = d_p
        mbuf[b] = top

        def step(c, state):
            old, total, weighted = state
            rows, s, d_p = both_of(c)
            new = jnp.maximum(old, jnp.max(s, axis=0, keepdims=True))
            p = jnp.exp(s - new)
            sbuf[rows, :] = p
            dpbuf[rows, :] = d_p
            mbuf[c] = new
            keep = jnp.exp(old - new)
            return new, total * keep + jnp.sum(p, axis=0, keepdims=True), weighted * keep + jnp.sum(p * d_p, axis=0, keepdims=True)

        top, total, weighted = lax.fori_loop(0, b, step, (top, jnp.sum(p, axis=0, keepdims=True), jnp.sum(p * d_p, axis=0, keepdims=True)))
        inv = 1.0 / total
        return top, inv, weighted * inv

    def second_part(b, stats, kvt_of, with_keys):
        top, inv, row_dot = stats
        adq[...] = jnp.zeros_like(adq)

        def step(c, carry):
            rows = part_of(c, pair)
            factor = jnp.exp(mbuf[c] - top) * inv
            d_k = d_v = None
            for at in groups:
                p = sbuf[rows, at] * factor[:, at]
                p_b = p.astype(BF)
                ds_b = (p * (dpbuf[rows, at] - row_dot[:, at])).astype(BF)
                adq[0:hd, at] += dot(kvt_of(slice(0, hd), rows), ds_b)
                adq[hd:hw, at] += dot(kvt_of(slice(hd, hw), rows), p_b)
                if with_keys:
                    more_k = dot_t(bmat[0:hd, at], ds_b)
                    more_v = dot_t(bmat[hd:hw, cols_q + at.start:cols_q + at.stop], p_b)
                    d_k = more_k if d_k is None else d_k + more_k
                    d_v = more_v if d_v is None else d_v + more_v
            if with_keys:
                dkvt[0:hd, rows] += d_k
                dkvt[hd:hw, rows] += d_v
            return carry

        lax.fori_loop(0, b + 1, step, 0)

    lane = lax.broadcasted_iota(jnp.int32, (pair, cols_q), 1)
    row = lax.broadcasted_iota(jnp.int32, (pair, cols_q), 0)

    @pl.loop(0, n_chip)
    def _(k):
        for turn in range(parts - 1):
            ring_service(y_ring, parts * k + turn)
        b = ring_origin(k)
        ring_mate(y_ring, k, b)

        @pl.when(k == 1)
        def _():
            for item in weight_loads:
                item.wait()

        @pl.when((k >= 1) & (k < 1 + n_far))
        def _():
            f = k - 1
            cos_t = trig[chip, 0:quarter, part_of(core, tok)]
            sin_t = trig[chip, quarter:2 * quarter, part_of(core, tok)]
            q_t = dot_t(wt[part_of(ring_origin(2 * near + 1 + f), 2 * hw), :], hb[chip, part_of(core, tok), :])
            for head in range(4):
                q_far[f, :, tok * head:tok * head + tok] = eighth(jnp.concatenate(turned(q_t[hd * head:hd * head + hd], cos_t, sin_t), axis=0))

        da_t = dot_t(woi[...], dyb[b]).astype(BF)
        bmat[0:hd, 0:cols_q] = qt[b]
        for t in range(2):
            for head in range(2):
                at = cols_q + pair * t + tok * head
                bmat[hd:hw, at:at + tok] = da_t[hd * head:hd * head + hd, tok * t:tok * t + tok]
        stats = first_part(b, row <= (lane // pair) * tok + lane % tok, lambda rows: kv[rows, :])
        ring_service(y_ring, parts * k + parts - 1)
        second_part(b, stats, lambda part, rows: kvt[part, rows], True)
        a_pair = []
        dq_pair = []
        for t in range(2):
            slot = 2 * b + t
            lanes = [slice(pair * t + tok * head, pair * t + tok * head + tok) for head in range(2)]
            a_t = jnp.concatenate([adq[hd:hw, at] for at in lanes], axis=0).astype(BF)
            cos_t = trig[b, 0:quarter, tok * t:tok * t + tok]
            sin_t = trig[b, quarter:2 * quarter, tok * t:tok * t + tok]
            dq_t = jnp.concatenate([piece for at in lanes for piece in turned(adq[0:hd, at] * scale, cos_t, -sin_t)], axis=0).astype(BF)
            a_pair.append(a_t)
            dq_pair.append(dq_t)

            @pl.when(slot == me)
            def _():
                at_rv[own_rows, :] = a_t
                dt_rv[own_rows, :] = dq_t

            @pl.when((slot != me) & (k < 1 + 2 * near))
            def _():
                at_st[slot] = a_t
                dqt_st[slot] = dq_t
                remote(dqt_st.at[slot], dt_rv.at[own_rows], q_s.at[slot], q_r.at[me], slot).start()
                remote(at_st.at[slot], at_rv.at[own_rows], a_s.at[slot], a_r.at[me], slot).start()

        a_pair = jnp.concatenate(a_pair, axis=1)
        dq_pair = jnp.concatenate(dq_pair, axis=1)
        for t in range(width // tile):
            cols = slice(tile * t, tile * t + tile)
            dwo[:, cols] += dot(a_pair, dyb[b, :, cols])
            dwt[0:hw, cols] += dot(dq_pair, hb[b, :, cols])

    far = [ring_origin(k) for k in range(n_chip - 1, 0, -1)]
    targets = [2 * c + p for c in far for p in range(2)] + [mate]
    near_targets = targets[-1 - 4 * near:]
    w_sends = [remote(dwt.at[pl.ds(0, hw), part_of(t, tok)], gw_hbm.at[own_rows], w_s.at[t], w_r.at[me], t) for t in targets]
    for item in w_sends[0:FIRST]:
        item.start()
    w_own = local(dwt.at[pl.ds(0, hw), part_of(me, tok)], gw_hbm.at[own_rows], loc_sem.at[0])
    w_own.start()

    swap = remote(dkvt.at[part_of(1 - core, hd)], kv_rv, x_s, x_r, mate)
    swap.start()
    store_wo = local(dwo, gwo_hbm, out_sem.at[0])
    store_wo.start()

    finish_ring(y_ring)
    wo_loads = [local(wo_hbm.at[pl.ds(pair * t, pair)], dyb.at[t], wo_sem.at[t]) for t in range(n_chip)]
    for item in wo_loads:
        item.start()

    swap.wait_recv()
    mine = part_of(core, hd)
    g_rows = pl.ds(pl.multiple_of(q_rows + core * kv_w + chip * hd, hd), hd)
    for t in range(n_chip):
        cols = slice(pair * t, pair * t + pair)
        g = dkvt[mine, cols] + kv_rv[:, cols]
        cos_t = jnp.where(core == 0, trig[t, 0:quarter, :], 1.0)
        sin_t = jnp.where(core == 0, trig[t, quarter:2 * quarter, :], 0.0)
        g_b = jnp.concatenate(turned(g, cos_t, -sin_t), axis=0).astype(BF)
        kv_mine[2 * t] = g_b[:, 0:tok]
        kv_mine[2 * t + 1] = g_b[:, tok:pair]
        kv_row[:, cols] = g_b
    dt_rv[g_rows, :] = kv_mine[me]
    kv_sends = [remote(kv_mine.at[t], dt_rv.at[g_rows], kv_s.at[t], kv_r.at[me], t) for t in targets]
    for item in kv_sends + w_sends[FIRST:]:
        item.start()
    for t in range(width // tile):
        cols = slice(tile * t, tile * t + tile)
        acc = jnp.zeros((hd, tile), F32)
        for s in range(n_chip):
            acc += dot(kv_row[:, pair * s:pair * s + pair], hb[s, :, cols])
        dwt[hw:hw + hd, cols] = acc
    wk_own = local(dwt.at[pl.ds(hw, hd), part_of(me, tok)], gw_hbm.at[g_rows], loc_sem.at[1])
    wk_own.start()
    wk_sends = [remote(dwt.at[pl.ds(hw, hd), part_of(t, tok)], gw_hbm.at[g_rows], wk_s.at[t], wk_r.at[me], t) for t in targets]
    for item in wk_sends[0:HELD]:
        item.start()

    @pl.loop(0, n_far)
    def _(f):
        c_far = ring_origin(2 * near + 1 + f)
        cos_t = trig[chip, 0:quarter, part_of(core, tok)]
        sin_t = trig[chip, quarter:2 * quarter, part_of(core, tok)]
        bmat[0:hd, 0:cols_q] = q_far[f]
        bmat[hd:hw, cols_q:2 * cols_q] = da_far[f]
        stats = first_part(chip, row <= core * tok + lane % tok, lambda rows: kv_far[f, rows, :])
        second_part(chip, stats, lambda part, rows: kvt_far[f, part, rows], False)
        for head in range(4):
            at = slice(tok * head, tok * head + tok)
            place = pl.ds(pl.multiple_of(c_far * 2 * hw + hd * head, hd), hd)
            at_rv[place, :] = adq[hd:hw, at].astype(BF)
            dt_rv[place, :] = jnp.concatenate(turned(adq[0:hd, at] * scale, cos_t, -sin_t), axis=0).astype(BF)

    for t in near_targets:
        remote(at_st.at[0], at_rv.at[part_of(t, hw)], a_s.at[t], a_r.at[t], t).wait_recv()
    for item in wo_loads:
        item.wait()
    for t in range(q_rows // tok):
        a_nat[:, tok * t:tok * t + tok] = at_rv[tok * t:tok * t + tok, :].T
    for t in range(width // tile):
        cols = slice(tile * t, tile * t + tile)
        prod = jnp.zeros((tok, tile), F32)
        for s in range(n_chip):
            prod += dot(a_nat[:, pair * s:pair * s + pair], dyb[s, :, cols])
        out_v[:, cols] = (x_v[:, cols].astype(F32) + prod).astype(BF)
    store_out = local(out_v, out_hbm, out_sem.at[1])
    store_out.start()

    def kv_place(t):
        return pl.ds(pl.multiple_of(q_rows + (t % 2) * kv_w + (t // 2) * hd, hd), hd)

    for t in near_targets:
        remote(dqt_st.at[0], dt_rv.at[part_of(t, hw)], q_s.at[t], q_r.at[t], t).wait_recv()
    for t in targets:
        remote(kv_mine.at[0], dt_rv.at[kv_place(t)], kv_s.at[t], kv_r.at[t], t).wait_recv()
    swap.wait_send()
    for t in range(n_rows // tok):
        d_nat[:, tok * t:tok * t + tok] = dt_rv[tok * t:tok * t + tok, :].T

    mean = stat[0, :, 0:1]
    inv_std = stat[1, :, 0:1]
    dh = dkvt
    for t in range(width // tile):
        cols = slice(tile * t, tile * t + tile)
        acc = jnp.zeros((tok, tile), F32)
        for s in range(n_rows // tile):
            acc += dot(d_nat[:, tile * s:tile * s + tile], wt[tile * s:tile * s + tile, cols])
        dh[:, cols] = acc
        gg_st[0, :, cols] = jnp.sum(acc * ((x_v[:, cols].astype(F32) - mean) * inv_std), axis=0, keepdims=True)
        gg_st[1, :, cols] = jnp.sum(acc, axis=0, keepdims=True)
    g_swap = remote(gg_st.at[1 - core], gg_mx, g_s.at[n_chip], g_r.at[n_chip], mate)
    g_swap.start()
    g_swap.wait_recv()
    gg_my[...] = jnp.where(core == 0, gg_st[0], gg_st[1]) + gg_mx[...]
    gg_rv[chip] = gg_my[...]
    g_sends = [remote(gg_my, gg_rv.at[chip], g_s.at[c], g_r.at[chip], 2 * c + core) for c in far]
    for item in g_sends + wk_sends[HELD:]:
        item.start()

    grad_hat = dh[...] * gain_one
    x_hat = (x_v[...].astype(F32) - mean) * inv_std
    mean_one = jnp.mean(grad_hat, axis=-1, keepdims=True)
    mean_two = jnp.mean(grad_hat * x_hat, axis=-1, keepdims=True)
    store_out.wait()
    out_v[...] = (dy_own[...].astype(F32) + inv_std * (grad_hat - mean_one - x_hat * mean_two)).astype(BF)
    store_gx = local(out_v, gx_hbm, out_sem.at[2])
    store_gx.start()

    for c in far:
        remote(gg_my, gg_rv.at[c], g_s.at[c], g_r.at[c], 2 * c + core).wait_recv()
    sums = gg_rv[0]
    for c in range(1, n_chip):
        sums = sums + gg_rv[c]
    gg_out[core] = sums
    g_swap_out = remote(gg_out.at[core], gg_out.at[core], g_s.at[n_chip + 1], g_r.at[n_chip + 1], mate)
    g_swap_out.start()
    remote(gg_out.at[core], gg_out.at[1 - core], g_s.at[n_chip + 1], g_r.at[n_chip + 1], mate).wait_recv()
    store_gg = local(gg_out, gg_hbm, out_sem.at[3])
    store_gg.start()

    finish_ring(h_ring)
    for item in pos_sends + [g_swap, g_swap_out]:
        item.wait_send()
    for t in near_targets:
        remote(at_st.at[0], at_rv.at[pl.ds(0, hw)], a_s.at[t], a_r.at[t], t).wait_send()
        remote(dqt_st.at[0], dt_rv.at[pl.ds(0, hw)], q_s.at[t], q_r.at[t], t).wait_send()
    for item in kv_sends + w_sends + g_sends + wk_sends:
        item.wait_send()
    for t in targets:
        remote(dwt.at[pl.ds(0, hw), part_of(t, tok)], gw_hbm.at[part_of(t, hw)], w_s.at[t], w_r.at[t], t).wait_recv()
        remote(dwt.at[pl.ds(hw, hd), part_of(t, tok)], gw_hbm.at[kv_place(t)], wk_s.at[t], wk_r.at[t], t).wait_recv()
    for item in (w_own, wk_own, store_wo, store_gx, store_gg):
        item.wait()


def settle_kernel(q_rows, kv_w, out_i, gx_i, gw_i, gwo_i, gg_i, out_o, gx_o, gq_o, gk_o, gv_o, gwo_o, gain_o, bias_o, b_act, b_q, b_kv, b_o, b_gg, sem_in, sem_out, sem_gg):
    half_q = q_rows // 2
    half_o = gwo_i.shape[0] // 2
    moves = [(out_i, b_act.at[0], out_o), (gx_i, b_act.at[1], gx_o)]
    for t in range(2):
        moves.append((gw_i.at[pl.ds(half_q * t, half_q)], b_q.at[t], gq_o.at[pl.ds(half_q * t, half_q)]))
        moves.append((gwo_i.at[pl.ds(half_o * t, half_o)], b_o.at[t], gwo_o.at[pl.ds(half_o * t, half_o)]))
    moves.append((gw_i.at[pl.ds(q_rows, kv_w)], b_kv.at[0], gk_o))
    moves.append((gw_i.at[pl.ds(q_rows + kv_w, kv_w)], b_kv.at[1], gv_o))
    loads = [pltpu.make_async_copy(src, mid, sem_in.at[i]) for i, (src, mid, _) in enumerate(moves)]
    stores = [pltpu.make_async_copy(mid, dst, sem_out.at[i]) for i, (_, mid, dst) in enumerate(moves)]
    load_gg = pltpu.make_async_copy(gg_i, b_gg, sem_gg)
    load_gg.start()
    for item in loads:
        item.start()
    for load, store in zip(loads, stores):
        load.wait()
        store.start()
    load_gg.wait()
    gain_o[...] = b_gg[0, 0]
    bias_o[...] = b_gg[1, 0]
    for item in stores:
        item.wait()


def solution(mesh):
    n_dev = mesh.shape['cp']

    def device_step(x_act, d_out, positions, ln_gain, ln_bias, w_query, w_key, w_value, w_out):
        tok, width = x_act.shape[1], x_act.shape[2]
        q_heads, hd = w_query.shape[1], w_query.shape[2]
        kv_heads = w_key.shape[1]
        q_w, kv_w = q_heads * hd, kv_heads * hd
        n_rows = q_w + 2 * kv_w
        seq = n_dev * tok
        hw = 2 * hd

        def flat_weight(w):
            return jnp.transpose(w, (1, 2, 0)).reshape(-1, width)

        hbm = pl.BlockSpec(memory_space=pltpu.HBM)
        vmem = pl.BlockSpec(memory_space=pltpu.VMEM)
        dma = pltpu.SemaphoreType.DMA
        n_chip = n_dev // 2
        n_far = n_chip - 1 - 2 * NEAR
        pair = 2 * tok
        scratch = [
            pltpu.VMEM((n_chip, pair, width), BF),
            pltpu.VMEM((n_chip, pair, width), BF),
            pltpu.VMEM((n_rows, width), BF),
            pltpu.VMEM((2 * hw, width), BF),
            pltpu.VMEM((hw, width), BF),
            pltpu.VMEM((n_far * hw, width), BF),
            pltpu.VMEM((n_dev, 1, tok), jnp.int32),
            pltpu.VMEM((n_chip, hd // 2, pair), F32),
            pltpu.VMEM((n_chip, hd, 2 * pair), BF),
            pltpu.VMEM((hw, seq), BF),
            pltpu.VMEM((seq, hw), BF),
            pltpu.VMEM((n_far, hw, seq), BF),
            pltpu.VMEM((n_far, seq, hw), BF),
            pltpu.VMEM((n_far, hd, 2 * pair), BF),
            pltpu.VMEM((n_far, hd, 2 * pair), BF),
            pltpu.VMEM((hw, 4 * pair), BF),
            pltpu.VMEM((seq, 2 * pair), F32),
            pltpu.VMEM((seq, 2 * pair), F32),
            pltpu.VMEM((n_chip, 1, 2 * pair), F32),
            pltpu.VMEM((hw, 2 * pair), F32),
            pltpu.VMEM((hw, seq), F32),
            pltpu.VMEM((hd, seq), F32),
            pltpu.VMEM((n_dev, hd, tok), BF),
            pltpu.VMEM((hd, seq), BF),
            pltpu.VMEM((hw, width), F32),
            pltpu.VMEM((hw + hd, width), F32),
            pltpu.VMEM((n_dev, hw, tok), BF),
            pltpu.VMEM((n_dev, hw, tok), BF),
            pltpu.VMEM((q_w, tok), BF),
            pltpu.VMEM((n_rows, tok), BF),
            pltpu.VMEM((tok, q_w), BF),
            pltpu.VMEM((tok, n_rows), BF),
            pltpu.VMEM((tok, width), BF),
            pltpu.VMEM((tok, width), BF),
            pltpu.VMEM((2, 1, width), F32),
            pltpu.VMEM((2, tok, 128), F32),
            pltpu.VMEM((tok, width), BF),
            pltpu.VMEM((2, 1, width), F32),
            pltpu.VMEM((1, width), F32),
            pltpu.VMEM((1, width), F32),
            pltpu.VMEM((n_chip, 1, width), F32),
            pltpu.VMEM((2, 1, width), F32),
            dma((10,)), dma((3 * n_far,)), dma((n_chip,)), dma((3,)), dma((4,)), dma((2,)),
        ] + [dma((9 * PARTS,)), dma((7 * PARTS,)), dma((8 * PARTS,)), dma((8 * PARTS,))] * 2 + [dma((n_dev,))] * 6 + [dma] * 2 + [dma((n_dev,))] * 8
        out, gx, gw, gwo, gg = pl.pallas_call(
            functools.partial(block_kernel, n_dev, hd, kv_w, NEAR, PARTS),
            out_shape=(
                jax.ShapeDtypeStruct((tok, width), BF),
                jax.ShapeDtypeStruct((tok, width), BF),
                jax.ShapeDtypeStruct((n_rows, tok), F32),
                jax.ShapeDtypeStruct((hw, width), F32),
                jax.ShapeDtypeStruct((2, 1, width), F32),
            ),
            in_specs=[hbm] * 9,
            out_specs=(hbm,) * 5,
            scratch_shapes=scratch,
            compiler_params=pltpu.CompilerParams(collective_id=0, has_side_effects=True, vmem_limit_bytes=67043328),
            name='attn_block',
        )(
            x_act.reshape(tok, width), d_out.reshape(tok, width), positions.reshape(1, tok),
            ln_gain.reshape(1, width), ln_bias.reshape(1, width),
            flat_weight(w_query), flat_weight(w_key), flat_weight(w_value), w_out,
        )

        out, gx, gq, gk, gv, gwo, gain, bias = pl.pallas_call(
            functools.partial(settle_kernel, q_w, kv_w),
            out_shape=(
                jax.ShapeDtypeStruct((tok, width), BF),
                jax.ShapeDtypeStruct((tok, width), BF),
                jax.ShapeDtypeStruct((q_w, tok), F32),
                jax.ShapeDtypeStruct((kv_w, tok), F32),
                jax.ShapeDtypeStruct((kv_w, tok), F32),
                jax.ShapeDtypeStruct((hw, width), F32),
                jax.ShapeDtypeStruct((width,), F32),
                jax.ShapeDtypeStruct((width,), F32),
            ),
            in_specs=[hbm] * 5,
            out_specs=(hbm,) * 6 + (vmem,) * 2,
            scratch_shapes=[
                pltpu.VMEM((2, tok, width), BF),
                pltpu.VMEM((2, q_w // 2, tok), F32),
                pltpu.VMEM((2, kv_w, tok), F32),
                pltpu.VMEM((2, hw // 2, width), F32),
                pltpu.VMEM((2, 1, width), F32),
                dma((8,)), dma((8,)), dma,
            ],
            name='settle',
        )(out, gx, gw, gwo, gg)

        def rows_out(block, heads):
            return jnp.transpose(block.reshape(heads, hd, tok), (2, 0, 1))

        return (
            out.reshape(1, tok, width), gx.reshape(1, tok, width),
            rows_out(gq, q_heads), rows_out(gk, kv_heads), rows_out(gv, kv_heads),
            gwo, gain, bias,
        )

    return jax.shard_map(device_step, mesh=mesh, in_specs=(P('dp', 'cp', None), P('dp', 'cp', None), P('dp', 'cp'), P(None), P(None), P(None, None, None), P(None, None, None), P(None, None, None), P(None, None)), out_specs=(P('dp', 'cp', None), P('dp', 'cp', None), P(('dp', 'cp'), None, None), P(('dp', 'cp'), None, None), P(('dp', 'cp'), None, None), P(('dp', 'cp'), None), P('dp'), P('dp')), check_vma=False)
```

```python
import functools
import math

import jax
import jax.numpy as jnp
from jax import lax
from jax.experimental import pallas as pl
from jax.experimental.pallas import tpu as pltpu
from jax.sharding import PartitionSpec as P

EPS = 1e-5
ROPE_BASE = 10000.0
MESH = pl.DeviceIdType.MESH
BF = jnp.bfloat16
F32 = jnp.float32
NEAR = 1
PARTS = 4
FIRST = 2
HELD = 4


def dot(lhs, rhs):
    return jnp.dot(lhs, rhs, preferred_element_type=F32)


def dot_t(lhs, rhs):
    return lax.dot_general(lhs, rhs, (((1,), (1,)), ((), ())), preferred_element_type=F32)


def block_kernel(
    n_dev, hd, kv_w, near, parts,
    x_hbm, dy_hbm, pos_hbm, gain_hbm, bias_hbm, wq_hbm, wk_hbm, wv_hbm, wo_hbm,
    out_hbm, gx_hbm, gw_hbm, gwo_hbm, gg_hbm,
    hb, dyb, wt, wi, woi, w_far, pos_all, trig,
    qt, kvt, kv, kvt_far, kv_far, q_far, da_far, bmat, sbuf, dpbuf, mbuf, adq, dkvt, kv_rv, kv_mine, kv_row,
    dwo, dwt, at_st, dqt_st, at_rv, dt_rv, a_nat, d_nat, x_v, dy_own, gb_v, stat, out_v, gg_st, gg_mx, gg_my, gg_rv, gg_out,
    in_sem, far_sem, wo_sem, w_sem, out_sem, loc_sem,
    hzs, hzr, hds, hdr, yzs, yzr, yds, ydr,
    pos_s, pos_r, a_s, a_r, q_s, q_r, x_s, x_r, kv_s, kv_r, w_s, w_r, wk_s, wk_r, g_s, g_r,
):
    tok, width = x_v.shape
    n_chip = n_dev // 2
    pair = 2 * tok
    me = lax.axis_index('cp')
    chip = me // 2
    core = me % 2
    right = 2 * ((chip + 1) % n_chip) + core
    left = 2 * ((chip + n_chip - 1) % n_chip) + core
    mate = 2 * chip + 1 - core
    q_rows = wq_hbm.shape[0]
    n_rows = q_rows + 2 * kv_w
    hw = 2 * hd
    quarter = hd // 4
    tile = 256
    scale = hd ** -0.5
    cols_q = 2 * pair
    n_far = n_chip - 1 - 2 * near

    def remote(src, dst, send, recv, target):
        return pltpu.make_async_remote_copy(src_ref=src, dst_ref=dst, send_sem=send, recv_sem=recv, device_id={'cp': target}, device_id_type=MESH)

    def local(src, dst, sem):
        return pltpu.make_async_copy(src, dst, sem)

    def part_of(i, size):
        return pl.ds(pl.multiple_of(i * size, size), size)

    def ring_steps(k):
        step = (k + 1) // 2
        return step, k % 2

    def ring_origin(k):
        step, ahead = ring_steps(k)
        return jnp.where(ahead == 1, chip + n_chip - step, chip + step) % n_chip

    own = (chip, part_of(core, tok))
    first_loads = [
        local(x_hbm, x_v, in_sem.at[0]),
        local(gain_hbm, gb_v.at[0], in_sem.at[1]),
        local(bias_hbm, gb_v.at[1], in_sem.at[2]),
        local(pos_hbm, pos_all.at[me], in_sem.at[3]),
    ]
    for item in first_loads:
        item.start()
    barrier = pltpu.get_barrier_semaphore()
    for step in range(1, n_dev):
        pl.semaphore_signal(barrier, inc=1, device_id={'cp': (me + step) % n_dev}, device_id_type=MESH)
    own_rows = part_of(me, hw)
    kv_rows = part_of(chip, hd)
    loads = [
        local(wq_hbm.at[own_rows], wi.at[pl.ds(0, hw)], in_sem.at[4]),
        local(wk_hbm.at[kv_rows], wi.at[pl.ds(hw, hd)], in_sem.at[5]),
        local(wv_hbm.at[kv_rows], wi.at[pl.ds(hw + hd, hd)], in_sem.at[6]),
        local(wo_hbm.at[own_rows], woi, in_sem.at[7]),
        local(dy_hbm, dyb.at[own], in_sem.at[8]),
        local(dy_hbm, dy_own, in_sem.at[9]),
    ]
    far_loads = []
    for f in range(n_far):
        far_rows = part_of(ring_origin(2 * near + 1 + f), hd)
        loads.append(local(wk_hbm.at[far_rows], w_far.at[pl.ds(hw * f, hd)], far_sem.at[2 * f]))
        loads.append(local(wv_hbm.at[far_rows], w_far.at[pl.ds(hw * f + hd, hd)], far_sem.at[2 * f + 1]))
        far_wo = part_of(ring_origin(2 * near + 1 + f), 2 * hw)
        far_loads.append(local(wo_hbm.at[far_wo], wt.at[pl.ds(2 * hw * f, 2 * hw)], far_sem.at[2 * n_far + f]))
    for item in loads + far_loads:
        item.start()

    for item in first_loads:
        item.wait()
    gain_one = 1.0 + gb_v[0]
    block = 16

    @pl.loop(0, tok // block)
    def _(i):
        rows = part_of(i, block)
        x_f = x_v[rows, :].astype(F32)
        mean = jnp.mean(x_f, axis=-1, keepdims=True)
        centered = x_f - mean
        inv_std = lax.rsqrt(jnp.mean(centered * centered, axis=-1, keepdims=True) + EPS)
        hb[chip, part_of(core * (tok // block) + i, block), :] = (centered * inv_std * gain_one + gb_v[1]).astype(BF)
        stat[0, rows, :] = jnp.broadcast_to(mean, (block, 128))
        stat[1, rows, :] = jnp.broadcast_to(inv_std, (block, 128))

    pl.semaphore_wait(barrier, n_dev - 1)

    def chunk(buf, origin, parity, part):
        return buf.at[origin, part_of(parts * parity + part, tok // parts)]

    turns = 2 * parts

    def own_sends(buf, zs, zr, ds, dr):
        copies = []
        for part in range(parts):
            piece = chunk(buf, chip, core, part)
            copies.append(remote(piece, piece, zs.at[2 * part], zr.at[2 * part], right))
            copies.append(remote(piece, piece, zs.at[2 * part + 1], zr.at[2 * part + 1], left))
            copies.append(remote(piece, piece, ds.at[7 * parts + part], dr.at[7 * parts + part], mate))
        return copies

    def event_place(event):
        step = event // turns + 1
        turn = event % turns
        direction = turn % 2
        part = jnp.where(step < 4, turn // 2, turn // 2 + direction * (parts // 2))
        origin = jnp.where(direction == 0, chip + n_chip - step, chip + step) % n_chip
        return step, direction, part, origin

    def last_event(part, direction):
        return 6 * parts + 2 * (part - direction * (parts // 2)) + direction

    def ring_event(ring, event):
        buf, zs, zr, ds, dr = ring
        step, direction, part, origin = event_place(event)
        piece = chunk(buf, origin, core, part)
        remote(piece, piece, zs.at[0], zr.at[event], right).wait_recv()
        onward = jnp.where(step < 3, event + turns, last_event(part, direction))

        @pl.when((step < 3) | ((step == 3) & ((part >= parts // 2) == (direction == 1))))
        def _():
            remote(piece, piece, zs.at[event + turns], zr.at[onward], jnp.where(direction == 0, right, left)).start()

        remote(piece, piece, ds.at[event], dr.at[event], mate).start()

    def ring_service(ring, event):
        @pl.when(event < 7 * parts)
        def _():
            ring_event(ring, event)

    def ring_mate(ring, k, origin):
        buf, zs, zr, ds, dr = ring
        step, ahead = ring_steps(k)
        for part in range(parts):
            event = jnp.where(k == 0, 7 * parts + part, jnp.where(step < 4, turns * (step - 1) + 2 * part + 1 - ahead, last_event(part, part // (parts // 2))))
            piece = chunk(buf, origin, 1 - core, part)
            remote(piece, piece, ds.at[0], dr.at[event], mate).wait_recv()

    def finish_ring(ring):
        buf, zs, zr, ds, dr = ring
        for item in own_sends(*ring):
            item.wait_send()

        @pl.loop(0, 7 * parts)
        def _(event):
            step, direction, part, origin = event_place(event)
            piece = chunk(buf, origin, core, part)

            @pl.when((step < 3) | ((step == 3) & ((part >= parts // 2) == (direction == 1))))
            def _():
                remote(piece, piece, zs.at[event + turns], zr.at[event], right).wait_send()

            remote(piece, piece, ds.at[event], dr.at[event], mate).wait_send()

    h_ring = (hb, hzs, hzr, hds, hdr)
    y_ring = (dyb, yzs, yzr, yds, ydr)
    for item in own_sends(*h_ring):
        item.start()
    pos_sends = [remote(pos_all.at[me], pos_all.at[me], pos_s.at[step], pos_r.at[me], (me + step) % n_dev) for step in range(1, n_dev)]
    for item in pos_sends:
        item.start()
    weight_loads = [
        local(wq_hbm, wt.at[pl.ds(0, q_rows)], w_sem.at[0]),
        local(wk_hbm, wt.at[pl.ds(q_rows, kv_w)], w_sem.at[1]),
        local(wv_hbm, wt.at[pl.ds(q_rows + kv_w, kv_w)], w_sem.at[2]),
    ]
    dkvt[...] = jnp.zeros_like(dkvt)
    dwo[...] = jnp.zeros_like(dwo)
    dwt[...] = jnp.zeros_like(dwt)
    bmat[...] = jnp.zeros_like(bmat)

    freq = jnp.exp(lax.broadcasted_iota(jnp.int32, (quarter, tok), 0).astype(F32) * (-2.0 * math.log(ROPE_BASE) / (hd // 2)))

    def make_trig(b):
        for t in range(2):
            slot = 2 * b + t

            @pl.when(slot != me)
            def _():
                remote(pos_all.at[slot], pos_all.at[slot], pos_s.at[0], pos_r.at[slot], me).wait_recv()

            angle = pos_all[slot].astype(F32) * freq
            trig[b, 0:quarter, tok * t:tok * t + tok] = jnp.cos(angle)
            trig[b, quarter:2 * quarter, tok * t:tok * t + tok] = jnp.sin(angle)

    def turned(val, cos_t, sin_t):
        u = val[0:quarter]
        w = val[quarter:2 * quarter]
        return [u * cos_t - w * sin_t, w * cos_t + u * sin_t, val[2 * quarter:hd]]

    def eighth(val):
        return val.astype(BF) * jnp.asarray(scale, BF)

    def keys_values(val, cos_t, sin_t):
        return jnp.concatenate(turned(val[0:hd], cos_t, sin_t) + [val[hd:hw]], axis=0).astype(BF)

    for event in range(2):
        ring_event(h_ring, jnp.int32(event))

    @pl.loop(0, n_chip)
    def _(k):
        for turn in range(2, parts):
            ring_service(h_ring, parts * k + turn)

        @pl.when(k == 5)
        def _():
            for item in own_sends(*y_ring):
                item.start()

        @pl.when(k == 0)
        def _():
            for item in loads:
                item.wait()

        @pl.when(k == 2)
        def _():
            for item in far_loads:
                item.wait()

        @pl.when((k >= 2) & (k < 2 + n_far))
        def _():
            f = k - 2
            da_t = dot_t(wt[part_of(f, 2 * hw), :], dy_own[...]).astype(BF)
            for head in range(4):
                da_far[f, :, tok * head:tok * head + tok] = da_t[hd * head:hd * head + hd]

        @pl.when(k == 1 + n_far)
        def _():
            for item in weight_loads:
                item.start()

        b = ring_origin(k)
        ring_mate(h_ring, k, b)
        make_trig(b)
        place = part_of(b, pair)
        cos_t = trig[b, 0:quarter, :]
        sin_t = trig[b, quarter:2 * quarter, :]
        flat = dot_t(wi[...], hb[b])
        for head in range(2):
            q_rot = eighth(jnp.concatenate(turned(flat[hd * head:hd * head + hd], cos_t, sin_t), axis=0))
            for t in range(2):
                lane = pair * t + tok * head
                qt[b, :, lane:lane + tok] = q_rot[:, tok * t:tok * t + tok]
        kv_rot = keys_values(flat[hw:2 * hw], cos_t, sin_t)
        kvt[:, place] = kv_rot
        kv[place, :] = kv_rot.T

        for turn in range(2):
            ring_service(h_ring, parts * (k + 1) + turn)

        @pl.when(b <= chip)
        def _():
            flat_far = dot_t(w_far[...], hb[b])
            for f in range(n_far):
                far_rot = keys_values(flat_far[hw * f:hw * f + hw], cos_t, sin_t)
                kvt_far[f, :, place] = far_rot
                kv_far[f, place, :] = far_rot.T

    groups = [slice(tile * g, tile * g + tile) for g in range(cols_q // tile)]

    def first_part(b, seen, kv_of):
        def both_of(c):
            rows = part_of(c, pair)
            both = dot(kv_of(rows), bmat[...])
            return rows, both[:, 0:cols_q], both[:, cols_q:2 * cols_q]

        rows, s, d_p = both_of(b)
        s = jnp.where(seen, s, -1e30)
        top = jnp.max(s, axis=0, keepdims=True)
        p = jnp.exp(s - top)
        sbuf[rows, :] = p
        dpbuf[rows, :] = d_p
        mbuf[b] = top

        def step(c, state):
            old, total, weighted = state
            rows, s, d_p = both_of(c)
            new = jnp.maximum(old, jnp.max(s, axis=0, keepdims=True))
            p = jnp.exp(s - new)
            sbuf[rows, :] = p
            dpbuf[rows, :] = d_p
            mbuf[c] = new
            keep = jnp.exp(old - new)
            return new, total * keep + jnp.sum(p, axis=0, keepdims=True), weighted * keep + jnp.sum(p * d_p, axis=0, keepdims=True)

        top, total, weighted = lax.fori_loop(0, b, step, (top, jnp.sum(p, axis=0, keepdims=True), jnp.sum(p * d_p, axis=0, keepdims=True)))
        inv = 1.0 / total
        return top, inv, weighted * inv

    def second_part(b, stats, kvt_of, with_keys):
        top, inv, row_dot = stats
        adq[...] = jnp.zeros_like(adq)

        def step(c, carry):
            rows = part_of(c, pair)
            factor = jnp.exp(mbuf[c] - top) * inv
            d_k = d_v = None
            for at in groups:
                p = sbuf[rows, at] * factor[:, at]
                p_b = p.astype(BF)
                ds_b = (p * (dpbuf[rows, at] - row_dot[:, at])).astype(BF)
                adq[0:hd, at] += dot(kvt_of(slice(0, hd), rows), ds_b)
                adq[hd:hw, at] += dot(kvt_of(slice(hd, hw), rows), p_b)
                if with_keys:
                    more_k = dot_t(bmat[0:hd, at], ds_b)
                    more_v = dot_t(bmat[hd:hw, cols_q + at.start:cols_q + at.stop], p_b)
                    d_k = more_k if d_k is None else d_k + more_k
                    d_v = more_v if d_v is None else d_v + more_v
            if with_keys:
                dkvt[0:hd, rows] += d_k
                dkvt[hd:hw, rows] += d_v
            return carry

        lax.fori_loop(0, b + 1, step, 0)

    lane = lax.broadcasted_iota(jnp.int32, (pair, cols_q), 1)
    row = lax.broadcasted_iota(jnp.int32, (pair, cols_q), 0)

    for event in range(2):
        ring_event(y_ring, jnp.int32(event))

    @pl.loop(0, n_chip)
    def _(k):
        for turn in range(2, parts):
            ring_service(y_ring, parts * k + turn)
        b = ring_origin(k)
        ring_mate(y_ring, k, b)

        @pl.when(k == 1)
        def _():
            for item in weight_loads:
                item.wait()

        @pl.when((k >= 1) & (k < 1 + n_far))
        def _():
            f = k - 1
            cos_t = trig[chip, 0:quarter, part_of(core, tok)]
            sin_t = trig[chip, quarter:2 * quarter, part_of(core, tok)]
            q_t = dot_t(wt[part_of(ring_origin(2 * near + 1 + f), 2 * hw), :], hb[chip, part_of(core, tok), :])
            for head in range(4):
                q_far[f, :, tok * head:tok * head + tok] = eighth(jnp.concatenate(turned(q_t[hd * head:hd * head + hd], cos_t, sin_t), axis=0))

        da_t = dot_t(woi[...], dyb[b]).astype(BF)
        bmat[0:hd, 0:cols_q] = qt[b]
        for t in range(2):
            for head in range(2):
                at = cols_q + pair * t + tok * head
                bmat[hd:hw, at:at + tok] = da_t[hd * head:hd * head + hd, tok * t:tok * t + tok]
        stats = first_part(b, row <= (lane // pair) * tok + lane % tok, lambda rows: kv[rows, :])
        for turn in range(2):
            ring_service(y_ring, parts * (k + 1) + turn)
        second_part(b, stats, lambda part, rows: kvt[part, rows], True)
        a_pair = []
        dq_pair = []
        for t in range(2):
            slot = 2 * b + t
            lanes = [slice(pair * t + tok * head, pair * t + tok * head + tok) for head in range(2)]
            a_t = jnp.concatenate([adq[hd:hw, at] for at in lanes], axis=0).astype(BF)
            cos_t = trig[b, 0:quarter, tok * t:tok * t + tok]
            sin_t = trig[b, quarter:2 * quarter, tok * t:tok * t + tok]
            dq_t = jnp.concatenate([piece for at in lanes for piece in turned(adq[0:hd, at] * scale, cos_t, -sin_t)], axis=0).astype(BF)
            a_pair.append(a_t)
            dq_pair.append(dq_t)

            @pl.when(slot == me)
            def _():
                at_rv[own_rows, :] = a_t
                dt_rv[own_rows, :] = dq_t

            @pl.when((slot != me) & (k < 1 + 2 * near))
            def _():
                at_st[slot] = a_t
                dqt_st[slot] = dq_t
                remote(dqt_st.at[slot], dt_rv.at[own_rows], q_s.at[slot], q_r.at[me], slot).start()
                remote(at_st.at[slot], at_rv.at[own_rows], a_s.at[slot], a_r.at[me], slot).start()

        a_pair = jnp.concatenate(a_pair, axis=1)
        dq_pair = jnp.concatenate(dq_pair, axis=1)
        for t in range(width // tile):
            cols = slice(tile * t, tile * t + tile)
            dwo[:, cols] += dot(a_pair, dyb[b, :, cols])
            dwt[0:hw, cols] += dot(dq_pair, hb[b, :, cols])

    far = [ring_origin(k) for k in range(n_chip - 1, 0, -1)]
    targets = [2 * c + p for c in far for p in range(2)] + [mate]
    near_targets = targets[-1 - 4 * near:]
    w_sends = [remote(dwt.at[pl.ds(0, hw), part_of(t, tok)], gw_hbm.at[own_rows], w_s.at[t], w_r.at[me], t) for t in targets]
    for item in w_sends[0:FIRST]:
        item.start()
    w_own = local(dwt.at[pl.ds(0, hw), part_of(me, tok)], gw_hbm.at[own_rows], loc_sem.at[0])
    w_own.start()

    swap = remote(dkvt.at[part_of(1 - core, hd)], kv_rv, x_s, x_r, mate)
    swap.start()
    store_wo = local(dwo, gwo_hbm, out_sem.at[0])
    store_wo.start()

    finish_ring(y_ring)
    wo_loads = [local(wo_hbm.at[pl.ds(pair * t, pair)], dyb.at[t], wo_sem.at[t]) for t in range(n_chip)]
    for item in wo_loads:
        item.start()

    swap.wait_recv()
    mine = part_of(core, hd)
    g_rows = pl.ds(pl.multiple_of(q_rows + core * kv_w + chip * hd, hd), hd)
    for t in range(n_chip):
        cols = slice(pair * t, pair * t + pair)
        g = dkvt[mine, cols] + kv_rv[:, cols]
        cos_t = jnp.where(core == 0, trig[t, 0:quarter, :], 1.0)
        sin_t = jnp.where(core == 0, trig[t, quarter:2 * quarter, :], 0.0)
        g_b = jnp.concatenate(turned(g, cos_t, -sin_t), axis=0).astype(BF)
        kv_mine[2 * t] = g_b[:, 0:tok]
        kv_mine[2 * t + 1] = g_b[:, tok:pair]
        kv_row[:, cols] = g_b
    dt_rv[g_rows, :] = kv_mine[me]
    kv_sends = [remote(kv_mine.at[t], dt_rv.at[g_rows], kv_s.at[t], kv_r.at[me], t) for t in targets]
    for item in kv_sends + w_sends[FIRST:]:
        item.start()
    for t in range(width // tile):
        cols = slice(tile * t, tile * t + tile)
        acc = jnp.zeros((hd, tile), F32)
        for s in range(n_chip):
            acc += dot(kv_row[:, pair * s:pair * s + pair], hb[s, :, cols])
        dwt[hw:hw + hd, cols] = acc
    wk_own = local(dwt.at[pl.ds(hw, hd), part_of(me, tok)], gw_hbm.at[g_rows], loc_sem.at[1])
    wk_own.start()
    wk_sends = [remote(dwt.at[pl.ds(hw, hd), part_of(t, tok)], gw_hbm.at[g_rows], wk_s.at[t], wk_r.at[me], t) for t in targets]
    for item in wk_sends[0:HELD]:
        item.start()

    @pl.loop(0, n_far)
    def _(f):
        c_far = ring_origin(2 * near + 1 + f)
        cos_t = trig[chip, 0:quarter, part_of(core, tok)]
        sin_t = trig[chip, quarter:2 * quarter, part_of(core, tok)]
        bmat[0:hd, 0:cols_q] = q_far[f]
        bmat[hd:hw, cols_q:2 * cols_q] = da_far[f]
        stats = first_part(chip, row <= core * tok + lane % tok, lambda rows: kv_far[f, rows, :])
        second_part(chip, stats, lambda part, rows: kvt_far[f, part, rows], False)
        for head in range(4):
            at = slice(tok * head, tok * head + tok)
            place = pl.ds(pl.multiple_of(c_far * 2 * hw + hd * head, hd), hd)
            at_rv[place, :] = adq[hd:hw, at].astype(BF)
            dt_rv[place, :] = jnp.concatenate(turned(adq[0:hd, at] * scale, cos_t, -sin_t), axis=0).astype(BF)

    for t in near_targets:
        remote(at_st.at[0], at_rv.at[part_of(t, hw)], a_s.at[t], a_r.at[t], t).wait_recv()
    for item in wo_loads:
        item.wait()
    for t in range(q_rows // tok):
        a_nat[:, tok * t:tok * t + tok] = at_rv[tok * t:tok * t + tok, :].T
    for t in range(width // tile):
        cols = slice(tile * t, tile * t + tile)
        prod = jnp.zeros((tok, tile), F32)
        for s in range(n_chip):
            prod += dot(a_nat[:, pair * s:pair * s + pair], dyb[s, :, cols])
        out_v[:, cols] = (x_v[:, cols].astype(F32) + prod).astype(BF)
    store_out = local(out_v, out_hbm, out_sem.at[1])
    store_out.start()

    def kv_place(t):
        return pl.ds(pl.multiple_of(q_rows + (t % 2) * kv_w + (t // 2) * hd, hd), hd)

    for t in near_targets:
        remote(dqt_st.at[0], dt_rv.at[part_of(t, hw)], q_s.at[t], q_r.at[t], t).wait_recv()
    for t in targets:
        remote(kv_mine.at[0], dt_rv.at[kv_place(t)], kv_s.at[t], kv_r.at[t], t).wait_recv()
    swap.wait_send()
    for t in range(n_rows // tok):
        d_nat[:, tok * t:tok * t + tok] = dt_rv[tok * t:tok * t + tok, :].T

    mean = stat[0, :, 0:1]
    inv_std = stat[1, :, 0:1]
    dh = dkvt
    for t in range(width // tile):
        cols = slice(tile * t, tile * t + tile)
        acc = jnp.zeros((tok, tile), F32)
        for s in range(n_rows // tile):
            acc += dot(d_nat[:, tile * s:tile * s + tile], wt[tile * s:tile * s + tile, cols])
        dh[:, cols] = acc
        gg_st[0, :, cols] = jnp.sum(acc * ((x_v[:, cols].astype(F32) - mean) * inv_std), axis=0, keepdims=True)
        gg_st[1, :, cols] = jnp.sum(acc, axis=0, keepdims=True)
    g_swap = remote(gg_st.at[1 - core], gg_mx, g_s.at[n_chip], g_r.at[n_chip], mate)
    g_swap.start()
    g_swap.wait_recv()
    gg_my[...] = jnp.where(core == 0, gg_st[0], gg_st[1]) + gg_mx[...]
    gg_rv[chip] = gg_my[...]
    g_sends = [remote(gg_my, gg_rv.at[chip], g_s.at[c], g_r.at[chip], 2 * c + core) for c in far]
    for item in g_sends + wk_sends[HELD:]:
        item.start()

    grad_hat = dh[...] * gain_one
    x_hat = (x_v[...].astype(F32) - mean) * inv_std
    mean_one = jnp.mean(grad_hat, axis=-1, keepdims=True)
    mean_two = jnp.mean(grad_hat * x_hat, axis=-1, keepdims=True)
    store_out.wait()
    out_v[...] = (dy_own[...].astype(F32) + inv_std * (grad_hat - mean_one - x_hat * mean_two)).astype(BF)
    store_gx = local(out_v, gx_hbm, out_sem.at[2])
    store_gx.start()

    for c in far:
        remote(gg_my, gg_rv.at[c], g_s.at[c], g_r.at[c], 2 * c + core).wait_recv()
    sums = gg_rv[0]
    for c in range(1, n_chip):
        sums = sums + gg_rv[c]
    gg_out[core] = sums
    g_swap_out = remote(gg_out.at[core], gg_out.at[core], g_s.at[n_chip + 1], g_r.at[n_chip + 1], mate)
    g_swap_out.start()
    remote(gg_out.at[core], gg_out.at[1 - core], g_s.at[n_chip + 1], g_r.at[n_chip + 1], mate).wait_recv()
    store_gg = local(gg_out, gg_hbm, out_sem.at[3])
    store_gg.start()

    finish_ring(h_ring)
    for item in pos_sends + [g_swap, g_swap_out]:
        item.wait_send()
    for t in near_targets:
        remote(at_st.at[0], at_rv.at[pl.ds(0, hw)], a_s.at[t], a_r.at[t], t).wait_send()
        remote(dqt_st.at[0], dt_rv.at[pl.ds(0, hw)], q_s.at[t], q_r.at[t], t).wait_send()
    for item in kv_sends + w_sends + g_sends + wk_sends:
        item.wait_send()
    for t in targets:
        remote(dwt.at[pl.ds(0, hw), part_of(t, tok)], gw_hbm.at[part_of(t, hw)], w_s.at[t], w_r.at[t], t).wait_recv()
        remote(dwt.at[pl.ds(hw, hd), part_of(t, tok)], gw_hbm.at[kv_place(t)], wk_s.at[t], wk_r.at[t], t).wait_recv()
    for item in (w_own, wk_own, store_wo, store_gx, store_gg):
        item.wait()


def settle_kernel(q_rows, kv_w, out_i, gx_i, gw_i, gwo_i, gg_i, out_o, gx_o, gq_o, gk_o, gv_o, gwo_o, gain_o, bias_o, b_act, b_q, b_kv, b_o, b_gg, sem_in, sem_out, sem_gg):
    half_q = q_rows // 2
    half_o = gwo_i.shape[0] // 2
    moves = [(out_i, b_act.at[0], out_o), (gx_i, b_act.at[1], gx_o)]
    for t in range(2):
        moves.append((gw_i.at[pl.ds(half_q * t, half_q)], b_q.at[t], gq_o.at[pl.ds(half_q * t, half_q)]))
        moves.append((gwo_i.at[pl.ds(half_o * t, half_o)], b_o.at[t], gwo_o.at[pl.ds(half_o * t, half_o)]))
    moves.append((gw_i.at[pl.ds(q_rows, kv_w)], b_kv.at[0], gk_o))
    moves.append((gw_i.at[pl.ds(q_rows + kv_w, kv_w)], b_kv.at[1], gv_o))
    loads = [pltpu.make_async_copy(src, mid, sem_in.at[i]) for i, (src, mid, _) in enumerate(moves)]
    stores = [pltpu.make_async_copy(mid, dst, sem_out.at[i]) for i, (_, mid, dst) in enumerate(moves)]
    load_gg = pltpu.make_async_copy(gg_i, b_gg, sem_gg)
    load_gg.start()
    for item in loads:
        item.start()
    for load, store in zip(loads, stores):
        load.wait()
        store.start()
    load_gg.wait()
    gain_o[...] = b_gg[0, 0]
    bias_o[...] = b_gg[1, 0]
    for item in stores:
        item.wait()


def solution(mesh):
    n_dev = mesh.shape['cp']

    def device_step(x_act, d_out, positions, ln_gain, ln_bias, w_query, w_key, w_value, w_out):
        tok, width = x_act.shape[1], x_act.shape[2]
        q_heads, hd = w_query.shape[1], w_query.shape[2]
        kv_heads = w_key.shape[1]
        q_w, kv_w = q_heads * hd, kv_heads * hd
        n_rows = q_w + 2 * kv_w
        seq = n_dev * tok
        hw = 2 * hd

        def flat_weight(w):
            return jnp.transpose(w, (1, 2, 0)).reshape(-1, width)

        hbm = pl.BlockSpec(memory_space=pltpu.HBM)
        vmem = pl.BlockSpec(memory_space=pltpu.VMEM)
        dma = pltpu.SemaphoreType.DMA
        n_chip = n_dev // 2
        n_far = n_chip - 1 - 2 * NEAR
        pair = 2 * tok
        scratch = [
            pltpu.VMEM((n_chip, pair, width), BF),
            pltpu.VMEM((n_chip, pair, width), BF),
            pltpu.VMEM((n_rows, width), BF),
            pltpu.VMEM((2 * hw, width), BF),
            pltpu.VMEM((hw, width), BF),
            pltpu.VMEM((n_far * hw, width), BF),
            pltpu.VMEM((n_dev, 1, tok), jnp.int32),
            pltpu.VMEM((n_chip, hd // 2, pair), F32),
            pltpu.VMEM((n_chip, hd, 2 * pair), BF),
            pltpu.VMEM((hw, seq), BF),
            pltpu.VMEM((seq, hw), BF),
            pltpu.VMEM((n_far, hw, seq), BF),
            pltpu.VMEM((n_far, seq, hw), BF),
            pltpu.VMEM((n_far, hd, 2 * pair), BF),
            pltpu.VMEM((n_far, hd, 2 * pair), BF),
            pltpu.VMEM((hw, 4 * pair), BF),
            pltpu.VMEM((seq, 2 * pair), F32),
            pltpu.VMEM((seq, 2 * pair), F32),
            pltpu.VMEM((n_chip, 1, 2 * pair), F32),
            pltpu.VMEM((hw, 2 * pair), F32),
            pltpu.VMEM((hw, seq), F32),
            pltpu.VMEM((hd, seq), F32),
            pltpu.VMEM((n_dev, hd, tok), BF),
            pltpu.VMEM((hd, seq), BF),
            pltpu.VMEM((hw, width), F32),
            pltpu.VMEM((hw + hd, width), F32),
            pltpu.VMEM((n_dev, hw, tok), BF),
            pltpu.VMEM((n_dev, hw, tok), BF),
            pltpu.VMEM((q_w, tok), BF),
            pltpu.VMEM((n_rows, tok), BF),
            pltpu.VMEM((tok, q_w), BF),
            pltpu.VMEM((tok, n_rows), BF),
            pltpu.VMEM((tok, width), BF),
            pltpu.VMEM((tok, width), BF),
            pltpu.VMEM((2, 1, width), F32),
            pltpu.VMEM((2, tok, 128), F32),
            pltpu.VMEM((tok, width), BF),
            pltpu.VMEM((2, 1, width), F32),
            pltpu.VMEM((1, width), F32),
            pltpu.VMEM((1, width), F32),
            pltpu.VMEM((n_chip, 1, width), F32),
            pltpu.VMEM((2, 1, width), F32),
            dma((10,)), dma((3 * n_far,)), dma((n_chip,)), dma((3,)), dma((4,)), dma((2,)),
        ] + [dma((9 * PARTS,)), dma((7 * PARTS,)), dma((8 * PARTS,)), dma((8 * PARTS,))] * 2 + [dma((n_dev,))] * 6 + [dma] * 2 + [dma((n_dev,))] * 8
        out, gx, gw, gwo, gg = pl.pallas_call(
            functools.partial(block_kernel, n_dev, hd, kv_w, NEAR, PARTS),
            out_shape=(
                jax.ShapeDtypeStruct((tok, width), BF),
                jax.ShapeDtypeStruct((tok, width), BF),
                jax.ShapeDtypeStruct((n_rows, tok), F32),
                jax.ShapeDtypeStruct((hw, width), F32),
                jax.ShapeDtypeStruct((2, 1, width), F32),
            ),
            in_specs=[hbm] * 9,
            out_specs=(hbm,) * 5,
            scratch_shapes=scratch,
            compiler_params=pltpu.CompilerParams(collective_id=0, has_side_effects=True, vmem_limit_bytes=67043328),
            name='attn_block',
        )(
            x_act.reshape(tok, width), d_out.reshape(tok, width), positions.reshape(1, tok),
            ln_gain.reshape(1, width), ln_bias.reshape(1, width),
            flat_weight(w_query), flat_weight(w_key), flat_weight(w_value), w_out,
        )

        out, gx, gq, gk, gv, gwo, gain, bias = pl.pallas_call(
            functools.partial(settle_kernel, q_w, kv_w),
            out_shape=(
                jax.ShapeDtypeStruct((tok, width), BF),
                jax.ShapeDtypeStruct((tok, width), BF),
                jax.ShapeDtypeStruct((q_w, tok), F32),
                jax.ShapeDtypeStruct((kv_w, tok), F32),
                jax.ShapeDtypeStruct((kv_w, tok), F32),
                jax.ShapeDtypeStruct((hw, width), F32),
                jax.ShapeDtypeStruct((width,), F32),
                jax.ShapeDtypeStruct((width,), F32),
            ),
            in_specs=[hbm] * 5,
            out_specs=(hbm,) * 6 + (vmem,) * 2,
            scratch_shapes=[
                pltpu.VMEM((2, tok, width), BF),
                pltpu.VMEM((2, q_w // 2, tok), F32),
                pltpu.VMEM((2, kv_w, tok), F32),
                pltpu.VMEM((2, hw // 2, width), F32),
                pltpu.VMEM((2, 1, width), F32),
                dma((8,)), dma((8,)), dma,
            ],
            name='settle',
        )(out, gx, gw, gwo, gg)

        def rows_out(block, heads):
            return jnp.transpose(block.reshape(heads, hd, tok), (2, 0, 1))

        return (
            out.reshape(1, tok, width), gx.reshape(1, tok, width),
            rows_out(gq, q_heads), rows_out(gk, kv_heads), rows_out(gv, kv_heads),
            gwo, gain, bias,
        )

    return jax.shard_map(device_step, mesh=mesh, in_specs=(P('dp', 'cp', None), P('dp', 'cp', None), P('dp', 'cp'), P(None), P(None), P(None, None, None), P(None, None, None), P(None, None, None), P(None, None)), out_specs=(P('dp', 'cp', None), P('dp', 'cp', None), P(('dp', 'cp'), None, None), P(('dp', 'cp'), None, None), P(('dp', 'cp'), None, None), P(('dp', 'cp'), None), P('dp'), P('dp')), check_vma=False)
```

```python
import functools
import math

import jax
import jax.numpy as jnp
from jax import lax
from jax.experimental import pallas as pl
from jax.experimental.pallas import tpu as pltpu
from jax.sharding import PartitionSpec as P

EPS = 1e-5
ROPE_BASE = 10000.0
MESH = pl.DeviceIdType.MESH
BF = jnp.bfloat16
F32 = jnp.float32
NEAR = 1
PARTS = 4
FIRST = 1
HELD = 4


def dot(lhs, rhs):
    return jnp.dot(lhs, rhs, preferred_element_type=F32)


def dot_t(lhs, rhs):
    return lax.dot_general(lhs, rhs, (((1,), (1,)), ((), ())), preferred_element_type=F32)


def block_kernel(
    n_dev, hd, kv_w, near, parts,
    x_hbm, dy_hbm, pos_hbm, gain_hbm, bias_hbm, wq_hbm, wk_hbm, wv_hbm, wo_hbm,
    out_hbm, gx_hbm, gw_hbm, gwo_hbm, gg_hbm,
    hb, dyb, wt, wi, woi, w_far, pos_all, trig,
    qt, kvt, kv, kvt_far, kv_far, da_far, bmat, sbuf, dpbuf, mbuf, adq, dkvt, kv_rv, kv_mine, kv_row,
    dwo, dwt, at_all, dq_all, at_rv, dt_rv, a_nat, d_nat, x_v, dy_own, gb_v, stat, out_v, gg_st, gg_mx, gg_my, gg_rv, gg_out,
    in_sem, far_sem, wo_sem, w_sem, out_sem, loc_sem,
    hzs, hzr, hds, hdr, yzs, yzr, yds, ydr,
    pos_s, pos_r, a_s, a_r, q_s, q_r, x_s, x_r, kv_s, kv_r, w_s, w_r, wk_s, wk_r, g_s, g_r,
):
    tok, width = x_v.shape
    n_chip = n_dev // 2
    pair = 2 * tok
    me = lax.axis_index('cp')
    chip = me // 2
    core = me % 2
    right = 2 * ((chip + 1) % n_chip) + core
    left = 2 * ((chip + n_chip - 1) % n_chip) + core
    mate = 2 * chip + 1 - core
    q_rows = wq_hbm.shape[0]
    n_rows = q_rows + 2 * kv_w
    hw = 2 * hd
    quarter = hd // 4
    tile = 256
    scale = hd ** -0.5
    cols_q = 2 * pair
    n_far = n_chip - 1 - 2 * near

    def remote(src, dst, send, recv, target):
        return pltpu.make_async_remote_copy(src_ref=src, dst_ref=dst, send_sem=send, recv_sem=recv, device_id={'cp': target}, device_id_type=MESH)

    def local(src, dst, sem):
        return pltpu.make_async_copy(src, dst, sem)

    def part_of(i, size):
        return pl.ds(pl.multiple_of(i * size, size), size)

    def ring_steps(k):
        step = (k + 1) // 2
        return step, k % 2

    def ring_origin(k):
        step, ahead = ring_steps(k)
        return jnp.where(ahead == 1, chip + n_chip - step, chip + step) % n_chip

    own = (chip, part_of(core, tok))
    first_loads = [
        local(x_hbm, x_v, in_sem.at[0]),
        local(gain_hbm, gb_v.at[0], in_sem.at[1]),
        local(bias_hbm, gb_v.at[1], in_sem.at[2]),
        local(pos_hbm, pos_all.at[me], in_sem.at[3]),
    ]
    for item in first_loads:
        item.start()
    barrier = pltpu.get_barrier_semaphore()
    for step in range(1, n_dev):
        pl.semaphore_signal(barrier, inc=1, device_id={'cp': (me + step) % n_dev}, device_id_type=MESH)
    own_rows = part_of(me, hw)
    kv_rows = part_of(chip, hd)
    loads = [
        local(wq_hbm.at[own_rows], wi.at[pl.ds(0, hw)], in_sem.at[4]),
        local(wk_hbm.at[kv_rows], wi.at[pl.ds(hw, hd)], in_sem.at[5]),
        local(wv_hbm.at[kv_rows], wi.at[pl.ds(hw + hd, hd)], in_sem.at[6]),
        local(wo_hbm.at[own_rows], woi, in_sem.at[7]),
        local(dy_hbm, dyb.at[own], in_sem.at[8]),
        local(dy_hbm, dy_own, in_sem.at[9]),
    ]
    far_loads = []
    for f in range(n_far):
        far_rows = part_of(ring_origin(2 * near + 1 + f), hd)
        loads.append(local(wk_hbm.at[far_rows], w_far.at[pl.ds(hw * f, hd)], far_sem.at[2 * f]))
        loads.append(local(wv_hbm.at[far_rows], w_far.at[pl.ds(hw * f + hd, hd)], far_sem.at[2 * f + 1]))
        far_wo = part_of(ring_origin(2 * near + 1 + f), 2 * hw)
        far_loads.append(local(wo_hbm.at[far_wo], wt.at[pl.ds(2 * hw * f, 2 * hw)], far_sem.at[2 * n_far + f]))
    for item in loads + far_loads:
        item.start()

    for item in first_loads:
        item.wait()
    gain_one = 1.0 + gb_v[0]
    block = 16

    @pl.loop(0, tok // block)
    def _(i):
        rows = part_of(i, block)
        x_f = x_v[rows, :].astype(F32)
        mean = jnp.mean(x_f, axis=-1, keepdims=True)
        centered = x_f - mean
        inv_std = lax.rsqrt(jnp.mean(centered * centered, axis=-1, keepdims=True) + EPS)
        hb[chip, part_of(core * (tok // block) + i, block), :] = (centered * inv_std * gain_one + gb_v[1]).astype(BF)
        stat[0, rows, :] = jnp.broadcast_to(mean, (block, 128))
        stat[1, rows, :] = jnp.broadcast_to(inv_std, (block, 128))

    pl.semaphore_wait(barrier, n_dev - 1)

    def chunk(buf, origin, parity, part):
        return buf.at[origin, part_of(parts * parity + part, tok // parts)]

    turns = 2 * parts

    def own_sends(buf, zs, zr, ds, dr):
        copies = []
        for part in range(parts):
            piece = chunk(buf, chip, core, part)
            copies.append(remote(piece, piece, zs.at[2 * part], zr.at[2 * part], right))
            copies.append(remote(piece, piece, zs.at[2 * part + 1], zr.at[2 * part + 1], left))
            copies.append(remote(piece, piece, ds.at[7 * parts + part], dr.at[7 * parts + part], mate))
        return copies

    def event_place(event):
        step = event // turns + 1
        turn = event % turns
        direction = turn % 2
        part = jnp.where(step < 4, turn // 2, turn // 2 + direction * (parts // 2))
        origin = jnp.where(direction == 0, chip + n_chip - step, chip + step) % n_chip
        return step, direction, part, origin

    def last_event(part, direction):
        return 6 * parts + 2 * (part - direction * (parts // 2)) + direction

    def ring_event(ring, event):
        buf, zs, zr, ds, dr = ring
        step, direction, part, origin = event_place(event)
        piece = chunk(buf, origin, core, part)
        remote(piece, piece, zs.at[0], zr.at[event], right).wait_recv()
        onward = jnp.where(step < 3, event + turns, last_event(part, direction))

        @pl.when((step < 3) | ((step == 3) & ((part >= parts // 2) == (direction == 1))))
        def _():
            remote(piece, piece, zs.at[event + turns], zr.at[onward], jnp.where(direction == 0, right, left)).start()

        remote(piece, piece, ds.at[event], dr.at[event], mate).start()

    def ring_service(ring, event):
        @pl.when(event < 7 * parts)
        def _():
            ring_event(ring, event)

    def ring_mate(ring, k, origin):
        buf, zs, zr, ds, dr = ring
        step, ahead = ring_steps(k)
        for part in range(parts):
            event = jnp.where(k == 0, 7 * parts + part, jnp.where(step < 4, turns * (step - 1) + 2 * part + 1 - ahead, last_event(part, part // (parts // 2))))
            piece = chunk(buf, origin, 1 - core, part)
            remote(piece, piece, ds.at[0], dr.at[event], mate).wait_recv()

    def finish_ring(ring):
        buf, zs, zr, ds, dr = ring
        for item in own_sends(*ring):
            item.wait_send()

        @pl.loop(0, 7 * parts)
        def _(event):
            step, direction, part, origin = event_place(event)
            piece = chunk(buf, origin, core, part)

            @pl.when((step < 3) | ((step == 3) & ((part >= parts // 2) == (direction == 1))))
            def _():
                remote(piece, piece, zs.at[event + turns], zr.at[event], right).wait_send()

            remote(piece, piece, ds.at[event], dr.at[event], mate).wait_send()

    h_ring = (hb, hzs, hzr, hds, hdr)
    y_ring = (dyb, yzs, yzr, yds, ydr)
    for item in own_sends(*h_ring):
        item.start()
    pos_sends = [remote(pos_all.at[me], pos_all.at[me], pos_s.at[step], pos_r.at[me], (me + step) % n_dev) for step in range(1, n_dev)]
    for item in pos_sends:
        item.start()
    weight_loads = [
        local(wq_hbm, wt.at[pl.ds(0, q_rows)], w_sem.at[0]),
        local(wk_hbm, wt.at[pl.ds(q_rows, kv_w)], w_sem.at[1]),
        local(wv_hbm, wt.at[pl.ds(q_rows + kv_w, kv_w)], w_sem.at[2]),
    ]
    dkvt[...] = jnp.zeros_like(dkvt)
    bmat[...] = jnp.zeros_like(bmat)

    freq = jnp.exp(lax.broadcasted_iota(jnp.int32, (quarter, tok), 0).astype(F32) * (-2.0 * math.log(ROPE_BASE) / (hd // 2)))

    def make_trig(b):
        for t in range(2):
            slot = 2 * b + t

            @pl.when(slot != me)
            def _():
                remote(pos_all.at[slot], pos_all.at[slot], pos_s.at[0], pos_r.at[slot], me).wait_recv()

            angle = pos_all[slot].astype(F32) * freq
            trig[b, 0:quarter, tok * t:tok * t + tok] = jnp.cos(angle)
            trig[b, quarter:2 * quarter, tok * t:tok * t + tok] = jnp.sin(angle)

    def turned(val, cos_t, sin_t):
        u = val[0:quarter]
        w = val[quarter:2 * quarter]
        return [u * cos_t - w * sin_t, w * cos_t + u * sin_t, val[2 * quarter:hd]]

    def eighth(val):
        return val.astype(BF) * jnp.asarray(scale, BF)

    def keys_values(val, cos_t, sin_t):
        return jnp.concatenate(turned(val[0:hd], cos_t, sin_t) + [val[hd:hw]], axis=0).astype(BF)

    @pl.loop(0, n_chip)
    def _(k):
        for turn in range(parts):
            ring_service(h_ring, parts * k + turn)

        @pl.when(k == 5)
        def _():
            for item in own_sends(*y_ring):
                item.start()

        @pl.when(k == 0)
        def _():
            for item in loads:
                item.wait()

        @pl.when(k == 2)
        def _():
            for item in far_loads:
                item.wait()

        @pl.when((k >= 2) & (k < 2 + n_far))
        def _():
            f = k - 2
            da_t = dot_t(wt[part_of(f, 2 * hw), :], dy_own[...]).astype(BF)
            for head in range(4):
                da_far[f, :, tok * head:tok * head + tok] = da_t[hd * head:hd * head + hd]

        @pl.when(k == 1 + n_far)
        def _():
            for item in weight_loads:
                item.start()

        b = ring_origin(k)
        ring_mate(h_ring, k, b)
        make_trig(b)
        place = part_of(b, pair)
        cos_t = trig[b, 0:quarter, :]
        sin_t = trig[b, quarter:2 * quarter, :]
        flat = dot_t(wi[...], hb[b])
        for head in range(2):
            q_rot = eighth(jnp.concatenate(turned(flat[hd * head:hd * head + hd], cos_t, sin_t), axis=0))
            for t in range(2):
                lane = pair * t + tok * head
                qt[b, :, lane:lane + tok] = q_rot[:, tok * t:tok * t + tok]
        kv_rot = keys_values(flat[hw:2 * hw], cos_t, sin_t)
        kvt[:, place] = kv_rot
        kv[place, :] = kv_rot.T

        @pl.when(b <= chip)
        def _():
            flat_far = dot_t(w_far[...], hb[b])
            for f in range(n_far):
                far_rot = keys_values(flat_far[hw * f:hw * f + hw], cos_t, sin_t)
                kvt_far[f, :, place] = far_rot
                kv_far[f, place, :] = far_rot.T

    groups = [slice(tile * g, tile * g + tile) for g in range(cols_q // tile)]

    def first_part(b, seen, kv_of):
        def both_of(c):
            rows = part_of(c, pair)
            both = dot(kv_of(rows), bmat[...])
            return rows, both[:, 0:cols_q], both[:, cols_q:2 * cols_q]

        rows, s, d_p = both_of(b)
        s = jnp.where(seen, s, -1e30)
        top = jnp.max(s, axis=0, keepdims=True)
        p = jnp.exp(s - top)
        sbuf[rows, :] = p
        dpbuf[rows, :] = d_p
        mbuf[b] = top

        def step(c, state):
            old, total, weighted = state
            rows, s, d_p = both_of(c)
            new = jnp.maximum(old, jnp.max(s, axis=0, keepdims=True))
            p = jnp.exp(s - new)
            sbuf[rows, :] = p
            dpbuf[rows, :] = d_p
            mbuf[c] = new
            keep = jnp.exp(old - new)
            return new, total * keep + jnp.sum(p, axis=0, keepdims=True), weighted * keep + jnp.sum(p * d_p, axis=0, keepdims=True)

        top, total, weighted = lax.fori_loop(0, b, step, (top, jnp.sum(p, axis=0, keepdims=True), jnp.sum(p * d_p, axis=0, keepdims=True)))
        inv = 1.0 / total
        return top, inv, weighted * inv

    def second_part(b, stats, kvt_of, with_keys):
        top, inv, row_dot = stats
        adq[...] = jnp.zeros_like(adq)

        def step(c, carry):
            rows = part_of(c, pair)
            factor = jnp.exp(mbuf[c] - top) * inv
            d_k = d_v = None
            for at in groups:
                p = sbuf[rows, at] * factor[:, at]
                p_b = p.astype(BF)
                ds_b = (p * (dpbuf[rows, at] - row_dot[:, at])).astype(BF)
                adq[0:hd, at] += dot(kvt_of(slice(0, hd), rows), ds_b)
                adq[hd:hw, at] += dot(kvt_of(slice(hd, hw), rows), p_b)
                if with_keys:
                    more_k = dot_t(bmat[0:hd, at], ds_b)
                    more_v = dot_t(bmat[hd:hw, cols_q + at.start:cols_q + at.stop], p_b)
                    d_k = more_k if d_k is None else d_k + more_k
                    d_v = more_v if d_v is None else d_v + more_v
            if with_keys:
                dkvt[0:hd, rows] += d_k
                dkvt[hd:hw, rows] += d_v
            return carry

        lax.fori_loop(0, b + 1, step, 0)

    lane = lax.broadcasted_iota(jnp.int32, (pair, cols_q), 1)
    row = lax.broadcasted_iota(jnp.int32, (pair, cols_q), 0)

    def send_rows(slot):
        cols = part_of(slot, tok)
        return [
            remote(dq_all.at[:, cols], dt_rv.at[own_rows], q_s.at[slot], q_r.at[me], slot),
            remote(at_all.at[:, cols], at_rv.at[own_rows], a_s.at[slot], a_r.at[me], slot),
        ]

    @pl.loop(0, n_chip)
    def _(k):
        for turn in range(parts - 1):
            ring_service(y_ring, parts * k + turn)
        b = ring_origin(k)
        ring_mate(y_ring, k, b)

        @pl.when(k == 1)
        def _():
            for item in weight_loads:
                item.wait()

        @pl.when(k == n_chip - 1)
        def _():
            for early in range(1 + 2 * near):
                for t in range(2):
                    slot = 2 * ring_origin(early) + t

                    @pl.when(slot != me)
                    def _():
                        for item in send_rows(slot):
                            item.start()

        da_t = dot_t(woi[...], dyb[b]).astype(BF)
        bmat[0:hd, 0:cols_q] = qt[b]
        for t in range(2):
            for head in range(2):
                at = cols_q + pair * t + tok * head
                bmat[hd:hw, at:at + tok] = da_t[hd * head:hd * head + hd, tok * t:tok * t + tok]
        stats = first_part(b, row <= (lane // pair) * tok + lane % tok, lambda rows: kv[rows, :])
        ring_service(y_ring, parts * k + parts - 1)
        second_part(b, stats, lambda part, rows: kvt[part, rows], True)
        for t in range(2):
            slot = 2 * b + t
            lanes = [slice(pair * t + tok * head, pair * t + tok * head + tok) for head in range(2)]
            a_t = jnp.concatenate([adq[hd:hw, at] for at in lanes], axis=0).astype(BF)
            cos_t = trig[b, 0:quarter, tok * t:tok * t + tok]
            sin_t = trig[b, quarter:2 * quarter, tok * t:tok * t + tok]
            dq_t = jnp.concatenate([piece for at in lanes for piece in turned(adq[0:hd, at] * scale, cos_t, -sin_t)], axis=0).astype(BF)
            at_all[:, part_of(slot, tok)] = a_t
            dq_all[:, part_of(slot, tok)] = dq_t

            @pl.when(slot == me)
            def _():
                at_rv[own_rows, :] = a_t
                dt_rv[own_rows, :] = dq_t

    far = [ring_origin(k) for k in range(n_chip - 1, 0, -1)]
    targets = [2 * c + p for c in far for p in range(2)] + [mate]
    near_targets = targets[-1 - 4 * near:]
    swap = remote(dkvt.at[part_of(1 - core, hd)], kv_rv, x_s, x_r, mate)
    swap.start()
    w_sends = [remote(dwt.at[pl.ds(0, hw), part_of(t, tok)], gw_hbm.at[own_rows], w_s.at[t], w_r.at[me], t) for t in targets]

    def columns(rows_all, buf, cols):
        acc = jnp.zeros((rows_all.shape[0], tile), F32)
        for s in range(n_chip):
            acc += dot(rows_all[:, pair * s:pair * s + pair], buf[s, :, cols])
        return acc

    def q_columns(i):
        cols = part_of(far[i] if i < n_chip - 1 else chip, pair)
        dwt[0:hw, cols] = columns(dq_all, hb, cols)
        for item in w_sends[max(2 * i - 2, 0):2 * i]:
            item.start()

    for i in range(FIRST + 1):
        q_columns(i)

    swap.wait_recv()
    mine = part_of(core, hd)
    g_rows = pl.ds(pl.multiple_of(q_rows + core * kv_w + chip * hd, hd), hd)
    for t in range(n_chip):
        cols = slice(pair * t, pair * t + pair)
        g = dkvt[mine, cols] + kv_rv[:, cols]
        cos_t = jnp.where(core == 0, trig[t, 0:quarter, :], 1.0)
        sin_t = jnp.where(core == 0, trig[t, quarter:2 * quarter, :], 0.0)
        g_b = jnp.concatenate(turned(g, cos_t, -sin_t), axis=0).astype(BF)
        kv_mine[2 * t] = g_b[:, 0:tok]
        kv_mine[2 * t + 1] = g_b[:, tok:pair]
        kv_row[:, cols] = g_b
    dt_rv[g_rows, :] = kv_mine[me]
    kv_sends = [remote(kv_mine.at[t], dt_rv.at[g_rows], kv_s.at[t], kv_r.at[me], t) for t in targets]
    for item in kv_sends:
        item.start()
    for i in range(FIRST + 1, n_chip):
        q_columns(i)
    w_sends[-1].start()
    w_own = local(dwt.at[pl.ds(0, hw), part_of(me, tok)], gw_hbm.at[own_rows], loc_sem.at[0])
    w_own.start()
    for t in range(width // tile):
        cols = slice(tile * t, tile * t + tile)
        dwt[hw:hw + hd, cols] = columns(kv_row, hb, cols)
    wk_own = local(dwt.at[pl.ds(hw, hd), part_of(me, tok)], gw_hbm.at[g_rows], loc_sem.at[1])
    wk_own.start()
    wk_sends = [remote(dwt.at[pl.ds(hw, hd), part_of(t, tok)], gw_hbm.at[g_rows], wk_s.at[t], wk_r.at[me], t) for t in targets]
    for item in wk_sends[0:HELD]:
        item.start()

    for t in range(width // tile):
        cols = slice(tile * t, tile * t + tile)
        dwo[:, cols] = columns(at_all, dyb, cols)
    store_wo = local(dwo, gwo_hbm, out_sem.at[0])
    store_wo.start()
    finish_ring(y_ring)
    wo_loads = [local(wo_hbm.at[pl.ds(pair * t, pair)], dyb.at[t], wo_sem.at[t]) for t in range(n_chip)]
    for item in wo_loads:
        item.start()

    @pl.loop(0, n_far)
    def _(f):
        c_far = ring_origin(2 * near + 1 + f)
        cos_t = trig[chip, 0:quarter, part_of(core, tok)]
        sin_t = trig[chip, quarter:2 * quarter, part_of(core, tok)]
        q_t = dot_t(wt[part_of(c_far, 2 * hw), :], hb[chip, part_of(core, tok), :])
        for head in range(4):
            bmat[0:hd, tok * head:tok * head + tok] = eighth(jnp.concatenate(turned(q_t[hd * head:hd * head + hd], cos_t, sin_t), axis=0))
        bmat[hd:hw, cols_q:2 * cols_q] = da_far[f]
        stats = first_part(chip, row <= core * tok + lane % tok, lambda rows: kv_far[f, rows, :])
        second_part(chip, stats, lambda part, rows: kvt_far[f, part, rows], False)
        for head in range(4):
            at = slice(tok * head, tok * head + tok)
            place = pl.ds(pl.multiple_of(c_far * 2 * hw + hd * head, hd), hd)
            at_rv[place, :] = adq[hd:hw, at].astype(BF)
            dt_rv[place, :] = jnp.concatenate(turned(adq[0:hd, at] * scale, cos_t, -sin_t), axis=0).astype(BF)

    for t in near_targets:
        remote(at_all.at[:, pl.ds(0, tok)], at_rv.at[part_of(t, hw)], a_s.at[t], a_r.at[t], t).wait_recv()
    for item in wo_loads:
        item.wait()
    for t in range(q_rows // tok):
        a_nat[:, tok * t:tok * t + tok] = at_rv[tok * t:tok * t + tok, :].T
    for t in range(width // tile):
        cols = slice(tile * t, tile * t + tile)
        prod = jnp.zeros((tok, tile), F32)
        for s in range(n_chip):
            prod += dot(a_nat[:, pair * s:pair * s + pair], dyb[s, :, cols])
        out_v[:, cols] = (x_v[:, cols].astype(F32) + prod).astype(BF)
    store_out = local(out_v, out_hbm, out_sem.at[1])
    store_out.start()

    def kv_place(t):
        return pl.ds(pl.multiple_of(q_rows + (t % 2) * kv_w + (t // 2) * hd, hd), hd)

    for t in near_targets:
        remote(dq_all.at[:, pl.ds(0, tok)], dt_rv.at[part_of(t, hw)], q_s.at[t], q_r.at[t], t).wait_recv()
    for t in targets:
        remote(kv_mine.at[0], dt_rv.at[kv_place(t)], kv_s.at[t], kv_r.at[t], t).wait_recv()
    swap.wait_send()
    for t in range(n_rows // tok):
        d_nat[:, tok * t:tok * t + tok] = dt_rv[tok * t:tok * t + tok, :].T

    mean = stat[0, :, 0:1]
    inv_std = stat[1, :, 0:1]
    dh = dkvt
    for t in range(width // tile):
        cols = slice(tile * t, tile * t + tile)
        acc = jnp.zeros((tok, tile), F32)
        for s in range(n_rows // tile):
            acc += dot(d_nat[:, tile * s:tile * s + tile], wt[tile * s:tile * s + tile, cols])
        dh[:, cols] = acc
        gg_st[0, :, cols] = jnp.sum(acc * ((x_v[:, cols].astype(F32) - mean) * inv_std), axis=0, keepdims=True)
        gg_st[1, :, cols] = jnp.sum(acc, axis=0, keepdims=True)
    g_swap = remote(gg_st.at[1 - core], gg_mx, g_s.at[n_chip], g_r.at[n_chip], mate)
    g_swap.start()
    g_swap.wait_recv()
    gg_my[...] = jnp.where(core == 0, gg_st[0], gg_st[1]) + gg_mx[...]
    gg_rv[chip] = gg_my[...]
    g_sends = [remote(gg_my, gg_rv.at[chip], g_s.at[c], g_r.at[chip], 2 * c + core) for c in far]
    for item in g_sends + wk_sends[HELD:]:
        item.start()

    grad_hat = dh[...] * gain_one
    x_hat = (x_v[...].astype(F32) - mean) * inv_std
    mean_one = jnp.mean(grad_hat, axis=-1, keepdims=True)
    mean_two = jnp.mean(grad_hat * x_hat, axis=-1, keepdims=True)
    store_out.wait()
    out_v[...] = (dy_own[...].astype(F32) + inv_std * (grad_hat - mean_one - x_hat * mean_two)).astype(BF)
    store_gx = local(out_v, gx_hbm, out_sem.at[2])
    store_gx.start()

    for c in far:
        remote(gg_my, gg_rv.at[c], g_s.at[c], g_r.at[c], 2 * c + core).wait_recv()
    sums = gg_rv[0]
    for c in range(1, n_chip):
        sums = sums + gg_rv[c]
    gg_out[core] = sums
    g_swap_out = remote(gg_out.at[core], gg_out.at[core], g_s.at[n_chip + 1], g_r.at[n_chip + 1], mate)
    g_swap_out.start()
    remote(gg_out.at[core], gg_out.at[1 - core], g_s.at[n_chip + 1], g_r.at[n_chip + 1], mate).wait_recv()
    store_gg = local(gg_out, gg_hbm, out_sem.at[3])
    store_gg.start()

    finish_ring(h_ring)
    for item in pos_sends + [g_swap, g_swap_out]:
        item.wait_send()
    for t in near_targets:
        remote(at_all.at[:, pl.ds(0, tok)], at_rv.at[pl.ds(0, hw)], a_s.at[t], a_r.at[t], t).wait_send()
        remote(dq_all.at[:, pl.ds(0, tok)], dt_rv.at[pl.ds(0, hw)], q_s.at[t], q_r.at[t], t).wait_send()
    for item in kv_sends + w_sends + g_sends + wk_sends:
        item.wait_send()
    for t in targets:
        remote(dwt.at[pl.ds(0, hw), part_of(t, tok)], gw_hbm.at[part_of(t, hw)], w_s.at[t], w_r.at[t], t).wait_recv()
        remote(dwt.at[pl.ds(hw, hd), part_of(t, tok)], gw_hbm.at[kv_place(t)], wk_s.at[t], wk_r.at[t], t).wait_recv()
    for item in (w_own, wk_own, store_wo, store_gx, store_gg):
        item.wait()


def settle_kernel(q_rows, kv_w, out_i, gx_i, gw_i, gwo_i, gg_i, out_o, gx_o, gq_o, gk_o, gv_o, gwo_o, gain_o, bias_o, b_act, b_q, b_kv, b_o, b_gg, sem_in, sem_out, sem_gg):
    half_q = q_rows // 2
    half_o = gwo_i.shape[0] // 2
    moves = [(out_i, b_act.at[0], out_o), (gx_i, b_act.at[1], gx_o)]
    for t in range(2):
        moves.append((gw_i.at[pl.ds(half_q * t, half_q)], b_q.at[t], gq_o.at[pl.ds(half_q * t, half_q)]))
        moves.append((gwo_i.at[pl.ds(half_o * t, half_o)], b_o.at[t], gwo_o.at[pl.ds(half_o * t, half_o)]))
    moves.append((gw_i.at[pl.ds(q_rows, kv_w)], b_kv.at[0], gk_o))
    moves.append((gw_i.at[pl.ds(q_rows + kv_w, kv_w)], b_kv.at[1], gv_o))
    loads = [pltpu.make_async_copy(src, mid, sem_in.at[i]) for i, (src, mid, _) in enumerate(moves)]
    stores = [pltpu.make_async_copy(mid, dst, sem_out.at[i]) for i, (_, mid, dst) in enumerate(moves)]
    load_gg = pltpu.make_async_copy(gg_i, b_gg, sem_gg)
    load_gg.start()
    for item in loads:
        item.start()
    for load, store in zip(loads, stores):
        load.wait()
        store.start()
    load_gg.wait()
    gain_o[...] = b_gg[0, 0]
    bias_o[...] = b_gg[1, 0]
    for item in stores:
        item.wait()


def solution(mesh):
    n_dev = mesh.shape['cp']

    def device_step(x_act, d_out, positions, ln_gain, ln_bias, w_query, w_key, w_value, w_out):
        tok, width = x_act.shape[1], x_act.shape[2]
        q_heads, hd = w_query.shape[1], w_query.shape[2]
        kv_heads = w_key.shape[1]
        q_w, kv_w = q_heads * hd, kv_heads * hd
        n_rows = q_w + 2 * kv_w
        seq = n_dev * tok
        hw = 2 * hd

        def flat_weight(w):
            return jnp.transpose(w, (1, 2, 0)).reshape(-1, width)

        hbm = pl.BlockSpec(memory_space=pltpu.HBM)
        vmem = pl.BlockSpec(memory_space=pltpu.VMEM)
        dma = pltpu.SemaphoreType.DMA
        n_chip = n_dev // 2
        n_far = n_chip - 1 - 2 * NEAR
        pair = 2 * tok
        scratch = [
            pltpu.VMEM((n_chip, pair, width), BF),
            pltpu.VMEM((n_chip, pair, width), BF),
            pltpu.VMEM((n_rows, width), BF),
            pltpu.VMEM((2 * hw, width), BF),
            pltpu.VMEM((hw, width), BF),
            pltpu.VMEM((n_far * hw, width), BF),
            pltpu.VMEM((n_dev, 1, tok), jnp.int32),
            pltpu.VMEM((n_chip, hd // 2, pair), F32),
            pltpu.VMEM((n_chip, hd, 2 * pair), BF),
            pltpu.VMEM((hw, seq), BF),
            pltpu.VMEM((seq, hw), BF),
            pltpu.VMEM((n_far, hw, seq), BF),
            pltpu.VMEM((n_far, seq, hw), BF),
            pltpu.VMEM((n_far, hd, 2 * pair), BF),
            pltpu.VMEM((hw, 4 * pair), BF),
            pltpu.VMEM((seq, 2 * pair), F32),
            pltpu.VMEM((seq, 2 * pair), F32),
            pltpu.VMEM((n_chip, 1, 2 * pair), F32),
            pltpu.VMEM((hw, 2 * pair), F32),
            pltpu.VMEM((hw, seq), F32),
            pltpu.VMEM((hd, seq), F32),
            pltpu.VMEM((n_dev, hd, tok), BF),
            pltpu.VMEM((hd, seq), BF),
            pltpu.VMEM((hw, width), F32),
            pltpu.VMEM((hw + hd, width), F32),
            pltpu.VMEM((hw, seq), BF),
            pltpu.VMEM((hw, seq), BF),
            pltpu.VMEM((q_w, tok), BF),
            pltpu.VMEM((n_rows, tok), BF),
            pltpu.VMEM((tok, q_w), BF),
            pltpu.VMEM((tok, n_rows), BF),
            pltpu.VMEM((tok, width), BF),
            pltpu.VMEM((tok, width), BF),
            pltpu.VMEM((2, 1, width), F32),
            pltpu.VMEM((2, tok, 128), F32),
            pltpu.VMEM((tok, width), BF),
            pltpu.VMEM((2, 1, width), F32),
            pltpu.VMEM((1, width), F32),
            pltpu.VMEM((1, width), F32),
            pltpu.VMEM((n_chip, 1, width), F32),
            pltpu.VMEM((2, 1, width), F32),
            dma((10,)), dma((3 * n_far,)), dma((n_chip,)), dma((3,)), dma((4,)), dma((2,)),
        ] + [dma((9 * PARTS,)), dma((7 * PARTS,)), dma((8 * PARTS,)), dma((8 * PARTS,))] * 2 + [dma((n_dev,))] * 6 + [dma] * 2 + [dma((n_dev,))] * 8
        out, gx, gw, gwo, gg = pl.pallas_call(
            functools.partial(block_kernel, n_dev, hd, kv_w, NEAR, PARTS),
            out_shape=(
                jax.ShapeDtypeStruct((tok, width), BF),
                jax.ShapeDtypeStruct((tok, width), BF),
                jax.ShapeDtypeStruct((n_rows, tok), F32),
                jax.ShapeDtypeStruct((hw, width), F32),
                jax.ShapeDtypeStruct((2, 1, width), F32),
            ),
            in_specs=[hbm] * 9,
            out_specs=(hbm,) * 5,
            scratch_shapes=scratch,
            compiler_params=pltpu.CompilerParams(collective_id=0, has_side_effects=True, vmem_limit_bytes=67043328),
            name='attn_block',
        )(
            x_act.reshape(tok, width), d_out.reshape(tok, width), positions.reshape(1, tok),
            ln_gain.reshape(1, width), ln_bias.reshape(1, width),
            flat_weight(w_query), flat_weight(w_key), flat_weight(w_value), w_out,
        )

        out, gx, gq, gk, gv, gwo, gain, bias = pl.pallas_call(
            functools.partial(settle_kernel, q_w, kv_w),
            out_shape=(
                jax.ShapeDtypeStruct((tok, width), BF),
                jax.ShapeDtypeStruct((tok, width), BF),
                jax.ShapeDtypeStruct((q_w, tok), F32),
                jax.ShapeDtypeStruct((kv_w, tok), F32),
                jax.ShapeDtypeStruct((kv_w, tok), F32),
                jax.ShapeDtypeStruct((hw, width), F32),
                jax.ShapeDtypeStruct((width,), F32),
                jax.ShapeDtypeStruct((width,), F32),
            ),
            in_specs=[hbm] * 5,
            out_specs=(hbm,) * 6 + (vmem,) * 2,
            scratch_shapes=[
                pltpu.VMEM((2, tok, width), BF),
                pltpu.VMEM((2, q_w // 2, tok), F32),
                pltpu.VMEM((2, kv_w, tok), F32),
                pltpu.VMEM((2, hw // 2, width), F32),
                pltpu.VMEM((2, 1, width), F32),
                dma((8,)), dma((8,)), dma,
            ],
            name='settle',
        )(out, gx, gw, gwo, gg)

        def rows_out(block, heads):
            return jnp.transpose(block.reshape(heads, hd, tok), (2, 0, 1))

        return (
            out.reshape(1, tok, width), gx.reshape(1, tok, width),
            rows_out(gq, q_heads), rows_out(gk, kv_heads), rows_out(gv, kv_heads),
            gwo, gain, bias,
        )

    return jax.shard_map(device_step, mesh=mesh, in_specs=(P('dp', 'cp', None), P('dp', 'cp', None), P('dp', 'cp'), P(None), P(None), P(None, None, None), P(None, None, None), P(None, None, None), P(None, None)), out_specs=(P('dp', 'cp', None), P('dp', 'cp', None), P(('dp', 'cp'), None, None), P(('dp', 'cp'), None, None), P(('dp', 'cp'), None, None), P(('dp', 'cp'), None), P('dp'), P('dp')), check_vma=False)
```

```python
import functools
import math

import jax
import jax.numpy as jnp
from jax import lax
from jax.experimental import pallas as pl
from jax.experimental.pallas import tpu as pltpu
from jax.sharding import PartitionSpec as P

EPS = 1e-5
ROPE_BASE = 10000.0
MESH = pl.DeviceIdType.MESH
BF = jnp.bfloat16
F32 = jnp.float32
NEAR = 1
PARTS = 4
FIRST = 1
HELD = 4


def dot(lhs, rhs):
    return jnp.dot(lhs, rhs, preferred_element_type=F32)


def dot_t(lhs, rhs):
    return lax.dot_general(lhs, rhs, (((1,), (1,)), ((), ())), preferred_element_type=F32)


def block_kernel(
    n_dev, hd, kv_w, near, parts,
    x_hbm, dy_hbm, pos_hbm, gain_hbm, bias_hbm, wq_hbm, wk_hbm, wv_hbm, wo_hbm,
    out_hbm, gx_hbm, gw_hbm, gwo_hbm, gg_hbm,
    hb, dyb, wt, wi, woi, w_far, pos_all, trig,
    qt, kvt, kv, kvt_far, kv_far, bmat_far, stat_far, bmat, sbuf, dpbuf, mbuf, adq, dkvt, kv_rv, kv_mine, kv_row,
    dwo, dwt, at_all, dq_all, at_rv, dt_rv, a_nat, d_nat, x_v, dy_own, gb_v, stat, out_v, gg_st, gg_mx, gg_my, gg_rv, gg_out,
    in_sem, far_sem, wo_sem, w_sem, out_sem, loc_sem,
    hzs, hzr, hds, hdr, yzs, yzr, yds, ydr,
    pos_s, pos_r, a_s, a_r, q_s, q_r, x_s, x_r, kv_s, kv_r, w_s, w_r, wk_s, wk_r, g_s, g_r,
):
    tok, width = x_v.shape
    n_chip = n_dev // 2
    pair = 2 * tok
    me = lax.axis_index('cp')
    chip = me // 2
    core = me % 2
    right = 2 * ((chip + 1) % n_chip) + core
    left = 2 * ((chip + n_chip - 1) % n_chip) + core
    mate = 2 * chip + 1 - core
    q_rows = wq_hbm.shape[0]
    n_rows = q_rows + 2 * kv_w
    hw = 2 * hd
    quarter = hd // 4
    tile = 256
    scale = hd ** -0.5
    cols_q = 2 * pair
    n_far = n_chip - 1 - 2 * near

    def remote(src, dst, send, recv, target):
        return pltpu.make_async_remote_copy(src_ref=src, dst_ref=dst, send_sem=send, recv_sem=recv, device_id={'cp': target}, device_id_type=MESH)

    def local(src, dst, sem):
        return pltpu.make_async_copy(src, dst, sem)

    def part_of(i, size):
        return pl.ds(pl.multiple_of(i * size, size), size)

    def ring_steps(k):
        step = (k + 1) // 2
        return step, k % 2

    def ring_origin(k):
        step, ahead = ring_steps(k)
        return jnp.where(ahead == 1, chip + n_chip - step, chip + step) % n_chip

    own = (chip, part_of(core, tok))
    first_loads = [
        local(x_hbm, x_v, in_sem.at[0]),
        local(gain_hbm, gb_v.at[0], in_sem.at[1]),
        local(bias_hbm, gb_v.at[1], in_sem.at[2]),
        local(pos_hbm, pos_all.at[me], in_sem.at[3]),
    ]
    for item in first_loads:
        item.start()
    barrier = pltpu.get_barrier_semaphore()
    for step in range(1, n_dev):
        pl.semaphore_signal(barrier, inc=1, device_id={'cp': (me + step) % n_dev}, device_id_type=MESH)
    own_rows = part_of(me, hw)
    kv_rows = part_of(chip, hd)
    loads = [
        local(wq_hbm.at[own_rows], wi.at[pl.ds(0, hw)], in_sem.at[4]),
        local(wk_hbm.at[kv_rows], wi.at[pl.ds(hw, hd)], in_sem.at[5]),
        local(wv_hbm.at[kv_rows], wi.at[pl.ds(hw + hd, hd)], in_sem.at[6]),
        local(wo_hbm.at[own_rows], woi, in_sem.at[7]),
        local(dy_hbm, dyb.at[own], in_sem.at[8]),
        local(dy_hbm, dy_own, in_sem.at[9]),
    ]
    far_loads = []
    for f in range(n_far):
        far_rows = part_of(ring_origin(2 * near + 1 + f), hd)
        loads.append(local(wk_hbm.at[far_rows], w_far.at[pl.ds(hw * f, hd)], far_sem.at[2 * f]))
        loads.append(local(wv_hbm.at[far_rows], w_far.at[pl.ds(hw * f + hd, hd)], far_sem.at[2 * f + 1]))
        far_wo = part_of(ring_origin(2 * near + 1 + f), 2 * hw)
        far_loads.append(local(wo_hbm.at[far_wo], wt.at[pl.ds(2 * hw * f, 2 * hw)], far_sem.at[2 * n_far + f]))
        far_loads.append(local(wq_hbm.at[far_wo], wt.at[pl.ds(2 * hw * (n_far + f), 2 * hw)], far_sem.at[3 * n_far + f]))
    for item in loads + far_loads:
        item.start()

    for item in first_loads:
        item.wait()
    gain_one = 1.0 + gb_v[0]
    block = 16

    @pl.loop(0, tok // block)
    def _(i):
        rows = part_of(i, block)
        x_f = x_v[rows, :].astype(F32)
        mean = jnp.mean(x_f, axis=-1, keepdims=True)
        centered = x_f - mean
        inv_std = lax.rsqrt(jnp.mean(centered * centered, axis=-1, keepdims=True) + EPS)
        hb[chip, part_of(core * (tok // block) + i, block), :] = (centered * inv_std * gain_one + gb_v[1]).astype(BF)
        stat[0, rows, :] = jnp.broadcast_to(mean, (block, 128))
        stat[1, rows, :] = jnp.broadcast_to(inv_std, (block, 128))

    pl.semaphore_wait(barrier, n_dev - 1)

    def chunk(buf, origin, parity, part):
        return buf.at[origin, part_of(parts * parity + part, tok // parts)]

    turns = 2 * parts

    def own_sends(buf, zs, zr, ds, dr):
        copies = []
        for part in range(parts):
            piece = chunk(buf, chip, core, part)
            copies.append(remote(piece, piece, zs.at[2 * part], zr.at[2 * part], right))
            copies.append(remote(piece, piece, zs.at[2 * part + 1], zr.at[2 * part + 1], left))
            copies.append(remote(piece, piece, ds.at[7 * parts + part], dr.at[7 * parts + part], mate))
        return copies

    def event_place(event):
        step = event // turns + 1
        turn = event % turns
        direction = turn % 2
        part = jnp.where(step < 4, turn // 2, turn // 2 + direction * (parts // 2))
        origin = jnp.where(direction == 0, chip + n_chip - step, chip + step) % n_chip
        return step, direction, part, origin

    def last_event(part, direction):
        return 6 * parts + 2 * (part - direction * (parts // 2)) + direction

    def ring_event(ring, event):
        buf, zs, zr, ds, dr = ring
        step, direction, part, origin = event_place(event)
        piece = chunk(buf, origin, core, part)
        remote(piece, piece, zs.at[0], zr.at[event], right).wait_recv()
        onward = jnp.where(step < 3, event + turns, last_event(part, direction))

        @pl.when((step < 3) | ((step == 3) & ((part >= parts // 2) == (direction == 1))))
        def _():
            remote(piece, piece, zs.at[event + turns], zr.at[onward], jnp.where(direction == 0, right, left)).start()

        remote(piece, piece, ds.at[event], dr.at[event], mate).start()

    def ring_service(ring, event):
        @pl.when(event < 7 * parts)
        def _():
            ring_event(ring, event)

    def ring_mate(ring, k, origin):
        buf, zs, zr, ds, dr = ring
        step, ahead = ring_steps(k)
        for part in range(parts):
            event = jnp.where(k == 0, 7 * parts + part, jnp.where(step < 4, turns * (step - 1) + 2 * part + 1 - ahead, last_event(part, part // (parts // 2))))
            piece = chunk(buf, origin, 1 - core, part)
            remote(piece, piece, ds.at[0], dr.at[event], mate).wait_recv()

    def finish_ring(ring):
        buf, zs, zr, ds, dr = ring
        for item in own_sends(*ring):
            item.wait_send()

        @pl.loop(0, 7 * parts)
        def _(event):
            step, direction, part, origin = event_place(event)
            piece = chunk(buf, origin, core, part)

            @pl.when((step < 3) | ((step == 3) & ((part >= parts // 2) == (direction == 1))))
            def _():
                remote(piece, piece, zs.at[event + turns], zr.at[event], right).wait_send()

            remote(piece, piece, ds.at[event], dr.at[event], mate).wait_send()

    h_ring = (hb, hzs, hzr, hds, hdr)
    y_ring = (dyb, yzs, yzr, yds, ydr)
    for item in own_sends(*h_ring):
        item.start()
    pos_sends = [remote(pos_all.at[me], pos_all.at[me], pos_s.at[step], pos_r.at[me], (me + step) % n_dev) for step in range(1, n_dev)]
    for item in pos_sends:
        item.start()
    weight_loads = [
        local(wq_hbm, wt.at[pl.ds(0, q_rows)], w_sem.at[0]),
        local(wk_hbm, wt.at[pl.ds(q_rows, kv_w)], w_sem.at[1]),
        local(wv_hbm, wt.at[pl.ds(q_rows + kv_w, kv_w)], w_sem.at[2]),
    ]
    dkvt[...] = jnp.zeros_like(dkvt)
    bmat[...] = jnp.zeros_like(bmat)
    bmat_far[...] = jnp.zeros_like(bmat_far)

    freq = jnp.exp(lax.broadcasted_iota(jnp.int32, (quarter, tok), 0).astype(F32) * (-2.0 * math.log(ROPE_BASE) / (hd // 2)))

    def make_trig(b):
        for t in range(2):
            slot = 2 * b + t

            @pl.when(slot != me)
            def _():
                remote(pos_all.at[slot], pos_all.at[slot], pos_s.at[0], pos_r.at[slot], me).wait_recv()

            angle = pos_all[slot].astype(F32) * freq
            trig[b, 0:quarter, tok * t:tok * t + tok] = jnp.cos(angle)
            trig[b, quarter:2 * quarter, tok * t:tok * t + tok] = jnp.sin(angle)

    def turned(val, cos_t, sin_t):
        u = val[0:quarter]
        w = val[quarter:2 * quarter]
        return [u * cos_t - w * sin_t, w * cos_t + u * sin_t, val[2 * quarter:hd]]

    def eighth(val):
        return val.astype(BF) * jnp.asarray(scale, BF)

    def keys_values(val, cos_t, sin_t):
        return jnp.concatenate(turned(val[0:hd], cos_t, sin_t) + [val[hd:hw]], axis=0).astype(BF)

    lane = lax.broadcasted_iota(jnp.int32, (pair, cols_q), 1)
    row = lax.broadcasted_iota(jnp.int32, (pair, cols_q), 0)
    seen_far = row <= core * tok + lane % tok

    @pl.loop(0, n_chip)
    def _(k):
        for turn in range(parts):
            ring_service(h_ring, parts * k + turn)

        @pl.when(k == 5)
        def _():
            for item in own_sends(*y_ring):
                item.start()

        @pl.when(k == 0)
        def _():
            for item in loads:
                item.wait()

        b = ring_origin(k)
        ring_mate(h_ring, k, b)
        make_trig(b)

        @pl.when(k == 0)
        def _():
            for item in far_loads:
                item.wait()
            cos_t = trig[chip, 0:quarter, part_of(core, tok)]
            sin_t = trig[chip, quarter:2 * quarter, part_of(core, tok)]

            @pl.loop(0, n_far)
            def _(f):
                da_t = dot_t(wt[part_of(f, 2 * hw), :], dy_own[...]).astype(BF)
                q_t = dot_t(wt[part_of(n_far + f, 2 * hw), :], hb[chip, part_of(core, tok), :])
                for head in range(4):
                    part = slice(hd * head, hd * head + hd)
                    at = tok * head
                    bmat_far[f, 0:hd, at:at + tok] = eighth(jnp.concatenate(turned(q_t[part], cos_t, sin_t), axis=0))
                    bmat_far[f, hd:hw, cols_q + at:cols_q + at + tok] = da_t[part]

            for item in weight_loads:
                item.start()

        place = part_of(b, pair)
        cos_t = trig[b, 0:quarter, :]
        sin_t = trig[b, quarter:2 * quarter, :]
        flat = dot_t(wi[...], hb[b])
        for head in range(2):
            q_rot = eighth(jnp.concatenate(turned(flat[hd * head:hd * head + hd], cos_t, sin_t), axis=0))
            for t in range(2):
                lane = pair * t + tok * head
                qt[b, :, lane:lane + tok] = q_rot[:, tok * t:tok * t + tok]
        kv_rot = keys_values(flat[hw:2 * hw], cos_t, sin_t)
        kvt[:, place] = kv_rot
        kv[place, :] = kv_rot.T

        @pl.when(b <= chip)
        def _():
            flat_far = dot_t(w_far[...], hb[b])
            for f in range(n_far):
                far_rot = keys_values(flat_far[hw * f:hw * f + hw], cos_t, sin_t)
                kvt_far[f, :, place] = far_rot
                kv_far[f, place, :] = far_rot.T

            @pl.loop(0, n_far)
            def _(f):
                both = dot(kv_far[f, place, :], bmat_far[f])
                d_p = both[:, cols_q:2 * cols_q]

                @pl.when(k == 0)
                def _():
                    s = jnp.where(seen_far, both[:, 0:cols_q], -1e30)
                    top = jnp.max(s, axis=0, keepdims=True)
                    p = jnp.exp(s - top)
                    stat_far[f, 0] = top
                    stat_far[f, 1] = jnp.sum(p, axis=0, keepdims=True)
                    stat_far[f, 2] = jnp.sum(p * d_p, axis=0, keepdims=True)

                @pl.when(k > 0)
                def _():
                    s = both[:, 0:cols_q]
                    old = stat_far[f, 0]
                    new = jnp.maximum(old, jnp.max(s, axis=0, keepdims=True))
                    p = jnp.exp(s - new)
                    keep = jnp.exp(old - new)
                    stat_far[f, 0] = new
                    stat_far[f, 1] = stat_far[f, 1] * keep + jnp.sum(p, axis=0, keepdims=True)
                    stat_far[f, 2] = stat_far[f, 2] * keep + jnp.sum(p * d_p, axis=0, keepdims=True)

    groups = [slice(tile * g, tile * g + tile) for g in range(cols_q // tile)]

    def first_part(b, seen):
        def both_of(rows):
            both = dot(kv[rows, :], bmat[...])
            return both[:, 0:cols_q], both[:, cols_q:2 * cols_q]

        rows = part_of(b, pair)
        s, d_p = both_of(rows)
        s = jnp.where(seen, s, -1e30)
        top = jnp.max(s, axis=0, keepdims=True)
        p = jnp.exp(s - top)
        sbuf[rows, :] = p
        dpbuf[rows, :] = d_p
        mbuf[b] = top

        def step(c, state, chunks=1):
            old, total, weighted = state
            rows = part_of(c, chunks * pair)
            s, d_p = both_of(rows)
            new = jnp.maximum(old, jnp.max(s, axis=0, keepdims=True))
            p = jnp.exp(s - new)
            sbuf[rows, :] = p
            dpbuf[rows, :] = d_p
            for i in range(chunks):
                mbuf[chunks * c + i] = new
            keep = jnp.exp(old - new)
            return new, total * keep + jnp.sum(p, axis=0, keepdims=True), weighted * keep + jnp.sum(p * d_p, axis=0, keepdims=True)

        state = (top, jnp.sum(p, axis=0, keepdims=True), jnp.sum(p * d_p, axis=0, keepdims=True))
        state = lax.fori_loop(0, b // 2, functools.partial(step, chunks=2), state)
        top, total, weighted = lax.fori_loop(2 * (b // 2), b, step, state)
        inv = 1.0 / total
        return top, inv, weighted * inv

    def second_part(b, stats):
        top, inv, row_dot = stats
        adq[...] = jnp.zeros_like(adq)

        def step(c, carry):
            rows = part_of(c, pair)
            factor = jnp.exp(mbuf[c] - top) * inv
            d_k = d_v = None
            for at in groups:
                p = sbuf[rows, at] * factor[:, at]
                p_b = p.astype(BF)
                ds_b = (p * (dpbuf[rows, at] - row_dot[:, at])).astype(BF)
                adq[0:hd, at] += dot(kvt[0:hd, rows], ds_b)
                adq[hd:hw, at] += dot(kvt[hd:hw, rows], p_b)
                more_k = dot_t(bmat[0:hd, at], ds_b)
                more_v = dot_t(bmat[hd:hw, cols_q + at.start:cols_q + at.stop], p_b)
                d_k = more_k if d_k is None else d_k + more_k
                d_v = more_v if d_v is None else d_v + more_v
            dkvt[0:hd, rows] += d_k
            dkvt[hd:hw, rows] += d_v
            return carry

        lax.fori_loop(0, b + 1, step, 0)


    def send_rows(slot):
        cols = part_of(slot, tok)
        return [
            remote(dq_all.at[:, cols], dt_rv.at[own_rows], q_s.at[slot], q_r.at[me], slot),
            remote(at_all.at[:, cols], at_rv.at[own_rows], a_s.at[slot], a_r.at[me], slot),
        ]

    @pl.loop(0, n_chip)
    def _(k):
        for turn in range(parts - 1):
            ring_service(y_ring, parts * k + turn)
        b = ring_origin(k)
        ring_mate(y_ring, k, b)

        @pl.when(k == 1)
        def _():
            for item in weight_loads:
                item.wait()

        @pl.when(k == n_chip - 1)
        def _():
            for early in range(1 + 2 * near):
                for t in range(2):
                    slot = 2 * ring_origin(early) + t

                    @pl.when(slot != me)
                    def _():
                        for item in send_rows(slot):
                            item.start()

        da_t = dot_t(woi[...], dyb[b]).astype(BF)
        bmat[0:hd, 0:cols_q] = qt[b]
        for t in range(2):
            for head in range(2):
                at = cols_q + pair * t + tok * head
                bmat[hd:hw, at:at + tok] = da_t[hd * head:hd * head + hd, tok * t:tok * t + tok]
        stats = first_part(b, row <= (lane // pair) * tok + lane % tok)
        ring_service(y_ring, parts * k + parts - 1)
        second_part(b, stats)
        for t in range(2):
            slot = 2 * b + t
            lanes = [slice(pair * t + tok * head, pair * t + tok * head + tok) for head in range(2)]
            a_t = jnp.concatenate([adq[hd:hw, at] for at in lanes], axis=0).astype(BF)
            cos_t = trig[b, 0:quarter, tok * t:tok * t + tok]
            sin_t = trig[b, quarter:2 * quarter, tok * t:tok * t + tok]
            dq_t = jnp.concatenate([piece for at in lanes for piece in turned(adq[0:hd, at] * scale, cos_t, -sin_t)], axis=0).astype(BF)
            at_all[:, part_of(slot, tok)] = a_t
            dq_all[:, part_of(slot, tok)] = dq_t

            @pl.when(slot == me)
            def _():
                at_rv[own_rows, :] = a_t
                dt_rv[own_rows, :] = dq_t

    far = [ring_origin(k) for k in range(n_chip - 1, 0, -1)]
    targets = [2 * c + p for c in far for p in range(2)] + [mate]
    near_targets = targets[-1 - 4 * near:]
    swap = remote(dkvt.at[part_of(1 - core, hd)], kv_rv, x_s, x_r, mate)
    swap.start()
    w_sends = [remote(dwt.at[pl.ds(0, hw), part_of(t, tok)], gw_hbm.at[own_rows], w_s.at[t], w_r.at[me], t) for t in targets]

    def columns(rows_all, buf, cols):
        acc = jnp.zeros((rows_all.shape[0], tile), F32)
        for s in range(n_chip):
            acc += dot(rows_all[:, pair * s:pair * s + pair], buf[s, :, cols])
        return acc

    def q_columns(i):
        cols = part_of(far[i] if i < n_chip - 1 else chip, pair)
        dwt[0:hw, cols] = columns(dq_all, hb, cols)
        for item in w_sends[max(2 * i - 2, 0):2 * i]:
            item.start()

    for i in range(FIRST + 1):
        q_columns(i)

    swap.wait_recv()
    mine = part_of(core, hd)
    g_rows = pl.ds(pl.multiple_of(q_rows + core * kv_w + chip * hd, hd), hd)
    for t in range(n_chip):
        cols = slice(pair * t, pair * t + pair)
        g = dkvt[mine, cols] + kv_rv[:, cols]
        cos_t = jnp.where(core == 0, trig[t, 0:quarter, :], 1.0)
        sin_t = jnp.where(core == 0, trig[t, quarter:2 * quarter, :], 0.0)
        g_b = jnp.concatenate(turned(g, cos_t, -sin_t), axis=0).astype(BF)
        kv_mine[2 * t] = g_b[:, 0:tok]
        kv_mine[2 * t + 1] = g_b[:, tok:pair]
        kv_row[:, cols] = g_b
    dt_rv[g_rows, :] = kv_mine[me]
    kv_sends = [remote(kv_mine.at[t], dt_rv.at[g_rows], kv_s.at[t], kv_r.at[me], t) for t in targets]
    for item in kv_sends:
        item.start()
    for i in range(FIRST + 1, n_chip):
        q_columns(i)
    w_sends[-1].start()
    w_own = local(dwt.at[pl.ds(0, hw), part_of(me, tok)], gw_hbm.at[own_rows], loc_sem.at[0])
    w_own.start()
    for t in range(width // tile):
        cols = slice(tile * t, tile * t + tile)
        dwt[hw:hw + hd, cols] = columns(kv_row, hb, cols)
    wk_own = local(dwt.at[pl.ds(hw, hd), part_of(me, tok)], gw_hbm.at[g_rows], loc_sem.at[1])
    wk_own.start()
    wk_sends = [remote(dwt.at[pl.ds(hw, hd), part_of(t, tok)], gw_hbm.at[g_rows], wk_s.at[t], wk_r.at[me], t) for t in targets]
    for item in wk_sends[0:HELD]:
        item.start()

    for t in range(width // tile):
        cols = slice(tile * t, tile * t + tile)
        dwo[:, cols] = columns(at_all, dyb, cols)
    store_wo = local(dwo, gwo_hbm, out_sem.at[0])
    store_wo.start()
    finish_ring(y_ring)
    wo_loads = [local(wo_hbm.at[pl.ds(pair * t, pair)], dyb.at[t], wo_sem.at[t]) for t in range(n_chip)]
    for item in wo_loads:
        item.start()

    @pl.loop(0, n_far)
    def _(f):
        c_far = ring_origin(2 * near + 1 + f)
        cos_t = trig[chip, 0:quarter, part_of(core, tok)]
        sin_t = trig[chip, quarter:2 * quarter, part_of(core, tok)]
        top = stat_far[f, 0]
        inv = 1.0 / stat_far[f, 1]
        row_dot = stat_far[f, 2] * inv

        def add_chunk(c, diagonal, chunks=1):
            rows = part_of(c, chunks * pair)
            for at in groups:
                keys = kv_far[f, rows, :]
                s = dot(keys, bmat_far[f, :, at])
                d_p = dot(keys, bmat_far[f, :, cols_q + at.start:cols_q + at.stop])
                if diagonal:
                    s = jnp.where(seen_far[:, at], s, -1e30)
                p = jnp.exp(s - top[:, at]) * inv[:, at]
                p_b = p.astype(BF)
                ds_b = (p * (d_p - row_dot[:, at])).astype(BF)
                d_q = dot(kvt_far[f, 0:hd, rows], ds_b)
                d_a = dot(kvt_far[f, hd:hw, rows], p_b)
                adq[0:hd, at] = d_q if diagonal else adq[0:hd, at] + d_q
                adq[hd:hw, at] = d_a if diagonal else adq[hd:hw, at] + d_a

        add_chunk(chip, True)

        @pl.loop(0, chip // 2)
        def _(c):
            add_chunk(c, False, 2)

        @pl.when(chip % 2 == 1)
        def _():
            add_chunk(chip - 1, False)

        for head in range(4):
            at = slice(tok * head, tok * head + tok)
            place = pl.ds(pl.multiple_of(c_far * 2 * hw + hd * head, hd), hd)
            at_rv[place, :] = adq[hd:hw, at].astype(BF)
            dt_rv[place, :] = jnp.concatenate(turned(adq[0:hd, at] * scale, cos_t, -sin_t), axis=0).astype(BF)

    for t in near_targets:
        remote(at_all.at[:, pl.ds(0, tok)], at_rv.at[part_of(t, hw)], a_s.at[t], a_r.at[t], t).wait_recv()
    for item in wo_loads:
        item.wait()
    for t in range(q_rows // tok):
        a_nat[:, tok * t:tok * t + tok] = at_rv[tok * t:tok * t + tok, :].T
    for t in range(width // tile):
        cols = slice(tile * t, tile * t + tile)
        prod = jnp.zeros((tok, tile), F32)
        for s in range(n_chip):
            prod += dot(a_nat[:, pair * s:pair * s + pair], dyb[s, :, cols])
        out_v[:, cols] = (x_v[:, cols].astype(F32) + prod).astype(BF)
    store_out = local(out_v, out_hbm, out_sem.at[1])
    store_out.start()

    def kv_place(t):
        return pl.ds(pl.multiple_of(q_rows + (t % 2) * kv_w + (t // 2) * hd, hd), hd)

    for t in near_targets:
        remote(dq_all.at[:, pl.ds(0, tok)], dt_rv.at[part_of(t, hw)], q_s.at[t], q_r.at[t], t).wait_recv()
    for t in targets:
        remote(kv_mine.at[0], dt_rv.at[kv_place(t)], kv_s.at[t], kv_r.at[t], t).wait_recv()
    swap.wait_send()
    for t in range(n_rows // tok):
        d_nat[:, tok * t:tok * t + tok] = dt_rv[tok * t:tok * t + tok, :].T

    mean = stat[0, :, 0:1]
    inv_std = stat[1, :, 0:1]
    dh = dkvt
    for t in range(width // tile):
        cols = slice(tile * t, tile * t + tile)
        acc = jnp.zeros((tok, tile), F32)
        for s in range(n_rows // tile):
            acc += dot(d_nat[:, tile * s:tile * s + tile], wt[tile * s:tile * s + tile, cols])
        dh[:, cols] = acc
        gg_st[0, :, cols] = jnp.sum(acc * ((x_v[:, cols].astype(F32) - mean) * inv_std), axis=0, keepdims=True)
        gg_st[1, :, cols] = jnp.sum(acc, axis=0, keepdims=True)
    g_swap = remote(gg_st.at[1 - core], gg_mx, g_s.at[n_chip], g_r.at[n_chip], mate)
    g_swap.start()
    g_swap.wait_recv()
    gg_my[...] = jnp.where(core == 0, gg_st[0], gg_st[1]) + gg_mx[...]
    gg_rv[chip] = gg_my[...]
    g_sends = [remote(gg_my, gg_rv.at[chip], g_s.at[c], g_r.at[chip], 2 * c + core) for c in far]
    for item in g_sends + wk_sends[HELD:]:
        item.start()

    grad_hat = dh[...] * gain_one
    x_hat = (x_v[...].astype(F32) - mean) * inv_std
    mean_one = jnp.mean(grad_hat, axis=-1, keepdims=True)
    mean_two = jnp.mean(grad_hat * x_hat, axis=-1, keepdims=True)
    store_out.wait()
    out_v[...] = (dy_own[...].astype(F32) + inv_std * (grad_hat - mean_one - x_hat * mean_two)).astype(BF)
    store_gx = local(out_v, gx_hbm, out_sem.at[2])
    store_gx.start()

    for c in far:
        remote(gg_my, gg_rv.at[c], g_s.at[c], g_r.at[c], 2 * c + core).wait_recv()
    sums = gg_rv[0]
    for c in range(1, n_chip):
        sums = sums + gg_rv[c]
    gg_out[core] = sums
    g_swap_out = remote(gg_out.at[core], gg_out.at[core], g_s.at[n_chip + 1], g_r.at[n_chip + 1], mate)
    g_swap_out.start()
    remote(gg_out.at[core], gg_out.at[1 - core], g_s.at[n_chip + 1], g_r.at[n_chip + 1], mate).wait_recv()
    store_gg = local(gg_out, gg_hbm, out_sem.at[3])
    store_gg.start()

    finish_ring(h_ring)
    for item in pos_sends + [g_swap, g_swap_out]:
        item.wait_send()
    for t in near_targets:
        remote(at_all.at[:, pl.ds(0, tok)], at_rv.at[pl.ds(0, hw)], a_s.at[t], a_r.at[t], t).wait_send()
        remote(dq_all.at[:, pl.ds(0, tok)], dt_rv.at[pl.ds(0, hw)], q_s.at[t], q_r.at[t], t).wait_send()
    for item in kv_sends + w_sends + g_sends + wk_sends:
        item.wait_send()
    for t in targets:
        remote(dwt.at[pl.ds(0, hw), part_of(t, tok)], gw_hbm.at[part_of(t, hw)], w_s.at[t], w_r.at[t], t).wait_recv()
        remote(dwt.at[pl.ds(hw, hd), part_of(t, tok)], gw_hbm.at[kv_place(t)], wk_s.at[t], wk_r.at[t], t).wait_recv()
    for item in (w_own, wk_own, store_wo, store_gx, store_gg):
        item.wait()


def settle_kernel(q_rows, kv_w, out_i, gx_i, gw_i, gwo_i, gg_i, out_o, gx_o, gq_o, gk_o, gv_o, gwo_o, gain_o, bias_o, b_act, b_q, b_kv, b_o, b_gg, sem_in, sem_out, sem_gg):
    half_q = q_rows // 2
    half_o = gwo_i.shape[0] // 2
    moves = [(out_i, b_act.at[0], out_o), (gx_i, b_act.at[1], gx_o)]
    for t in range(2):
        moves.append((gw_i.at[pl.ds(half_q * t, half_q)], b_q.at[t], gq_o.at[pl.ds(half_q * t, half_q)]))
        moves.append((gwo_i.at[pl.ds(half_o * t, half_o)], b_o.at[t], gwo_o.at[pl.ds(half_o * t, half_o)]))
    moves.append((gw_i.at[pl.ds(q_rows, kv_w)], b_kv.at[0], gk_o))
    moves.append((gw_i.at[pl.ds(q_rows + kv_w, kv_w)], b_kv.at[1], gv_o))
    loads = [pltpu.make_async_copy(src, mid, sem_in.at[i]) for i, (src, mid, _) in enumerate(moves)]
    stores = [pltpu.make_async_copy(mid, dst, sem_out.at[i]) for i, (_, mid, dst) in enumerate(moves)]
    load_gg = pltpu.make_async_copy(gg_i, b_gg, sem_gg)
    load_gg.start()
    for item in loads:
        item.start()
    for load, store in zip(loads, stores):
        load.wait()
        store.start()
    load_gg.wait()
    gain_o[...] = b_gg[0, 0]
    bias_o[...] = b_gg[1, 0]
    for item in stores:
        item.wait()


def solution(mesh):
    n_dev = mesh.shape['cp']

    def device_step(x_act, d_out, positions, ln_gain, ln_bias, w_query, w_key, w_value, w_out):
        tok, width = x_act.shape[1], x_act.shape[2]
        q_heads, hd = w_query.shape[1], w_query.shape[2]
        kv_heads = w_key.shape[1]
        q_w, kv_w = q_heads * hd, kv_heads * hd
        n_rows = q_w + 2 * kv_w
        seq = n_dev * tok
        hw = 2 * hd

        def flat_weight(w):
            return jnp.transpose(w, (1, 2, 0)).reshape(-1, width)

        hbm = pl.BlockSpec(memory_space=pltpu.HBM)
        vmem = pl.BlockSpec(memory_space=pltpu.VMEM)
        dma = pltpu.SemaphoreType.DMA
        n_chip = n_dev // 2
        n_far = n_chip - 1 - 2 * NEAR
        pair = 2 * tok
        scratch = [
            pltpu.VMEM((n_chip, pair, width), BF),
            pltpu.VMEM((n_chip, pair, width), BF),
            pltpu.VMEM((n_rows, width), BF),
            pltpu.VMEM((2 * hw, width), BF),
            pltpu.VMEM((hw, width), BF),
            pltpu.VMEM((n_far * hw, width), BF),
            pltpu.VMEM((n_dev, 1, tok), jnp.int32),
            pltpu.VMEM((n_chip, hd // 2, pair), F32),
            pltpu.VMEM((n_chip, hd, 2 * pair), BF),
            pltpu.VMEM((hw, seq), BF),
            pltpu.VMEM((seq, hw), BF),
            pltpu.VMEM((n_far, hw, seq), BF),
            pltpu.VMEM((n_far, seq, hw), BF),
            pltpu.VMEM((n_far, hw, 4 * pair), BF),
            pltpu.VMEM((n_far, 3, 1, 2 * pair), F32),
            pltpu.VMEM((hw, 4 * pair), BF),
            pltpu.VMEM((seq, 2 * pair), F32),
            pltpu.VMEM((seq, 2 * pair), F32),
            pltpu.VMEM((n_chip, 1, 2 * pair), F32),
            pltpu.VMEM((hw, 2 * pair), F32),
            pltpu.VMEM((hw, seq), F32),
            pltpu.VMEM((hd, seq), F32),
            pltpu.VMEM((n_dev, hd, tok), BF),
            pltpu.VMEM((hd, seq), BF),
            pltpu.VMEM((hw, width), F32),
            pltpu.VMEM((hw + hd, width), F32),
            pltpu.VMEM((hw, seq), BF),
            pltpu.VMEM((hw, seq), BF),
            pltpu.VMEM((q_w, tok), BF),
            pltpu.VMEM((n_rows, tok), BF),
            pltpu.VMEM((tok, q_w), BF),
            pltpu.VMEM((tok, n_rows), BF),
            pltpu.VMEM((tok, width), BF),
            pltpu.VMEM((tok, width), BF),
            pltpu.VMEM((2, 1, width), F32),
            pltpu.VMEM((2, tok, 128), F32),
            pltpu.VMEM((tok, width), BF),
            pltpu.VMEM((2, 1, width), F32),
            pltpu.VMEM((1, width), F32),
            pltpu.VMEM((1, width), F32),
            pltpu.VMEM((n_chip, 1, width), F32),
            pltpu.VMEM((2, 1, width), F32),
            dma((10,)), dma((4 * n_far,)), dma((n_chip,)), dma((3,)), dma((4,)), dma((2,)),
        ] + [dma((9 * PARTS,)), dma((7 * PARTS,)), dma((8 * PARTS,)), dma((8 * PARTS,))] * 2 + [dma((n_dev,))] * 6 + [dma] * 2 + [dma((n_dev,))] * 8
        out, gx, gw, gwo, gg = pl.pallas_call(
            functools.partial(block_kernel, n_dev, hd, kv_w, NEAR, PARTS),
            out_shape=(
                jax.ShapeDtypeStruct((tok, width), BF),
                jax.ShapeDtypeStruct((tok, width), BF),
                jax.ShapeDtypeStruct((n_rows, tok), F32),
                jax.ShapeDtypeStruct((hw, width), F32),
                jax.ShapeDtypeStruct((2, 1, width), F32),
            ),
            in_specs=[hbm] * 9,
            out_specs=(hbm,) * 5,
            scratch_shapes=scratch,
            compiler_params=pltpu.CompilerParams(collective_id=0, has_side_effects=True, vmem_limit_bytes=67043328),
            name='attn_block',
        )(
            x_act.reshape(tok, width), d_out.reshape(tok, width), positions.reshape(1, tok),
            ln_gain.reshape(1, width), ln_bias.reshape(1, width),
            flat_weight(w_query), flat_weight(w_key), flat_weight(w_value), w_out,
        )

        out, gx, gq, gk, gv, gwo, gain, bias = pl.pallas_call(
            functools.partial(settle_kernel, q_w, kv_w),
            out_shape=(
                jax.ShapeDtypeStruct((tok, width), BF),
                jax.ShapeDtypeStruct((tok, width), BF),
                jax.ShapeDtypeStruct((q_w, tok), F32),
                jax.ShapeDtypeStruct((kv_w, tok), F32),
                jax.ShapeDtypeStruct((kv_w, tok), F32),
                jax.ShapeDtypeStruct((hw, width), F32),
                jax.ShapeDtypeStruct((width,), F32),
                jax.ShapeDtypeStruct((width,), F32),
            ),
            in_specs=[hbm] * 5,
            out_specs=(hbm,) * 6 + (vmem,) * 2,
            scratch_shapes=[
                pltpu.VMEM((2, tok, width), BF),
                pltpu.VMEM((2, q_w // 2, tok), F32),
                pltpu.VMEM((2, kv_w, tok), F32),
                pltpu.VMEM((2, hw // 2, width), F32),
                pltpu.VMEM((2, 1, width), F32),
                dma((8,)), dma((8,)), dma,
            ],
            name='settle',
        )(out, gx, gw, gwo, gg)

        def rows_out(block, heads):
            return jnp.transpose(block.reshape(heads, hd, tok), (2, 0, 1))

        return (
            out.reshape(1, tok, width), gx.reshape(1, tok, width),
            rows_out(gq, q_heads), rows_out(gk, kv_heads), rows_out(gv, kv_heads),
            gwo, gain, bias,
        )

    return jax.shard_map(device_step, mesh=mesh, in_specs=(P('dp', 'cp', None), P('dp', 'cp', None), P('dp', 'cp'), P(None), P(None), P(None, None, None), P(None, None, None), P(None, None, None), P(None, None)), out_specs=(P('dp', 'cp', None), P('dp', 'cp', None), P(('dp', 'cp'), None, None), P(('dp', 'cp'), None, None), P(('dp', 'cp'), None, None), P(('dp', 'cp'), None), P('dp'), P('dp')), check_vma=False)
```

```python
import functools
import math

import jax
import jax.numpy as jnp
from jax import lax
from jax.experimental import pallas as pl
from jax.experimental.pallas import tpu as pltpu
from jax.sharding import PartitionSpec as P

EPS = 1e-5
ROPE_BASE = 10000.0
MESH = pl.DeviceIdType.MESH
BF = jnp.bfloat16
F32 = jnp.float32
NEAR = 1
PARTS = 4
FIRST = 1
HELD = 4


def dot(lhs, rhs):
    return jnp.dot(lhs, rhs, preferred_element_type=F32)


def dot_t(lhs, rhs):
    return lax.dot_general(lhs, rhs, (((1,), (1,)), ((), ())), preferred_element_type=F32)


def block_kernel(
    n_dev, hd, kv_w, near, parts,
    x_hbm, dy_hbm, pos_hbm, gain_hbm, bias_hbm, wq_hbm, wk_hbm, wv_hbm, wo_hbm,
    out_hbm, gx_hbm, gw_hbm, gwo_hbm, gg_hbm,
    hb, dyb, wt, wi, woi, w_far, pos_all, trig,
    qt, kvt, kv, kvt_far, kv_far, bmat_far, stat_far, bmat, sbuf, dpbuf, mbuf, adq, dkvt, kv_rv, kv_mine, kv_row,
    dwo, dwt, at_all, dq_all, at_rv, dt_rv, a_nat, d_nat, x_v, dy_own, gb_v, stat, out_v, gg_st, gg_mx, gg_my, gg_rv, gg_out,
    in_sem, far_sem, wo_sem, w_sem, out_sem, loc_sem,
    hzs, hzr, hds, hdr, yzs, yzr, yds, ydr,
    pos_s, pos_r, a_s, a_r, q_s, q_r, x_s, x_r, kv_s, kv_r, w_s, w_r, wk_s, wk_r, g_s, g_r,
):
    tok, width = x_v.shape
    n_chip = n_dev // 2
    pair = 2 * tok
    me = lax.axis_index('cp')
    chip = me // 2
    core = me % 2
    right = 2 * ((chip + 1) % n_chip) + core
    left = 2 * ((chip + n_chip - 1) % n_chip) + core
    mate = 2 * chip + 1 - core
    q_rows = wq_hbm.shape[0]
    n_rows = q_rows + 2 * kv_w
    hw = 2 * hd
    quarter = hd // 4
    tile = 256
    scale = hd ** -0.5
    cols_q = 2 * pair
    n_far = n_chip - 1 - 2 * near

    def remote(src, dst, send, recv, target):
        return pltpu.make_async_remote_copy(src_ref=src, dst_ref=dst, send_sem=send, recv_sem=recv, device_id={'cp': target}, device_id_type=MESH)

    def local(src, dst, sem):
        return pltpu.make_async_copy(src, dst, sem)

    def part_of(i, size):
        return pl.ds(pl.multiple_of(i * size, size), size)

    def ring_steps(k):
        step = (k + 1) // 2
        return step, k % 2

    def ring_origin(k):
        step, ahead = ring_steps(k)
        return jnp.where(ahead == 1, chip + n_chip - step, chip + step) % n_chip

    own = (chip, part_of(core, tok))
    first_loads = [
        local(x_hbm, x_v, in_sem.at[0]),
        local(gain_hbm, gb_v.at[0], in_sem.at[1]),
        local(bias_hbm, gb_v.at[1], in_sem.at[2]),
        local(pos_hbm, pos_all.at[me], in_sem.at[3]),
    ]
    for item in first_loads:
        item.start()
    barrier = pltpu.get_barrier_semaphore()
    for step in range(1, n_dev):
        pl.semaphore_signal(barrier, inc=1, device_id={'cp': (me + step) % n_dev}, device_id_type=MESH)
    own_rows = part_of(me, hw)
    kv_rows = part_of(chip, hd)
    loads = [
        local(wq_hbm.at[own_rows], wi.at[pl.ds(0, hw)], in_sem.at[4]),
        local(wk_hbm.at[kv_rows], wi.at[pl.ds(hw, hd)], in_sem.at[5]),
        local(wv_hbm.at[kv_rows], wi.at[pl.ds(hw + hd, hd)], in_sem.at[6]),
        local(wo_hbm.at[own_rows], woi, in_sem.at[7]),
        local(dy_hbm, dyb.at[own], in_sem.at[8]),
        local(dy_hbm, dy_own, in_sem.at[9]),
    ]
    far_loads = []
    for f in range(n_far):
        far_rows = part_of(ring_origin(2 * near + 1 + f), hd)
        loads.append(local(wk_hbm.at[far_rows], w_far.at[pl.ds(hw * f, hd)], far_sem.at[2 * f]))
        loads.append(local(wv_hbm.at[far_rows], w_far.at[pl.ds(hw * f + hd, hd)], far_sem.at[2 * f + 1]))
        far_wo = part_of(ring_origin(2 * near + 1 + f), 2 * hw)
        far_loads.append(local(wo_hbm.at[far_wo], wt.at[pl.ds(2 * hw * f, 2 * hw)], far_sem.at[2 * n_far + f]))
        far_loads.append(local(wq_hbm.at[far_wo], wt.at[pl.ds(2 * hw * (n_far + f), 2 * hw)], far_sem.at[3 * n_far + f]))
    for item in loads + far_loads:
        item.start()

    for item in first_loads:
        item.wait()
    gain_one = 1.0 + gb_v[0]
    block = 16

    @pl.loop(0, tok // block)
    def _(i):
        rows = part_of(i, block)
        x_f = x_v[rows, :].astype(F32)
        mean = jnp.mean(x_f, axis=-1, keepdims=True)
        centered = x_f - mean
        inv_std = lax.rsqrt(jnp.mean(centered * centered, axis=-1, keepdims=True) + EPS)
        hb[chip, part_of(core * (tok // block) + i, block), :] = (centered * inv_std * gain_one + gb_v[1]).astype(BF)
        stat[0, rows, :] = jnp.broadcast_to(mean, (block, 128))
        stat[1, rows, :] = jnp.broadcast_to(inv_std, (block, 128))

    pl.semaphore_wait(barrier, n_dev - 1)

    def chunk(buf, origin, parity, part):
        return buf.at[origin, part_of(parts * parity + part, tok // parts)]

    turns = 2 * parts

    def own_sends(buf, zs, zr, ds, dr):
        copies = []
        for part in range(parts):
            piece = chunk(buf, chip, core, part)
            copies.append(remote(piece, piece, zs.at[2 * part], zr.at[2 * part], right))
            copies.append(remote(piece, piece, zs.at[2 * part + 1], zr.at[2 * part + 1], left))
            copies.append(remote(piece, piece, ds.at[7 * parts + part], dr.at[7 * parts + part], mate))
        return copies

    def event_place(event):
        step = event // turns + 1
        turn = event % turns
        direction = turn % 2
        part = jnp.where(step < 4, turn // 2, turn // 2 + direction * (parts // 2))
        origin = jnp.where(direction == 0, chip + n_chip - step, chip + step) % n_chip
        return step, direction, part, origin

    def last_event(part, direction):
        return 6 * parts + 2 * (part - direction * (parts // 2)) + direction

    def ring_event(ring, event):
        buf, zs, zr, ds, dr = ring
        step, direction, part, origin = event_place(event)
        piece = chunk(buf, origin, core, part)
        remote(piece, piece, zs.at[0], zr.at[event], right).wait_recv()
        onward = jnp.where(step < 3, event + turns, last_event(part, direction))

        @pl.when((step < 3) | ((step == 3) & ((part >= parts // 2) == (direction == 1))))
        def _():
            remote(piece, piece, zs.at[event + turns], zr.at[onward], jnp.where(direction == 0, right, left)).start()

        remote(piece, piece, ds.at[event], dr.at[event], mate).start()

    def ring_service(ring, event):
        @pl.when(event < 7 * parts)
        def _():
            ring_event(ring, event)

    def ring_mate(ring, k, origin):
        buf, zs, zr, ds, dr = ring
        step, ahead = ring_steps(k)
        for part in range(parts):
            event = jnp.where(k == 0, 7 * parts + part, jnp.where(step < 4, turns * (step - 1) + 2 * part + 1 - ahead, last_event(part, part // (parts // 2))))
            piece = chunk(buf, origin, 1 - core, part)
            remote(piece, piece, ds.at[0], dr.at[event], mate).wait_recv()

    def finish_ring(ring):
        buf, zs, zr, ds, dr = ring
        for item in own_sends(*ring):
            item.wait_send()

        @pl.loop(0, 7 * parts)
        def _(event):
            step, direction, part, origin = event_place(event)
            piece = chunk(buf, origin, core, part)

            @pl.when((step < 3) | ((step == 3) & ((part >= parts // 2) == (direction == 1))))
            def _():
                remote(piece, piece, zs.at[event + turns], zr.at[event], right).wait_send()

            remote(piece, piece, ds.at[event], dr.at[event], mate).wait_send()

    h_ring = (hb, hzs, hzr, hds, hdr)
    y_ring = (dyb, yzs, yzr, yds, ydr)
    for item in own_sends(*h_ring):
        item.start()
    pos_sends = [remote(pos_all.at[me], pos_all.at[me], pos_s.at[step], pos_r.at[me], (me + step) % n_dev) for step in range(1, n_dev)]
    for item in pos_sends:
        item.start()
    weight_loads = [
        local(wq_hbm, wt.at[pl.ds(0, q_rows)], w_sem.at[0]),
        local(wk_hbm, wt.at[pl.ds(q_rows, kv_w)], w_sem.at[1]),
        local(wv_hbm, wt.at[pl.ds(q_rows + kv_w, kv_w)], w_sem.at[2]),
    ]
    dkvt[...] = jnp.zeros_like(dkvt)
    bmat[...] = jnp.zeros_like(bmat)
    bmat_far[...] = jnp.zeros_like(bmat_far)

    freq = jnp.exp(lax.broadcasted_iota(jnp.int32, (quarter, tok), 0).astype(F32) * (-2.0 * math.log(ROPE_BASE) / (hd // 2)))

    def make_trig(b):
        for t in range(2):
            slot = 2 * b + t

            @pl.when(slot != me)
            def _():
                remote(pos_all.at[slot], pos_all.at[slot], pos_s.at[0], pos_r.at[slot], me).wait_recv()

            angle = pos_all[slot].astype(F32) * freq
            trig[b, 0:quarter, tok * t:tok * t + tok] = jnp.cos(angle)
            trig[b, quarter:2 * quarter, tok * t:tok * t + tok] = jnp.sin(angle)

    def turned(val, cos_t, sin_t):
        u = val[0:quarter]
        w = val[quarter:2 * quarter]
        return [u * cos_t - w * sin_t, w * cos_t + u * sin_t, val[2 * quarter:hd]]

    def eighth(val):
        return val.astype(BF) * jnp.asarray(scale, BF)

    def keys_values(val, cos_t, sin_t):
        return jnp.concatenate(turned(val[0:hd], cos_t, sin_t) + [val[hd:hw]], axis=0).astype(BF)

    lane = lax.broadcasted_iota(jnp.int32, (pair, cols_q), 1)
    row = lax.broadcasted_iota(jnp.int32, (pair, cols_q), 0)
    seen_far = row <= core * tok + lane % tok

    @pl.loop(0, n_chip)
    def _(k):
        for turn in range(parts):
            ring_service(h_ring, parts * k + turn)

        @pl.when(k == 5)
        def _():
            for item in own_sends(*y_ring):
                item.start()

        @pl.when(k == 0)
        def _():
            for item in loads:
                item.wait()

        b = ring_origin(k)
        ring_mate(h_ring, k, b)
        make_trig(b)

        @pl.when(k == 0)
        def _():
            for item in far_loads:
                item.wait()
            cos_t = trig[chip, 0:quarter, part_of(core, tok)]
            sin_t = trig[chip, quarter:2 * quarter, part_of(core, tok)]

            @pl.loop(0, n_far)
            def _(f):
                da_t = dot_t(wt[part_of(f, 2 * hw), :], dy_own[...]).astype(BF)
                q_t = dot_t(wt[part_of(n_far + f, 2 * hw), :], hb[chip, part_of(core, tok), :])
                for head in range(4):
                    part = slice(hd * head, hd * head + hd)
                    at = tok * head
                    bmat_far[f, 0:hd, at:at + tok] = eighth(jnp.concatenate(turned(q_t[part], cos_t, sin_t), axis=0))
                    bmat_far[f, hd:hw, cols_q + at:cols_q + at + tok] = da_t[part]

            for item in weight_loads:
                item.start()

        place = part_of(b, pair)
        cos_t = trig[b, 0:quarter, :]
        sin_t = trig[b, quarter:2 * quarter, :]
        flat = dot_t(wi[...], hb[b])
        for head in range(2):
            q_rot = eighth(jnp.concatenate(turned(flat[hd * head:hd * head + hd], cos_t, sin_t), axis=0))
            for t in range(2):
                lane = pair * t + tok * head
                qt[b, :, lane:lane + tok] = q_rot[:, tok * t:tok * t + tok]
        kv_rot = keys_values(flat[hw:2 * hw], cos_t, sin_t)
        kvt[:, place] = kv_rot
        kv[place, :] = kv_rot.T

        @pl.when(b <= chip)
        def _():
            flat_far = dot_t(w_far[...], hb[b])
            for f in range(n_far):
                far_rot = keys_values(flat_far[hw * f:hw * f + hw], cos_t, sin_t)
                kvt_far[f, :, place] = far_rot
                kv_far[f, place, :] = far_rot.T

            @pl.loop(0, n_far)
            def _(f):
                both = dot(kv_far[f, place, :], bmat_far[f])
                d_p = both[:, cols_q:2 * cols_q]

                @pl.when(k == 0)
                def _():
                    s = jnp.where(seen_far, both[:, 0:cols_q], -1e30)
                    top = jnp.max(s, axis=0, keepdims=True)
                    p = jnp.exp(s - top)
                    stat_far[f, 0] = top
                    stat_far[f, 1] = jnp.sum(p, axis=0, keepdims=True)
                    stat_far[f, 2] = jnp.sum(p * d_p, axis=0, keepdims=True)

                @pl.when(k > 0)
                def _():
                    s = both[:, 0:cols_q]
                    old = stat_far[f, 0]
                    new = jnp.maximum(old, jnp.max(s, axis=0, keepdims=True))
                    p = jnp.exp(s - new)
                    keep = jnp.exp(old - new)
                    stat_far[f, 0] = new
                    stat_far[f, 1] = stat_far[f, 1] * keep + jnp.sum(p, axis=0, keepdims=True)
                    stat_far[f, 2] = stat_far[f, 2] * keep + jnp.sum(p * d_p, axis=0, keepdims=True)

    groups = [slice(tile * g, tile * g + tile) for g in range(cols_q // tile)]

    def first_part(b, seen):
        def both_of(rows):
            both = dot(kv[rows, :], bmat[...])
            return both[:, 0:cols_q], both[:, cols_q:2 * cols_q]

        rows = part_of(b, pair)
        s, d_p = both_of(rows)
        s = jnp.where(seen, s, -1e30)
        top = jnp.max(s, axis=0, keepdims=True)
        p = jnp.exp(s - top)
        sbuf[rows, :] = p
        dpbuf[rows, :] = d_p
        mbuf[b] = top

        def step(c, state, chunks=1):
            old, total, weighted = state
            rows = part_of(c, chunks * pair)
            s, d_p = both_of(rows)
            new = jnp.maximum(old, jnp.max(s, axis=0, keepdims=True))
            p = jnp.exp(s - new)
            sbuf[rows, :] = p
            dpbuf[rows, :] = d_p
            for i in range(chunks):
                mbuf[chunks * c + i] = new
            keep = jnp.exp(old - new)
            return new, total * keep + jnp.sum(p, axis=0, keepdims=True), weighted * keep + jnp.sum(p * d_p, axis=0, keepdims=True)

        state = (top, jnp.sum(p, axis=0, keepdims=True), jnp.sum(p * d_p, axis=0, keepdims=True))
        state = lax.fori_loop(0, b // 2, functools.partial(step, chunks=2), state)
        top, total, weighted = lax.fori_loop(2 * (b // 2), b, step, state)
        inv = 1.0 / total
        return top, inv, weighted * inv

    def second_part(b, stats):
        top, inv, row_dot = stats
        adq[...] = jnp.zeros_like(adq)

        def step(c, carry):
            rows = part_of(c, pair)
            factor = jnp.exp(mbuf[c] - top) * inv
            d_k = d_v = None
            for at in groups:
                p = sbuf[rows, at] * factor[:, at]
                p_b = p.astype(BF)
                ds_b = (p * (dpbuf[rows, at] - row_dot[:, at])).astype(BF)
                adq[0:hd, at] += dot(kvt[0:hd, rows], ds_b)
                adq[hd:hw, at] += dot(kvt[hd:hw, rows], p_b)
                more_k = dot_t(bmat[0:hd, at], ds_b)
                more_v = dot_t(bmat[hd:hw, cols_q + at.start:cols_q + at.stop], p_b)
                d_k = more_k if d_k is None else d_k + more_k
                d_v = more_v if d_v is None else d_v + more_v
            dkvt[0:hd, rows] += d_k
            dkvt[hd:hw, rows] += d_v
            return carry

        lax.fori_loop(0, b + 1, step, 0)


    def send_rows(slot):
        cols = part_of(slot, tok)
        return [
            remote(dq_all.at[:, cols], dt_rv.at[own_rows], q_s.at[slot], q_r.at[me], slot),
            remote(at_all.at[:, cols], at_rv.at[own_rows], a_s.at[slot], a_r.at[me], slot),
        ]

    for event in range(2):
        ring_event(y_ring, jnp.int32(event))

    @pl.loop(0, n_chip)
    def _(k):
        @pl.when(k % 2 == 1)
        def _():
            for turn in range(2, parts):
                ring_service(y_ring, parts * k + turn)

        b = ring_origin(k)
        ring_mate(y_ring, k, b)

        @pl.when(k == 1)
        def _():
            for item in weight_loads:
                item.wait()

        @pl.when(k == n_chip - 1)
        def _():
            for early in range(1 + 2 * near):
                for t in range(2):
                    slot = 2 * ring_origin(early) + t

                    @pl.when(slot != me)
                    def _():
                        for item in send_rows(slot):
                            item.start()

        da_t = dot_t(woi[...], dyb[b]).astype(BF)
        bmat[0:hd, 0:cols_q] = qt[b]
        for t in range(2):
            for head in range(2):
                at = cols_q + pair * t + tok * head
                bmat[hd:hw, at:at + tok] = da_t[hd * head:hd * head + hd, tok * t:tok * t + tok]
        stats = first_part(b, row <= (lane // pair) * tok + lane % tok)
        for turn in range(2):
            ring_service(y_ring, parts * k + 2 + 2 * (k % 2) + turn)
        second_part(b, stats)
        for t in range(2):
            slot = 2 * b + t
            lanes = [slice(pair * t + tok * head, pair * t + tok * head + tok) for head in range(2)]
            a_t = jnp.concatenate([adq[hd:hw, at] for at in lanes], axis=0).astype(BF)
            cos_t = trig[b, 0:quarter, tok * t:tok * t + tok]
            sin_t = trig[b, quarter:2 * quarter, tok * t:tok * t + tok]
            dq_t = jnp.concatenate([piece for at in lanes for piece in turned(adq[0:hd, at] * scale, cos_t, -sin_t)], axis=0).astype(BF)
            at_all[:, part_of(slot, tok)] = a_t
            dq_all[:, part_of(slot, tok)] = dq_t

            @pl.when(slot == me)
            def _():
                at_rv[own_rows, :] = a_t
                dt_rv[own_rows, :] = dq_t

        @pl.when(k % 2 == 0)
        def _():
            for turn in range(2):
                ring_service(y_ring, parts * (k + 1) + turn)

    far = [ring_origin(k) for k in range(n_chip - 1, 0, -1)]
    targets = [2 * c + p for c in far for p in range(2)] + [mate]
    near_targets = targets[-1 - 4 * near:]
    swap = remote(dkvt.at[part_of(1 - core, hd)], kv_rv, x_s, x_r, mate)
    swap.start()
    w_sends = [remote(dwt.at[pl.ds(0, hw), part_of(t, tok)], gw_hbm.at[own_rows], w_s.at[t], w_r.at[me], t) for t in targets]

    def columns(rows_all, buf, cols):
        acc = jnp.zeros((rows_all.shape[0], tile), F32)
        for s in range(n_chip):
            acc += dot(rows_all[:, pair * s:pair * s + pair], buf[s, :, cols])
        return acc

    def q_columns(i):
        cols = part_of(far[i] if i < n_chip - 1 else chip, pair)
        dwt[0:hw, cols] = columns(dq_all, hb, cols)
        for item in w_sends[max(2 * i - 2, 0):2 * i]:
            item.start()

    for i in range(FIRST + 1):
        q_columns(i)

    swap.wait_recv()
    mine = part_of(core, hd)
    g_rows = pl.ds(pl.multiple_of(q_rows + core * kv_w + chip * hd, hd), hd)
    for t in range(n_chip):
        cols = slice(pair * t, pair * t + pair)
        g = dkvt[mine, cols] + kv_rv[:, cols]
        cos_t = jnp.where(core == 0, trig[t, 0:quarter, :], 1.0)
        sin_t = jnp.where(core == 0, trig[t, quarter:2 * quarter, :], 0.0)
        g_b = jnp.concatenate(turned(g, cos_t, -sin_t), axis=0).astype(BF)
        kv_mine[2 * t] = g_b[:, 0:tok]
        kv_mine[2 * t + 1] = g_b[:, tok:pair]
        kv_row[:, cols] = g_b
    dt_rv[g_rows, :] = kv_mine[me]
    kv_sends = [remote(kv_mine.at[t], dt_rv.at[g_rows], kv_s.at[t], kv_r.at[me], t) for t in targets]
    for item in kv_sends:
        item.start()
    for i in range(FIRST + 1, n_chip):
        q_columns(i)
    w_sends[-1].start()
    w_own = local(dwt.at[pl.ds(0, hw), part_of(me, tok)], gw_hbm.at[own_rows], loc_sem.at[0])
    w_own.start()
    for t in range(width // tile):
        cols = slice(tile * t, tile * t + tile)
        dwt[hw:hw + hd, cols] = columns(kv_row, hb, cols)
    wk_own = local(dwt.at[pl.ds(hw, hd), part_of(me, tok)], gw_hbm.at[g_rows], loc_sem.at[1])
    wk_own.start()
    wk_sends = [remote(dwt.at[pl.ds(hw, hd), part_of(t, tok)], gw_hbm.at[g_rows], wk_s.at[t], wk_r.at[me], t) for t in targets]
    for item in wk_sends[0:HELD]:
        item.start()

    for t in range(width // tile):
        cols = slice(tile * t, tile * t + tile)
        dwo[:, cols] = columns(at_all, dyb, cols)
    store_wo = local(dwo, gwo_hbm, out_sem.at[0])
    store_wo.start()
    finish_ring(y_ring)
    wo_loads = [local(wo_hbm.at[pl.ds(pair * t, pair)], dyb.at[t], wo_sem.at[t]) for t in range(n_chip)]
    for item in wo_loads:
        item.start()

    @pl.loop(0, n_far)
    def _(f):
        c_far = ring_origin(2 * near + 1 + f)
        cos_t = trig[chip, 0:quarter, part_of(core, tok)]
        sin_t = trig[chip, quarter:2 * quarter, part_of(core, tok)]
        top = stat_far[f, 0]
        inv = 1.0 / stat_far[f, 1]
        row_dot = stat_far[f, 2] * inv

        def add_chunk(c, diagonal, chunks=1):
            rows = part_of(c, chunks * pair)
            for at in groups:
                keys = kv_far[f, rows, :]
                s = dot(keys, bmat_far[f, :, at])
                d_p = dot(keys, bmat_far[f, :, cols_q + at.start:cols_q + at.stop])
                if diagonal:
                    s = jnp.where(seen_far[:, at], s, -1e30)
                p = jnp.exp(s - top[:, at]) * inv[:, at]
                p_b = p.astype(BF)
                ds_b = (p * (d_p - row_dot[:, at])).astype(BF)
                d_q = dot(kvt_far[f, 0:hd, rows], ds_b)
                d_a = dot(kvt_far[f, hd:hw, rows], p_b)
                adq[0:hd, at] = d_q if diagonal else adq[0:hd, at] + d_q
                adq[hd:hw, at] = d_a if diagonal else adq[hd:hw, at] + d_a

        add_chunk(chip, True)

        @pl.loop(0, chip // 2)
        def _(c):
            add_chunk(c, False, 2)

        @pl.when(chip % 2 == 1)
        def _():
            add_chunk(chip - 1, False)

        for head in range(4):
            at = slice(tok * head, tok * head + tok)
            place = pl.ds(pl.multiple_of(c_far * 2 * hw + hd * head, hd), hd)
            at_rv[place, :] = adq[hd:hw, at].astype(BF)
            dt_rv[place, :] = jnp.concatenate(turned(adq[0:hd, at] * scale, cos_t, -sin_t), axis=0).astype(BF)

    for t in near_targets:
        remote(at_all.at[:, pl.ds(0, tok)], at_rv.at[part_of(t, hw)], a_s.at[t], a_r.at[t], t).wait_recv()
    for item in wo_loads:
        item.wait()
    for t in range(q_rows // tok):
        a_nat[:, tok * t:tok * t + tok] = at_rv[tok * t:tok * t + tok, :].T
    for t in range(width // tile):
        cols = slice(tile * t, tile * t + tile)
        prod = jnp.zeros((tok, tile), F32)
        for s in range(n_chip):
            prod += dot(a_nat[:, pair * s:pair * s + pair], dyb[s, :, cols])
        out_v[:, cols] = (x_v[:, cols].astype(F32) + prod).astype(BF)
    store_out = local(out_v, out_hbm, out_sem.at[1])
    store_out.start()

    def kv_place(t):
        return pl.ds(pl.multiple_of(q_rows + (t % 2) * kv_w + (t // 2) * hd, hd), hd)

    for t in near_targets:
        remote(dq_all.at[:, pl.ds(0, tok)], dt_rv.at[part_of(t, hw)], q_s.at[t], q_r.at[t], t).wait_recv()
    for t in targets:
        remote(kv_mine.at[0], dt_rv.at[kv_place(t)], kv_s.at[t], kv_r.at[t], t).wait_recv()
    swap.wait_send()
    for t in range(n_rows // tok):
        d_nat[:, tok * t:tok * t + tok] = dt_rv[tok * t:tok * t + tok, :].T

    mean = stat[0, :, 0:1]
    inv_std = stat[1, :, 0:1]
    dh = dkvt
    for t in range(width // tile):
        cols = slice(tile * t, tile * t + tile)
        acc = jnp.zeros((tok, tile), F32)
        for s in range(n_rows // tile):
            acc += dot(d_nat[:, tile * s:tile * s + tile], wt[tile * s:tile * s + tile, cols])
        dh[:, cols] = acc
        gg_st[0, :, cols] = jnp.sum(acc * ((x_v[:, cols].astype(F32) - mean) * inv_std), axis=0, keepdims=True)
        gg_st[1, :, cols] = jnp.sum(acc, axis=0, keepdims=True)
    g_swap = remote(gg_st.at[1 - core], gg_mx, g_s.at[n_chip], g_r.at[n_chip], mate)
    g_swap.start()
    g_swap.wait_recv()
    gg_my[...] = jnp.where(core == 0, gg_st[0], gg_st[1]) + gg_mx[...]
    gg_rv[chip] = gg_my[...]
    g_sends = [remote(gg_my, gg_rv.at[chip], g_s.at[c], g_r.at[chip], 2 * c + core) for c in far]
    for item in g_sends + wk_sends[HELD:]:
        item.start()

    grad_hat = dh[...] * gain_one
    x_hat = (x_v[...].astype(F32) - mean) * inv_std
    mean_one = jnp.mean(grad_hat, axis=-1, keepdims=True)
    mean_two = jnp.mean(grad_hat * x_hat, axis=-1, keepdims=True)
    store_out.wait()
    out_v[...] = (dy_own[...].astype(F32) + inv_std * (grad_hat - mean_one - x_hat * mean_two)).astype(BF)
    store_gx = local(out_v, gx_hbm, out_sem.at[2])
    store_gx.start()

    for c in far:
        remote(gg_my, gg_rv.at[c], g_s.at[c], g_r.at[c], 2 * c + core).wait_recv()
    sums = gg_rv[0]
    for c in range(1, n_chip):
        sums = sums + gg_rv[c]
    gg_out[core] = sums
    g_swap_out = remote(gg_out.at[core], gg_out.at[core], g_s.at[n_chip + 1], g_r.at[n_chip + 1], mate)
    g_swap_out.start()
    remote(gg_out.at[core], gg_out.at[1 - core], g_s.at[n_chip + 1], g_r.at[n_chip + 1], mate).wait_recv()
    store_gg = local(gg_out, gg_hbm, out_sem.at[3])
    store_gg.start()

    finish_ring(h_ring)
    for item in pos_sends + [g_swap, g_swap_out]:
        item.wait_send()
    for t in near_targets:
        remote(at_all.at[:, pl.ds(0, tok)], at_rv.at[pl.ds(0, hw)], a_s.at[t], a_r.at[t], t).wait_send()
        remote(dq_all.at[:, pl.ds(0, tok)], dt_rv.at[pl.ds(0, hw)], q_s.at[t], q_r.at[t], t).wait_send()
    for item in kv_sends + w_sends + g_sends + wk_sends:
        item.wait_send()
    for t in targets:
        remote(dwt.at[pl.ds(0, hw), part_of(t, tok)], gw_hbm.at[part_of(t, hw)], w_s.at[t], w_r.at[t], t).wait_recv()
        remote(dwt.at[pl.ds(hw, hd), part_of(t, tok)], gw_hbm.at[kv_place(t)], wk_s.at[t], wk_r.at[t], t).wait_recv()
    for item in (w_own, wk_own, store_wo, store_gx, store_gg):
        item.wait()


def settle_kernel(q_rows, kv_w, out_i, gx_i, gw_i, gwo_i, gg_i, out_o, gx_o, gq_o, gk_o, gv_o, gwo_o, gain_o, bias_o, b_act, b_q, b_kv, b_o, b_gg, sem_in, sem_out, sem_gg):
    half_q = q_rows // 2
    half_o = gwo_i.shape[0] // 2
    moves = [(out_i, b_act.at[0], out_o), (gx_i, b_act.at[1], gx_o)]
    for t in range(2):
        moves.append((gw_i.at[pl.ds(half_q * t, half_q)], b_q.at[t], gq_o.at[pl.ds(half_q * t, half_q)]))
        moves.append((gwo_i.at[pl.ds(half_o * t, half_o)], b_o.at[t], gwo_o.at[pl.ds(half_o * t, half_o)]))
    moves.append((gw_i.at[pl.ds(q_rows, kv_w)], b_kv.at[0], gk_o))
    moves.append((gw_i.at[pl.ds(q_rows + kv_w, kv_w)], b_kv.at[1], gv_o))
    loads = [pltpu.make_async_copy(src, mid, sem_in.at[i]) for i, (src, mid, _) in enumerate(moves)]
    stores = [pltpu.make_async_copy(mid, dst, sem_out.at[i]) for i, (_, mid, dst) in enumerate(moves)]
    load_gg = pltpu.make_async_copy(gg_i, b_gg, sem_gg)
    load_gg.start()
    for item in loads:
        item.start()
    for load, store in zip(loads, stores):
        load.wait()
        store.start()
    load_gg.wait()
    gain_o[...] = b_gg[0, 0]
    bias_o[...] = b_gg[1, 0]
    for item in stores:
        item.wait()


def solution(mesh):
    n_dev = mesh.shape['cp']

    def device_step(x_act, d_out, positions, ln_gain, ln_bias, w_query, w_key, w_value, w_out):
        tok, width = x_act.shape[1], x_act.shape[2]
        q_heads, hd = w_query.shape[1], w_query.shape[2]
        kv_heads = w_key.shape[1]
        q_w, kv_w = q_heads * hd, kv_heads * hd
        n_rows = q_w + 2 * kv_w
        seq = n_dev * tok
        hw = 2 * hd

        def flat_weight(w):
            return jnp.transpose(w, (1, 2, 0)).reshape(-1, width)

        hbm = pl.BlockSpec(memory_space=pltpu.HBM)
        vmem = pl.BlockSpec(memory_space=pltpu.VMEM)
        dma = pltpu.SemaphoreType.DMA
        n_chip = n_dev // 2
        n_far = n_chip - 1 - 2 * NEAR
        pair = 2 * tok
        scratch = [
            pltpu.VMEM((n_chip, pair, width), BF),
            pltpu.VMEM((n_chip, pair, width), BF),
            pltpu.VMEM((n_rows, width), BF),
            pltpu.VMEM((2 * hw, width), BF),
            pltpu.VMEM((hw, width), BF),
            pltpu.VMEM((n_far * hw, width), BF),
            pltpu.VMEM((n_dev, 1, tok), jnp.int32),
            pltpu.VMEM((n_chip, hd // 2, pair), F32),
            pltpu.VMEM((n_chip, hd, 2 * pair), BF),
            pltpu.VMEM((hw, seq), BF),
            pltpu.VMEM((seq, hw), BF),
            pltpu.VMEM((n_far, hw, seq), BF),
            pltpu.VMEM((n_far, seq, hw), BF),
            pltpu.VMEM((n_far, hw, 4 * pair), BF),
            pltpu.VMEM((n_far, 3, 1, 2 * pair), F32),
            pltpu.VMEM((hw, 4 * pair), BF),
            pltpu.VMEM((seq, 2 * pair), F32),
            pltpu.VMEM((seq, 2 * pair), F32),
            pltpu.VMEM((n_chip, 1, 2 * pair), F32),
            pltpu.VMEM((hw, 2 * pair), F32),
            pltpu.VMEM((hw, seq), F32),
            pltpu.VMEM((hd, seq), F32),
            pltpu.VMEM((n_dev, hd, tok), BF),
            pltpu.VMEM((hd, seq), BF),
            pltpu.VMEM((hw, width), F32),
            pltpu.VMEM((hw + hd, width), F32),
            pltpu.VMEM((hw, seq), BF),
            pltpu.VMEM((hw, seq), BF),
            pltpu.VMEM((q_w, tok), BF),
            pltpu.VMEM((n_rows, tok), BF),
            pltpu.VMEM((tok, q_w), BF),
            pltpu.VMEM((tok, n_rows), BF),
            pltpu.VMEM((tok, width), BF),
            pltpu.VMEM((tok, width), BF),
            pltpu.VMEM((2, 1, width), F32),
            pltpu.VMEM((2, tok, 128), F32),
            pltpu.VMEM((tok, width), BF),
            pltpu.VMEM((2, 1, width), F32),
            pltpu.VMEM((1, width), F32),
            pltpu.VMEM((1, width), F32),
            pltpu.VMEM((n_chip, 1, width), F32),
            pltpu.VMEM((2, 1, width), F32),
            dma((10,)), dma((4 * n_far,)), dma((n_chip,)), dma((3,)), dma((4,)), dma((2,)),
        ] + [dma((9 * PARTS,)), dma((7 * PARTS,)), dma((8 * PARTS,)), dma((8 * PARTS,))] * 2 + [dma((n_dev,))] * 6 + [dma] * 2 + [dma((n_dev,))] * 8
        out, gx, gw, gwo, gg = pl.pallas_call(
            functools.partial(block_kernel, n_dev, hd, kv_w, NEAR, PARTS),
            out_shape=(
                jax.ShapeDtypeStruct((tok, width), BF),
                jax.ShapeDtypeStruct((tok, width), BF),
                jax.ShapeDtypeStruct((n_rows, tok), F32),
                jax.ShapeDtypeStruct((hw, width), F32),
                jax.ShapeDtypeStruct((2, 1, width), F32),
            ),
            in_specs=[hbm] * 9,
            out_specs=(hbm,) * 5,
            scratch_shapes=scratch,
            compiler_params=pltpu.CompilerParams(collective_id=0, has_side_effects=True, vmem_limit_bytes=67043328),
            name='attn_block',
        )(
            x_act.reshape(tok, width), d_out.reshape(tok, width), positions.reshape(1, tok),
            ln_gain.reshape(1, width), ln_bias.reshape(1, width),
            flat_weight(w_query), flat_weight(w_key), flat_weight(w_value), w_out,
        )

        out, gx, gq, gk, gv, gwo, gain, bias = pl.pallas_call(
            functools.partial(settle_kernel, q_w, kv_w),
            out_shape=(
                jax.ShapeDtypeStruct((tok, width), BF),
                jax.ShapeDtypeStruct((tok, width), BF),
                jax.ShapeDtypeStruct((q_w, tok), F32),
                jax.ShapeDtypeStruct((kv_w, tok), F32),
                jax.ShapeDtypeStruct((kv_w, tok), F32),
                jax.ShapeDtypeStruct((hw, width), F32),
                jax.ShapeDtypeStruct((width,), F32),
                jax.ShapeDtypeStruct((width,), F32),
            ),
            in_specs=[hbm] * 5,
            out_specs=(hbm,) * 6 + (vmem,) * 2,
            scratch_shapes=[
                pltpu.VMEM((2, tok, width), BF),
                pltpu.VMEM((2, q_w // 2, tok), F32),
                pltpu.VMEM((2, kv_w, tok), F32),
                pltpu.VMEM((2, hw // 2, width), F32),
                pltpu.VMEM((2, 1, width), F32),
                dma((8,)), dma((8,)), dma,
            ],
            name='settle',
        )(out, gx, gw, gwo, gg)

        def rows_out(block, heads):
            return jnp.transpose(block.reshape(heads, hd, tok), (2, 0, 1))

        return (
            out.reshape(1, tok, width), gx.reshape(1, tok, width),
            rows_out(gq, q_heads), rows_out(gk, kv_heads), rows_out(gv, kv_heads),
            gwo, gain, bias,
        )

    return jax.shard_map(device_step, mesh=mesh, in_specs=(P('dp', 'cp', None), P('dp', 'cp', None), P('dp', 'cp'), P(None), P(None), P(None, None, None), P(None, None, None), P(None, None, None), P(None, None)), out_specs=(P('dp', 'cp', None), P('dp', 'cp', None), P(('dp', 'cp'), None, None), P(('dp', 'cp'), None, None), P(('dp', 'cp'), None, None), P(('dp', 'cp'), None), P('dp'), P('dp')), check_vma=False)
```

```python
import functools
import math

import jax
import jax.numpy as jnp
from jax import lax
from jax.experimental import pallas as pl
from jax.experimental.pallas import tpu as pltpu
from jax.sharding import PartitionSpec as P

EPS = 1e-5
ROPE_BASE = 10000.0
MESH = pl.DeviceIdType.MESH
BF = jnp.bfloat16
F32 = jnp.float32
NEAR = 1
PARTS = 4
FIRST = 1
HELD = 4


def dot(lhs, rhs):
    return jnp.dot(lhs, rhs, preferred_element_type=F32)


def dot_t(lhs, rhs):
    return lax.dot_general(lhs, rhs, (((1,), (1,)), ((), ())), preferred_element_type=F32)


def block_kernel(
    n_dev, hd, kv_w, near, parts,
    x_hbm, dy_hbm, pos_hbm, gain_hbm, bias_hbm, wq_hbm, wk_hbm, wv_hbm, wo_hbm,
    out_hbm, gx_hbm, gw_hbm, gwo_hbm, gg_hbm,
    hb, dyb, wt, wi, woi, w_far, pos_all, trig,
    qt, kvt, kv, kvt_far, kv_far, bmat_far, stat_far, bmat, sbuf, dpbuf, mbuf, adq, dkvt, kv_rv, kv_mine, kv_row,
    dwo, dwt, at_all, dq_all, at_rv, dt_rv, a_nat, d_nat, x_v, dy_own, gb_v, stat, out_v, gg_st, gg_mx, gg_my, gg_rv, gg_out,
    in_sem, far_sem, wo_sem, w_sem, out_sem, loc_sem,
    hzs, hzr, hds, hdr, yzs, yzr, yds, ydr,
    pos_s, pos_r, a_s, a_r, q_s, q_r, x_s, x_r, kv_s, kv_r, w_s, w_r, wk_s, wk_r, g_s, g_r,
):
    tok, width = x_v.shape
    n_chip = n_dev // 2
    pair = 2 * tok
    me = lax.axis_index('cp')
    chip = me // 2
    core = me % 2
    right = 2 * ((chip + 1) % n_chip) + core
    left = 2 * ((chip + n_chip - 1) % n_chip) + core
    mate = 2 * chip + 1 - core
    q_rows = wq_hbm.shape[0]
    n_rows = q_rows + 2 * kv_w
    hw = 2 * hd
    quarter = hd // 4
    tile = 256
    scale = hd ** -0.5
    cols_q = 2 * pair
    n_far = n_chip - 1 - 2 * near

    def remote(src, dst, send, recv, target):
        return pltpu.make_async_remote_copy(src_ref=src, dst_ref=dst, send_sem=send, recv_sem=recv, device_id={'cp': target}, device_id_type=MESH)

    def local(src, dst, sem):
        return pltpu.make_async_copy(src, dst, sem)

    def part_of(i, size):
        return pl.ds(pl.multiple_of(i * size, size), size)

    def once(cond):
        return pl.loop(0, jnp.where(cond, 1, 0))

    def ring_steps(k):
        step = (k + 1) // 2
        return step, k % 2

    def ring_origin(k):
        step, ahead = ring_steps(k)
        return jnp.where(ahead == 1, chip + n_chip - step, chip + step) % n_chip

    own = (chip, part_of(core, tok))
    first_loads = [
        local(x_hbm, x_v, in_sem.at[0]),
        local(gain_hbm, gb_v.at[0], in_sem.at[1]),
        local(bias_hbm, gb_v.at[1], in_sem.at[2]),
        local(pos_hbm, pos_all.at[me], in_sem.at[3]),
    ]
    for item in first_loads:
        item.start()
    barrier = pltpu.get_barrier_semaphore()
    for step in range(1, n_dev):
        pl.semaphore_signal(barrier, inc=1, device_id={'cp': (me + step) % n_dev}, device_id_type=MESH)
    own_rows = part_of(me, hw)
    kv_rows = part_of(chip, hd)
    loads = [
        local(wq_hbm.at[own_rows], wi.at[pl.ds(0, hw)], in_sem.at[4]),
        local(wk_hbm.at[kv_rows], wi.at[pl.ds(hw, hd)], in_sem.at[5]),
        local(wv_hbm.at[kv_rows], wi.at[pl.ds(hw + hd, hd)], in_sem.at[6]),
        local(wo_hbm.at[own_rows], woi, in_sem.at[7]),
        local(dy_hbm, dyb.at[own], in_sem.at[8]),
        local(dy_hbm, dy_own, in_sem.at[9]),
    ]
    far_loads = []
    for f in range(n_far):
        far_rows = part_of(ring_origin(2 * near + 1 + f), hd)
        loads.append(local(wk_hbm.at[far_rows], w_far.at[pl.ds(hw * f, hd)], far_sem.at[2 * f]))
        loads.append(local(wv_hbm.at[far_rows], w_far.at[pl.ds(hw * f + hd, hd)], far_sem.at[2 * f + 1]))
        far_wo = part_of(ring_origin(2 * near + 1 + f), 2 * hw)
        far_loads.append(local(wo_hbm.at[far_wo], wt.at[pl.ds(2 * hw * f, 2 * hw)], far_sem.at[2 * n_far + f]))
        far_loads.append(local(wq_hbm.at[far_wo], wt.at[pl.ds(2 * hw * (n_far + f), 2 * hw)], far_sem.at[3 * n_far + f]))
    for item in loads + far_loads:
        item.start()

    for item in first_loads:
        item.wait()
    gain_one = 1.0 + gb_v[0]
    block = 16

    @pl.loop(0, tok // block)
    def _(i):
        rows = part_of(i, block)
        x_f = x_v[rows, :].astype(F32)
        mean = jnp.mean(x_f, axis=-1, keepdims=True)
        centered = x_f - mean
        inv_std = lax.rsqrt(jnp.mean(centered * centered, axis=-1, keepdims=True) + EPS)
        hb[chip, part_of(core * (tok // block) + i, block), :] = (centered * inv_std * gain_one + gb_v[1]).astype(BF)
        stat[0, rows, :] = jnp.broadcast_to(mean, (block, 128))
        stat[1, rows, :] = jnp.broadcast_to(inv_std, (block, 128))

    pl.semaphore_wait(barrier, n_dev - 1)

    def chunk(buf, origin, parity, part):
        return buf.at[origin, part_of(parts * parity + part, tok // parts)]

    turns = 2 * parts

    def own_sends(buf, zs, zr, ds, dr):
        copies = []
        for part in range(parts):
            piece = chunk(buf, chip, core, part)
            copies.append(remote(piece, piece, zs.at[2 * part], zr.at[2 * part], right))
            copies.append(remote(piece, piece, zs.at[2 * part + 1], zr.at[2 * part + 1], left))
            copies.append(remote(piece, piece, ds.at[7 * parts + part], dr.at[7 * parts + part], mate))
        return copies

    def event_place(event):
        step = event // turns + 1
        turn = event % turns
        direction = turn % 2
        part = jnp.where(step < 4, turn // 2, turn // 2 + direction * (parts // 2))
        origin = jnp.where(direction == 0, chip + n_chip - step, chip + step) % n_chip
        return step, direction, part, origin

    def last_event(part, direction):
        return 6 * parts + 2 * (part - direction * (parts // 2)) + direction

    def ring_event(ring, event):
        buf, zs, zr, ds, dr = ring
        step, direction, part, origin = event_place(event)
        piece = chunk(buf, origin, core, part)
        remote(piece, piece, zs.at[0], zr.at[event], right).wait_recv()
        onward = jnp.where(step < 3, event + turns, last_event(part, direction))

        @pl.when((step < 3) | ((step == 3) & ((part >= parts // 2) == (direction == 1))))
        def _():
            remote(piece, piece, zs.at[event + turns], zr.at[onward], jnp.where(direction == 0, right, left)).start()

        remote(piece, piece, ds.at[event], dr.at[event], mate).start()

    def ring_service(ring, event):
        @pl.when(event < 7 * parts)
        def _():
            ring_event(ring, event)

    def ring_mate(ring, k, origin):
        buf, zs, zr, ds, dr = ring
        step, ahead = ring_steps(k)
        for part in range(parts):
            event = jnp.where(k == 0, 7 * parts + part, jnp.where(step < 4, turns * (step - 1) + 2 * part + 1 - ahead, last_event(part, part // (parts // 2))))
            piece = chunk(buf, origin, 1 - core, part)
            remote(piece, piece, ds.at[0], dr.at[event], mate).wait_recv()

    def finish_ring(ring):
        buf, zs, zr, ds, dr = ring
        for item in own_sends(*ring):
            item.wait_send()

        @pl.loop(0, 7 * parts)
        def _(event):
            step, direction, part, origin = event_place(event)
            piece = chunk(buf, origin, core, part)

            @pl.when((step < 3) | ((step == 3) & ((part >= parts // 2) == (direction == 1))))
            def _():
                remote(piece, piece, zs.at[event + turns], zr.at[event], right).wait_send()

            remote(piece, piece, ds.at[event], dr.at[event], mate).wait_send()

    h_ring = (hb, hzs, hzr, hds, hdr)
    y_ring = (dyb, yzs, yzr, yds, ydr)
    for item in own_sends(*h_ring):
        item.start()
    pos_sends = [remote(pos_all.at[me], pos_all.at[me], pos_s.at[step], pos_r.at[me], (me + step) % n_dev) for step in range(1, n_dev)]
    for item in pos_sends:
        item.start()
    weight_loads = [
        local(wq_hbm, wt.at[pl.ds(0, q_rows)], w_sem.at[0]),
        local(wk_hbm, wt.at[pl.ds(q_rows, kv_w)], w_sem.at[1]),
        local(wv_hbm, wt.at[pl.ds(q_rows + kv_w, kv_w)], w_sem.at[2]),
    ]
    dkvt[...] = jnp.zeros_like(dkvt)
    bmat[...] = jnp.zeros_like(bmat)
    bmat_far[...] = jnp.zeros_like(bmat_far)
    for f in range(n_far):
        stat_far[f, 0] = jnp.full((1, cols_q), -3e38, F32)
        stat_far[f, 1] = jnp.zeros((1, cols_q), F32)
        stat_far[f, 2] = jnp.zeros((1, cols_q), F32)

    freq = jnp.exp(lax.broadcasted_iota(jnp.int32, (quarter, tok), 0).astype(F32) * (-2.0 * math.log(ROPE_BASE) / (hd // 2)))

    def make_trig(b):
        for t in range(2):
            slot = 2 * b + t

            @pl.when(slot != me)
            def _():
                remote(pos_all.at[slot], pos_all.at[slot], pos_s.at[0], pos_r.at[slot], me).wait_recv()

            angle = pos_all[slot].astype(F32) * freq
            trig[b, 0:quarter, tok * t:tok * t + tok] = jnp.cos(angle)
            trig[b, quarter:2 * quarter, tok * t:tok * t + tok] = jnp.sin(angle)

    def turned(val, cos_t, sin_t):
        u = val[0:quarter]
        w = val[quarter:2 * quarter]
        return [u * cos_t - w * sin_t, w * cos_t + u * sin_t, val[2 * quarter:hd]]

    def eighth(val):
        return val.astype(BF) * jnp.asarray(scale, BF)

    def keys_values(val, cos_t, sin_t):
        return jnp.concatenate(turned(val[0:hd], cos_t, sin_t) + [val[hd:hw]], axis=0).astype(BF)

    lane = lax.broadcasted_iota(jnp.int32, (pair, cols_q), 1)
    row = lax.broadcasted_iota(jnp.int32, (pair, cols_q), 0)
    seen_far = row <= core * tok + lane % tok

    @pl.loop(0, n_chip)
    def _(k):
        for turn in range(parts):
            ring_service(h_ring, parts * k + turn)

        @once(k == 5)
        def _(_):
            for item in own_sends(*y_ring):
                item.start()

        @once(k == 0)
        def _(_):
            for item in loads:
                item.wait()

        b = ring_origin(k)
        ring_mate(h_ring, k, b)
        make_trig(b)

        @once(k == 0)
        def _(_):
            for item in far_loads:
                item.wait()
            cos_t = trig[chip, 0:quarter, part_of(core, tok)]
            sin_t = trig[chip, quarter:2 * quarter, part_of(core, tok)]

            @pl.loop(0, n_far)
            def _(f):
                da_t = dot_t(wt[part_of(f, 2 * hw), :], dy_own[...]).astype(BF)
                q_t = dot_t(wt[part_of(n_far + f, 2 * hw), :], hb[chip, part_of(core, tok), :])
                for head in range(4):
                    part = slice(hd * head, hd * head + hd)
                    at = tok * head
                    bmat_far[f, 0:hd, at:at + tok] = eighth(jnp.concatenate(turned(q_t[part], cos_t, sin_t), axis=0))
                    bmat_far[f, hd:hw, cols_q + at:cols_q + at + tok] = da_t[part]

            for item in weight_loads:
                item.start()

        place = part_of(b, pair)
        cos_t = trig[b, 0:quarter, :]
        sin_t = trig[b, quarter:2 * quarter, :]
        flat = dot_t(wi[...], hb[b])
        for head in range(2):
            q_rot = eighth(jnp.concatenate(turned(flat[hd * head:hd * head + hd], cos_t, sin_t), axis=0))
            for t in range(2):
                lane = pair * t + tok * head
                qt[b, :, lane:lane + tok] = q_rot[:, tok * t:tok * t + tok]
        kv_rot = keys_values(flat[hw:2 * hw], cos_t, sin_t)
        kvt[:, place] = kv_rot
        kv[place, :] = kv_rot.T

        @pl.when(b <= chip)
        def _():
            flat_far = dot_t(w_far[...], hb[b])
            for f in range(n_far):
                far_rot = keys_values(flat_far[hw * f:hw * f + hw], cos_t, sin_t)
                kvt_far[f, :, place] = far_rot
                kv_far[f, place, :] = far_rot.T

            @pl.loop(0, n_far)
            def _(f):
                both = dot(kv_far[f, place, :], bmat_far[f])
                s = jnp.where(seen_far | (k > 0), both[:, 0:cols_q], -1e30)
                old = stat_far[f, 0]
                new = jnp.maximum(old, jnp.max(s, axis=0, keepdims=True))
                p = jnp.exp(s - new)
                keep = jnp.exp(old - new)
                stat_far[f, 0] = new
                stat_far[f, 1] = stat_far[f, 1] * keep + jnp.sum(p, axis=0, keepdims=True)
                stat_far[f, 2] = stat_far[f, 2] * keep + jnp.sum(p * both[:, cols_q:2 * cols_q], axis=0, keepdims=True)

    groups = [slice(tile * g, tile * g + tile) for g in range(cols_q // tile)]

    def first_part(b, seen):
        def both_of(rows):
            both = dot(kv[rows, :], bmat[...])
            return both[:, 0:cols_q], both[:, cols_q:2 * cols_q]

        rows = part_of(b, pair)
        s, d_p = both_of(rows)
        s = jnp.where(seen, s, -1e30)
        top = jnp.max(s, axis=0, keepdims=True)
        p = jnp.exp(s - top)
        sbuf[rows, :] = p
        dpbuf[rows, :] = d_p
        mbuf[b] = top

        def step(c, state, chunks=1):
            old, total, weighted = state
            rows = part_of(c, chunks * pair)
            s, d_p = both_of(rows)
            new = jnp.maximum(old, jnp.max(s, axis=0, keepdims=True))
            p = jnp.exp(s - new)
            sbuf[rows, :] = p
            dpbuf[rows, :] = d_p
            for i in range(chunks):
                mbuf[chunks * c + i] = new
            keep = jnp.exp(old - new)
            return new, total * keep + jnp.sum(p, axis=0, keepdims=True), weighted * keep + jnp.sum(p * d_p, axis=0, keepdims=True)

        state = (top, jnp.sum(p, axis=0, keepdims=True), jnp.sum(p * d_p, axis=0, keepdims=True))
        state = lax.fori_loop(0, b // 2, functools.partial(step, chunks=2), state)
        top, total, weighted = lax.fori_loop(2 * (b // 2), b, step, state)
        inv = 1.0 / total
        return top, inv, weighted * inv

    def second_part(b, stats):
        top, inv, row_dot = stats
        adq[...] = jnp.zeros_like(adq)

        def step(c, carry):
            rows = part_of(c, pair)
            factor = jnp.exp(mbuf[c] - top) * inv
            d_k = d_v = None
            for at in groups:
                p = sbuf[rows, at] * factor[:, at]
                p_b = p.astype(BF)
                ds_b = (p * (dpbuf[rows, at] - row_dot[:, at])).astype(BF)
                adq[0:hd, at] += dot(kvt[0:hd, rows], ds_b)
                adq[hd:hw, at] += dot(kvt[hd:hw, rows], p_b)
                more_k = dot_t(bmat[0:hd, at], ds_b)
                more_v = dot_t(bmat[hd:hw, cols_q + at.start:cols_q + at.stop], p_b)
                d_k = more_k if d_k is None else d_k + more_k
                d_v = more_v if d_v is None else d_v + more_v
            dkvt[0:hd, rows] += d_k
            dkvt[hd:hw, rows] += d_v
            return carry

        lax.fori_loop(0, b + 1, step, 0)


    def send_rows(slot):
        cols = part_of(slot, tok)
        return [
            remote(dq_all.at[:, cols], dt_rv.at[own_rows], q_s.at[slot], q_r.at[me], slot),
            remote(at_all.at[:, cols], at_rv.at[own_rows], a_s.at[slot], a_r.at[me], slot),
        ]

    for event in range(2):
        ring_event(y_ring, jnp.int32(event))

    @pl.loop(0, n_chip)
    def _(k):
        @pl.when(k % 2 == 1)
        def _():
            for turn in range(2, parts):
                ring_service(y_ring, parts * k + turn)

        b = ring_origin(k)
        ring_mate(y_ring, k, b)

        @pl.when(k == 1)
        def _():
            for item in weight_loads:
                item.wait()

        @pl.loop(0, jnp.where(k == n_chip - 1, 2 + 4 * near, 0))
        def _(early):
            slot = 2 * ring_origin(early // 2) + early % 2

            @pl.when(slot != me)
            def _():
                for item in send_rows(slot):
                    item.start()

        da_t = dot_t(woi[...], dyb[b]).astype(BF)
        bmat[0:hd, 0:cols_q] = qt[b]
        for t in range(2):
            for head in range(2):
                at = cols_q + pair * t + tok * head
                bmat[hd:hw, at:at + tok] = da_t[hd * head:hd * head + hd, tok * t:tok * t + tok]
        stats = first_part(b, row <= (lane // pair) * tok + lane % tok)
        for turn in range(2):
            ring_service(y_ring, parts * k + 2 + 2 * (k % 2) + turn)
        second_part(b, stats)
        for t in range(2):
            slot = 2 * b + t
            lanes = [slice(pair * t + tok * head, pair * t + tok * head + tok) for head in range(2)]
            a_t = jnp.concatenate([adq[hd:hw, at] for at in lanes], axis=0).astype(BF)
            cos_t = trig[b, 0:quarter, tok * t:tok * t + tok]
            sin_t = trig[b, quarter:2 * quarter, tok * t:tok * t + tok]
            dq_t = jnp.concatenate([piece for at in lanes for piece in turned(adq[0:hd, at] * scale, cos_t, -sin_t)], axis=0).astype(BF)
            at_all[:, part_of(slot, tok)] = a_t
            dq_all[:, part_of(slot, tok)] = dq_t

            @pl.when(slot == me)
            def _():
                at_rv[own_rows, :] = a_t
                dt_rv[own_rows, :] = dq_t

        @pl.when(k % 2 == 0)
        def _():
            for turn in range(2):
                ring_service(y_ring, parts * (k + 1) + turn)

    far = [ring_origin(k) for k in range(n_chip - 1, 0, -1)]
    targets = [2 * c + p for c in far for p in range(2)] + [mate]
    near_targets = targets[-1 - 4 * near:]
    swap = remote(dkvt.at[part_of(1 - core, hd)], kv_rv, x_s, x_r, mate)
    swap.start()
    w_sends = [remote(dwt.at[pl.ds(0, hw), part_of(t, tok)], gw_hbm.at[own_rows], w_s.at[t], w_r.at[me], t) for t in targets]

    def columns(rows_all, buf, cols):
        acc = jnp.zeros((rows_all.shape[0], tile), F32)
        for s in range(n_chip):
            acc += dot(rows_all[:, pair * s:pair * s + pair], buf[s, :, cols])
        return acc

    def q_columns(i):
        cols = part_of(far[i] if i < n_chip - 1 else chip, pair)
        dwt[0:hw, cols] = columns(dq_all, hb, cols)
        for item in w_sends[max(2 * i - 2, 0):2 * i]:
            item.start()

    for i in range(FIRST + 1):
        q_columns(i)

    swap.wait_recv()
    mine = part_of(core, hd)
    g_rows = pl.ds(pl.multiple_of(q_rows + core * kv_w + chip * hd, hd), hd)
    for t in range(n_chip):
        cols = slice(pair * t, pair * t + pair)
        g = dkvt[mine, cols] + kv_rv[:, cols]
        cos_t = jnp.where(core == 0, trig[t, 0:quarter, :], 1.0)
        sin_t = jnp.where(core == 0, trig[t, quarter:2 * quarter, :], 0.0)
        g_b = jnp.concatenate(turned(g, cos_t, -sin_t), axis=0).astype(BF)
        kv_mine[2 * t] = g_b[:, 0:tok]
        kv_mine[2 * t + 1] = g_b[:, tok:pair]
        kv_row[:, cols] = g_b
    dt_rv[g_rows, :] = kv_mine[me]
    kv_sends = [remote(kv_mine.at[t], dt_rv.at[g_rows], kv_s.at[t], kv_r.at[me], t) for t in targets]
    for item in kv_sends:
        item.start()
    for i in range(FIRST + 1, n_chip):
        q_columns(i)
    w_sends[-1].start()
    w_own = local(dwt.at[pl.ds(0, hw), part_of(me, tok)], gw_hbm.at[own_rows], loc_sem.at[0])
    w_own.start()
    for t in range(width // tile):
        cols = slice(tile * t, tile * t + tile)
        dwt[hw:hw + hd, cols] = columns(kv_row, hb, cols)
    wk_own = local(dwt.at[pl.ds(hw, hd), part_of(me, tok)], gw_hbm.at[g_rows], loc_sem.at[1])
    wk_own.start()
    wk_sends = [remote(dwt.at[pl.ds(hw, hd), part_of(t, tok)], gw_hbm.at[g_rows], wk_s.at[t], wk_r.at[me], t) for t in targets]
    for item in wk_sends[0:HELD]:
        item.start()

    for t in range(width // tile):
        cols = slice(tile * t, tile * t + tile)
        dwo[:, cols] = columns(at_all, dyb, cols)
    store_wo = local(dwo, gwo_hbm, out_sem.at[0])
    store_wo.start()
    finish_ring(y_ring)
    wo_loads = [local(wo_hbm.at[pl.ds(pair * t, pair)], dyb.at[t], wo_sem.at[t]) for t in range(n_chip)]
    for item in wo_loads:
        item.start()

    @pl.loop(0, n_far)
    def _(f):
        c_far = ring_origin(2 * near + 1 + f)
        cos_t = trig[chip, 0:quarter, part_of(core, tok)]
        sin_t = trig[chip, quarter:2 * quarter, part_of(core, tok)]
        top = stat_far[f, 0]
        inv = 1.0 / stat_far[f, 1]
        row_dot = stat_far[f, 2] * inv

        def add_chunk(c, diagonal, chunks=1):
            rows = part_of(c, chunks * pair)
            for at in groups:
                keys = kv_far[f, rows, :]
                s = dot(keys, bmat_far[f, :, at])
                d_p = dot(keys, bmat_far[f, :, cols_q + at.start:cols_q + at.stop])
                if diagonal:
                    s = jnp.where(seen_far[:, at], s, -1e30)
                p = jnp.exp(s - top[:, at]) * inv[:, at]
                p_b = p.astype(BF)
                ds_b = (p * (d_p - row_dot[:, at])).astype(BF)
                d_q = dot(kvt_far[f, 0:hd, rows], ds_b)
                d_a = dot(kvt_far[f, hd:hw, rows], p_b)
                adq[0:hd, at] = d_q if diagonal else adq[0:hd, at] + d_q
                adq[hd:hw, at] = d_a if diagonal else adq[hd:hw, at] + d_a

        add_chunk(chip, True)

        @pl.loop(0, chip // 2)
        def _(c):
            add_chunk(c, False, 2)

        @pl.when(chip % 2 == 1)
        def _():
            add_chunk(chip - 1, False)

        for head in range(4):
            at = slice(tok * head, tok * head + tok)
            place = pl.ds(pl.multiple_of(c_far * 2 * hw + hd * head, hd), hd)
            at_rv[place, :] = adq[hd:hw, at].astype(BF)
            dt_rv[place, :] = jnp.concatenate(turned(adq[0:hd, at] * scale, cos_t, -sin_t), axis=0).astype(BF)

    for t in near_targets:
        remote(at_all.at[:, pl.ds(0, tok)], at_rv.at[part_of(t, hw)], a_s.at[t], a_r.at[t], t).wait_recv()
    for item in wo_loads:
        item.wait()
    for t in range(q_rows // tok):
        a_nat[:, tok * t:tok * t + tok] = at_rv[tok * t:tok * t + tok, :].T
    for t in range(width // tile):
        cols = slice(tile * t, tile * t + tile)
        prod = jnp.zeros((tok, tile), F32)
        for s in range(n_chip):
            prod += dot(a_nat[:, pair * s:pair * s + pair], dyb[s, :, cols])
        out_v[:, cols] = (x_v[:, cols].astype(F32) + prod).astype(BF)
    store_out = local(out_v, out_hbm, out_sem.at[1])
    store_out.start()

    def kv_place(t):
        return pl.ds(pl.multiple_of(q_rows + (t % 2) * kv_w + (t // 2) * hd, hd), hd)

    for t in near_targets:
        remote(dq_all.at[:, pl.ds(0, tok)], dt_rv.at[part_of(t, hw)], q_s.at[t], q_r.at[t], t).wait_recv()
    for t in targets:
        remote(kv_mine.at[0], dt_rv.at[kv_place(t)], kv_s.at[t], kv_r.at[t], t).wait_recv()
    swap.wait_send()
    for t in range(n_rows // tok):
        d_nat[:, tok * t:tok * t + tok] = dt_rv[tok * t:tok * t + tok, :].T

    mean = stat[0, :, 0:1]
    inv_std = stat[1, :, 0:1]
    dh = dkvt
    for t in range(width // tile):
        cols = slice(tile * t, tile * t + tile)
        acc = jnp.zeros((tok, tile), F32)
        for s in range(n_rows // tile):
            acc += dot(d_nat[:, tile * s:tile * s + tile], wt[tile * s:tile * s + tile, cols])
        dh[:, cols] = acc
        gg_st[0, :, cols] = jnp.sum(acc * ((x_v[:, cols].astype(F32) - mean) * inv_std), axis=0, keepdims=True)
        gg_st[1, :, cols] = jnp.sum(acc, axis=0, keepdims=True)
    g_swap = remote(gg_st.at[1 - core], gg_mx, g_s.at[n_chip], g_r.at[n_chip], mate)
    g_swap.start()
    g_swap.wait_recv()
    gg_my[...] = jnp.where(core == 0, gg_st[0], gg_st[1]) + gg_mx[...]
    gg_rv[chip] = gg_my[...]
    g_sends = [remote(gg_my, gg_rv.at[chip], g_s.at[c], g_r.at[chip], 2 * c + core) for c in far]
    for item in g_sends + wk_sends[HELD:]:
        item.start()

    grad_hat = dh[...] * gain_one
    x_hat = (x_v[...].astype(F32) - mean) * inv_std
    mean_one = jnp.mean(grad_hat, axis=-1, keepdims=True)
    mean_two = jnp.mean(grad_hat * x_hat, axis=-1, keepdims=True)
    store_out.wait()
    out_v[...] = (dy_own[...].astype(F32) + inv_std * (grad_hat - mean_one - x_hat * mean_two)).astype(BF)
    store_gx = local(out_v, gx_hbm, out_sem.at[2])
    store_gx.start()

    for c in far:
        remote(gg_my, gg_rv.at[c], g_s.at[c], g_r.at[c], 2 * c + core).wait_recv()
    sums = gg_rv[0]
    for c in range(1, n_chip):
        sums = sums + gg_rv[c]
    gg_out[core] = sums
    g_swap_out = remote(gg_out.at[core], gg_out.at[core], g_s.at[n_chip + 1], g_r.at[n_chip + 1], mate)
    g_swap_out.start()
    remote(gg_out.at[core], gg_out.at[1 - core], g_s.at[n_chip + 1], g_r.at[n_chip + 1], mate).wait_recv()
    store_gg = local(gg_out, gg_hbm, out_sem.at[3])
    store_gg.start()

    finish_ring(h_ring)
    for item in pos_sends + [g_swap, g_swap_out]:
        item.wait_send()
    for t in near_targets:
        remote(at_all.at[:, pl.ds(0, tok)], at_rv.at[pl.ds(0, hw)], a_s.at[t], a_r.at[t], t).wait_send()
        remote(dq_all.at[:, pl.ds(0, tok)], dt_rv.at[pl.ds(0, hw)], q_s.at[t], q_r.at[t], t).wait_send()
    for item in kv_sends + w_sends + g_sends + wk_sends:
        item.wait_send()
    for t in targets:
        remote(dwt.at[pl.ds(0, hw), part_of(t, tok)], gw_hbm.at[part_of(t, hw)], w_s.at[t], w_r.at[t], t).wait_recv()
        remote(dwt.at[pl.ds(hw, hd), part_of(t, tok)], gw_hbm.at[kv_place(t)], wk_s.at[t], wk_r.at[t], t).wait_recv()
    for item in (w_own, wk_own, store_wo, store_gx, store_gg):
        item.wait()


def settle_kernel(q_rows, kv_w, out_i, gx_i, gw_i, gwo_i, gg_i, out_o, gx_o, gq_o, gk_o, gv_o, gwo_o, gain_o, bias_o, b_act, b_q, b_kv, b_o, b_gg, sem_in, sem_out, sem_gg):
    half_q = q_rows // 2
    half_o = gwo_i.shape[0] // 2
    moves = [(out_i, b_act.at[0], out_o), (gx_i, b_act.at[1], gx_o)]
    for t in range(2):
        moves.append((gw_i.at[pl.ds(half_q * t, half_q)], b_q.at[t], gq_o.at[pl.ds(half_q * t, half_q)]))
        moves.append((gwo_i.at[pl.ds(half_o * t, half_o)], b_o.at[t], gwo_o.at[pl.ds(half_o * t, half_o)]))
    moves.append((gw_i.at[pl.ds(q_rows, kv_w)], b_kv.at[0], gk_o))
    moves.append((gw_i.at[pl.ds(q_rows + kv_w, kv_w)], b_kv.at[1], gv_o))
    loads = [pltpu.make_async_copy(src, mid, sem_in.at[i]) for i, (src, mid, _) in enumerate(moves)]
    stores = [pltpu.make_async_copy(mid, dst, sem_out.at[i]) for i, (_, mid, dst) in enumerate(moves)]
    load_gg = pltpu.make_async_copy(gg_i, b_gg, sem_gg)
    load_gg.start()
    for item in loads:
        item.start()
    for load, store in zip(loads, stores):
        load.wait()
        store.start()
    load_gg.wait()
    gain_o[...] = b_gg[0, 0]
    bias_o[...] = b_gg[1, 0]
    for item in stores:
        item.wait()


def solution(mesh):
    n_dev = mesh.shape['cp']

    def device_step(x_act, d_out, positions, ln_gain, ln_bias, w_query, w_key, w_value, w_out):
        tok, width = x_act.shape[1], x_act.shape[2]
        q_heads, hd = w_query.shape[1], w_query.shape[2]
        kv_heads = w_key.shape[1]
        q_w, kv_w = q_heads * hd, kv_heads * hd
        n_rows = q_w + 2 * kv_w
        seq = n_dev * tok
        hw = 2 * hd

        def flat_weight(w):
            return jnp.transpose(w, (1, 2, 0)).reshape(-1, width)

        hbm = pl.BlockSpec(memory_space=pltpu.HBM)
        vmem = pl.BlockSpec(memory_space=pltpu.VMEM)
        dma = pltpu.SemaphoreType.DMA
        n_chip = n_dev // 2
        n_far = n_chip - 1 - 2 * NEAR
        pair = 2 * tok
        scratch = [
            pltpu.VMEM((n_chip, pair, width), BF),
            pltpu.VMEM((n_chip, pair, width), BF),
            pltpu.VMEM((n_rows, width), BF),
            pltpu.VMEM((2 * hw, width), BF),
            pltpu.VMEM((hw, width), BF),
            pltpu.VMEM((n_far * hw, width), BF),
            pltpu.VMEM((n_dev, 1, tok), jnp.int32),
            pltpu.VMEM((n_chip, hd // 2, pair), F32),
            pltpu.VMEM((n_chip, hd, 2 * pair), BF),
            pltpu.VMEM((hw, seq), BF),
            pltpu.VMEM((seq, hw), BF),
            pltpu.VMEM((n_far, hw, seq), BF),
            pltpu.VMEM((n_far, seq, hw), BF),
            pltpu.VMEM((n_far, hw, 4 * pair), BF),
            pltpu.VMEM((n_far, 3, 1, 2 * pair), F32),
            pltpu.VMEM((hw, 4 * pair), BF),
            pltpu.VMEM((seq, 2 * pair), F32),
            pltpu.VMEM((seq, 2 * pair), F32),
            pltpu.VMEM((n_chip, 1, 2 * pair), F32),
            pltpu.VMEM((hw, 2 * pair), F32),
            pltpu.VMEM((hw, seq), F32),
            pltpu.VMEM((hd, seq), F32),
            pltpu.VMEM((n_dev, hd, tok), BF),
            pltpu.VMEM((hd, seq), BF),
            pltpu.VMEM((hw, width), F32),
            pltpu.VMEM((hw + hd, width), F32),
            pltpu.VMEM((hw, seq), BF),
            pltpu.VMEM((hw, seq), BF),
            pltpu.VMEM((q_w, tok), BF),
            pltpu.VMEM((n_rows, tok), BF),
            pltpu.VMEM((tok, q_w), BF),
            pltpu.VMEM((tok, n_rows), BF),
            pltpu.VMEM((tok, width), BF),
            pltpu.VMEM((tok, width), BF),
            pltpu.VMEM((2, 1, width), F32),
            pltpu.VMEM((2, tok, 128), F32),
            pltpu.VMEM((tok, width), BF),
            pltpu.VMEM((2, 1, width), F32),
            pltpu.VMEM((1, width), F32),
            pltpu.VMEM((1, width), F32),
            pltpu.VMEM((n_chip, 1, width), F32),
            pltpu.VMEM((2, 1, width), F32),
            dma((10,)), dma((4 * n_far,)), dma((n_chip,)), dma((3,)), dma((4,)), dma((2,)),
        ] + [dma((9 * PARTS,)), dma((7 * PARTS,)), dma((8 * PARTS,)), dma((8 * PARTS,))] * 2 + [dma((n_dev,))] * 6 + [dma] * 2 + [dma((n_dev,))] * 8
        out, gx, gw, gwo, gg = pl.pallas_call(
            functools.partial(block_kernel, n_dev, hd, kv_w, NEAR, PARTS),
            out_shape=(
                jax.ShapeDtypeStruct((tok, width), BF),
                jax.ShapeDtypeStruct((tok, width), BF),
                jax.ShapeDtypeStruct((n_rows, tok), F32),
                jax.ShapeDtypeStruct((hw, width), F32),
                jax.ShapeDtypeStruct((2, 1, width), F32),
            ),
            in_specs=[hbm] * 9,
            out_specs=(hbm,) * 5,
            scratch_shapes=scratch,
            compiler_params=pltpu.CompilerParams(collective_id=0, has_side_effects=True, vmem_limit_bytes=67043328),
            name='attn_block',
        )(
            x_act.reshape(tok, width), d_out.reshape(tok, width), positions.reshape(1, tok),
            ln_gain.reshape(1, width), ln_bias.reshape(1, width),
            flat_weight(w_query), flat_weight(w_key), flat_weight(w_value), w_out,
        )

        out, gx, gq, gk, gv, gwo, gain, bias = pl.pallas_call(
            functools.partial(settle_kernel, q_w, kv_w),
            out_shape=(
                jax.ShapeDtypeStruct((tok, width), BF),
                jax.ShapeDtypeStruct((tok, width), BF),
                jax.ShapeDtypeStruct((q_w, tok), F32),
                jax.ShapeDtypeStruct((kv_w, tok), F32),
                jax.ShapeDtypeStruct((kv_w, tok), F32),
                jax.ShapeDtypeStruct((hw, width), F32),
                jax.ShapeDtypeStruct((width,), F32),
                jax.ShapeDtypeStruct((width,), F32),
            ),
            in_specs=[hbm] * 5,
            out_specs=(hbm,) * 6 + (vmem,) * 2,
            scratch_shapes=[
                pltpu.VMEM((2, tok, width), BF),
                pltpu.VMEM((2, q_w // 2, tok), F32),
                pltpu.VMEM((2, kv_w, tok), F32),
                pltpu.VMEM((2, hw // 2, width), F32),
                pltpu.VMEM((2, 1, width), F32),
                dma((8,)), dma((8,)), dma,
            ],
            name='settle',
        )(out, gx, gw, gwo, gg)

        def rows_out(block, heads):
            return jnp.transpose(block.reshape(heads, hd, tok), (2, 0, 1))

        return (
            out.reshape(1, tok, width), gx.reshape(1, tok, width),
            rows_out(gq, q_heads), rows_out(gk, kv_heads), rows_out(gv, kv_heads),
            gwo, gain, bias,
        )

    return jax.shard_map(device_step, mesh=mesh, in_specs=(P('dp', 'cp', None), P('dp', 'cp', None), P('dp', 'cp'), P(None), P(None), P(None, None, None), P(None, None, None), P(None, None, None), P(None, None)), out_specs=(P('dp', 'cp', None), P('dp', 'cp', None), P(('dp', 'cp'), None, None), P(('dp', 'cp'), None, None), P(('dp', 'cp'), None, None), P(('dp', 'cp'), None), P('dp'), P('dp')), check_vma=False)
```

```python
import functools
import math

import jax
import jax.numpy as jnp
from jax import lax
from jax.experimental import pallas as pl
from jax.experimental.pallas import tpu as pltpu
from jax.sharding import PartitionSpec as P

EPS = 1e-5
ROPE_BASE = 10000.0
MESH = pl.DeviceIdType.MESH
BF = jnp.bfloat16
F32 = jnp.float32
NEAR = 1
PARTS = 4
FIRST = 1
HELD = 4


def dot(lhs, rhs):
    return jnp.dot(lhs, rhs, preferred_element_type=F32)


def dot_t(lhs, rhs):
    return lax.dot_general(lhs, rhs, (((1,), (1,)), ((), ())), preferred_element_type=F32)


def block_kernel(
    n_dev, hd, kv_w, near, parts,
    x_hbm, dy_hbm, pos_hbm, gain_hbm, bias_hbm, wq_hbm, wk_hbm, wv_hbm, wo_hbm,
    out_hbm, gx_hbm, gw_hbm, gwo_hbm, gg_hbm,
    hb, dyb, wt, wi, woi, w_far, pos_all, trig,
    qt, kvt, kv, kvt_far, kv_far, bmat_far, stat_far, bmat, da_rv, sbuf, dpbuf, mbuf, adq, dkvt, kv_rv, kv_mine, kv_row,
    dwo, dwt, at_all, dq_all, at_rv, dt_rv, a_nat, d_nat, x_v, dy_own, gb_v, stat, out_v, gg_st, gg_mx, gg_my, gg_rv, gg_out,
    in_sem, far_sem, wo_sem, w_sem, out_sem, loc_sem,
    hzs, hzr, hds, hdr, yzs, yzr, yds, ydr,
    d_s, d_r, pos_s, pos_r, a_s, a_r, q_s, q_r, x_s, x_r, kv_s, kv_r, w_s, w_r, wk_s, wk_r, g_s, g_r,
):
    tok, width = x_v.shape
    n_chip = n_dev // 2
    pair = 2 * tok
    me = lax.axis_index('cp')
    chip = me // 2
    core = me % 2
    right = 2 * ((chip + 1) % n_chip) + core
    left = 2 * ((chip + n_chip - 1) % n_chip) + core
    mate = 2 * chip + 1 - core
    q_rows = wq_hbm.shape[0]
    n_rows = q_rows + 2 * kv_w
    hw = 2 * hd
    quarter = hd // 4
    tile = 256
    scale = hd ** -0.5
    cols_q = 2 * pair
    n_far = n_chip - 1 - 2 * near

    def remote(src, dst, send, recv, target):
        return pltpu.make_async_remote_copy(src_ref=src, dst_ref=dst, send_sem=send, recv_sem=recv, device_id={'cp': target}, device_id_type=MESH)

    def local(src, dst, sem):
        return pltpu.make_async_copy(src, dst, sem)

    def part_of(i, size):
        return pl.ds(pl.multiple_of(i * size, size), size)

    def once(cond):
        return pl.loop(0, jnp.where(cond, 1, 0))

    def ring_steps(k):
        step = (k + 1) // 2
        return step, k % 2

    def ring_origin(k):
        step, ahead = ring_steps(k)
        return jnp.where(ahead == 1, chip + n_chip - step, chip + step) % n_chip

    own = (chip, part_of(core, tok))
    first_loads = [
        local(x_hbm, x_v, in_sem.at[0]),
        local(gain_hbm, gb_v.at[0], in_sem.at[1]),
        local(bias_hbm, gb_v.at[1], in_sem.at[2]),
        local(pos_hbm, pos_all.at[me], in_sem.at[3]),
    ]
    for item in first_loads:
        item.start()
    barrier = pltpu.get_barrier_semaphore()
    for step in range(1, n_dev):
        pl.semaphore_signal(barrier, inc=1, device_id={'cp': (me + step) % n_dev}, device_id_type=MESH)
    own_rows = part_of(me, hw)
    kv_rows = part_of(chip, hd)
    loads = [
        local(wq_hbm.at[own_rows], wi.at[pl.ds(0, hw)], in_sem.at[4]),
        local(wk_hbm.at[kv_rows], wi.at[pl.ds(hw, hd)], in_sem.at[5]),
        local(wv_hbm.at[kv_rows], wi.at[pl.ds(hw + hd, hd)], in_sem.at[6]),
        local(wo_hbm.at[own_rows], woi, in_sem.at[7]),
        local(dy_hbm, dyb.at[own], in_sem.at[8]),
        local(dy_hbm, dy_own, in_sem.at[9]),
    ]
    far_loads = []
    for f in range(n_far):
        far_rows = part_of(ring_origin(2 * near + 1 + f), hd)
        loads.append(local(wk_hbm.at[far_rows], w_far.at[pl.ds(hw * f, hd)], far_sem.at[2 * f]))
        loads.append(local(wv_hbm.at[far_rows], w_far.at[pl.ds(hw * f + hd, hd)], far_sem.at[2 * f + 1]))
        far_wo = part_of(ring_origin(2 * near + 1 + f), 2 * hw)
        far_loads.append(local(wo_hbm.at[far_wo], wt.at[pl.ds(2 * hw * f, 2 * hw)], far_sem.at[2 * n_far + f]))
        far_loads.append(local(wq_hbm.at[far_wo], wt.at[pl.ds(2 * hw * (n_far + f), 2 * hw)], far_sem.at[3 * n_far + f]))
    for item in loads + far_loads:
        item.start()

    for item in first_loads:
        item.wait()
    gain_one = 1.0 + gb_v[0]
    block = 16

    @pl.loop(0, tok // block)
    def _(i):
        rows = part_of(i, block)
        x_f = x_v[rows, :].astype(F32)
        mean = jnp.mean(x_f, axis=-1, keepdims=True)
        centered = x_f - mean
        inv_std = lax.rsqrt(jnp.mean(centered * centered, axis=-1, keepdims=True) + EPS)
        hb[chip, part_of(core * (tok // block) + i, block), :] = (centered * inv_std * gain_one + gb_v[1]).astype(BF)
        stat[0, rows, :] = jnp.broadcast_to(mean, (block, 128))
        stat[1, rows, :] = jnp.broadcast_to(inv_std, (block, 128))

    pl.semaphore_wait(barrier, n_dev - 1)

    def chunk(buf, origin, parity, part):
        return buf.at[origin, part_of(parts * parity + part, tok // parts)]

    turns = 2 * parts

    def own_sends(buf, zs, zr, ds, dr):
        copies = []
        for part in range(parts):
            piece = chunk(buf, chip, core, part)
            copies.append(remote(piece, piece, zs.at[2 * part], zr.at[2 * part], right))
            copies.append(remote(piece, piece, zs.at[2 * part + 1], zr.at[2 * part + 1], left))
            copies.append(remote(piece, piece, ds.at[7 * parts + part], dr.at[7 * parts + part], mate))
        return copies

    def event_place(event):
        step = event // turns + 1
        turn = event % turns
        direction = turn % 2
        part = jnp.where(step < 4, turn // 2, turn // 2 + direction * (parts // 2))
        origin = jnp.where(direction == 0, chip + n_chip - step, chip + step) % n_chip
        return step, direction, part, origin

    def last_event(part, direction):
        return 6 * parts + 2 * (part - direction * (parts // 2)) + direction

    def ring_event(ring, event):
        buf, zs, zr, ds, dr = ring
        step, direction, part, origin = event_place(event)
        piece = chunk(buf, origin, core, part)
        remote(piece, piece, zs.at[0], zr.at[event], right).wait_recv()
        onward = jnp.where(step < 3, event + turns, last_event(part, direction))

        @pl.when((step < 3) | ((step == 3) & ((part >= parts // 2) == (direction == 1))))
        def _():
            remote(piece, piece, zs.at[event + turns], zr.at[onward], jnp.where(direction == 0, right, left)).start()

        remote(piece, piece, ds.at[event], dr.at[event], mate).start()

    def ring_service(ring, event):
        @pl.when(event < 7 * parts)
        def _():
            ring_event(ring, event)

    def ring_mate(ring, k, origin):
        buf, zs, zr, ds, dr = ring
        step, ahead = ring_steps(k)
        for part in range(parts):
            event = jnp.where(k == 0, 7 * parts + part, jnp.where(step < 4, turns * (step - 1) + 2 * part + 1 - ahead, last_event(part, part // (parts // 2))))
            piece = chunk(buf, origin, 1 - core, part)
            remote(piece, piece, ds.at[0], dr.at[event], mate).wait_recv()

    def finish_ring(ring):
        buf, zs, zr, ds, dr = ring
        for item in own_sends(*ring):
            item.wait_send()

        @pl.loop(0, 7 * parts)
        def _(event):
            step, direction, part, origin = event_place(event)
            piece = chunk(buf, origin, core, part)

            @pl.when((step < 3) | ((step == 3) & ((part >= parts // 2) == (direction == 1))))
            def _():
                remote(piece, piece, zs.at[event + turns], zr.at[event], right).wait_send()

            remote(piece, piece, ds.at[event], dr.at[event], mate).wait_send()

    h_ring = (hb, hzs, hzr, hds, hdr)
    y_ring = (dyb, yzs, yzr, yds, ydr)
    for item in own_sends(*h_ring):
        item.start()
    pos_sends = [remote(pos_all.at[me], pos_all.at[me], pos_s.at[step], pos_r.at[me], (me + step) % n_dev) for step in range(1, n_dev)]
    for item in pos_sends:
        item.start()
    weight_loads = [
        local(wq_hbm, wt.at[pl.ds(0, q_rows)], w_sem.at[0]),
        local(wk_hbm, wt.at[pl.ds(q_rows, kv_w)], w_sem.at[1]),
        local(wv_hbm, wt.at[pl.ds(q_rows + kv_w, kv_w)], w_sem.at[2]),
    ]
    dkvt[...] = jnp.zeros_like(dkvt)
    bmat[...] = jnp.zeros_like(bmat)
    bmat_far[...] = jnp.zeros_like(bmat_far)
    for f in range(n_far):
        stat_far[f, 0] = jnp.full((1, cols_q), -3e38, F32)
        stat_far[f, 1] = jnp.zeros((1, cols_q), F32)
        stat_far[f, 2] = jnp.zeros((1, cols_q), F32)

    freq = jnp.exp(lax.broadcasted_iota(jnp.int32, (quarter, tok), 0).astype(F32) * (-2.0 * math.log(ROPE_BASE) / (hd // 2)))

    def make_trig(b):
        for t in range(2):
            slot = 2 * b + t

            @pl.when(slot != me)
            def _():
                remote(pos_all.at[slot], pos_all.at[slot], pos_s.at[0], pos_r.at[slot], me).wait_recv()

            angle = pos_all[slot].astype(F32) * freq
            trig[b, 0:quarter, tok * t:tok * t + tok] = jnp.cos(angle)
            trig[b, quarter:2 * quarter, tok * t:tok * t + tok] = jnp.sin(angle)

    def turned(val, cos_t, sin_t):
        u = val[0:quarter]
        w = val[quarter:2 * quarter]
        return [u * cos_t - w * sin_t, w * cos_t + u * sin_t, val[2 * quarter:hd]]

    def eighth(val):
        return val.astype(BF) * jnp.asarray(scale, BF)

    def keys_values(val, cos_t, sin_t):
        return jnp.concatenate(turned(val[0:hd], cos_t, sin_t) + [val[hd:hw]], axis=0).astype(BF)

    lane = lax.broadcasted_iota(jnp.int32, (pair, cols_q), 1)
    row = lax.broadcasted_iota(jnp.int32, (pair, cols_q), 0)
    seen_far = row <= core * tok + lane % tok

    opposite = ring_origin(n_chip - 1)

    def opposite_send(head):
        block = bmat_far.at[n_far - 1, pl.ds(hd, hd), pl.ds(cols_q + tok * head, tok)]
        return remote(block, da_rv.at[2 * core + head % 2], d_s.at[head], d_r.at[2 * core + head % 2], 2 * opposite + head // 2)

    @pl.loop(0, n_chip)
    def _(k):
        for turn in range(parts):
            ring_service(h_ring, parts * k + turn)

        @once(k == 5)
        def _(_):
            for item in own_sends(*y_ring):
                item.start()

        @once(k == 0)
        def _(_):
            for item in loads:
                item.wait()

        b = ring_origin(k)
        ring_mate(h_ring, k, b)
        make_trig(b)

        @once(k == 0)
        def _(_):
            for item in far_loads:
                item.wait()
            cos_t = trig[chip, 0:quarter, part_of(core, tok)]
            sin_t = trig[chip, quarter:2 * quarter, part_of(core, tok)]

            @pl.loop(0, n_far)
            def _(f):
                da_t = dot_t(wt[part_of(f, 2 * hw), :], dy_own[...]).astype(BF)
                q_t = dot_t(wt[part_of(n_far + f, 2 * hw), :], hb[chip, part_of(core, tok), :])
                for head in range(4):
                    part = slice(hd * head, hd * head + hd)
                    at = tok * head
                    bmat_far[f, 0:hd, at:at + tok] = eighth(jnp.concatenate(turned(q_t[part], cos_t, sin_t), axis=0))
                    bmat_far[f, hd:hw, cols_q + at:cols_q + at + tok] = da_t[part]

            for item in weight_loads:
                item.start()

        @once(k == 1)
        def _(_):
            for head in range(4):
                opposite_send(head).start()

        place = part_of(b, pair)
        cos_t = trig[b, 0:quarter, :]
        sin_t = trig[b, quarter:2 * quarter, :]
        flat = dot_t(wi[...], hb[b])
        for head in range(2):
            q_rot = eighth(jnp.concatenate(turned(flat[hd * head:hd * head + hd], cos_t, sin_t), axis=0))
            for t in range(2):
                lane = pair * t + tok * head
                qt[b, :, lane:lane + tok] = q_rot[:, tok * t:tok * t + tok]
        kv_rot = keys_values(flat[hw:2 * hw], cos_t, sin_t)
        kvt[:, place] = kv_rot
        kv[place, :] = kv_rot.T

        @pl.when(b <= chip)
        def _():
            flat_far = dot_t(w_far[...], hb[b])
            for f in range(n_far):
                far_rot = keys_values(flat_far[hw * f:hw * f + hw], cos_t, sin_t)
                kvt_far[f, :, place] = far_rot
                kv_far[f, place, :] = far_rot.T

            @pl.loop(0, n_far)
            def _(f):
                both = dot(kv_far[f, place, :], bmat_far[f])
                s = jnp.where(seen_far | (k > 0), both[:, 0:cols_q], -1e30)
                old = stat_far[f, 0]
                new = jnp.maximum(old, jnp.max(s, axis=0, keepdims=True))
                p = jnp.exp(s - new)
                keep = jnp.exp(old - new)
                stat_far[f, 0] = new
                stat_far[f, 1] = stat_far[f, 1] * keep + jnp.sum(p, axis=0, keepdims=True)
                stat_far[f, 2] = stat_far[f, 2] * keep + jnp.sum(p * both[:, cols_q:2 * cols_q], axis=0, keepdims=True)

    groups = [slice(tile * g, tile * g + tile) for g in range(cols_q // tile)]

    def first_part(b, seen):
        def both_of(rows):
            both = dot(kv[rows, :], bmat[...])
            return both[:, 0:cols_q], both[:, cols_q:2 * cols_q]

        rows = part_of(b, pair)
        s, d_p = both_of(rows)
        s = jnp.where(seen, s, -1e30)
        top = jnp.max(s, axis=0, keepdims=True)
        p = jnp.exp(s - top)
        sbuf[rows, :] = p
        dpbuf[rows, :] = d_p
        mbuf[b] = top

        def step(c, state, chunks=1):
            old, total, weighted = state
            rows = part_of(c, chunks * pair)
            s, d_p = both_of(rows)
            new = jnp.maximum(old, jnp.max(s, axis=0, keepdims=True))
            p = jnp.exp(s - new)
            sbuf[rows, :] = p
            dpbuf[rows, :] = d_p
            for i in range(chunks):
                mbuf[chunks * c + i] = new
            keep = jnp.exp(old - new)
            return new, total * keep + jnp.sum(p, axis=0, keepdims=True), weighted * keep + jnp.sum(p * d_p, axis=0, keepdims=True)

        state = (top, jnp.sum(p, axis=0, keepdims=True), jnp.sum(p * d_p, axis=0, keepdims=True))
        state = lax.fori_loop(0, b // 2, functools.partial(step, chunks=2), state)
        top, total, weighted = lax.fori_loop(2 * (b // 2), b, step, state)
        inv = 1.0 / total
        return top, inv, weighted * inv

    def second_part(b, stats):
        top, inv, row_dot = stats
        adq[...] = jnp.zeros_like(adq)

        def step(c, carry):
            rows = part_of(c, pair)
            factor = jnp.exp(mbuf[c] - top) * inv
            d_k = d_v = None
            for at in groups:
                p = sbuf[rows, at] * factor[:, at]
                p_b = p.astype(BF)
                ds_b = (p * (dpbuf[rows, at] - row_dot[:, at])).astype(BF)
                adq[0:hd, at] += dot(kvt[0:hd, rows], ds_b)
                adq[hd:hw, at] += dot(kvt[hd:hw, rows], p_b)
                more_k = dot_t(bmat[0:hd, at], ds_b)
                more_v = dot_t(bmat[hd:hw, cols_q + at.start:cols_q + at.stop], p_b)
                d_k = more_k if d_k is None else d_k + more_k
                d_v = more_v if d_v is None else d_v + more_v
            dkvt[0:hd, rows] += d_k
            dkvt[hd:hw, rows] += d_v
            return carry

        lax.fori_loop(0, b + 1, step, 0)


    def send_rows(slot):
        cols = part_of(slot, tok)
        return [
            remote(dq_all.at[:, cols], dt_rv.at[own_rows], q_s.at[slot], q_r.at[me], slot),
            remote(at_all.at[:, cols], at_rv.at[own_rows], a_s.at[slot], a_r.at[me], slot),
        ]

    last = 6 * parts

    def serve(event):
        @pl.when((event >= 0) & (event < last))
        def _():
            ring_event(y_ring, event)

    @pl.loop(0, n_chip)
    def _(j):
        k = j - 1

        @pl.when(k == 0)
        def _():
            for turn in range(2):
                ring_event(y_ring, k + turn)

        @pl.when((k % 2 == 1) & (k > 0))
        def _():
            for turn in range(2, parts):
                serve(parts * k + turn)

        b = jnp.where(j == 0, opposite, ring_origin(jnp.maximum(k, 0)))

        @once(k == 1)
        def _(_):
            for item in weight_loads:
                item.wait()

        @pl.loop(0, jnp.where(j == n_chip - 1, 2 + 4 * near, 0))
        def _(early):
            slot = 2 * ring_origin(early // 2) + early % 2

            @pl.when(slot != me)
            def _():
                for item in send_rows(slot):
                    item.start()

        bmat[0:hd, 0:cols_q] = qt[b]

        @once(j == 0)
        def _(_):
            for i in range(4):
                remote(da_rv.at[i], da_rv.at[i], d_s.at[0], d_r.at[i], mate).wait_recv()
                bmat[hd:hw, cols_q + tok * i:cols_q + tok * i + tok] = da_rv[i]

        @once(j > 0)
        def _(_):
            ring_mate(y_ring, k, b)
            da_t = dot_t(woi[...], dyb[b]).astype(BF)
            for t in range(2):
                for head in range(2):
                    at = cols_q + pair * t + tok * head
                    bmat[hd:hw, at:at + tok] = da_t[hd * head:hd * head + hd, tok * t:tok * t + tok]

        stats = first_part(b, row <= (lane // pair) * tok + lane % tok)
        for turn in range(2):
            serve(jnp.where(k < 0, -1, parts * k + 2 + 2 * (k % 2) + turn))
        second_part(b, stats)
        for t in range(2):
            slot = 2 * b + t
            lanes = [slice(pair * t + tok * head, pair * t + tok * head + tok) for head in range(2)]
            a_t = jnp.concatenate([adq[hd:hw, at] for at in lanes], axis=0).astype(BF)
            cos_t = trig[b, 0:quarter, tok * t:tok * t + tok]
            sin_t = trig[b, quarter:2 * quarter, tok * t:tok * t + tok]
            dq_t = jnp.concatenate([piece for at in lanes for piece in turned(adq[0:hd, at] * scale, cos_t, -sin_t)], axis=0).astype(BF)
            at_all[:, part_of(slot, tok)] = a_t
            dq_all[:, part_of(slot, tok)] = dq_t

            @pl.when(slot == me)
            def _():
                at_rv[own_rows, :] = a_t
                dt_rv[own_rows, :] = dq_t

        @pl.when((k % 2 == 0) & (k >= 0))
        def _():
            for turn in range(2):
                serve(parts * (k + 1) + turn)

    far = [ring_origin(k) for k in range(n_chip - 1, 0, -1)]
    targets = [2 * c + p for c in far for p in range(2)] + [mate]
    near_targets = targets[-1 - 4 * near:]
    swap = remote(dkvt.at[part_of(1 - core, hd)], kv_rv, x_s, x_r, mate)
    swap.start()
    w_sends = [remote(dwt.at[pl.ds(0, hw), part_of(t, tok)], gw_hbm.at[own_rows], w_s.at[t], w_r.at[me], t) for t in targets]

    def columns(rows_all, buf, cols):
        acc = jnp.zeros((rows_all.shape[0], tile), F32)
        for s in range(n_chip):
            acc += dot(rows_all[:, pair * s:pair * s + pair], buf[s, :, cols])
        return acc

    def q_columns(i):
        cols = part_of(far[i] if i < n_chip - 1 else chip, pair)
        dwt[0:hw, cols] = columns(dq_all, hb, cols)
        for item in w_sends[max(2 * i - 2, 0):2 * i]:
            item.start()

    for i in range(FIRST + 1):
        q_columns(i)

    swap.wait_recv()
    mine = part_of(core, hd)
    g_rows = pl.ds(pl.multiple_of(q_rows + core * kv_w + chip * hd, hd), hd)
    for t in range(n_chip):
        cols = slice(pair * t, pair * t + pair)
        g = dkvt[mine, cols] + kv_rv[:, cols]
        cos_t = jnp.where(core == 0, trig[t, 0:quarter, :], 1.0)
        sin_t = jnp.where(core == 0, trig[t, quarter:2 * quarter, :], 0.0)
        g_b = jnp.concatenate(turned(g, cos_t, -sin_t), axis=0).astype(BF)
        kv_mine[2 * t] = g_b[:, 0:tok]
        kv_mine[2 * t + 1] = g_b[:, tok:pair]
        kv_row[:, cols] = g_b
    dt_rv[g_rows, :] = kv_mine[me]
    kv_sends = [remote(kv_mine.at[t], dt_rv.at[g_rows], kv_s.at[t], kv_r.at[me], t) for t in targets]
    for item in kv_sends:
        item.start()
    for i in range(FIRST + 1, n_chip):
        q_columns(i)
    w_sends[-1].start()
    w_own = local(dwt.at[pl.ds(0, hw), part_of(me, tok)], gw_hbm.at[own_rows], loc_sem.at[0])
    w_own.start()
    for t in range(width // tile):
        cols = slice(tile * t, tile * t + tile)
        dwt[hw:hw + hd, cols] = columns(kv_row, hb, cols)
    wk_own = local(dwt.at[pl.ds(hw, hd), part_of(me, tok)], gw_hbm.at[g_rows], loc_sem.at[1])
    wk_own.start()
    wk_sends = [remote(dwt.at[pl.ds(hw, hd), part_of(t, tok)], gw_hbm.at[g_rows], wk_s.at[t], wk_r.at[me], t) for t in targets]
    for item in wk_sends[0:HELD]:
        item.start()

    @pl.loop(last, 7 * parts)
    def _(event):
        ring_event(y_ring, event)

    ring_mate(y_ring, n_chip - 1, opposite)
    for t in range(width // tile):
        cols = slice(tile * t, tile * t + tile)
        dwo[:, cols] = columns(at_all, dyb, cols)
    store_wo = local(dwo, gwo_hbm, out_sem.at[0])
    store_wo.start()
    finish_ring(y_ring)
    wo_loads = [local(wo_hbm.at[pl.ds(pair * t, pair)], dyb.at[t], wo_sem.at[t]) for t in range(n_chip)]
    for item in wo_loads:
        item.start()

    @pl.loop(0, n_far)
    def _(f):
        c_far = ring_origin(2 * near + 1 + f)
        cos_t = trig[chip, 0:quarter, part_of(core, tok)]
        sin_t = trig[chip, quarter:2 * quarter, part_of(core, tok)]
        top = stat_far[f, 0]
        inv = 1.0 / stat_far[f, 1]
        row_dot = stat_far[f, 2] * inv

        def add_chunk(c, diagonal, chunks=1):
            rows = part_of(c, chunks * pair)
            for at in groups:
                keys = kv_far[f, rows, :]
                s = dot(keys, bmat_far[f, :, at])
                d_p = dot(keys, bmat_far[f, :, cols_q + at.start:cols_q + at.stop])
                if diagonal:
                    s = jnp.where(seen_far[:, at], s, -1e30)
                p = jnp.exp(s - top[:, at]) * inv[:, at]
                p_b = p.astype(BF)
                ds_b = (p * (d_p - row_dot[:, at])).astype(BF)
                d_q = dot(kvt_far[f, 0:hd, rows], ds_b)
                d_a = dot(kvt_far[f, hd:hw, rows], p_b)
                adq[0:hd, at] = d_q if diagonal else adq[0:hd, at] + d_q
                adq[hd:hw, at] = d_a if diagonal else adq[hd:hw, at] + d_a

        add_chunk(chip, True)

        @pl.loop(0, chip // 2)
        def _(c):
            add_chunk(c, False, 2)

        @pl.when(chip % 2 == 1)
        def _():
            add_chunk(chip - 1, False)

        for head in range(4):
            at = slice(tok * head, tok * head + tok)
            place = pl.ds(pl.multiple_of(c_far * 2 * hw + hd * head, hd), hd)
            at_rv[place, :] = adq[hd:hw, at].astype(BF)
            dt_rv[place, :] = jnp.concatenate(turned(adq[0:hd, at] * scale, cos_t, -sin_t), axis=0).astype(BF)

    for t in near_targets:
        remote(at_all.at[:, pl.ds(0, tok)], at_rv.at[part_of(t, hw)], a_s.at[t], a_r.at[t], t).wait_recv()
    for item in wo_loads:
        item.wait()
    for t in range(q_rows // tok):
        a_nat[:, tok * t:tok * t + tok] = at_rv[tok * t:tok * t + tok, :].T
    for t in range(width // tile):
        cols = slice(tile * t, tile * t + tile)
        prod = jnp.zeros((tok, tile), F32)
        for s in range(n_chip):
            prod += dot(a_nat[:, pair * s:pair * s + pair], dyb[s, :, cols])
        out_v[:, cols] = (x_v[:, cols].astype(F32) + prod).astype(BF)
    store_out = local(out_v, out_hbm, out_sem.at[1])
    store_out.start()

    def kv_place(t):
        return pl.ds(pl.multiple_of(q_rows + (t % 2) * kv_w + (t // 2) * hd, hd), hd)

    for t in near_targets:
        remote(dq_all.at[:, pl.ds(0, tok)], dt_rv.at[part_of(t, hw)], q_s.at[t], q_r.at[t], t).wait_recv()
    for t in targets:
        remote(kv_mine.at[0], dt_rv.at[kv_place(t)], kv_s.at[t], kv_r.at[t], t).wait_recv()
    swap.wait_send()
    for t in range(n_rows // tok):
        d_nat[:, tok * t:tok * t + tok] = dt_rv[tok * t:tok * t + tok, :].T

    mean = stat[0, :, 0:1]
    inv_std = stat[1, :, 0:1]
    dh = dkvt
    for t in range(width // tile):
        cols = slice(tile * t, tile * t + tile)
        acc = jnp.zeros((tok, tile), F32)
        for s in range(n_rows // tile):
            acc += dot(d_nat[:, tile * s:tile * s + tile], wt[tile * s:tile * s + tile, cols])
        dh[:, cols] = acc
        gg_st[0, :, cols] = jnp.sum(acc * ((x_v[:, cols].astype(F32) - mean) * inv_std), axis=0, keepdims=True)
        gg_st[1, :, cols] = jnp.sum(acc, axis=0, keepdims=True)
    g_swap = remote(gg_st.at[1 - core], gg_mx, g_s.at[n_chip], g_r.at[n_chip], mate)
    g_swap.start()
    g_swap.wait_recv()
    gg_my[...] = jnp.where(core == 0, gg_st[0], gg_st[1]) + gg_mx[...]
    gg_rv[chip] = gg_my[...]
    g_sends = [remote(gg_my, gg_rv.at[chip], g_s.at[c], g_r.at[chip], 2 * c + core) for c in far]
    for item in g_sends + wk_sends[HELD:]:
        item.start()

    grad_hat = dh[...] * gain_one
    x_hat = (x_v[...].astype(F32) - mean) * inv_std
    mean_one = jnp.mean(grad_hat, axis=-1, keepdims=True)
    mean_two = jnp.mean(grad_hat * x_hat, axis=-1, keepdims=True)
    store_out.wait()
    out_v[...] = (dy_own[...].astype(F32) + inv_std * (grad_hat - mean_one - x_hat * mean_two)).astype(BF)
    store_gx = local(out_v, gx_hbm, out_sem.at[2])
    store_gx.start()

    for c in far:
        remote(gg_my, gg_rv.at[c], g_s.at[c], g_r.at[c], 2 * c + core).wait_recv()
    sums = gg_rv[0]
    for c in range(1, n_chip):
        sums = sums + gg_rv[c]
    gg_out[core] = sums
    g_swap_out = remote(gg_out.at[core], gg_out.at[core], g_s.at[n_chip + 1], g_r.at[n_chip + 1], mate)
    g_swap_out.start()
    remote(gg_out.at[core], gg_out.at[1 - core], g_s.at[n_chip + 1], g_r.at[n_chip + 1], mate).wait_recv()
    store_gg = local(gg_out, gg_hbm, out_sem.at[3])
    store_gg.start()

    finish_ring(h_ring)
    for item in pos_sends + [g_swap, g_swap_out] + [opposite_send(head) for head in range(4)]:
        item.wait_send()
    for t in near_targets:
        remote(at_all.at[:, pl.ds(0, tok)], at_rv.at[pl.ds(0, hw)], a_s.at[t], a_r.at[t], t).wait_send()
        remote(dq_all.at[:, pl.ds(0, tok)], dt_rv.at[pl.ds(0, hw)], q_s.at[t], q_r.at[t], t).wait_send()
    for item in kv_sends + w_sends + g_sends + wk_sends:
        item.wait_send()
    for t in targets:
        remote(dwt.at[pl.ds(0, hw), part_of(t, tok)], gw_hbm.at[part_of(t, hw)], w_s.at[t], w_r.at[t], t).wait_recv()
        remote(dwt.at[pl.ds(hw, hd), part_of(t, tok)], gw_hbm.at[kv_place(t)], wk_s.at[t], wk_r.at[t], t).wait_recv()
    for item in (w_own, wk_own, store_wo, store_gx, store_gg):
        item.wait()


def settle_kernel(q_rows, kv_w, out_i, gx_i, gw_i, gwo_i, gg_i, out_o, gx_o, gq_o, gk_o, gv_o, gwo_o, gain_o, bias_o, b_act, b_q, b_kv, b_o, b_gg, sem_in, sem_out, sem_gg):
    half_q = q_rows // 2
    half_o = gwo_i.shape[0] // 2
    moves = [(out_i, b_act.at[0], out_o), (gx_i, b_act.at[1], gx_o)]
    for t in range(2):
        moves.append((gw_i.at[pl.ds(half_q * t, half_q)], b_q.at[t], gq_o.at[pl.ds(half_q * t, half_q)]))
        moves.append((gwo_i.at[pl.ds(half_o * t, half_o)], b_o.at[t], gwo_o.at[pl.ds(half_o * t, half_o)]))
    moves.append((gw_i.at[pl.ds(q_rows, kv_w)], b_kv.at[0], gk_o))
    moves.append((gw_i.at[pl.ds(q_rows + kv_w, kv_w)], b_kv.at[1], gv_o))
    loads = [pltpu.make_async_copy(src, mid, sem_in.at[i]) for i, (src, mid, _) in enumerate(moves)]
    stores = [pltpu.make_async_copy(mid, dst, sem_out.at[i]) for i, (_, mid, dst) in enumerate(moves)]
    load_gg = pltpu.make_async_copy(gg_i, b_gg, sem_gg)
    load_gg.start()
    for item in loads:
        item.start()
    for load, store in zip(loads, stores):
        load.wait()
        store.start()
    load_gg.wait()
    gain_o[...] = b_gg[0, 0]
    bias_o[...] = b_gg[1, 0]
    for item in stores:
        item.wait()


def solution(mesh):
    n_dev = mesh.shape['cp']

    def device_step(x_act, d_out, positions, ln_gain, ln_bias, w_query, w_key, w_value, w_out):
        tok, width = x_act.shape[1], x_act.shape[2]
        q_heads, hd = w_query.shape[1], w_query.shape[2]
        kv_heads = w_key.shape[1]
        q_w, kv_w = q_heads * hd, kv_heads * hd
        n_rows = q_w + 2 * kv_w
        seq = n_dev * tok
        hw = 2 * hd

        def flat_weight(w):
            return jnp.transpose(w, (1, 2, 0)).reshape(-1, width)

        hbm = pl.BlockSpec(memory_space=pltpu.HBM)
        vmem = pl.BlockSpec(memory_space=pltpu.VMEM)
        dma = pltpu.SemaphoreType.DMA
        n_chip = n_dev // 2
        n_far = n_chip - 1 - 2 * NEAR
        pair = 2 * tok
        scratch = [
            pltpu.VMEM((n_chip, pair, width), BF),
            pltpu.VMEM((n_chip, pair, width), BF),
            pltpu.VMEM((n_rows, width), BF),
            pltpu.VMEM((2 * hw, width), BF),
            pltpu.VMEM((hw, width), BF),
            pltpu.VMEM((n_far * hw, width), BF),
            pltpu.VMEM((n_dev, 1, tok), jnp.int32),
            pltpu.VMEM((n_chip, hd // 2, pair), F32),
            pltpu.VMEM((n_chip, hd, 2 * pair), BF),
            pltpu.VMEM((hw, seq), BF),
            pltpu.VMEM((seq, hw), BF),
            pltpu.VMEM((n_far, hw, seq), BF),
            pltpu.VMEM((n_far, seq, hw), BF),
            pltpu.VMEM((n_far, hw, 4 * pair), BF),
            pltpu.VMEM((n_far, 3, 1, 2 * pair), F32),
            pltpu.VMEM((hw, 4 * pair), BF),
            pltpu.VMEM((4, hd, tok), BF),
            pltpu.VMEM((seq, 2 * pair), F32),
            pltpu.VMEM((seq, 2 * pair), F32),
            pltpu.VMEM((n_chip, 1, 2 * pair), F32),
            pltpu.VMEM((hw, 2 * pair), F32),
            pltpu.VMEM((hw, seq), F32),
            pltpu.VMEM((hd, seq), F32),
            pltpu.VMEM((n_dev, hd, tok), BF),
            pltpu.VMEM((hd, seq), BF),
            pltpu.VMEM((hw, width), F32),
            pltpu.VMEM((hw + hd, width), F32),
            pltpu.VMEM((hw, seq), BF),
            pltpu.VMEM((hw, seq), BF),
            pltpu.VMEM((q_w, tok), BF),
            pltpu.VMEM((n_rows, tok), BF),
            pltpu.VMEM((tok, q_w), BF),
            pltpu.VMEM((tok, n_rows), BF),
            pltpu.VMEM((tok, width), BF),
            pltpu.VMEM((tok, width), BF),
            pltpu.VMEM((2, 1, width), F32),
            pltpu.VMEM((2, tok, 128), F32),
            pltpu.VMEM((tok, width), BF),
            pltpu.VMEM((2, 1, width), F32),
            pltpu.VMEM((1, width), F32),
            pltpu.VMEM((1, width), F32),
            pltpu.VMEM((n_chip, 1, width), F32),
            pltpu.VMEM((2, 1, width), F32),
            dma((10,)), dma((4 * n_far,)), dma((n_chip,)), dma((3,)), dma((4,)), dma((2,)),
        ] + [dma((9 * PARTS,)), dma((7 * PARTS,)), dma((8 * PARTS,)), dma((8 * PARTS,))] * 2 + [dma((4,))] * 2 + [dma((n_dev,))] * 6 + [dma] * 2 + [dma((n_dev,))] * 8
        out, gx, gw, gwo, gg = pl.pallas_call(
            functools.partial(block_kernel, n_dev, hd, kv_w, NEAR, PARTS),
            out_shape=(
                jax.ShapeDtypeStruct((tok, width), BF),
                jax.ShapeDtypeStruct((tok, width), BF),
                jax.ShapeDtypeStruct((n_rows, tok), F32),
                jax.ShapeDtypeStruct((hw, width), F32),
                jax.ShapeDtypeStruct((2, 1, width), F32),
            ),
            in_specs=[hbm] * 9,
            out_specs=(hbm,) * 5,
            scratch_shapes=scratch,
            compiler_params=pltpu.CompilerParams(collective_id=0, has_side_effects=True, vmem_limit_bytes=67043328),
            name='attn_block',
        )(
            x_act.reshape(tok, width), d_out.reshape(tok, width), positions.reshape(1, tok),
            ln_gain.reshape(1, width), ln_bias.reshape(1, width),
            flat_weight(w_query), flat_weight(w_key), flat_weight(w_value), w_out,
        )

        out, gx, gq, gk, gv, gwo, gain, bias = pl.pallas_call(
            functools.partial(settle_kernel, q_w, kv_w),
            out_shape=(
                jax.ShapeDtypeStruct((tok, width), BF),
                jax.ShapeDtypeStruct((tok, width), BF),
                jax.ShapeDtypeStruct((q_w, tok), F32),
                jax.ShapeDtypeStruct((kv_w, tok), F32),
                jax.ShapeDtypeStruct((kv_w, tok), F32),
                jax.ShapeDtypeStruct((hw, width), F32),
                jax.ShapeDtypeStruct((width,), F32),
                jax.ShapeDtypeStruct((width,), F32),
            ),
            in_specs=[hbm] * 5,
            out_specs=(hbm,) * 6 + (vmem,) * 2,
            scratch_shapes=[
                pltpu.VMEM((2, tok, width), BF),
                pltpu.VMEM((2, q_w // 2, tok), F32),
                pltpu.VMEM((2, kv_w, tok), F32),
                pltpu.VMEM((2, hw // 2, width), F32),
                pltpu.VMEM((2, 1, width), F32),
                dma((8,)), dma((8,)), dma,
            ],
            name='settle',
        )(out, gx, gw, gwo, gg)

        def rows_out(block, heads):
            return jnp.transpose(block.reshape(heads, hd, tok), (2, 0, 1))

        return (
            out.reshape(1, tok, width), gx.reshape(1, tok, width),
            rows_out(gq, q_heads), rows_out(gk, kv_heads), rows_out(gv, kv_heads),
            gwo, gain, bias,
        )

    return jax.shard_map(device_step, mesh=mesh, in_specs=(P('dp', 'cp', None), P('dp', 'cp', None), P('dp', 'cp'), P(None), P(None), P(None, None, None), P(None, None, None), P(None, None, None), P(None, None)), out_specs=(P('dp', 'cp', None), P('dp', 'cp', None), P(('dp', 'cp'), None, None), P(('dp', 'cp'), None, None), P(('dp', 'cp'), None, None), P(('dp', 'cp'), None), P('dp'), P('dp')), check_vma=False)
```

```python
import functools
import math

import jax
import jax.numpy as jnp
from jax import lax
from jax.experimental import pallas as pl
from jax.experimental.pallas import tpu as pltpu
from jax.sharding import PartitionSpec as P

EPS = 1e-5
ROPE_BASE = 10000.0
MESH = pl.DeviceIdType.MESH
BF = jnp.bfloat16
F32 = jnp.float32
NEAR = 1
PARTS = 4
FIRST = 1
HELD = 4


def dot(lhs, rhs):
    return jnp.dot(lhs, rhs, preferred_element_type=F32)


def col_sum(val):
    return jnp.sum(val, axis=0, keepdims=True)


def col_max(val):
    return jnp.max(val, axis=0, keepdims=True)


def row_mean(val):
    return jnp.mean(val, axis=-1, keepdims=True)


def dot_t(lhs, rhs):
    return lax.dot_general(lhs, rhs, (((1,), (1,)), ((), ())), preferred_element_type=F32)


def block_kernel(
    n_dev, hd, kv_w, near, parts,
    x_hbm, dy_hbm, pos_hbm, gain_hbm, bias_hbm, wq_hbm, wk_hbm, wv_hbm, wo_hbm,
    out_hbm, gx_hbm, gw_hbm, gwo_hbm, gg_hbm,
    hb, dyb, wt, wi, woi, w_far, pos_all, trig,
    qt, kvt, kv, kvt_far, kv_far, bmat_far, stat_far, bmat, da_rv, sbuf, dpbuf, mbuf, adq, dkvt, kv_rv, kv_mine, kv_row,
    dwo, dwt, at_all, dq_all, at_rv, dt_rv, a_nat, d_nat, x_v, dy_own, gb_v, stat, out_v, gg_st, gg_mx, gg_my, gg_rv, gg_out,
    in_sem, far_sem, wo_sem, w_sem, out_sem, loc_sem,
    hzs, hzr, hds, hdr, yzs, yzr, yds, ydr,
    d_s, d_r, pos_s, pos_r, a_s, a_r, q_s, q_r, x_s, x_r, kv_s, kv_r, w_s, w_r, wk_s, wk_r, g_s, g_r,
):
    tok, width = x_v.shape
    n_chip = n_dev // 2
    pair = 2 * tok
    me = lax.axis_index('cp')
    chip = me // 2
    core = me % 2
    right = 2 * ((chip + 1) % n_chip) + core
    left = 2 * ((chip + n_chip - 1) % n_chip) + core
    mate = 2 * chip + 1 - core
    q_rows = wq_hbm.shape[0]
    n_rows = q_rows + 2 * kv_w
    hw = 2 * hd
    quarter = hd // 4
    tile = 256
    scale = hd ** -0.5
    cols_q = 2 * pair
    n_far = n_chip - 1 - 2 * near

    def remote(src, dst, send, recv, target):
        return pltpu.make_async_remote_copy(src_ref=src, dst_ref=dst, send_sem=send, recv_sem=recv, device_id={'cp': target}, device_id_type=MESH)

    def local(src, dst, sem):
        return pltpu.make_async_copy(src, dst, sem)

    def part_of(i, size):
        return pl.ds(pl.multiple_of(i * size, size), size)

    def once(cond):
        return pl.loop(0, jnp.where(cond, 1, 0))

    def ring_steps(k):
        step = (k + 1) // 2
        return step, k % 2

    def ring_origin(k):
        step, ahead = ring_steps(k)
        return jnp.where(ahead == 1, chip + n_chip - step, chip + step) % n_chip

    own = (chip, part_of(core, tok))
    first_loads = [
        local(x_hbm, x_v, in_sem.at[0]),
        local(gain_hbm, gb_v.at[0], in_sem.at[1]),
        local(bias_hbm, gb_v.at[1], in_sem.at[2]),
        local(pos_hbm, pos_all.at[me], in_sem.at[3]),
    ]
    for item in first_loads:
        item.start()
    barrier = pltpu.get_barrier_semaphore()
    for step in range(1, n_dev):
        pl.semaphore_signal(barrier, inc=1, device_id={'cp': (me + step) % n_dev}, device_id_type=MESH)
    own_rows = part_of(me, hw)
    kv_rows = part_of(chip, hd)
    loads = [
        local(wq_hbm.at[own_rows], wi.at[pl.ds(0, hw)], in_sem.at[4]),
        local(wk_hbm.at[kv_rows], wi.at[pl.ds(hw, hd)], in_sem.at[5]),
        local(wv_hbm.at[kv_rows], wi.at[pl.ds(hw + hd, hd)], in_sem.at[6]),
        local(wo_hbm.at[own_rows], woi, in_sem.at[7]),
        local(dy_hbm, dyb.at[own], in_sem.at[8]),
        local(dy_hbm, dy_own, in_sem.at[9]),
    ]
    far_loads = []
    for f in range(n_far):
        far_rows = part_of(ring_origin(2 * near + 1 + f), hd)
        loads.append(local(wk_hbm.at[far_rows], w_far.at[pl.ds(hw * f, hd)], far_sem.at[2 * f]))
        loads.append(local(wv_hbm.at[far_rows], w_far.at[pl.ds(hw * f + hd, hd)], far_sem.at[2 * f + 1]))
        far_wo = part_of(ring_origin(2 * near + 1 + f), 2 * hw)
        far_loads.append(local(wo_hbm.at[far_wo], wt.at[pl.ds(2 * hw * f, 2 * hw)], far_sem.at[2 * n_far + f]))
        far_loads.append(local(wq_hbm.at[far_wo], wt.at[pl.ds(2 * hw * (n_far + f), 2 * hw)], far_sem.at[3 * n_far + f]))
    for item in loads + far_loads:
        item.start()

    for item in first_loads:
        item.wait()
    gain_one = 1.0 + gb_v[0]
    block = 16

    @pl.loop(0, tok // block)
    def _(i):
        rows = part_of(i, block)
        x_f = x_v[rows, :].astype(F32)
        mean = row_mean(x_f)
        centered = x_f - mean
        inv_std = lax.rsqrt(row_mean(centered * centered) + EPS)
        hb[chip, part_of(core * (tok // block) + i, block), :] = (centered * inv_std * gain_one + gb_v[1]).astype(BF)
        stat[0, rows, :] = jnp.broadcast_to(mean, (block, 128))
        stat[1, rows, :] = jnp.broadcast_to(inv_std, (block, 128))

    pl.semaphore_wait(barrier, n_dev - 1)

    def chunk(buf, origin, parity, part):
        return buf.at[origin, part_of(parts * parity + part, tok // parts)]

    turns = 2 * parts

    def own_sends(buf, zs, zr, ds, dr):
        copies = []
        for part in range(parts):
            piece = chunk(buf, chip, core, part)
            copies.append(remote(piece, piece, zs.at[2 * part], zr.at[2 * part], right))
            copies.append(remote(piece, piece, zs.at[2 * part + 1], zr.at[2 * part + 1], left))
            copies.append(remote(piece, piece, ds.at[7 * parts + part], dr.at[7 * parts + part], mate))
        return copies

    def event_place(event):
        step = event // turns + 1
        turn = event % turns
        direction = turn % 2
        part = jnp.where(step < 4, turn // 2, turn // 2 + direction * (parts // 2))
        origin = jnp.where(direction == 0, chip + n_chip - step, chip + step) % n_chip
        return step, direction, part, origin

    def last_event(part, direction):
        return 6 * parts + 2 * (part - direction * (parts // 2)) + direction

    def ring_event(ring, event):
        buf, zs, zr, ds, dr = ring
        step, direction, part, origin = event_place(event)
        piece = chunk(buf, origin, core, part)
        remote(piece, piece, zs.at[0], zr.at[event], right).wait_recv()
        onward = jnp.where(step < 3, event + turns, last_event(part, direction))

        @pl.when((step < 3) | ((step == 3) & ((part >= parts // 2) == (direction == 1))))
        def _():
            remote(piece, piece, zs.at[event + turns], zr.at[onward], jnp.where(direction == 0, right, left)).start()

        remote(piece, piece, ds.at[event], dr.at[event], mate).start()

    def ring_service(ring, event):
        @pl.when(event < 7 * parts)
        def _():
            ring_event(ring, event)

    def ring_mate(ring, k, origin):
        buf, zs, zr, ds, dr = ring
        step, ahead = ring_steps(k)
        for part in range(parts):
            event = jnp.where(k == 0, 7 * parts + part, jnp.where(step < 4, turns * (step - 1) + 2 * part + 1 - ahead, last_event(part, part // (parts // 2))))
            piece = chunk(buf, origin, 1 - core, part)
            remote(piece, piece, ds.at[0], dr.at[event], mate).wait_recv()

    def finish_ring(ring):
        buf, zs, zr, ds, dr = ring
        for item in own_sends(*ring):
            item.wait_send()

        @pl.loop(0, 7 * parts)
        def _(event):
            step, direction, part, origin = event_place(event)
            piece = chunk(buf, origin, core, part)

            @pl.when((step < 3) | ((step == 3) & ((part >= parts // 2) == (direction == 1))))
            def _():
                remote(piece, piece, zs.at[event + turns], zr.at[event], right).wait_send()

            remote(piece, piece, ds.at[event], dr.at[event], mate).wait_send()

    h_ring = (hb, hzs, hzr, hds, hdr)
    y_ring = (dyb, yzs, yzr, yds, ydr)
    for item in own_sends(*h_ring):
        item.start()
    pos_sends = [remote(pos_all.at[me], pos_all.at[me], pos_s.at[step], pos_r.at[me], (me + step) % n_dev) for step in range(1, n_dev)]
    for item in pos_sends:
        item.start()
    weight_loads = [
        local(wq_hbm, wt.at[pl.ds(0, q_rows)], w_sem.at[0]),
        local(wk_hbm, wt.at[pl.ds(q_rows, kv_w)], w_sem.at[1]),
        local(wv_hbm, wt.at[pl.ds(q_rows + kv_w, kv_w)], w_sem.at[2]),
    ]
    dkvt[...] = jnp.zeros_like(dkvt)
    bmat[...] = jnp.zeros_like(bmat)
    bmat_far[...] = jnp.zeros_like(bmat_far)
    for f in range(n_far):
        stat_far[f, 0] = jnp.full((1, cols_q), -3e38, F32)
        stat_far[f, 1] = jnp.zeros((1, cols_q), F32)
        stat_far[f, 2] = jnp.zeros((1, cols_q), F32)

    freq = jnp.exp(lax.broadcasted_iota(jnp.int32, (quarter, tok), 0).astype(F32) * (-2.0 * math.log(ROPE_BASE) / (hd // 2)))

    def make_trig(b):
        for t in range(2):
            slot = 2 * b + t

            @pl.when(slot != me)
            def _():
                remote(pos_all.at[slot], pos_all.at[slot], pos_s.at[0], pos_r.at[slot], me).wait_recv()

            angle = pos_all[slot].astype(F32) * freq
            trig[b, 0:quarter, tok * t:tok * t + tok] = jnp.cos(angle)
            trig[b, quarter:2 * quarter, tok * t:tok * t + tok] = jnp.sin(angle)

    def turned(val, cos_t, sin_t):
        u = val[0:quarter]
        w = val[quarter:2 * quarter]
        return [u * cos_t - w * sin_t, w * cos_t + u * sin_t, val[2 * quarter:hd]]

    def eighth(val):
        return val.astype(BF) * jnp.asarray(scale, BF)

    def keys_values(val, cos_t, sin_t):
        return jnp.concatenate(turned(val[0:hd], cos_t, sin_t) + [val[hd:hw]], axis=0).astype(BF)

    lane = lax.broadcasted_iota(jnp.int32, (pair, cols_q), 1)
    row = lax.broadcasted_iota(jnp.int32, (pair, cols_q), 0)
    seen_far = row <= core * tok + lane % tok

    opposite = ring_origin(n_chip - 1)

    def opposite_send(head):
        block = bmat_far.at[n_far - 1, pl.ds(hd, hd), pl.ds(cols_q + tok * head, tok)]
        return remote(block, da_rv.at[2 * core + head % 2], d_s.at[head], d_r.at[2 * core + head % 2], 2 * opposite + head // 2)

    @pl.loop(0, n_chip)
    def _(k):
        for turn in range(parts):
            ring_service(h_ring, parts * k + turn)

        @once(k == 5)
        def _(_):
            for item in own_sends(*y_ring):
                item.start()

        @once(k == 0)
        def _(_):
            for item in loads:
                item.wait()

        b = ring_origin(k)
        ring_mate(h_ring, k, b)
        make_trig(b)

        @once(k == 0)
        def _(_):
            for item in far_loads:
                item.wait()
            cos_t = trig[chip, 0:quarter, part_of(core, tok)]
            sin_t = trig[chip, quarter:2 * quarter, part_of(core, tok)]

            @pl.loop(0, n_far)
            def _(f):
                da_t = dot_t(wt[part_of(f, 2 * hw), :], dy_own[...]).astype(BF)
                q_t = dot_t(wt[part_of(n_far + f, 2 * hw), :], hb[chip, part_of(core, tok), :])
                for head in range(4):
                    part = slice(hd * head, hd * head + hd)
                    at = tok * head
                    bmat_far[f, 0:hd, at:at + tok] = eighth(jnp.concatenate(turned(q_t[part], cos_t, sin_t), axis=0))
                    bmat_far[f, hd:hw, cols_q + at:cols_q + at + tok] = da_t[part]

            for item in weight_loads:
                item.start()

        @once(k == 1)
        def _(_):
            for head in range(4):
                opposite_send(head).start()

        place = part_of(b, pair)
        cos_t = trig[b, 0:quarter, :]
        sin_t = trig[b, quarter:2 * quarter, :]
        flat = dot_t(wi[...], hb[b])
        for head in range(2):
            q_rot = eighth(jnp.concatenate(turned(flat[hd * head:hd * head + hd], cos_t, sin_t), axis=0))
            for t in range(2):
                lane = pair * t + tok * head
                qt[b, :, lane:lane + tok] = q_rot[:, tok * t:tok * t + tok]
        kv_rot = keys_values(flat[hw:2 * hw], cos_t, sin_t)
        kvt[:, place] = kv_rot
        kv[place, :] = kv_rot.T

        @pl.when(b <= chip)
        def _():
            flat_far = dot_t(w_far[...], hb[b])
            for f in range(n_far):
                far_rot = keys_values(flat_far[hw * f:hw * f + hw], cos_t, sin_t)
                kvt_far[f, :, place] = far_rot
                kv_far[f, place, :] = far_rot.T

            @pl.loop(0, n_far)
            def _(f):
                both = dot(kv_far[f, place, :], bmat_far[f])
                s = jnp.where(seen_far | (k > 0), both[:, 0:cols_q], -1e30)
                old = stat_far[f, 0]
                new = jnp.maximum(old, col_max(s))
                p = jnp.exp(s - new)
                keep = jnp.exp(old - new)
                stat_far[f, 0] = new
                stat_far[f, 1] = stat_far[f, 1] * keep + col_sum(p)
                stat_far[f, 2] = stat_far[f, 2] * keep + col_sum(p * both[:, cols_q:2 * cols_q])

    groups = [slice(tile * g, tile * g + tile) for g in range(cols_q // tile)]

    def first_part(b, seen):
        def both_of(rows):
            both = dot(kv[rows, :], bmat[...])
            return both[:, 0:cols_q], both[:, cols_q:2 * cols_q]

        rows = part_of(b, pair)
        s, d_p = both_of(rows)
        s = jnp.where(seen, s, -1e30)
        top = col_max(s)
        p = jnp.exp(s - top)
        sbuf[rows, :] = p
        dpbuf[rows, :] = d_p
        mbuf[b] = top

        def step(c, state, chunks=1):
            old, total, weighted = state
            rows = part_of(c, chunks * pair)
            s, d_p = both_of(rows)
            new = jnp.maximum(old, col_max(s))
            p = jnp.exp(s - new)
            sbuf[rows, :] = p
            dpbuf[rows, :] = d_p
            for i in range(chunks):
                mbuf[chunks * c + i] = new
            keep = jnp.exp(old - new)
            return new, total * keep + col_sum(p), weighted * keep + col_sum(p * d_p)

        state = (top, col_sum(p), col_sum(p * d_p))
        state = lax.fori_loop(0, b // 2, functools.partial(step, chunks=2), state)
        top, total, weighted = lax.fori_loop(2 * (b // 2), b, step, state)
        inv = 1.0 / total
        return top, inv, weighted * inv

    def second_part(b, stats):
        top, inv, row_dot = stats
        adq[...] = jnp.zeros_like(adq)

        def step(c, carry):
            rows = part_of(c, pair)
            factor = jnp.exp(mbuf[c] - top) * inv
            d_k = d_v = None
            for at in groups:
                p = sbuf[rows, at] * factor[:, at]
                p_b = p.astype(BF)
                ds_b = (p * (dpbuf[rows, at] - row_dot[:, at])).astype(BF)
                adq[0:hd, at] += dot(kvt[0:hd, rows], ds_b)
                adq[hd:hw, at] += dot(kvt[hd:hw, rows], p_b)
                more_k = dot_t(bmat[0:hd, at], ds_b)
                more_v = dot_t(bmat[hd:hw, cols_q + at.start:cols_q + at.stop], p_b)
                d_k = more_k if d_k is None else d_k + more_k
                d_v = more_v if d_v is None else d_v + more_v
            dkvt[0:hd, rows] += d_k
            dkvt[hd:hw, rows] += d_v
            return carry

        lax.fori_loop(0, b + 1, step, 0)


    def send_rows(slot):
        cols = part_of(slot, tok)
        return [
            remote(dq_all.at[:, cols], dt_rv.at[own_rows], q_s.at[slot], q_r.at[me], slot),
            remote(at_all.at[:, cols], at_rv.at[own_rows], a_s.at[slot], a_r.at[me], slot),
        ]

    last = 6 * parts

    def serve(event):
        @pl.when(event < last)
        def _():
            ring_event(y_ring, event)

    @pl.loop(0, n_chip)
    def _(j):
        k = j - 1

        @pl.when((k % 2 == 1) & (k > 1))
        def _():
            for turn in range(2, parts):
                serve(parts * k + turn)

        b = jnp.where(j == 0, opposite, ring_origin(jnp.maximum(k, 0)))

        @once(k == 1)
        def _(_):
            for item in weight_loads:
                item.wait()

        @pl.loop(0, jnp.where(j == n_chip - 1, 2 + 4 * near, 0))
        def _(early):
            slot = 2 * ring_origin(early // 2) + early % 2

            @pl.when(slot != me)
            def _():
                for item in send_rows(slot):
                    item.start()

        bmat[0:hd, 0:cols_q] = qt[b]

        @once(j == 0)
        def _(_):
            for i in range(4):
                remote(da_rv.at[i], da_rv.at[i], d_s.at[0], d_r.at[i], mate).wait_recv()
                bmat[hd:hw, cols_q + tok * i:cols_q + tok * i + tok] = da_rv[i]

        @once(j > 0)
        def _(_):
            ring_mate(y_ring, k, b)
            da_t = dot_t(woi[...], dyb[b]).astype(BF)
            for t in range(2):
                for head in range(2):
                    at = cols_q + pair * t + tok * head
                    bmat[hd:hw, at:at + tok] = da_t[hd * head:hd * head + hd, tok * t:tok * t + tok]

        stats = first_part(b, row <= (lane // pair) * tok + lane % tok)
        for turn in range(2):
            serve(jnp.where(k < 1, parts * j, parts * k + 2 + 2 * (k % 2)) + turn)
        second_part(b, stats)
        for t in range(2):
            slot = 2 * b + t
            lanes = [slice(pair * t + tok * head, pair * t + tok * head + tok) for head in range(2)]
            a_t = jnp.concatenate([adq[hd:hw, at] for at in lanes], axis=0).astype(BF)
            cos_t = trig[b, 0:quarter, tok * t:tok * t + tok]
            sin_t = trig[b, quarter:2 * quarter, tok * t:tok * t + tok]
            dq_t = jnp.concatenate([piece for at in lanes for piece in turned(adq[0:hd, at] * scale, cos_t, -sin_t)], axis=0).astype(BF)
            at_all[:, part_of(slot, tok)] = a_t
            dq_all[:, part_of(slot, tok)] = dq_t

            @pl.when(slot == me)
            def _():
                at_rv[own_rows, :] = a_t
                dt_rv[own_rows, :] = dq_t

        @pl.when((k % 2 == 0) | (j == 0))
        def _():
            for turn in range(2):
                serve(parts * j + jnp.where(k < 1, 2, 0) + turn)

    far = [ring_origin(k) for k in range(n_chip - 1, 0, -1)]
    targets = [2 * c + p for c in far for p in range(2)] + [mate]
    near_targets = targets[-1 - 4 * near:]
    swap = remote(dkvt.at[part_of(1 - core, hd)], kv_rv, x_s, x_r, mate)
    swap.start()
    w_sends = [remote(dwt.at[pl.ds(0, hw), part_of(t, tok)], gw_hbm.at[own_rows], w_s.at[t], w_r.at[me], t) for t in targets]

    def columns(rows_all, buf, cols):
        acc = jnp.zeros((rows_all.shape[0], tile), F32)
        for s in range(n_chip):
            acc += dot(rows_all[:, pair * s:pair * s + pair], buf[s, :, cols])
        return acc

    def q_columns(i):
        cols = part_of(far[i] if i < n_chip - 1 else chip, pair)
        dwt[0:hw, cols] = columns(dq_all, hb, cols)
        for item in w_sends[max(2 * i - 2, 0):2 * i]:
            item.start()

    for i in range(FIRST + 1):
        q_columns(i)

    swap.wait_recv()
    mine = part_of(core, hd)
    g_rows = pl.ds(pl.multiple_of(q_rows + core * kv_w + chip * hd, hd), hd)
    for t in range(n_chip):
        cols = slice(pair * t, pair * t + pair)
        g = dkvt[mine, cols] + kv_rv[:, cols]
        cos_t = jnp.where(core == 0, trig[t, 0:quarter, :], 1.0)
        sin_t = jnp.where(core == 0, trig[t, quarter:2 * quarter, :], 0.0)
        g_b = jnp.concatenate(turned(g, cos_t, -sin_t), axis=0).astype(BF)
        kv_mine[2 * t] = g_b[:, 0:tok]
        kv_mine[2 * t + 1] = g_b[:, tok:pair]
        kv_row[:, cols] = g_b
    dt_rv[g_rows, :] = kv_mine[me]
    kv_sends = [remote(kv_mine.at[t], dt_rv.at[g_rows], kv_s.at[t], kv_r.at[me], t) for t in targets]
    for item in kv_sends:
        item.start()
    for i in range(FIRST + 1, n_chip):
        q_columns(i)
    w_sends[-1].start()
    w_own = local(dwt.at[pl.ds(0, hw), part_of(me, tok)], gw_hbm.at[own_rows], loc_sem.at[0])
    w_own.start()
    for t in range(width // tile):
        cols = slice(tile * t, tile * t + tile)
        dwt[hw:hw + hd, cols] = columns(kv_row, hb, cols)
    wk_own = local(dwt.at[pl.ds(hw, hd), part_of(me, tok)], gw_hbm.at[g_rows], loc_sem.at[1])
    wk_own.start()
    wk_sends = [remote(dwt.at[pl.ds(hw, hd), part_of(t, tok)], gw_hbm.at[g_rows], wk_s.at[t], wk_r.at[me], t) for t in targets]
    for item in wk_sends[0:HELD]:
        item.start()

    @pl.loop(last, 7 * parts)
    def _(event):
        ring_event(y_ring, event)

    ring_mate(y_ring, n_chip - 1, opposite)
    for t in range(width // tile):
        cols = slice(tile * t, tile * t + tile)
        dwo[:, cols] = columns(at_all, dyb, cols)
    store_wo = local(dwo, gwo_hbm, out_sem.at[0])
    store_wo.start()
    finish_ring(y_ring)
    wo_loads = [local(wo_hbm.at[pl.ds(pair * t, pair)], dyb.at[t], wo_sem.at[t]) for t in range(n_chip)]
    for item in wo_loads:
        item.start()

    @pl.loop(0, n_far)
    def _(f):
        c_far = ring_origin(2 * near + 1 + f)
        cos_t = trig[chip, 0:quarter, part_of(core, tok)]
        sin_t = trig[chip, quarter:2 * quarter, part_of(core, tok)]
        top = stat_far[f, 0]
        inv = 1.0 / stat_far[f, 1]
        row_dot = stat_far[f, 2] * inv

        def add_chunk(c, diagonal, chunks=1):
            rows = part_of(c, chunks * pair)
            for at in groups:
                keys = kv_far[f, rows, :]
                s = dot(keys, bmat_far[f, :, at])
                d_p = dot(keys, bmat_far[f, :, cols_q + at.start:cols_q + at.stop])
                if diagonal:
                    s = jnp.where(seen_far[:, at], s, -1e30)
                p = jnp.exp(s - top[:, at]) * inv[:, at]
                p_b = p.astype(BF)
                ds_b = (p * (d_p - row_dot[:, at])).astype(BF)
                d_q = dot(kvt_far[f, 0:hd, rows], ds_b)
                d_a = dot(kvt_far[f, hd:hw, rows], p_b)
                adq[0:hd, at] = d_q if diagonal else adq[0:hd, at] + d_q
                adq[hd:hw, at] = d_a if diagonal else adq[hd:hw, at] + d_a

        add_chunk(chip, True)

        @pl.loop(0, chip // 2)
        def _(c):
            add_chunk(c, False, 2)

        @pl.when(chip % 2 == 1)
        def _():
            add_chunk(chip - 1, False)

        for head in range(4):
            at = slice(tok * head, tok * head + tok)
            place = pl.ds(pl.multiple_of(c_far * 2 * hw + hd * head, hd), hd)
            at_rv[place, :] = adq[hd:hw, at].astype(BF)
            dt_rv[place, :] = jnp.concatenate(turned(adq[0:hd, at] * scale, cos_t, -sin_t), axis=0).astype(BF)

    for t in near_targets:
        remote(at_all.at[:, pl.ds(0, tok)], at_rv.at[part_of(t, hw)], a_s.at[t], a_r.at[t], t).wait_recv()
    for item in wo_loads:
        item.wait()
    for t in range(q_rows // tok):
        a_nat[:, tok * t:tok * t + tok] = at_rv[tok * t:tok * t + tok, :].T
    for t in range(width // tile):
        cols = slice(tile * t, tile * t + tile)
        prod = jnp.zeros((tok, tile), F32)
        for s in range(n_chip):
            prod += dot(a_nat[:, pair * s:pair * s + pair], dyb[s, :, cols])
        out_v[:, cols] = (x_v[:, cols].astype(F32) + prod).astype(BF)
    store_out = local(out_v, out_hbm, out_sem.at[1])
    store_out.start()

    def kv_place(t):
        return pl.ds(pl.multiple_of(q_rows + (t % 2) * kv_w + (t // 2) * hd, hd), hd)

    for t in near_targets:
        remote(dq_all.at[:, pl.ds(0, tok)], dt_rv.at[part_of(t, hw)], q_s.at[t], q_r.at[t], t).wait_recv()
    for t in targets:
        remote(kv_mine.at[0], dt_rv.at[kv_place(t)], kv_s.at[t], kv_r.at[t], t).wait_recv()
    swap.wait_send()
    for t in range(n_rows // tok):
        d_nat[:, tok * t:tok * t + tok] = dt_rv[tok * t:tok * t + tok, :].T

    mean = stat[0, :, 0:1]
    inv_std = stat[1, :, 0:1]
    dh = dkvt
    for t in range(width // tile):
        cols = slice(tile * t, tile * t + tile)
        acc = jnp.zeros((tok, tile), F32)
        for s in range(n_rows // tile):
            acc += dot(d_nat[:, tile * s:tile * s + tile], wt[tile * s:tile * s + tile, cols])
        dh[:, cols] = acc
        gg_st[0, :, cols] = col_sum(acc * ((x_v[:, cols].astype(F32) - mean) * inv_std))
        gg_st[1, :, cols] = col_sum(acc)
    g_swap = remote(gg_st.at[1 - core], gg_mx, g_s.at[n_chip], g_r.at[n_chip], mate)
    g_swap.start()
    g_swap.wait_recv()
    gg_my[...] = jnp.where(core == 0, gg_st[0], gg_st[1]) + gg_mx[...]
    gg_rv[chip] = gg_my[...]
    g_sends = [remote(gg_my, gg_rv.at[chip], g_s.at[c], g_r.at[chip], 2 * c + core) for c in far]
    for item in g_sends + wk_sends[HELD:]:
        item.start()

    grad_hat = dh[...] * gain_one
    x_hat = (x_v[...].astype(F32) - mean) * inv_std
    mean_one = row_mean(grad_hat)
    mean_two = row_mean(grad_hat * x_hat)
    store_out.wait()
    out_v[...] = (dy_own[...].astype(F32) + inv_std * (grad_hat - mean_one - x_hat * mean_two)).astype(BF)
    store_gx = local(out_v, gx_hbm, out_sem.at[2])
    store_gx.start()

    for c in far:
        remote(gg_my, gg_rv.at[c], g_s.at[c], g_r.at[c], 2 * c + core).wait_recv()
    sums = gg_rv[0]
    for c in range(1, n_chip):
        sums = sums + gg_rv[c]
    gg_out[core] = sums
    g_swap_out = remote(gg_out.at[core], gg_out.at[core], g_s.at[n_chip + 1], g_r.at[n_chip + 1], mate)
    g_swap_out.start()
    remote(gg_out.at[core], gg_out.at[1 - core], g_s.at[n_chip + 1], g_r.at[n_chip + 1], mate).wait_recv()
    store_gg = local(gg_out, gg_hbm, out_sem.at[3])
    store_gg.start()

    finish_ring(h_ring)
    for item in pos_sends + [g_swap, g_swap_out] + [opposite_send(head) for head in range(4)]:
        item.wait_send()
    for t in near_targets:
        remote(at_all.at[:, pl.ds(0, tok)], at_rv.at[pl.ds(0, hw)], a_s.at[t], a_r.at[t], t).wait_send()
        remote(dq_all.at[:, pl.ds(0, tok)], dt_rv.at[pl.ds(0, hw)], q_s.at[t], q_r.at[t], t).wait_send()
    for item in kv_sends + w_sends + g_sends + wk_sends:
        item.wait_send()
    for t in targets:
        remote(dwt.at[pl.ds(0, hw), part_of(t, tok)], gw_hbm.at[part_of(t, hw)], w_s.at[t], w_r.at[t], t).wait_recv()
        remote(dwt.at[pl.ds(hw, hd), part_of(t, tok)], gw_hbm.at[kv_place(t)], wk_s.at[t], wk_r.at[t], t).wait_recv()
    for item in (w_own, wk_own, store_wo, store_gx, store_gg):
        item.wait()


def settle_kernel(q_rows, kv_w, out_i, gx_i, gw_i, gwo_i, gg_i, out_o, gx_o, gq_o, gk_o, gv_o, gwo_o, gain_o, bias_o, b_act, b_q, b_kv, b_o, b_gg, sem_in, sem_out, sem_gg):
    half_q = q_rows // 2
    half_o = gwo_i.shape[0] // 2
    moves = [(out_i, b_act.at[0], out_o), (gx_i, b_act.at[1], gx_o)]
    for t in range(2):
        moves.append((gw_i.at[pl.ds(half_q * t, half_q)], b_q.at[t], gq_o.at[pl.ds(half_q * t, half_q)]))
        moves.append((gwo_i.at[pl.ds(half_o * t, half_o)], b_o.at[t], gwo_o.at[pl.ds(half_o * t, half_o)]))
    moves.append((gw_i.at[pl.ds(q_rows, kv_w)], b_kv.at[0], gk_o))
    moves.append((gw_i.at[pl.ds(q_rows + kv_w, kv_w)], b_kv.at[1], gv_o))
    loads = [pltpu.make_async_copy(src, mid, sem_in.at[i]) for i, (src, mid, _) in enumerate(moves)]
    stores = [pltpu.make_async_copy(mid, dst, sem_out.at[i]) for i, (_, mid, dst) in enumerate(moves)]
    load_gg = pltpu.make_async_copy(gg_i, b_gg, sem_gg)
    load_gg.start()
    for item in loads:
        item.start()
    for load, store in zip(loads, stores):
        load.wait()
        store.start()
    load_gg.wait()
    gain_o[...] = b_gg[0, 0]
    bias_o[...] = b_gg[1, 0]
    for item in stores:
        item.wait()


def solution(mesh):
    n_dev = mesh.shape['cp']

    def device_step(x_act, d_out, positions, ln_gain, ln_bias, w_query, w_key, w_value, w_out):
        tok, width = x_act.shape[1], x_act.shape[2]
        q_heads, hd = w_query.shape[1], w_query.shape[2]
        kv_heads = w_key.shape[1]
        q_w, kv_w = q_heads * hd, kv_heads * hd
        n_rows = q_w + 2 * kv_w
        seq = n_dev * tok
        hw = 2 * hd

        def flat_weight(w):
            return jnp.transpose(w, (1, 2, 0)).reshape(-1, width)

        hbm = pl.BlockSpec(memory_space=pltpu.HBM)
        vmem = pl.BlockSpec(memory_space=pltpu.VMEM)
        dma = pltpu.SemaphoreType.DMA
        n_chip = n_dev // 2
        n_far = n_chip - 1 - 2 * NEAR
        pair = 2 * tok
        scratch = [
            pltpu.VMEM((n_chip, pair, width), BF),
            pltpu.VMEM((n_chip, pair, width), BF),
            pltpu.VMEM((n_rows, width), BF),
            pltpu.VMEM((2 * hw, width), BF),
            pltpu.VMEM((hw, width), BF),
            pltpu.VMEM((n_far * hw, width), BF),
            pltpu.VMEM((n_dev, 1, tok), jnp.int32),
            pltpu.VMEM((n_chip, hd // 2, pair), F32),
            pltpu.VMEM((n_chip, hd, 2 * pair), BF),
            pltpu.VMEM((hw, seq), BF),
            pltpu.VMEM((seq, hw), BF),
            pltpu.VMEM((n_far, hw, seq), BF),
            pltpu.VMEM((n_far, seq, hw), BF),
            pltpu.VMEM((n_far, hw, 4 * pair), BF),
            pltpu.VMEM((n_far, 3, 1, 2 * pair), F32),
            pltpu.VMEM((hw, 4 * pair), BF),
            pltpu.VMEM((4, hd, tok), BF),
            pltpu.VMEM((seq, 2 * pair), F32),
            pltpu.VMEM((seq, 2 * pair), F32),
            pltpu.VMEM((n_chip, 1, 2 * pair), F32),
            pltpu.VMEM((hw, 2 * pair), F32),
            pltpu.VMEM((hw, seq), F32),
            pltpu.VMEM((hd, seq), F32),
            pltpu.VMEM((n_dev, hd, tok), BF),
            pltpu.VMEM((hd, seq), BF),
            pltpu.VMEM((hw, width), F32),
            pltpu.VMEM((hw + hd, width), F32),
            pltpu.VMEM((hw, seq), BF),
            pltpu.VMEM((hw, seq), BF),
            pltpu.VMEM((q_w, tok), BF),
            pltpu.VMEM((n_rows, tok), BF),
            pltpu.VMEM((tok, q_w), BF),
            pltpu.VMEM((tok, n_rows), BF),
            pltpu.VMEM((tok, width), BF),
            pltpu.VMEM((tok, width), BF),
            pltpu.VMEM((2, 1, width), F32),
            pltpu.VMEM((2, tok, 128), F32),
            pltpu.VMEM((tok, width), BF),
            pltpu.VMEM((2, 1, width), F32),
            pltpu.VMEM((1, width), F32),
            pltpu.VMEM((1, width), F32),
            pltpu.VMEM((n_chip, 1, width), F32),
            pltpu.VMEM((2, 1, width), F32),
            dma((10,)), dma((4 * n_far,)), dma((n_chip,)), dma((3,)), dma((4,)), dma((2,)),
        ] + [dma((9 * PARTS,)), dma((7 * PARTS,)), dma((8 * PARTS,)), dma((8 * PARTS,))] * 2 + [dma((4,))] * 2 + [dma((n_dev,))] * 6 + [dma] * 2 + [dma((n_dev,))] * 8
        out, gx, gw, gwo, gg = pl.pallas_call(
            functools.partial(block_kernel, n_dev, hd, kv_w, NEAR, PARTS),
            out_shape=(
                jax.ShapeDtypeStruct((tok, width), BF),
                jax.ShapeDtypeStruct((tok, width), BF),
                jax.ShapeDtypeStruct((n_rows, tok), F32),
                jax.ShapeDtypeStruct((hw, width), F32),
                jax.ShapeDtypeStruct((2, 1, width), F32),
            ),
            in_specs=[hbm] * 9,
            out_specs=(hbm,) * 5,
            scratch_shapes=scratch,
            compiler_params=pltpu.CompilerParams(collective_id=0, has_side_effects=True, vmem_limit_bytes=67043328),
            name='attn_block',
        )(
            x_act.reshape(tok, width), d_out.reshape(tok, width), positions.reshape(1, tok),
            ln_gain.reshape(1, width), ln_bias.reshape(1, width),
            flat_weight(w_query), flat_weight(w_key), flat_weight(w_value), w_out,
        )

        out, gx, gq, gk, gv, gwo, gain, bias = pl.pallas_call(
            functools.partial(settle_kernel, q_w, kv_w),
            out_shape=(
                jax.ShapeDtypeStruct((tok, width), BF),
                jax.ShapeDtypeStruct((tok, width), BF),
                jax.ShapeDtypeStruct((q_w, tok), F32),
                jax.ShapeDtypeStruct((kv_w, tok), F32),
                jax.ShapeDtypeStruct((kv_w, tok), F32),
                jax.ShapeDtypeStruct((hw, width), F32),
                jax.ShapeDtypeStruct((width,), F32),
                jax.ShapeDtypeStruct((width,), F32),
            ),
            in_specs=[hbm] * 5,
            out_specs=(hbm,) * 6 + (vmem,) * 2,
            scratch_shapes=[
                pltpu.VMEM((2, tok, width), BF),
                pltpu.VMEM((2, q_w // 2, tok), F32),
                pltpu.VMEM((2, kv_w, tok), F32),
                pltpu.VMEM((2, hw // 2, width), F32),
                pltpu.VMEM((2, 1, width), F32),
                dma((8,)), dma((8,)), dma,
            ],
            name='settle',
        )(out, gx, gw, gwo, gg)

        def rows_out(block, heads):
            return jnp.transpose(block.reshape(heads, hd, tok), (2, 0, 1))

        return (
            out.reshape(1, tok, width), gx.reshape(1, tok, width),
            rows_out(gq, q_heads), rows_out(gk, kv_heads), rows_out(gv, kv_heads),
            gwo, gain, bias,
        )

    return jax.shard_map(device_step, mesh=mesh, in_specs=(P('dp', 'cp', None), P('dp', 'cp', None), P('dp', 'cp'), P(None), P(None), P(None, None, None), P(None, None, None), P(None, None, None), P(None, None)), out_specs=(P('dp', 'cp', None), P('dp', 'cp', None), P(('dp', 'cp'), None, None), P(('dp', 'cp'), None, None), P(('dp', 'cp'), None, None), P(('dp', 'cp'), None), P('dp'), P('dp')), check_vma=False)
```

```python
import functools
import math

import jax
import jax.numpy as jnp
from jax import lax
from jax.experimental import pallas as pl
from jax.experimental.pallas import tpu as pltpu
from jax.sharding import PartitionSpec as P

EPS = 1e-5
ROPE_BASE = 10000.0
MESH = pl.DeviceIdType.MESH
BF = jnp.bfloat16
F32 = jnp.float32
NEAR = 0
PARTS = 4
FIRST = 1
HELD = 4


def dot(lhs, rhs):
    return jnp.dot(lhs, rhs, preferred_element_type=F32)


def col_sum(val):
    return jnp.sum(val, axis=0, keepdims=True)


def col_max(val):
    return jnp.max(val, axis=0, keepdims=True)


def row_mean(val):
    return jnp.mean(val, axis=-1, keepdims=True)


def dot_t(lhs, rhs):
    return lax.dot_general(lhs, rhs, (((1,), (1,)), ((), ())), preferred_element_type=F32)


def block_kernel(
    n_dev, hd, kv_w, near, parts,
    x_hbm, dy_hbm, pos_hbm, gain_hbm, bias_hbm, wq_hbm, wk_hbm, wv_hbm, wo_hbm,
    out_hbm, gx_hbm, gw_hbm, gwo_hbm, gg_hbm,
    hb, dyb, wt, wi, woi, pos_all, trig,
    qt, kvt, kv, kvt_far, kv_far, bmat_far, stat_far, bmat, da_rv, sbuf, dpbuf, mbuf, adq, dkvt, kv_rv, kv_mine, kv_row,
    dwo, dwt, at_all, dq_all, at_rv, dt_rv, a_nat, d_nat, x_v, dy_own, gb_v, stat, out_v, gg_st, gg_mx, gg_my, gg_rv, gg_out,
    in_sem, far_sem, wo_sem, w_sem, out_sem, loc_sem,
    hzs, hzr, hds, hdr, yzs, yzr, yds, ydr,
    d_s, d_r, pos_s, pos_r, a_s, a_r, q_s, q_r, x_s, x_r, kv_s, kv_r, w_s, w_r, wk_s, wk_r, g_s, g_r,
):
    tok, width = x_v.shape
    n_chip = n_dev // 2
    pair = 2 * tok
    me = lax.axis_index('cp')
    chip = me // 2
    core = me % 2
    right = 2 * ((chip + 1) % n_chip) + core
    left = 2 * ((chip + n_chip - 1) % n_chip) + core
    mate = 2 * chip + 1 - core
    q_rows = wq_hbm.shape[0]
    n_rows = q_rows + 2 * kv_w
    hw = 2 * hd
    quarter = hd // 4
    tile = 256
    scale = hd ** -0.5
    cols_q = 2 * pair
    n_far = n_chip - 1 - 2 * near

    def remote(src, dst, send, recv, target):
        return pltpu.make_async_remote_copy(src_ref=src, dst_ref=dst, send_sem=send, recv_sem=recv, device_id={'cp': target}, device_id_type=MESH)

    def local(src, dst, sem):
        return pltpu.make_async_copy(src, dst, sem)

    def part_of(i, size):
        return pl.ds(pl.multiple_of(i * size, size), size)

    def once(cond):
        return pl.loop(0, jnp.where(cond, 1, 0))

    def ring_steps(k):
        step = (k + 1) // 2
        return step, k % 2

    def ring_origin(k):
        step, ahead = ring_steps(k)
        return jnp.where(ahead == 1, chip + n_chip - step, chip + step) % n_chip

    own = (chip, part_of(core, tok))
    first_loads = [
        local(x_hbm, x_v, in_sem.at[0]),
        local(gain_hbm, gb_v.at[0], in_sem.at[1]),
        local(bias_hbm, gb_v.at[1], in_sem.at[2]),
        local(pos_hbm, pos_all.at[me], in_sem.at[3]),
    ]
    for item in first_loads:
        item.start()
    barrier = pltpu.get_barrier_semaphore()
    for step in range(1, n_dev):
        pl.semaphore_signal(barrier, inc=1, device_id={'cp': (me + step) % n_dev}, device_id_type=MESH)
    own_rows = part_of(me, hw)
    kv_rows = part_of(chip, hd)
    loads = [
        local(wq_hbm.at[own_rows], wi.at[pl.ds(0, hw)], in_sem.at[4]),
        local(wk_hbm.at[kv_rows], wi.at[pl.ds(hw, hd)], in_sem.at[5]),
        local(wv_hbm.at[kv_rows], wi.at[pl.ds(hw + hd, hd)], in_sem.at[6]),
        local(wo_hbm.at[own_rows], woi, in_sem.at[7]),
        local(dy_hbm, dyb.at[own], in_sem.at[8]),
        local(dy_hbm, dy_own, in_sem.at[9]),
    ]
    far_loads = []
    far_first = n_far * 2 * hw
    for f in range(n_far):
        c_far = ring_origin(2 * near + 1 + f)
        far_rows = part_of(c_far, hd)
        loads.append(local(wk_hbm.at[far_rows], wt.at[pl.ds(far_first + hw * f, hd)], far_sem.at[f]))
        loads.append(local(wv_hbm.at[far_rows], wt.at[pl.ds(far_first + hw * f + hd, hd)], far_sem.at[n_far + f]))
        far_w = part_of(c_far, pair)
        far_loads.append(local(wo_hbm.at[far_w], wt.at[pl.ds(pair * f, pair)], far_sem.at[2 * n_far + f]))
        far_loads.append(local(wq_hbm.at[far_w], dyb.at[c_far], far_sem.at[3 * n_far + f]))
    for item in loads + far_loads:
        item.start()

    for item in first_loads:
        item.wait()
    gain_one = 1.0 + gb_v[0]
    block = 16

    @pl.loop(0, tok // block)
    def _(i):
        rows = part_of(i, block)
        x_f = x_v[rows, :].astype(F32)
        mean = row_mean(x_f)
        centered = x_f - mean
        inv_std = lax.rsqrt(row_mean(centered * centered) + EPS)
        hb[chip, part_of(core * (tok // block) + i, block), :] = (centered * inv_std * gain_one + gb_v[1]).astype(BF)
        stat[0, rows, :] = jnp.broadcast_to(mean, (block, 128))
        stat[1, rows, :] = jnp.broadcast_to(inv_std, (block, 128))

    pl.semaphore_wait(barrier, n_dev - 1)

    def chunk(buf, origin, parity, part):
        return buf.at[origin, part_of(parts * parity + part, tok // parts)]

    turns = 2 * parts

    def own_sends(buf, zs, zr, ds, dr):
        copies = []
        for part in range(parts):
            piece = chunk(buf, chip, core, part)
            copies.append(remote(piece, piece, zs.at[2 * part], zr.at[2 * part], right))
            copies.append(remote(piece, piece, zs.at[2 * part + 1], zr.at[2 * part + 1], left))
            copies.append(remote(piece, piece, ds.at[7 * parts + part], dr.at[7 * parts + part], mate))
        return copies

    def event_place(event):
        step = event // turns + 1
        turn = event % turns
        direction = turn % 2
        part = jnp.where(step < 4, turn // 2, turn // 2 + direction * (parts // 2))
        origin = jnp.where(direction == 0, chip + n_chip - step, chip + step) % n_chip
        return step, direction, part, origin

    def last_event(part, direction):
        return 6 * parts + 2 * (part - direction * (parts // 2)) + direction

    def ring_event(ring, event):
        buf, zs, zr, ds, dr = ring
        step, direction, part, origin = event_place(event)
        piece = chunk(buf, origin, core, part)
        remote(piece, piece, zs.at[0], zr.at[event], right).wait_recv()
        onward = jnp.where(step < 3, event + turns, last_event(part, direction))

        @pl.when((step < 3) | ((step == 3) & ((part >= parts // 2) == (direction == 1))))
        def _():
            remote(piece, piece, zs.at[event + turns], zr.at[onward], jnp.where(direction == 0, right, left)).start()

        remote(piece, piece, ds.at[event], dr.at[event], mate).start()

    def ring_service(ring, event):
        @pl.when(event < 7 * parts)
        def _():
            ring_event(ring, event)

    def ring_mate(ring, k, origin):
        buf, zs, zr, ds, dr = ring
        step, ahead = ring_steps(k)
        for part in range(parts):
            event = jnp.where(k == 0, 7 * parts + part, jnp.where(step < 4, turns * (step - 1) + 2 * part + 1 - ahead, last_event(part, part // (parts // 2))))
            piece = chunk(buf, origin, 1 - core, part)
            remote(piece, piece, ds.at[0], dr.at[event], mate).wait_recv()

    def finish_ring(ring):
        buf, zs, zr, ds, dr = ring
        for item in own_sends(*ring):
            item.wait_send()

        @pl.loop(0, 7 * parts)
        def _(event):
            step, direction, part, origin = event_place(event)
            piece = chunk(buf, origin, core, part)

            @pl.when((step < 3) | ((step == 3) & ((part >= parts // 2) == (direction == 1))))
            def _():
                remote(piece, piece, zs.at[event + turns], zr.at[event], right).wait_send()

            remote(piece, piece, ds.at[event], dr.at[event], mate).wait_send()

    h_ring = (hb, hzs, hzr, hds, hdr)
    y_ring = (dyb, yzs, yzr, yds, ydr)
    for item in own_sends(*h_ring):
        item.start()
    pos_sends = [remote(pos_all.at[me], pos_all.at[me], pos_s.at[step], pos_r.at[me], (me + step) % n_dev) for step in range(1, n_dev)]
    for item in pos_sends:
        item.start()
    weight_loads = [
        local(wq_hbm, wt.at[pl.ds(0, q_rows)], w_sem.at[0]),
        local(wk_hbm, wt.at[pl.ds(q_rows, kv_w)], w_sem.at[1]),
        local(wv_hbm, wt.at[pl.ds(q_rows + kv_w, kv_w)], w_sem.at[2]),
    ]
    dkvt[...] = jnp.zeros_like(dkvt)
    bmat[...] = jnp.zeros_like(bmat)
    bmat_far[...] = jnp.zeros_like(bmat_far)
    for f in range(n_far):
        stat_far[f, 0] = jnp.full((1, cols_q), -3e38, F32)
        stat_far[f, 1] = jnp.zeros((1, cols_q), F32)
        stat_far[f, 2] = jnp.zeros((1, cols_q), F32)

    freq = jnp.exp(lax.broadcasted_iota(jnp.int32, (quarter, tok), 0).astype(F32) * (-2.0 * math.log(ROPE_BASE) / (hd // 2)))

    def make_trig(b):
        for t in range(2):
            slot = 2 * b + t

            @pl.when(slot != me)
            def _():
                remote(pos_all.at[slot], pos_all.at[slot], pos_s.at[0], pos_r.at[slot], me).wait_recv()

            angle = pos_all[slot].astype(F32) * freq
            trig[b, 0:quarter, tok * t:tok * t + tok] = jnp.cos(angle)
            trig[b, quarter:2 * quarter, tok * t:tok * t + tok] = jnp.sin(angle)

    def turned(val, cos_t, sin_t):
        u = val[0:quarter]
        w = val[quarter:2 * quarter]
        return [u * cos_t - w * sin_t, w * cos_t + u * sin_t, val[2 * quarter:hd]]

    def eighth(val):
        return val.astype(BF) * jnp.asarray(scale, BF)

    def keys_values(val, cos_t, sin_t):
        return jnp.concatenate(turned(val[0:hd], cos_t, sin_t) + [val[hd:hw]], axis=0).astype(BF)

    lane = lax.broadcasted_iota(jnp.int32, (pair, cols_q), 1)
    row = lax.broadcasted_iota(jnp.int32, (pair, cols_q), 0)
    seen_far = row <= core * tok + lane % tok

    opposite = ring_origin(n_chip - 1)

    def opposite_send(head):
        block = bmat_far.at[n_far - 1, pl.ds(hd, hd), pl.ds(cols_q + tok * head, tok)]
        return remote(block, da_rv.at[2 * core + head % 2], d_s.at[head], d_r.at[2 * core + head % 2], 2 * opposite + head // 2)

    @pl.loop(0, n_chip)
    def _(k):
        for turn in range(2):
            ring_service(h_ring, parts * k + turn)

        @pl.when(k % 2 == 1)
        def _():
            ring_service(h_ring, parts * k + 2)


        @once(k == 5)
        def _(_):
            for item in own_sends(*y_ring):
                item.start()

        @once(k == 0)
        def _(_):
            for item in loads:
                item.wait()

        b = ring_origin(k)
        ring_mate(h_ring, k, b)
        make_trig(b)

        @once(k == 0)
        def _(_):
            for item in far_loads:
                item.wait()
            cos_t = trig[chip, 0:quarter, part_of(core, tok)]
            sin_t = trig[chip, quarter:2 * quarter, part_of(core, tok)]

            @pl.loop(0, n_far)
            def _(f):
                da_t = dot_t(wt[part_of(f, 2 * hw), :], dy_own[...]).astype(BF)
                q_t = dot_t(dyb[ring_origin(2 * near + 1 + f)], hb[chip, part_of(core, tok), :])
                for head in range(4):
                    part = slice(hd * head, hd * head + hd)
                    at = tok * head
                    bmat_far[f, 0:hd, at:at + tok] = eighth(jnp.concatenate(turned(q_t[part], cos_t, sin_t), axis=0))
                    bmat_far[f, hd:hw, cols_q + at:cols_q + at + tok] = da_t[part]

        @once(k == 1)
        def _(_):
            for head in range(4):
                opposite_send(head).start()

        place = part_of(b, pair)
        cos_t = trig[b, 0:quarter, :]
        sin_t = trig[b, quarter:2 * quarter, :]
        flat = dot_t(wi[...], hb[b])
        for head in range(2):
            q_rot = eighth(jnp.concatenate(turned(flat[hd * head:hd * head + hd], cos_t, sin_t), axis=0))
            for t in range(2):
                lane = pair * t + tok * head
                qt[b, :, lane:lane + tok] = q_rot[:, tok * t:tok * t + tok]
        kv_rot = keys_values(flat[hw:2 * hw], cos_t, sin_t)
        kvt[:, place] = kv_rot
        kv[place, :] = kv_rot.T

        @pl.when(k % 2 == 0)
        def _():
            ring_service(h_ring, parts * k + 2)

        ring_service(h_ring, parts * k + parts - 1)

        @pl.when(b <= chip)
        def _():
            flat_far = dot_t(wt[far_first:far_first + n_far * hw, :], hb[b])
            for f in range(n_far):
                far_rot = keys_values(flat_far[hw * f:hw * f + hw], cos_t, sin_t)
                kvt_far[f, :, place] = far_rot
                kv_far[f, place, :] = far_rot.T

            @pl.loop(0, n_far)
            def _(f):
                both = dot(kv_far[f, place, :], bmat_far[f])
                s = jnp.where(seen_far | (k > 0), both[:, 0:cols_q], -1e30)
                old = stat_far[f, 0]
                new = jnp.maximum(old, col_max(s))
                p = jnp.exp(s - new)
                keep = jnp.exp(old - new)
                stat_far[f, 0] = new
                stat_far[f, 1] = stat_far[f, 1] * keep + col_sum(p)
                stat_far[f, 2] = stat_far[f, 2] * keep + col_sum(p * both[:, cols_q:2 * cols_q])

    groups = [slice(tile * g, tile * g + tile) for g in range(cols_q // tile)]

    def first_part(b, seen):
        def both_of(rows):
            both = dot(kv[rows, :], bmat[...])
            return both[:, 0:cols_q], both[:, cols_q:2 * cols_q]

        rows = part_of(b, pair)
        s, d_p = both_of(rows)
        s = jnp.where(seen, s, -1e30)
        top = col_max(s)
        p = jnp.exp(s - top)
        sbuf[rows, :] = p
        dpbuf[rows, :] = d_p
        mbuf[b] = top

        def step(c, state, chunks=1):
            old, total, weighted = state
            rows = part_of(c, chunks * pair)
            s, d_p = both_of(rows)
            new = jnp.maximum(old, col_max(s))
            p = jnp.exp(s - new)
            sbuf[rows, :] = p
            dpbuf[rows, :] = d_p
            for i in range(chunks):
                mbuf[chunks * c + i] = new
            keep = jnp.exp(old - new)
            return new, total * keep + col_sum(p), weighted * keep + col_sum(p * d_p)

        state = (top, col_sum(p), col_sum(p * d_p))
        state = lax.fori_loop(0, b // 2, functools.partial(step, chunks=2), state)
        top, total, weighted = lax.fori_loop(2 * (b // 2), b, step, state)
        inv = 1.0 / total
        return top, inv, weighted * inv

    def second_part(b, stats):
        top, inv, row_dot = stats
        adq[...] = jnp.zeros_like(adq)

        def step(c, carry):
            rows = part_of(c, pair)
            factor = jnp.exp(mbuf[c] - top) * inv
            d_k = d_v = None
            for at in groups:
                p = sbuf[rows, at] * factor[:, at]
                p_b = p.astype(BF)
                ds_b = (p * (dpbuf[rows, at] - row_dot[:, at])).astype(BF)
                adq[0:hd, at] += dot(kvt[0:hd, rows], ds_b)
                adq[hd:hw, at] += dot(kvt[hd:hw, rows], p_b)
                more_k = dot_t(bmat[0:hd, at], ds_b)
                more_v = dot_t(bmat[hd:hw, cols_q + at.start:cols_q + at.stop], p_b)
                d_k = more_k if d_k is None else d_k + more_k
                d_v = more_v if d_v is None else d_v + more_v
            dkvt[0:hd, rows] += d_k
            dkvt[hd:hw, rows] += d_v
            return carry

        lax.fori_loop(0, b + 1, step, 0)


    def send_rows(slot):
        cols = part_of(slot, tok)
        return [
            remote(dq_all.at[:, cols], dt_rv.at[own_rows], q_s.at[slot], q_r.at[me], slot),
            remote(at_all.at[:, cols], at_rv.at[own_rows], a_s.at[slot], a_r.at[me], slot),
        ]

    last = 6 * parts

    def serve(event):
        @pl.when(event < last)
        def _():
            ring_event(y_ring, event)

    @pl.loop(0, n_chip)
    def _(j):
        k = j - 1

        @pl.when(k == 0)
        def _():
            for turn in range(2):
                ring_event(y_ring, k + turn)

        @pl.when((k % 2 == 1) & (k > 0))
        def _():
            for turn in range(2, parts):
                serve(parts * k + turn)

        b = jnp.where(j == 0, opposite, ring_origin(jnp.maximum(k, 0)))

        @once(j == 0)
        def _(_):
            for item in weight_loads:
                item.start()

        @pl.loop(0, jnp.where(j == n_chip - 1, 2 + 4 * near, 0))
        def _(early):
            slot = 2 * ring_origin(early // 2) + early % 2

            @pl.when(slot != me)
            def _():
                for item in send_rows(slot):
                    item.start()

        bmat[0:hd, 0:cols_q] = qt[b]

        @once(j == 0)
        def _(_):
            for i in range(4):
                remote(da_rv.at[i], da_rv.at[i], d_s.at[0], d_r.at[i], mate).wait_recv()
                bmat[hd:hw, cols_q + tok * i:cols_q + tok * i + tok] = da_rv[i]

        @once(j > 0)
        def _(_):
            ring_mate(y_ring, k, b)
            da_t = dot_t(woi[...], dyb[b]).astype(BF)
            for t in range(2):
                for head in range(2):
                    at = cols_q + pair * t + tok * head
                    bmat[hd:hw, at:at + tok] = da_t[hd * head:hd * head + hd, tok * t:tok * t + tok]

        stats = first_part(b, row <= (lane // pair) * tok + lane % tok)
        for turn in range(2):
            serve(jnp.where(k < 0, last, parts * k + 2 + 2 * (k % 2)) + turn)
        second_part(b, stats)
        for t in range(2):
            slot = 2 * b + t
            lanes = [slice(pair * t + tok * head, pair * t + tok * head + tok) for head in range(2)]
            a_t = jnp.concatenate([adq[hd:hw, at] for at in lanes], axis=0).astype(BF)
            cos_t = trig[b, 0:quarter, tok * t:tok * t + tok]
            sin_t = trig[b, quarter:2 * quarter, tok * t:tok * t + tok]
            dq_t = jnp.concatenate([piece for at in lanes for piece in turned(adq[0:hd, at] * scale, cos_t, -sin_t)], axis=0).astype(BF)
            at_all[:, part_of(slot, tok)] = a_t
            dq_all[:, part_of(slot, tok)] = dq_t

            @pl.when(slot == me)
            def _():
                at_rv[own_rows, :] = a_t
                dt_rv[own_rows, :] = dq_t

        @pl.when((k % 2 == 0) & (k >= 0))
        def _():
            for turn in range(2):
                serve(parts * j + turn)

    far = [ring_origin(k) for k in range(n_chip - 1, 0, -1)]
    targets = [2 * c + p for c in far for p in range(2)] + [mate]
    near_targets = targets[-1 - 4 * near:]
    swap = remote(dkvt.at[part_of(1 - core, hd)], kv_rv, x_s, x_r, mate)
    swap.start()
    w_sends = [remote(dwt.at[pl.ds(0, hw), part_of(t, tok)], gw_hbm.at[own_rows], w_s.at[t], w_r.at[me], t) for t in targets]

    def columns(rows_all, buf, cols):
        acc = jnp.zeros((rows_all.shape[0], tile), F32)
        for s in range(n_chip):
            acc += dot(rows_all[:, pair * s:pair * s + pair], buf[s, :, cols])
        return acc

    def q_columns(i):
        cols = part_of(far[i] if i < n_chip - 1 else chip, pair)
        dwt[0:hw, cols] = columns(dq_all, hb, cols)
        for item in w_sends[max(2 * i - 2, 0):2 * i]:
            item.start()

    for i in range(FIRST + 1):
        q_columns(i)

    swap.wait_recv()
    mine = part_of(core, hd)
    g_rows = pl.ds(pl.multiple_of(q_rows + core * kv_w + chip * hd, hd), hd)
    for t in range(n_chip):
        cols = slice(pair * t, pair * t + pair)
        g = dkvt[mine, cols] + kv_rv[:, cols]
        cos_t = jnp.where(core == 0, trig[t, 0:quarter, :], 1.0)
        sin_t = jnp.where(core == 0, trig[t, quarter:2 * quarter, :], 0.0)
        g_b = jnp.concatenate(turned(g, cos_t, -sin_t), axis=0).astype(BF)
        kv_mine[2 * t] = g_b[:, 0:tok]
        kv_mine[2 * t + 1] = g_b[:, tok:pair]
        kv_row[:, cols] = g_b
    dt_rv[g_rows, :] = kv_mine[me]
    kv_sends = [remote(kv_mine.at[t], dt_rv.at[g_rows], kv_s.at[t], kv_r.at[me], t) for t in targets]
    for item in kv_sends:
        item.start()
    for i in range(FIRST + 1, n_chip):
        q_columns(i)
    w_sends[-1].start()
    w_own = local(dwt.at[pl.ds(0, hw), part_of(me, tok)], gw_hbm.at[own_rows], loc_sem.at[0])
    w_own.start()
    for t in range(width // tile):
        cols = slice(tile * t, tile * t + tile)
        dwt[hw:hw + hd, cols] = columns(kv_row, hb, cols)
    wk_own = local(dwt.at[pl.ds(hw, hd), part_of(me, tok)], gw_hbm.at[g_rows], loc_sem.at[1])
    wk_own.start()
    wk_sends = [remote(dwt.at[pl.ds(hw, hd), part_of(t, tok)], gw_hbm.at[g_rows], wk_s.at[t], wk_r.at[me], t) for t in targets]
    for item in wk_sends[0:HELD]:
        item.start()

    @pl.loop(last, 7 * parts)
    def _(event):
        ring_event(y_ring, event)

    ring_mate(y_ring, n_chip - 1, opposite)
    for t in range(width // tile):
        cols = slice(tile * t, tile * t + tile)
        dwo[:, cols] = columns(at_all, dyb, cols)
    store_wo = local(dwo, gwo_hbm, out_sem.at[0])
    store_wo.start()
    finish_ring(y_ring)
    wo_loads = [local(wo_hbm.at[pl.ds(pair * t, pair)], dyb.at[t], wo_sem.at[t]) for t in range(n_chip)]
    for item in wo_loads:
        item.start()

    @pl.loop(0, n_far)
    def _(f):
        c_far = ring_origin(2 * near + 1 + f)
        cos_t = trig[chip, 0:quarter, part_of(core, tok)]
        sin_t = trig[chip, quarter:2 * quarter, part_of(core, tok)]
        top = stat_far[f, 0]
        inv = 1.0 / stat_far[f, 1]
        row_dot = stat_far[f, 2] * inv

        def add_chunk(c, diagonal, chunks=1):
            rows = part_of(c, chunks * pair)
            for at in groups:
                keys = kv_far[f, rows, :]
                s = dot(keys, bmat_far[f, :, at])
                d_p = dot(keys, bmat_far[f, :, cols_q + at.start:cols_q + at.stop])
                if diagonal:
                    s = jnp.where(seen_far[:, at], s, -1e30)
                p = jnp.exp(s - top[:, at]) * inv[:, at]
                p_b = p.astype(BF)
                ds_b = (p * (d_p - row_dot[:, at])).astype(BF)
                d_q = dot(kvt_far[f, 0:hd, rows], ds_b)
                d_a = dot(kvt_far[f, hd:hw, rows], p_b)
                adq[0:hd, at] = d_q if diagonal else adq[0:hd, at] + d_q
                adq[hd:hw, at] = d_a if diagonal else adq[hd:hw, at] + d_a

        add_chunk(chip, True)

        @pl.loop(0, chip // 2)
        def _(c):
            add_chunk(c, False, 2)

        @pl.when(chip % 2 == 1)
        def _():
            add_chunk(chip - 1, False)

        for head in range(4):
            at = slice(tok * head, tok * head + tok)
            place = pl.ds(pl.multiple_of(c_far * 2 * hw + hd * head, hd), hd)
            at_rv[place, :] = adq[hd:hw, at].astype(BF)
            dt_rv[place, :] = jnp.concatenate(turned(adq[0:hd, at] * scale, cos_t, -sin_t), axis=0).astype(BF)

    for t in near_targets:
        remote(at_all.at[:, pl.ds(0, tok)], at_rv.at[part_of(t, hw)], a_s.at[t], a_r.at[t], t).wait_recv()
    for item in wo_loads:
        item.wait()
    for t in range(q_rows // tok):
        a_nat[:, tok * t:tok * t + tok] = at_rv[tok * t:tok * t + tok, :].T
    for t in range(width // tile):
        cols = slice(tile * t, tile * t + tile)
        prod = jnp.zeros((tok, tile), F32)
        for s in range(n_chip):
            prod += dot(a_nat[:, pair * s:pair * s + pair], dyb[s, :, cols])
        out_v[:, cols] = (x_v[:, cols].astype(F32) + prod).astype(BF)
    store_out = local(out_v, out_hbm, out_sem.at[1])
    store_out.start()

    for item in weight_loads:
        item.wait()

    def kv_place(t):
        return pl.ds(pl.multiple_of(q_rows + (t % 2) * kv_w + (t // 2) * hd, hd), hd)

    for t in near_targets:
        remote(dq_all.at[:, pl.ds(0, tok)], dt_rv.at[part_of(t, hw)], q_s.at[t], q_r.at[t], t).wait_recv()
    for t in targets:
        remote(kv_mine.at[0], dt_rv.at[kv_place(t)], kv_s.at[t], kv_r.at[t], t).wait_recv()
    swap.wait_send()
    for t in range(n_rows // tok):
        d_nat[:, tok * t:tok * t + tok] = dt_rv[tok * t:tok * t + tok, :].T

    mean = stat[0, :, 0:1]
    inv_std = stat[1, :, 0:1]
    dh = dkvt
    for t in range(width // tile):
        cols = slice(tile * t, tile * t + tile)
        acc = jnp.zeros((tok, tile), F32)
        for s in range(n_rows // tile):
            acc += dot(d_nat[:, tile * s:tile * s + tile], wt[tile * s:tile * s + tile, cols])
        dh[:, cols] = acc
        gg_st[0, :, cols] = col_sum(acc * ((x_v[:, cols].astype(F32) - mean) * inv_std))
        gg_st[1, :, cols] = col_sum(acc)
    g_swap = remote(gg_st.at[1 - core], gg_mx, g_s.at[n_chip], g_r.at[n_chip], mate)
    g_swap.start()
    g_swap.wait_recv()
    gg_my[...] = jnp.where(core == 0, gg_st[0], gg_st[1]) + gg_mx[...]
    gg_rv[chip] = gg_my[...]
    g_sends = [remote(gg_my, gg_rv.at[chip], g_s.at[c], g_r.at[chip], 2 * c + core) for c in far]
    for item in g_sends + wk_sends[HELD:]:
        item.start()

    grad_hat = dh[...] * gain_one
    x_hat = (x_v[...].astype(F32) - mean) * inv_std
    mean_one = row_mean(grad_hat)
    mean_two = row_mean(grad_hat * x_hat)
    store_out.wait()
    out_v[...] = (dy_own[...].astype(F32) + inv_std * (grad_hat - mean_one - x_hat * mean_two)).astype(BF)
    store_gx = local(out_v, gx_hbm, out_sem.at[2])
    store_gx.start()

    for c in far:
        remote(gg_my, gg_rv.at[c], g_s.at[c], g_r.at[c], 2 * c + core).wait_recv()
    sums = gg_rv[0]
    for c in range(1, n_chip):
        sums = sums + gg_rv[c]
    gg_out[core] = sums
    g_swap_out = remote(gg_out.at[core], gg_out.at[core], g_s.at[n_chip + 1], g_r.at[n_chip + 1], mate)
    g_swap_out.start()
    remote(gg_out.at[core], gg_out.at[1 - core], g_s.at[n_chip + 1], g_r.at[n_chip + 1], mate).wait_recv()
    store_gg = local(gg_out, gg_hbm, out_sem.at[3])
    store_gg.start()

    finish_ring(h_ring)
    for item in pos_sends + [g_swap, g_swap_out] + [opposite_send(head) for head in range(4)]:
        item.wait_send()
    for t in near_targets:
        remote(at_all.at[:, pl.ds(0, tok)], at_rv.at[pl.ds(0, hw)], a_s.at[t], a_r.at[t], t).wait_send()
        remote(dq_all.at[:, pl.ds(0, tok)], dt_rv.at[pl.ds(0, hw)], q_s.at[t], q_r.at[t], t).wait_send()
    for item in kv_sends + w_sends + g_sends + wk_sends:
        item.wait_send()
    for t in targets:
        remote(dwt.at[pl.ds(0, hw), part_of(t, tok)], gw_hbm.at[part_of(t, hw)], w_s.at[t], w_r.at[t], t).wait_recv()
        remote(dwt.at[pl.ds(hw, hd), part_of(t, tok)], gw_hbm.at[kv_place(t)], wk_s.at[t], wk_r.at[t], t).wait_recv()
    for item in (w_own, wk_own, store_wo, store_gx, store_gg):
        item.wait()


def settle_kernel(q_rows, kv_w, out_i, gx_i, gw_i, gwo_i, gg_i, out_o, gx_o, gq_o, gk_o, gv_o, gwo_o, gain_o, bias_o, b_act, b_q, b_kv, b_o, b_gg, sem_in, sem_out, sem_gg):
    half_q = q_rows // 2
    half_o = gwo_i.shape[0] // 2
    moves = [(out_i, b_act.at[0], out_o), (gx_i, b_act.at[1], gx_o)]
    for t in range(2):
        moves.append((gw_i.at[pl.ds(half_q * t, half_q)], b_q.at[t], gq_o.at[pl.ds(half_q * t, half_q)]))
        moves.append((gwo_i.at[pl.ds(half_o * t, half_o)], b_o.at[t], gwo_o.at[pl.ds(half_o * t, half_o)]))
    moves.append((gw_i.at[pl.ds(q_rows, kv_w)], b_kv.at[0], gk_o))
    moves.append((gw_i.at[pl.ds(q_rows + kv_w, kv_w)], b_kv.at[1], gv_o))
    loads = [pltpu.make_async_copy(src, mid, sem_in.at[i]) for i, (src, mid, _) in enumerate(moves)]
    stores = [pltpu.make_async_copy(mid, dst, sem_out.at[i]) for i, (_, mid, dst) in enumerate(moves)]
    load_gg = pltpu.make_async_copy(gg_i, b_gg, sem_gg)
    load_gg.start()
    for item in loads:
        item.start()
    for load, store in zip(loads, stores):
        load.wait()
        store.start()
    load_gg.wait()
    gain_o[...] = b_gg[0, 0]
    bias_o[...] = b_gg[1, 0]
    for item in stores:
        item.wait()


def solution(mesh):
    n_dev = mesh.shape['cp']

    def device_step(x_act, d_out, positions, ln_gain, ln_bias, w_query, w_key, w_value, w_out):
        tok, width = x_act.shape[1], x_act.shape[2]
        q_heads, hd = w_query.shape[1], w_query.shape[2]
        kv_heads = w_key.shape[1]
        q_w, kv_w = q_heads * hd, kv_heads * hd
        n_rows = q_w + 2 * kv_w
        seq = n_dev * tok
        hw = 2 * hd

        def flat_weight(w):
            return jnp.transpose(w, (1, 2, 0)).reshape(-1, width)

        hbm = pl.BlockSpec(memory_space=pltpu.HBM)
        vmem = pl.BlockSpec(memory_space=pltpu.VMEM)
        dma = pltpu.SemaphoreType.DMA
        n_chip = n_dev // 2
        n_far = n_chip - 1 - 2 * NEAR
        pair = 2 * tok
        scratch = [
            pltpu.VMEM((n_chip, pair, width), BF),
            pltpu.VMEM((n_chip, pair, width), BF),
            pltpu.VMEM((n_rows, width), BF),
            pltpu.VMEM((2 * hw, width), BF),
            pltpu.VMEM((hw, width), BF),
            pltpu.VMEM((n_dev, 1, tok), jnp.int32),
            pltpu.VMEM((n_chip, hd // 2, pair), F32),
            pltpu.VMEM((n_chip, hd, 2 * pair), BF),
            pltpu.VMEM((hw, seq), BF),
            pltpu.VMEM((seq, hw), BF),
            pltpu.VMEM((n_far, hw, seq), BF),
            pltpu.VMEM((n_far, seq, hw), BF),
            pltpu.VMEM((n_far, hw, 4 * pair), BF),
            pltpu.VMEM((n_far, 3, 1, 2 * pair), F32),
            pltpu.VMEM((hw, 4 * pair), BF),
            pltpu.VMEM((4, hd, tok), BF),
            pltpu.VMEM((seq, 2 * pair), F32),
            pltpu.VMEM((seq, 2 * pair), F32),
            pltpu.VMEM((n_chip, 1, 2 * pair), F32),
            pltpu.VMEM((hw, 2 * pair), F32),
            pltpu.VMEM((hw, seq), F32),
            pltpu.VMEM((hd, seq), F32),
            pltpu.VMEM((n_dev, hd, tok), BF),
            pltpu.VMEM((hd, seq), BF),
            pltpu.VMEM((hw, width), F32),
            pltpu.VMEM((hw + hd, width), F32),
            pltpu.VMEM((hw, seq), BF),
            pltpu.VMEM((hw, seq), BF),
            pltpu.VMEM((q_w, tok), BF),
            pltpu.VMEM((n_rows, tok), BF),
            pltpu.VMEM((tok, q_w), BF),
            pltpu.VMEM((tok, n_rows), BF),
            pltpu.VMEM((tok, width), BF),
            pltpu.VMEM((tok, width), BF),
            pltpu.VMEM((2, 1, width), F32),
            pltpu.VMEM((2, tok, 128), F32),
            pltpu.VMEM((tok, width), BF),
            pltpu.VMEM((2, 1, width), F32),
            pltpu.VMEM((1, width), F32),
            pltpu.VMEM((1, width), F32),
            pltpu.VMEM((n_chip, 1, width), F32),
            pltpu.VMEM((2, 1, width), F32),
            dma((10,)), dma((4 * n_far,)), dma((n_chip,)), dma((3,)), dma((4,)), dma((2,)),
        ] + [dma((9 * PARTS,)), dma((7 * PARTS,)), dma((8 * PARTS,)), dma((8 * PARTS,))] * 2 + [dma((4,))] * 2 + [dma((n_dev,))] * 6 + [dma] * 2 + [dma((n_dev,))] * 8
        out, gx, gw, gwo, gg = pl.pallas_call(
            functools.partial(block_kernel, n_dev, hd, kv_w, NEAR, PARTS),
            out_shape=(
                jax.ShapeDtypeStruct((tok, width), BF),
                jax.ShapeDtypeStruct((tok, width), BF),
                jax.ShapeDtypeStruct((n_rows, tok), F32),
                jax.ShapeDtypeStruct((hw, width), F32),
                jax.ShapeDtypeStruct((2, 1, width), F32),
            ),
            in_specs=[hbm] * 9,
            out_specs=(hbm,) * 5,
            scratch_shapes=scratch,
            compiler_params=pltpu.CompilerParams(collective_id=0, has_side_effects=True, vmem_limit_bytes=67043328),
            name='attn_block',
        )(
            x_act.reshape(tok, width), d_out.reshape(tok, width), positions.reshape(1, tok),
            ln_gain.reshape(1, width), ln_bias.reshape(1, width),
            flat_weight(w_query), flat_weight(w_key), flat_weight(w_value), w_out,
        )

        out, gx, gq, gk, gv, gwo, gain, bias = pl.pallas_call(
            functools.partial(settle_kernel, q_w, kv_w),
            out_shape=(
                jax.ShapeDtypeStruct((tok, width), BF),
                jax.ShapeDtypeStruct((tok, width), BF),
                jax.ShapeDtypeStruct((q_w, tok), F32),
                jax.ShapeDtypeStruct((kv_w, tok), F32),
                jax.ShapeDtypeStruct((kv_w, tok), F32),
                jax.ShapeDtypeStruct((hw, width), F32),
                jax.ShapeDtypeStruct((width,), F32),
                jax.ShapeDtypeStruct((width,), F32),
            ),
            in_specs=[hbm] * 5,
            out_specs=(hbm,) * 6 + (vmem,) * 2,
            scratch_shapes=[
                pltpu.VMEM((2, tok, width), BF),
                pltpu.VMEM((2, q_w // 2, tok), F32),
                pltpu.VMEM((2, kv_w, tok), F32),
                pltpu.VMEM((2, hw // 2, width), F32),
                pltpu.VMEM((2, 1, width), F32),
                dma((8,)), dma((8,)), dma,
            ],
            name='settle',
        )(out, gx, gw, gwo, gg)

        def rows_out(block, heads):
            return jnp.transpose(block.reshape(heads, hd, tok), (2, 0, 1))

        return (
            out.reshape(1, tok, width), gx.reshape(1, tok, width),
            rows_out(gq, q_heads), rows_out(gk, kv_heads), rows_out(gv, kv_heads),
            gwo, gain, bias,
        )

    return jax.shard_map(device_step, mesh=mesh, in_specs=(P('dp', 'cp', None), P('dp', 'cp', None), P('dp', 'cp'), P(None), P(None), P(None, None, None), P(None, None, None), P(None, None, None), P(None, None)), out_specs=(P('dp', 'cp', None), P('dp', 'cp', None), P(('dp', 'cp'), None, None), P(('dp', 'cp'), None, None), P(('dp', 'cp'), None, None), P(('dp', 'cp'), None), P('dp'), P('dp')), check_vma=False)
```

```python
import functools
import math

import jax
import jax.numpy as jnp
from jax import lax
from jax.experimental import pallas as pl
from jax.experimental.pallas import tpu as pltpu
from jax.sharding import PartitionSpec as P

EPS = 1e-5
ROPE_BASE = 10000.0
MESH = pl.DeviceIdType.MESH
BF = jnp.bfloat16
F32 = jnp.float32
NEAR = 1
PARTS = 4
FIRST = 1
HELD = 4


def dot(lhs, rhs):
    return jnp.dot(lhs, rhs, preferred_element_type=F32)


def col_sum(val):
    return jnp.sum(val, axis=0, keepdims=True)


def col_max(val):
    return jnp.max(val, axis=0, keepdims=True)


def row_mean(val):
    return jnp.mean(val, axis=-1, keepdims=True)


def dot_t(lhs, rhs):
    return lax.dot_general(lhs, rhs, (((1,), (1,)), ((), ())), preferred_element_type=F32)


def block_kernel(
    n_dev, hd, kv_w, near, parts,
    x_hbm, dy_hbm, pos_hbm, gain_hbm, bias_hbm, wq_hbm, wk_hbm, wv_hbm, wo_hbm,
    out_hbm, gx_hbm, gw_hbm, gwo_hbm, gg_hbm,
    hb, dyb, wt, wi, woi, w_far, pos_all, trig,
    qt, kvt, kv, kvt_far, kv_far, bmat_far, stat_far, bmat, da_rv, sbuf, dpbuf, mbuf, adq, dkvt, kv_rv, kv_mine, kv_row,
    dwo, dwt, at_all, dq_all, at_rv, dt_rv, a_nat, d_nat, x_v, dy_own, gb_v, stat, out_v, gg_st, gg_mx, gg_my, gg_rv, gg_out,
    in_sem, far_sem, wo_sem, w_sem, out_sem, loc_sem,
    hzs, hzr, hds, hdr, yzs, yzr, yds, ydr,
    d_s, d_r, pos_s, pos_r, a_s, a_r, q_s, q_r, x_s, x_r, kv_s, kv_r, w_s, w_r, wk_s, wk_r, g_s, g_r,
):
    tok, width = x_v.shape
    n_chip = n_dev // 2
    pair = 2 * tok
    me = lax.axis_index('cp')
    chip = me // 2
    core = me % 2
    right = 2 * ((chip + 1) % n_chip) + core
    left = 2 * ((chip + n_chip - 1) % n_chip) + core
    mate = 2 * chip + 1 - core
    q_rows = wq_hbm.shape[0]
    n_rows = q_rows + 2 * kv_w
    hw = 2 * hd
    quarter = hd // 4
    tile = 256
    scale = hd ** -0.5
    cols_q = 2 * pair
    n_far = n_chip - 1 - 2 * near

    def remote(src, dst, send, recv, target):
        return pltpu.make_async_remote_copy(src_ref=src, dst_ref=dst, send_sem=send, recv_sem=recv, device_id={'cp': target}, device_id_type=MESH)

    def local(src, dst, sem):
        return pltpu.make_async_copy(src, dst, sem)

    def part_of(i, size):
        return pl.ds(pl.multiple_of(i * size, size), size)

    def once(cond):
        return pl.loop(0, jnp.where(cond, 1, 0))

    def ring_steps(k):
        step = (k + 1) // 2
        return step, k % 2

    def ring_origin(k):
        step, ahead = ring_steps(k)
        return jnp.where(ahead == 1, chip + n_chip - step, chip + step) % n_chip

    own = (chip, part_of(core, tok))
    first_loads = [
        local(x_hbm, x_v, in_sem.at[0]),
        local(gain_hbm, gb_v.at[0], in_sem.at[1]),
        local(bias_hbm, gb_v.at[1], in_sem.at[2]),
        local(pos_hbm, pos_all.at[me], in_sem.at[3]),
    ]
    for item in first_loads:
        item.start()
    barrier = pltpu.get_barrier_semaphore()
    for step in range(1, n_dev):
        pl.semaphore_signal(barrier, inc=1, device_id={'cp': (me + step) % n_dev}, device_id_type=MESH)
    own_rows = part_of(me, hw)
    kv_rows = part_of(chip, hd)
    loads = [
        local(wq_hbm.at[own_rows], wi.at[pl.ds(0, hw)], in_sem.at[4]),
        local(wk_hbm.at[kv_rows], wi.at[pl.ds(hw, hd)], in_sem.at[5]),
        local(wv_hbm.at[kv_rows], wi.at[pl.ds(hw + hd, hd)], in_sem.at[6]),
        local(wo_hbm.at[own_rows], woi, in_sem.at[7]),
        local(dy_hbm, dyb.at[own], in_sem.at[8]),
        local(dy_hbm, dy_own, in_sem.at[9]),
    ]
    far_loads = []
    for f in range(n_far):
        far_rows = part_of(ring_origin(2 * near + 1 + f), hd)
        loads.append(local(wk_hbm.at[far_rows], w_far.at[pl.ds(hw * f, hd)], far_sem.at[2 * f]))
        loads.append(local(wv_hbm.at[far_rows], w_far.at[pl.ds(hw * f + hd, hd)], far_sem.at[2 * f + 1]))
        far_wo = part_of(ring_origin(2 * near + 1 + f), 2 * hw)
        far_loads.append(local(wo_hbm.at[far_wo], wt.at[pl.ds(2 * hw * f, 2 * hw)], far_sem.at[2 * n_far + f]))
        far_loads.append(local(wq_hbm.at[far_wo], wt.at[pl.ds(2 * hw * (n_far + f), 2 * hw)], far_sem.at[3 * n_far + f]))
    for item in loads + far_loads:
        item.start()

    for item in first_loads:
        item.wait()
    gain_one = 1.0 + gb_v[0]
    block = 16

    @pl.loop(0, tok // block)
    def _(i):
        rows = part_of(i, block)
        x_f = x_v[rows, :].astype(F32)
        mean = row_mean(x_f)
        centered = x_f - mean
        inv_std = lax.rsqrt(row_mean(centered * centered) + EPS)
        hb[chip, part_of(core * (tok // block) + i, block), :] = (centered * inv_std * gain_one + gb_v[1]).astype(BF)
        stat[0, rows, :] = jnp.broadcast_to(mean, (block, 128))
        stat[1, rows, :] = jnp.broadcast_to(inv_std, (block, 128))

    pl.semaphore_wait(barrier, n_dev - 1)

    def chunk(buf, origin, parity, part):
        return buf.at[origin, part_of(parts * parity + part, tok // parts)]

    turns = 2 * parts

    def own_sends(buf, zs, zr, ds, dr):
        copies = []
        for part in range(parts):
            piece = chunk(buf, chip, core, part)
            copies.append(remote(piece, piece, zs.at[2 * part], zr.at[2 * part], right))
            copies.append(remote(piece, piece, zs.at[2 * part + 1], zr.at[2 * part + 1], left))
            copies.append(remote(piece, piece, ds.at[7 * parts + part], dr.at[7 * parts + part], mate))
        return copies

    def event_place(event):
        step = event // turns + 1
        turn = event % turns
        direction = turn % 2
        part = jnp.where(step < 4, turn // 2, turn // 2 + direction * (parts // 2))
        origin = jnp.where(direction == 0, chip + n_chip - step, chip + step) % n_chip
        return step, direction, part, origin

    def last_event(part, direction):
        return 6 * parts + 2 * (part - direction * (parts // 2)) + direction

    def ring_event(ring, event):
        buf, zs, zr, ds, dr = ring
        step, direction, part, origin = event_place(event)
        piece = chunk(buf, origin, core, part)
        remote(piece, piece, zs.at[0], zr.at[event], right).wait_recv()
        onward = jnp.where(step < 3, event + turns, last_event(part, direction))

        @pl.when((step < 3) | ((step == 3) & ((part >= parts // 2) == (direction == 1))))
        def _():
            remote(piece, piece, zs.at[event + turns], zr.at[onward], jnp.where(direction == 0, right, left)).start()

        remote(piece, piece, ds.at[event], dr.at[event], mate).start()

    def ring_service(ring, event):
        @pl.when(event < 7 * parts)
        def _():
            ring_event(ring, event)

    def ring_mate(ring, k, origin):
        buf, zs, zr, ds, dr = ring
        step, ahead = ring_steps(k)
        for part in range(parts):
            event = jnp.where(k == 0, 7 * parts + part, jnp.where(step < 4, turns * (step - 1) + 2 * part + 1 - ahead, last_event(part, part // (parts // 2))))
            piece = chunk(buf, origin, 1 - core, part)
            remote(piece, piece, ds.at[0], dr.at[event], mate).wait_recv()

    def finish_ring(ring):
        buf, zs, zr, ds, dr = ring
        for item in own_sends(*ring):
            item.wait_send()

        @pl.loop(0, 7 * parts)
        def _(event):
            step, direction, part, origin = event_place(event)
            piece = chunk(buf, origin, core, part)

            @pl.when((step < 3) | ((step == 3) & ((part >= parts // 2) == (direction == 1))))
            def _():
                remote(piece, piece, zs.at[event + turns], zr.at[event], right).wait_send()

            remote(piece, piece, ds.at[event], dr.at[event], mate).wait_send()

    h_ring = (hb, hzs, hzr, hds, hdr)
    y_ring = (dyb, yzs, yzr, yds, ydr)
    for item in own_sends(*h_ring):
        item.start()
    pos_sends = [remote(pos_all.at[me], pos_all.at[me], pos_s.at[step], pos_r.at[me], (me + step) % n_dev) for step in range(1, n_dev)]
    for item in pos_sends:
        item.start()
    weight_loads = [
        local(wq_hbm, wt.at[pl.ds(0, q_rows)], w_sem.at[0]),
        local(wk_hbm, wt.at[pl.ds(q_rows, kv_w)], w_sem.at[1]),
        local(wv_hbm, wt.at[pl.ds(q_rows + kv_w, kv_w)], w_sem.at[2]),
    ]
    dkvt[...] = jnp.zeros_like(dkvt)
    bmat[...] = jnp.zeros_like(bmat)
    bmat_far[...] = jnp.zeros_like(bmat_far)
    for f in range(n_far):
        stat_far[f, 0] = jnp.full((1, cols_q), -3e38, F32)
        stat_far[f, 1] = jnp.zeros((1, cols_q), F32)
        stat_far[f, 2] = jnp.zeros((1, cols_q), F32)

    freq = jnp.exp(lax.broadcasted_iota(jnp.int32, (quarter, tok), 0).astype(F32) * (-2.0 * math.log(ROPE_BASE) / (hd // 2)))

    def make_trig(b):
        for t in range(2):
            slot = 2 * b + t

            @pl.when(slot != me)
            def _():
                remote(pos_all.at[slot], pos_all.at[slot], pos_s.at[0], pos_r.at[slot], me).wait_recv()

            angle = pos_all[slot].astype(F32) * freq
            trig[b, 0:quarter, tok * t:tok * t + tok] = jnp.cos(angle)
            trig[b, quarter:2 * quarter, tok * t:tok * t + tok] = jnp.sin(angle)

    def turned(val, cos_t, sin_t):
        u = val[0:quarter]
        w = val[quarter:2 * quarter]
        return [u * cos_t - w * sin_t, w * cos_t + u * sin_t, val[2 * quarter:hd]]

    def eighth(val):
        return val.astype(BF) * jnp.asarray(scale, BF)

    def keys_values(val, cos_t, sin_t):
        return jnp.concatenate(turned(val[0:hd], cos_t, sin_t) + [val[hd:hw]], axis=0).astype(BF)

    lane = lax.broadcasted_iota(jnp.int32, (pair, cols_q), 1)
    row = lax.broadcasted_iota(jnp.int32, (pair, cols_q), 0)
    seen_far = row <= core * tok + lane % tok

    opposite = ring_origin(n_chip - 1)

    def opposite_send(head):
        block = bmat_far.at[n_far - 1, pl.ds(hd, hd), pl.ds(cols_q + tok * head, tok)]
        return remote(block, da_rv.at[2 * core + head % 2], d_s.at[head], d_r.at[2 * core + head % 2], 2 * opposite + head // 2)

    @pl.loop(0, n_chip)
    def _(k):
        for turn in range(2):
            ring_service(h_ring, parts * k + turn)

        @pl.when(k % 2 == 1)
        def _():
            ring_service(h_ring, parts * k + 2)


        @once(k == 5)
        def _(_):
            for item in own_sends(*y_ring):
                item.start()

        @once(k == 0)
        def _(_):
            for item in loads:
                item.wait()

        b = ring_origin(k)
        ring_mate(h_ring, k, b)
        make_trig(b)

        @once(k == 0)
        def _(_):
            for item in far_loads:
                item.wait()
            cos_t = trig[chip, 0:quarter, part_of(core, tok)]
            sin_t = trig[chip, quarter:2 * quarter, part_of(core, tok)]

            @pl.loop(0, n_far)
            def _(f):
                da_t = dot_t(wt[part_of(f, 2 * hw), :], dy_own[...]).astype(BF)
                q_t = dot_t(wt[part_of(n_far + f, 2 * hw), :], hb[chip, part_of(core, tok), :])
                for head in range(4):
                    part = slice(hd * head, hd * head + hd)
                    at = tok * head
                    bmat_far[f, 0:hd, at:at + tok] = eighth(jnp.concatenate(turned(q_t[part], cos_t, sin_t), axis=0))
                    bmat_far[f, hd:hw, cols_q + at:cols_q + at + tok] = da_t[part]

            for item in weight_loads:
                item.start()

        @once(k == 1)
        def _(_):
            for head in range(4):
                opposite_send(head).start()

        place = part_of(b, pair)
        cos_t = trig[b, 0:quarter, :]
        sin_t = trig[b, quarter:2 * quarter, :]
        flat = dot_t(wi[...], hb[b])
        for head in range(2):
            q_rot = eighth(jnp.concatenate(turned(flat[hd * head:hd * head + hd], cos_t, sin_t), axis=0))
            for t in range(2):
                lane = pair * t + tok * head
                qt[b, :, lane:lane + tok] = q_rot[:, tok * t:tok * t + tok]
        kv_rot = keys_values(flat[hw:2 * hw], cos_t, sin_t)
        kvt[:, place] = kv_rot
        kv[place, :] = kv_rot.T

        @pl.when(k % 2 == 0)
        def _():
            ring_service(h_ring, parts * k + 2)

        ring_service(h_ring, parts * k + parts - 1)

        @pl.when(b <= chip)
        def _():
            flat_far = dot_t(w_far[...], hb[b])
            for f in range(n_far):
                far_rot = keys_values(flat_far[hw * f:hw * f + hw], cos_t, sin_t)
                kvt_far[f, :, place] = far_rot
                kv_far[f, place, :] = far_rot.T

            @pl.loop(0, n_far)
            def _(f):
                both = dot(kv_far[f, place, :], bmat_far[f])
                s = jnp.where(seen_far | (k > 0), both[:, 0:cols_q], -1e30)
                old = stat_far[f, 0]
                new = jnp.maximum(old, col_max(s))
                p = jnp.exp(s - new)
                keep = jnp.exp(old - new)
                stat_far[f, 0] = new
                stat_far[f, 1] = stat_far[f, 1] * keep + col_sum(p)
                stat_far[f, 2] = stat_far[f, 2] * keep + col_sum(p * both[:, cols_q:2 * cols_q])

    groups = [slice(tile * g, tile * g + tile) for g in range(cols_q // tile)]

    def first_part(b, seen):
        def both_of(rows):
            both = dot(kv[rows, :], bmat[...])
            return both[:, 0:cols_q], both[:, cols_q:2 * cols_q]

        rows = part_of(b, pair)
        s, d_p = both_of(rows)
        s = jnp.where(seen, s, -1e30)
        top = col_max(s)
        p = jnp.exp(s - top)
        sbuf[rows, :] = p
        dpbuf[rows, :] = d_p
        mbuf[b] = top

        def step(c, state, chunks=1):
            old, total, weighted = state
            rows = part_of(c, chunks * pair)
            s, d_p = both_of(rows)
            new = jnp.maximum(old, col_max(s))
            p = jnp.exp(s - new)
            sbuf[rows, :] = p
            dpbuf[rows, :] = d_p
            for i in range(chunks):
                mbuf[chunks * c + i] = new
            keep = jnp.exp(old - new)
            return new, total * keep + col_sum(p), weighted * keep + col_sum(p * d_p)

        state = (top, col_sum(p), col_sum(p * d_p))
        state = lax.fori_loop(0, b // 2, functools.partial(step, chunks=2), state)
        top, total, weighted = lax.fori_loop(2 * (b // 2), b, step, state)
        inv = 1.0 / total
        return top, inv, weighted * inv

    def second_part(b, stats):
        top, inv, row_dot = stats
        adq[...] = jnp.zeros_like(adq)

        def step(c, carry):
            rows = part_of(c, pair)
            factor = jnp.exp(mbuf[c] - top) * inv
            d_k = d_v = None
            for at in groups:
                p = sbuf[rows, at] * factor[:, at]
                p_b = p.astype(BF)
                ds_b = (p * (dpbuf[rows, at] - row_dot[:, at])).astype(BF)
                adq[0:hd, at] += dot(kvt[0:hd, rows], ds_b)
                adq[hd:hw, at] += dot(kvt[hd:hw, rows], p_b)
                more_k = dot_t(bmat[0:hd, at], ds_b)
                more_v = dot_t(bmat[hd:hw, cols_q + at.start:cols_q + at.stop], p_b)
                d_k = more_k if d_k is None else d_k + more_k
                d_v = more_v if d_v is None else d_v + more_v
            dkvt[0:hd, rows] += d_k
            dkvt[hd:hw, rows] += d_v
            return carry

        lax.fori_loop(0, b + 1, step, 0)


    def send_rows(slot):
        cols = part_of(slot, tok)
        return [
            remote(dq_all.at[:, cols], dt_rv.at[own_rows], q_s.at[slot], q_r.at[me], slot),
            remote(at_all.at[:, cols], at_rv.at[own_rows], a_s.at[slot], a_r.at[me], slot),
        ]

    last = 6 * parts

    def serve(event):
        @pl.when(event < last)
        def _():
            ring_event(y_ring, event)

    @pl.loop(0, n_chip)
    def _(j):
        k = j - 1

        @pl.when(k == 0)
        def _():
            for turn in range(2):
                ring_event(y_ring, k + turn)

        @pl.when((k % 2 == 1) & (k > 0))
        def _():
            for turn in range(2, parts):
                serve(parts * k + turn)

        b = jnp.where(j == 0, opposite, ring_origin(jnp.maximum(k, 0)))

        @once(k == 1)
        def _(_):
            for item in weight_loads:
                item.wait()

        @pl.loop(0, jnp.where(j == n_chip - 1, 2 + 4 * near, 0))
        def _(early):
            slot = 2 * ring_origin(early // 2) + early % 2

            @pl.when(slot != me)
            def _():
                for item in send_rows(slot):
                    item.start()

        bmat[0:hd, 0:cols_q] = qt[b]

        @once(j == 0)
        def _(_):
            for i in range(4):
                remote(da_rv.at[i], da_rv.at[i], d_s.at[0], d_r.at[i], mate).wait_recv()
                bmat[hd:hw, cols_q + tok * i:cols_q + tok * i + tok] = da_rv[i]

        @once(j > 0)
        def _(_):
            ring_mate(y_ring, k, b)
            da_t = dot_t(woi[...], dyb[b]).astype(BF)
            for t in range(2):
                for head in range(2):
                    at = cols_q + pair * t + tok * head
                    bmat[hd:hw, at:at + tok] = da_t[hd * head:hd * head + hd, tok * t:tok * t + tok]

        stats = first_part(b, row <= (lane // pair) * tok + lane % tok)
        for turn in range(2):
            serve(jnp.where(k < 0, last, parts * k + 2 + 2 * (k % 2)) + turn)
        second_part(b, stats)
        for t in range(2):
            slot = 2 * b + t
            lanes = [slice(pair * t + tok * head, pair * t + tok * head + tok) for head in range(2)]
            a_t = jnp.concatenate([adq[hd:hw, at] for at in lanes], axis=0).astype(BF)
            cos_t = trig[b, 0:quarter, tok * t:tok * t + tok]
            sin_t = trig[b, quarter:2 * quarter, tok * t:tok * t + tok]
            dq_t = jnp.concatenate([piece for at in lanes for piece in turned(adq[0:hd, at] * scale, cos_t, -sin_t)], axis=0).astype(BF)
            at_all[:, part_of(slot, tok)] = a_t
            dq_all[:, part_of(slot, tok)] = dq_t

            @pl.when(slot == me)
            def _():
                at_rv[own_rows, :] = a_t
                dt_rv[own_rows, :] = dq_t

        @pl.when((k % 2 == 0) & (k >= 0))
        def _():
            for turn in range(2):
                serve(parts * j + turn)

    far = [ring_origin(k) for k in range(n_chip - 1, 0, -1)]
    targets = [2 * c + p for c in far for p in range(2)] + [mate]
    near_targets = targets[-1 - 4 * near:]
    swap = remote(dkvt.at[part_of(1 - core, hd)], kv_rv, x_s, x_r, mate)
    swap.start()
    w_sends = [remote(dwt.at[pl.ds(0, hw), part_of(t, tok)], gw_hbm.at[own_rows], w_s.at[t], w_r.at[me], t) for t in targets]

    def columns(rows_all, buf, cols):
        acc = jnp.zeros((rows_all.shape[0], tile), F32)
        for s in range(n_chip):
            acc += dot(rows_all[:, pair * s:pair * s + pair], buf[s, :, cols])
        return acc

    def q_columns(i):
        cols = part_of(far[i] if i < n_chip - 1 else chip, pair)
        dwt[0:hw, cols] = columns(dq_all, hb, cols)
        for item in w_sends[max(2 * i - 2, 0):2 * i]:
            item.start()

    for i in range(FIRST + 1):
        q_columns(i)

    swap.wait_recv()
    mine = part_of(core, hd)
    g_rows = pl.ds(pl.multiple_of(q_rows + core * kv_w + chip * hd, hd), hd)
    for t in range(n_chip):
        cols = slice(pair * t, pair * t + pair)
        g = dkvt[mine, cols] + kv_rv[:, cols]
        cos_t = jnp.where(core == 0, trig[t, 0:quarter, :], 1.0)
        sin_t = jnp.where(core == 0, trig[t, quarter:2 * quarter, :], 0.0)
        g_b = jnp.concatenate(turned(g, cos_t, -sin_t), axis=0).astype(BF)
        kv_mine[2 * t] = g_b[:, 0:tok]
        kv_mine[2 * t + 1] = g_b[:, tok:pair]
        kv_row[:, cols] = g_b
    dt_rv[g_rows, :] = kv_mine[me]
    kv_sends = [remote(kv_mine.at[t], dt_rv.at[g_rows], kv_s.at[t], kv_r.at[me], t) for t in targets]
    for item in kv_sends:
        item.start()
    for i in range(FIRST + 1, n_chip):
        q_columns(i)
    w_sends[-1].start()
    w_own = local(dwt.at[pl.ds(0, hw), part_of(me, tok)], gw_hbm.at[own_rows], loc_sem.at[0])
    w_own.start()
    for t in range(width // tile):
        cols = slice(tile * t, tile * t + tile)
        dwt[hw:hw + hd, cols] = columns(kv_row, hb, cols)
    wk_own = local(dwt.at[pl.ds(hw, hd), part_of(me, tok)], gw_hbm.at[g_rows], loc_sem.at[1])
    wk_own.start()
    wk_sends = [remote(dwt.at[pl.ds(hw, hd), part_of(t, tok)], gw_hbm.at[g_rows], wk_s.at[t], wk_r.at[me], t) for t in targets]
    for item in wk_sends[0:HELD]:
        item.start()

    @pl.loop(last, 7 * parts)
    def _(event):
        ring_event(y_ring, event)

    ring_mate(y_ring, n_chip - 1, opposite)
    for t in range(width // tile):
        cols = slice(tile * t, tile * t + tile)
        dwo[:, cols] = columns(at_all, dyb, cols)
    store_wo = local(dwo, gwo_hbm, out_sem.at[0])
    store_wo.start()
    finish_ring(y_ring)
    wo_loads = [local(wo_hbm.at[pl.ds(pair * t, pair)], dyb.at[t], wo_sem.at[t]) for t in range(n_chip)]
    for item in wo_loads:
        item.start()

    @pl.loop(0, n_far)
    def _(f):
        c_far = ring_origin(2 * near + 1 + f)
        cos_t = trig[chip, 0:quarter, part_of(core, tok)]
        sin_t = trig[chip, quarter:2 * quarter, part_of(core, tok)]
        top = stat_far[f, 0]
        inv = 1.0 / stat_far[f, 1]
        row_dot = stat_far[f, 2] * inv

        def add_chunk(c, diagonal, chunks=1):
            rows = part_of(c, chunks * pair)
            for at in groups:
                keys = kv_far[f, rows, :]
                s = dot(keys, bmat_far[f, :, at])
                d_p = dot(keys, bmat_far[f, :, cols_q + at.start:cols_q + at.stop])
                if diagonal:
                    s = jnp.where(seen_far[:, at], s, -1e30)
                p = jnp.exp(s - top[:, at]) * inv[:, at]
                p_b = p.astype(BF)
                ds_b = (p * (d_p - row_dot[:, at])).astype(BF)
                d_q = dot(kvt_far[f, 0:hd, rows], ds_b)
                d_a = dot(kvt_far[f, hd:hw, rows], p_b)
                adq[0:hd, at] = d_q if diagonal else adq[0:hd, at] + d_q
                adq[hd:hw, at] = d_a if diagonal else adq[hd:hw, at] + d_a

        add_chunk(chip, True)

        @pl.loop(0, chip // 2)
        def _(c):
            add_chunk(c, False, 2)

        @pl.when(chip % 2 == 1)
        def _():
            add_chunk(chip - 1, False)

        for head in range(4):
            at = slice(tok * head, tok * head + tok)
            place = pl.ds(pl.multiple_of(c_far * 2 * hw + hd * head, hd), hd)
            at_rv[place, :] = adq[hd:hw, at].astype(BF)
            dt_rv[place, :] = jnp.concatenate(turned(adq[0:hd, at] * scale, cos_t, -sin_t), axis=0).astype(BF)

    for t in near_targets:
        remote(at_all.at[:, pl.ds(0, tok)], at_rv.at[part_of(t, hw)], a_s.at[t], a_r.at[t], t).wait_recv()
    for item in wo_loads:
        item.wait()
    for t in range(q_rows // tok):
        a_nat[:, tok * t:tok * t + tok] = at_rv[tok * t:tok * t + tok, :].T
    for t in range(width // tile):
        cols = slice(tile * t, tile * t + tile)
        prod = jnp.zeros((tok, tile), F32)
        for s in range(n_chip):
            prod += dot(a_nat[:, pair * s:pair * s + pair], dyb[s, :, cols])
        out_v[:, cols] = (x_v[:, cols].astype(F32) + prod).astype(BF)
    store_out = local(out_v, out_hbm, out_sem.at[1])
    store_out.start()

    def kv_place(t):
        return pl.ds(pl.multiple_of(q_rows + (t % 2) * kv_w + (t // 2) * hd, hd), hd)

    for t in near_targets:
        remote(dq_all.at[:, pl.ds(0, tok)], dt_rv.at[part_of(t, hw)], q_s.at[t], q_r.at[t], t).wait_recv()
    for t in targets:
        remote(kv_mine.at[0], dt_rv.at[kv_place(t)], kv_s.at[t], kv_r.at[t], t).wait_recv()
    swap.wait_send()
    for t in range(n_rows // tok):
        d_nat[:, tok * t:tok * t + tok] = dt_rv[tok * t:tok * t + tok, :].T

    mean = stat[0, :, 0:1]
    inv_std = stat[1, :, 0:1]
    dh = dkvt
    for t in range(width // tile):
        cols = slice(tile * t, tile * t + tile)
        acc = jnp.zeros((tok, tile), F32)
        for s in range(n_rows // tile):
            acc += dot(d_nat[:, tile * s:tile * s + tile], wt[tile * s:tile * s + tile, cols])
        dh[:, cols] = acc
        gg_st[0, :, cols] = col_sum(acc * ((x_v[:, cols].astype(F32) - mean) * inv_std))
        gg_st[1, :, cols] = col_sum(acc)
    g_swap = remote(gg_st.at[1 - core], gg_mx, g_s.at[n_chip], g_r.at[n_chip], mate)
    g_swap.start()
    g_swap.wait_recv()
    gg_my[...] = jnp.where(core == 0, gg_st[0], gg_st[1]) + gg_mx[...]
    gg_rv[chip] = gg_my[...]
    g_sends = [remote(gg_my, gg_rv.at[chip], g_s.at[c], g_r.at[chip], 2 * c + core) for c in far]
    for item in g_sends + wk_sends[HELD:]:
        item.start()

    grad_hat = dh[...] * gain_one
    x_hat = (x_v[...].astype(F32) - mean) * inv_std
    mean_one = row_mean(grad_hat)
    mean_two = row_mean(grad_hat * x_hat)
    store_out.wait()
    out_v[...] = (dy_own[...].astype(F32) + inv_std * (grad_hat - mean_one - x_hat * mean_two)).astype(BF)
    store_gx = local(out_v, gx_hbm, out_sem.at[2])
    store_gx.start()

    for c in far:
        remote(gg_my, gg_rv.at[c], g_s.at[c], g_r.at[c], 2 * c + core).wait_recv()
    sums = gg_rv[0]
    for c in range(1, n_chip):
        sums = sums + gg_rv[c]
    gg_out[core] = sums
    g_swap_out = remote(gg_out.at[core], gg_out.at[core], g_s.at[n_chip + 1], g_r.at[n_chip + 1], mate)
    g_swap_out.start()
    remote(gg_out.at[core], gg_out.at[1 - core], g_s.at[n_chip + 1], g_r.at[n_chip + 1], mate).wait_recv()
    store_gg = local(gg_out, gg_hbm, out_sem.at[3])
    store_gg.start()

    finish_ring(h_ring)
    for item in pos_sends + [g_swap, g_swap_out] + [opposite_send(head) for head in range(4)]:
        item.wait_send()
    for t in near_targets:
        remote(at_all.at[:, pl.ds(0, tok)], at_rv.at[pl.ds(0, hw)], a_s.at[t], a_r.at[t], t).wait_send()
        remote(dq_all.at[:, pl.ds(0, tok)], dt_rv.at[pl.ds(0, hw)], q_s.at[t], q_r.at[t], t).wait_send()
    for item in kv_sends + w_sends + g_sends + wk_sends:
        item.wait_send()
    for t in targets:
        remote(dwt.at[pl.ds(0, hw), part_of(t, tok)], gw_hbm.at[part_of(t, hw)], w_s.at[t], w_r.at[t], t).wait_recv()
        remote(dwt.at[pl.ds(hw, hd), part_of(t, tok)], gw_hbm.at[kv_place(t)], wk_s.at[t], wk_r.at[t], t).wait_recv()
    for item in (w_own, wk_own, store_wo, store_gx, store_gg):
        item.wait()


def settle_kernel(q_rows, kv_w, out_i, gx_i, gw_i, gwo_i, gg_i, out_o, gx_o, gq_o, gk_o, gv_o, gwo_o, gain_o, bias_o, b_act, b_q, b_kv, b_o, b_gg, sem_in, sem_out, sem_gg):
    half_q = q_rows // 2
    half_o = gwo_i.shape[0] // 2
    moves = [(out_i, b_act.at[0], out_o), (gx_i, b_act.at[1], gx_o)]
    for t in range(2):
        moves.append((gw_i.at[pl.ds(half_q * t, half_q)], b_q.at[t], gq_o.at[pl.ds(half_q * t, half_q)]))
        moves.append((gwo_i.at[pl.ds(half_o * t, half_o)], b_o.at[t], gwo_o.at[pl.ds(half_o * t, half_o)]))
    moves.append((gw_i.at[pl.ds(q_rows, kv_w)], b_kv.at[0], gk_o))
    moves.append((gw_i.at[pl.ds(q_rows + kv_w, kv_w)], b_kv.at[1], gv_o))
    loads = [pltpu.make_async_copy(src, mid, sem_in.at[i]) for i, (src, mid, _) in enumerate(moves)]
    stores = [pltpu.make_async_copy(mid, dst, sem_out.at[i]) for i, (_, mid, dst) in enumerate(moves)]
    load_gg = pltpu.make_async_copy(gg_i, b_gg, sem_gg)
    load_gg.start()
    for item in loads:
        item.start()
    for load, store in zip(loads, stores):
        load.wait()
        store.start()
    load_gg.wait()
    gain_o[...] = b_gg[0, 0]
    bias_o[...] = b_gg[1, 0]
    for item in stores:
        item.wait()


def solution(mesh):
    n_dev = mesh.shape['cp']

    def device_step(x_act, d_out, positions, ln_gain, ln_bias, w_query, w_key, w_value, w_out):
        tok, width = x_act.shape[1], x_act.shape[2]
        q_heads, hd = w_query.shape[1], w_query.shape[2]
        kv_heads = w_key.shape[1]
        q_w, kv_w = q_heads * hd, kv_heads * hd
        n_rows = q_w + 2 * kv_w
        seq = n_dev * tok
        hw = 2 * hd

        def flat_weight(w):
            return jnp.transpose(w, (1, 2, 0)).reshape(-1, width)

        hbm = pl.BlockSpec(memory_space=pltpu.HBM)
        vmem = pl.BlockSpec(memory_space=pltpu.VMEM)
        dma = pltpu.SemaphoreType.DMA
        n_chip = n_dev // 2
        n_far = n_chip - 1 - 2 * NEAR
        pair = 2 * tok
        scratch = [
            pltpu.VMEM((n_chip, pair, width), BF),
            pltpu.VMEM((n_chip, pair, width), BF),
            pltpu.VMEM((n_rows, width), BF),
            pltpu.VMEM((2 * hw, width), BF),
            pltpu.VMEM((hw, width), BF),
            pltpu.VMEM((n_far * hw, width), BF),
            pltpu.VMEM((n_dev, 1, tok), jnp.int32),
            pltpu.VMEM((n_chip, hd // 2, pair), F32),
            pltpu.VMEM((n_chip, hd, 2 * pair), BF),
            pltpu.VMEM((hw, seq), BF),
            pltpu.VMEM((seq, hw), BF),
            pltpu.VMEM((n_far, hw, seq), BF),
            pltpu.VMEM((n_far, seq, hw), BF),
            pltpu.VMEM((n_far, hw, 4 * pair), BF),
            pltpu.VMEM((n_far, 3, 1, 2 * pair), F32),
            pltpu.VMEM((hw, 4 * pair), BF),
            pltpu.VMEM((4, hd, tok), BF),
            pltpu.VMEM((seq, 2 * pair), F32),
            pltpu.VMEM((seq, 2 * pair), F32),
            pltpu.VMEM((n_chip, 1, 2 * pair), F32),
            pltpu.VMEM((hw, 2 * pair), F32),
            pltpu.VMEM((hw, seq), F32),
            pltpu.VMEM((hd, seq), F32),
            pltpu.VMEM((n_dev, hd, tok), BF),
            pltpu.VMEM((hd, seq), BF),
            pltpu.VMEM((hw, width), F32),
            pltpu.VMEM((hw + hd, width), F32),
            pltpu.VMEM((hw, seq), BF),
            pltpu.VMEM((hw, seq), BF),
            pltpu.VMEM((q_w, tok), BF),
            pltpu.VMEM((n_rows, tok), BF),
            pltpu.VMEM((tok, q_w), BF),
            pltpu.VMEM((tok, n_rows), BF),
            pltpu.VMEM((tok, width), BF),
            pltpu.VMEM((tok, width), BF),
            pltpu.VMEM((2, 1, width), F32),
            pltpu.VMEM((2, tok, 128), F32),
            pltpu.VMEM((tok, width), BF),
            pltpu.VMEM((2, 1, width), F32),
            pltpu.VMEM((1, width), F32),
            pltpu.VMEM((1, width), F32),
            pltpu.VMEM((n_chip, 1, width), F32),
            pltpu.VMEM((2, 1, width), F32),
            dma((10,)), dma((4 * n_far,)), dma((n_chip,)), dma((3,)), dma((4,)), dma((2,)),
        ] + [dma((9 * PARTS,)), dma((7 * PARTS,)), dma((8 * PARTS,)), dma((8 * PARTS,))] * 2 + [dma((4,))] * 2 + [dma((n_dev,))] * 6 + [dma] * 2 + [dma((n_dev,))] * 8
        out, gx, gw, gwo, gg = pl.pallas_call(
            functools.partial(block_kernel, n_dev, hd, kv_w, NEAR, PARTS),
            out_shape=(
                jax.ShapeDtypeStruct((tok, width), BF),
                jax.ShapeDtypeStruct((tok, width), BF),
                jax.ShapeDtypeStruct((n_rows, tok), F32),
                jax.ShapeDtypeStruct((hw, width), F32),
                jax.ShapeDtypeStruct((2, 1, width), F32),
            ),
            in_specs=[hbm] * 9,
            out_specs=(hbm,) * 5,
            scratch_shapes=scratch,
            compiler_params=pltpu.CompilerParams(collective_id=0, has_side_effects=True, vmem_limit_bytes=67043328),
            name='attn_block',
        )(
            x_act.reshape(tok, width), d_out.reshape(tok, width), positions.reshape(1, tok),
            ln_gain.reshape(1, width), ln_bias.reshape(1, width),
            flat_weight(w_query), flat_weight(w_key), flat_weight(w_value), w_out,
        )

        out, gx, gq, gk, gv, gwo, gain, bias = pl.pallas_call(
            functools.partial(settle_kernel, q_w, kv_w),
            out_shape=(
                jax.ShapeDtypeStruct((tok, width), BF),
                jax.ShapeDtypeStruct((tok, width), BF),
                jax.ShapeDtypeStruct((q_w, tok), F32),
                jax.ShapeDtypeStruct((kv_w, tok), F32),
                jax.ShapeDtypeStruct((kv_w, tok), F32),
                jax.ShapeDtypeStruct((hw, width), F32),
                jax.ShapeDtypeStruct((width,), F32),
                jax.ShapeDtypeStruct((width,), F32),
            ),
            in_specs=[hbm] * 5,
            out_specs=(hbm,) * 6 + (vmem,) * 2,
            scratch_shapes=[
                pltpu.VMEM((2, tok, width), BF),
                pltpu.VMEM((2, q_w // 2, tok), F32),
                pltpu.VMEM((2, kv_w, tok), F32),
                pltpu.VMEM((2, hw // 2, width), F32),
                pltpu.VMEM((2, 1, width), F32),
                dma((8,)), dma((8,)), dma,
            ],
            name='settle',
        )(out, gx, gw, gwo, gg)

        def rows_out(block, heads):
            return jnp.transpose(block.reshape(heads, hd, tok), (2, 0, 1))

        return (
            out.reshape(1, tok, width), gx.reshape(1, tok, width),
            rows_out(gq, q_heads), rows_out(gk, kv_heads), rows_out(gv, kv_heads),
            gwo, gain, bias,
        )

    return jax.shard_map(device_step, mesh=mesh, in_specs=(P('dp', 'cp', None), P('dp', 'cp', None), P('dp', 'cp'), P(None), P(None), P(None, None, None), P(None, None, None), P(None, None, None), P(None, None)), out_specs=(P('dp', 'cp', None), P('dp', 'cp', None), P(('dp', 'cp'), None, None), P(('dp', 'cp'), None, None), P(('dp', 'cp'), None, None), P(('dp', 'cp'), None), P('dp'), P('dp')), check_vma=False)
```

```python
import functools
import math

import jax
import jax.numpy as jnp
from jax import lax
from jax.experimental import pallas as pl
from jax.experimental.pallas import tpu as pltpu
from jax.sharding import PartitionSpec as P

EPS = 1e-5
ROPE_BASE = 10000.0
MESH = pl.DeviceIdType.MESH
BF = jnp.bfloat16
F32 = jnp.float32
NEAR = 0
PARTS = 4
FIRST = 1
HELD = 4


def dot(lhs, rhs):
    return jnp.dot(lhs, rhs, preferred_element_type=F32)


def col_sum(val):
    return jnp.sum(val, axis=0, keepdims=True)


def col_max(val):
    return jnp.max(val, axis=0, keepdims=True)


def row_mean(val):
    return jnp.mean(val, axis=-1, keepdims=True)


def dot_t(lhs, rhs):
    return lax.dot_general(lhs, rhs, (((1,), (1,)), ((), ())), preferred_element_type=F32)


def block_kernel(
    n_dev, hd, kv_w, near, parts,
    x_hbm, dy_hbm, pos_hbm, gain_hbm, bias_hbm, wq_hbm, wk_hbm, wv_hbm, wo_hbm,
    out_hbm, gx_hbm, gw_hbm, gwo_hbm, gg_hbm,
    hb, dyb, wt, wi, woi, pos_all, trig,
    qt, kvt, kv, kvt_far, kv_far, bmat_far, stat_far, bmat, da_rv, sbuf, dpbuf, mbuf, adq, dkvt, kv_rv, kv_mine, kv_row,
    dwo, dwt, at_all, dq_all, at_rv, dt_rv, a_nat, d_nat, x_v, dy_own, gb_v, stat, out_v, gg_st, gg_mx, gg_my, gg_rv, gg_out,
    in_sem, far_sem, wo_sem, w_sem, out_sem, loc_sem,
    hzs, hzr, hds, hdr, yzs, yzr, yds, ydr,
    d_s, d_r, pos_s, pos_r, a_s, a_r, q_s, q_r, x_s, x_r, kv_s, kv_r, w_s, w_r, wk_s, wk_r, g_s, g_r,
):
    tok, width = x_v.shape
    n_chip = n_dev // 2
    pair = 2 * tok
    me = lax.axis_index('cp')
    chip = me // 2
    core = me % 2
    right = 2 * ((chip + 1) % n_chip) + core
    left = 2 * ((chip + n_chip - 1) % n_chip) + core
    mate = 2 * chip + 1 - core
    q_rows = wq_hbm.shape[0]
    n_rows = q_rows + 2 * kv_w
    hw = 2 * hd
    quarter = hd // 4
    tile = 256
    scale = hd ** -0.5
    cols_q = 2 * pair
    n_far = n_chip - 1 - 2 * near

    def remote(src, dst, send, recv, target):
        return pltpu.make_async_remote_copy(src_ref=src, dst_ref=dst, send_sem=send, recv_sem=recv, device_id={'cp': target}, device_id_type=MESH)

    def local(src, dst, sem):
        return pltpu.make_async_copy(src, dst, sem)

    def part_of(i, size):
        return pl.ds(pl.multiple_of(i * size, size), size)

    def once(cond):
        return pl.loop(0, jnp.where(cond, 1, 0))

    def ring_steps(k):
        step = (k + 1) // 2
        return step, k % 2

    def ring_origin(k):
        step, ahead = ring_steps(k)
        return jnp.where(ahead == 1, chip + n_chip - step, chip + step) % n_chip

    own = (chip, part_of(core, tok))
    first_loads = [
        local(x_hbm, x_v, in_sem.at[0]),
        local(gain_hbm, gb_v.at[0], in_sem.at[1]),
        local(bias_hbm, gb_v.at[1], in_sem.at[2]),
        local(pos_hbm, pos_all.at[me], in_sem.at[3]),
    ]
    for item in first_loads:
        item.start()
    barrier = pltpu.get_barrier_semaphore()
    for step in range(1, n_dev):
        pl.semaphore_signal(barrier, inc=1, device_id={'cp': (me + step) % n_dev}, device_id_type=MESH)
    own_rows = part_of(me, hw)
    kv_rows = part_of(chip, hd)
    loads = [
        local(wq_hbm.at[own_rows], wi.at[pl.ds(0, hw)], in_sem.at[4]),
        local(wk_hbm.at[kv_rows], wi.at[pl.ds(hw, hd)], in_sem.at[5]),
        local(wv_hbm.at[kv_rows], wi.at[pl.ds(hw + hd, hd)], in_sem.at[6]),
        local(wo_hbm.at[own_rows], woi, in_sem.at[7]),
        local(dy_hbm, dyb.at[own], in_sem.at[8]),
        local(dy_hbm, dy_own, in_sem.at[9]),
    ]
    far_loads = []
    far_first = n_far * 2 * hw
    for f in range(n_far):
        c_far = ring_origin(2 * near + 1 + f)
        far_rows = part_of(c_far, hd)
        loads.append(local(wk_hbm.at[far_rows], wt.at[pl.ds(far_first + hw * f, hd)], far_sem.at[f]))
        loads.append(local(wv_hbm.at[far_rows], wt.at[pl.ds(far_first + hw * f + hd, hd)], far_sem.at[n_far + f]))
        far_w = part_of(c_far, pair)
        far_loads.append(local(wo_hbm.at[far_w], wt.at[pl.ds(pair * f, pair)], far_sem.at[2 * n_far + f]))
        far_loads.append(local(wq_hbm.at[far_w], dyb.at[c_far], far_sem.at[3 * n_far + f]))
    for item in loads + far_loads:
        item.start()

    for item in first_loads:
        item.wait()
    gain_one = 1.0 + gb_v[0]
    block = 16

    @pl.loop(0, tok // block)
    def _(i):
        rows = part_of(i, block)
        x_f = x_v[rows, :].astype(F32)
        mean = row_mean(x_f)
        centered = x_f - mean
        inv_std = lax.rsqrt(row_mean(centered * centered) + EPS)
        hb[chip, part_of(core * (tok // block) + i, block), :] = (centered * inv_std * gain_one + gb_v[1]).astype(BF)
        stat[0, rows, :] = jnp.broadcast_to(mean, (block, 128))
        stat[1, rows, :] = jnp.broadcast_to(inv_std, (block, 128))

    pl.semaphore_wait(barrier, n_dev - 1)

    def chunk(buf, origin, parity, part):
        return buf.at[origin, part_of(parts * parity + part, tok // parts)]

    turns = 2 * parts

    def own_sends(buf, zs, zr, ds, dr):
        copies = []
        for part in range(parts):
            piece = chunk(buf, chip, core, part)
            copies.append(remote(piece, piece, zs.at[2 * part], zr.at[2 * part], right))
            copies.append(remote(piece, piece, zs.at[2 * part + 1], zr.at[2 * part + 1], left))
            copies.append(remote(piece, piece, ds.at[7 * parts + part], dr.at[7 * parts + part], mate))
        return copies

    def event_place(event):
        step = event // turns + 1
        turn = event % turns
        direction = turn % 2
        part = jnp.where(step < 4, turn // 2, turn // 2 + direction * (parts // 2))
        origin = jnp.where(direction == 0, chip + n_chip - step, chip + step) % n_chip
        return step, direction, part, origin

    def last_event(part, direction):
        return 6 * parts + 2 * (part - direction * (parts // 2)) + direction

    def ring_event(ring, event):
        buf, zs, zr, ds, dr = ring
        step, direction, part, origin = event_place(event)
        piece = chunk(buf, origin, core, part)
        remote(piece, piece, zs.at[0], zr.at[event], right).wait_recv()
        onward = jnp.where(step < 3, event + turns, last_event(part, direction))

        @pl.when((step < 3) | ((step == 3) & ((part >= parts // 2) == (direction == 1))))
        def _():
            remote(piece, piece, zs.at[event + turns], zr.at[onward], jnp.where(direction == 0, right, left)).start()

        remote(piece, piece, ds.at[event], dr.at[event], mate).start()

    def ring_service(ring, event):
        @pl.when(event < 7 * parts)
        def _():
            ring_event(ring, event)

    def ring_mate(ring, k, origin):
        buf, zs, zr, ds, dr = ring
        step, ahead = ring_steps(k)
        for part in range(parts):
            event = jnp.where(k == 0, 7 * parts + part, jnp.where(step < 4, turns * (step - 1) + 2 * part + 1 - ahead, last_event(part, part // (parts // 2))))
            piece = chunk(buf, origin, 1 - core, part)
            remote(piece, piece, ds.at[0], dr.at[event], mate).wait_recv()

    def finish_ring(ring):
        buf, zs, zr, ds, dr = ring
        for item in own_sends(*ring):
            item.wait_send()

        @pl.loop(0, 7 * parts)
        def _(event):
            step, direction, part, origin = event_place(event)
            piece = chunk(buf, origin, core, part)

            @pl.when((step < 3) | ((step == 3) & ((part >= parts // 2) == (direction == 1))))
            def _():
                remote(piece, piece, zs.at[event + turns], zr.at[event], right).wait_send()

            remote(piece, piece, ds.at[event], dr.at[event], mate).wait_send()

    h_ring = (hb, hzs, hzr, hds, hdr)
    y_ring = (dyb, yzs, yzr, yds, ydr)
    for item in own_sends(*h_ring):
        item.start()
    pos_sends = [remote(pos_all.at[me], pos_all.at[me], pos_s.at[step], pos_r.at[me], (me + step) % n_dev) for step in range(1, n_dev)]
    for item in pos_sends:
        item.start()
    weight_loads = [
        local(wq_hbm, wt.at[pl.ds(0, q_rows)], w_sem.at[0]),
        local(wk_hbm, wt.at[pl.ds(q_rows, kv_w)], w_sem.at[1]),
        local(wv_hbm, wt.at[pl.ds(q_rows + kv_w, kv_w)], w_sem.at[2]),
    ]
    dkvt[...] = jnp.zeros_like(dkvt)
    bmat[...] = jnp.zeros_like(bmat)
    bmat_far[...] = jnp.zeros_like(bmat_far)
    for f in range(n_far):
        stat_far[f, 0] = jnp.full((1, cols_q), -3e38, F32)
        stat_far[f, 1] = jnp.zeros((1, cols_q), F32)
        stat_far[f, 2] = jnp.zeros((1, cols_q), F32)

    freq = jnp.exp(lax.broadcasted_iota(jnp.int32, (quarter, tok), 0).astype(F32) * (-2.0 * math.log(ROPE_BASE) / (hd // 2)))

    def make_trig(b):
        for t in range(2):
            slot = 2 * b + t

            @pl.when(slot != me)
            def _():
                remote(pos_all.at[slot], pos_all.at[slot], pos_s.at[0], pos_r.at[slot], me).wait_recv()

            angle = pos_all[slot].astype(F32) * freq
            trig[b, 0:quarter, tok * t:tok * t + tok] = jnp.cos(angle)
            trig[b, quarter:2 * quarter, tok * t:tok * t + tok] = jnp.sin(angle)

    def turned(val, cos_t, sin_t):
        u = val[0:quarter]
        w = val[quarter:2 * quarter]
        return [u * cos_t - w * sin_t, w * cos_t + u * sin_t, val[2 * quarter:hd]]

    def eighth(val):
        return val.astype(BF) * jnp.asarray(scale, BF)

    def keys_values(val, cos_t, sin_t):
        return jnp.concatenate(turned(val[0:hd], cos_t, sin_t) + [val[hd:hw]], axis=0).astype(BF)

    lane = lax.broadcasted_iota(jnp.int32, (pair, cols_q), 1)
    row = lax.broadcasted_iota(jnp.int32, (pair, cols_q), 0)
    seen_far = row <= core * tok + lane % tok

    opposite = ring_origin(n_chip - 1)

    def opposite_send(head):
        block = bmat_far.at[n_far - 1, pl.ds(hd, hd), pl.ds(cols_q + tok * head, tok)]
        return remote(block, da_rv.at[2 * core + head % 2], d_s.at[head], d_r.at[2 * core + head % 2], 2 * opposite + head // 2)

    @pl.loop(0, n_chip)
    def _(k):
        for turn in range(2):
            ring_service(h_ring, parts * k + turn)

        @pl.when(k % 2 == 1)
        def _():
            ring_service(h_ring, parts * k + 2)


        @once(k == 0)
        def _(_):
            for item in loads:
                item.wait()

        b = ring_origin(k)
        ring_mate(h_ring, k, b)
        make_trig(b)

        @once(k == 0)
        def _(_):
            for item in far_loads:
                item.wait()
            cos_t = trig[chip, 0:quarter, part_of(core, tok)]
            sin_t = trig[chip, quarter:2 * quarter, part_of(core, tok)]

            @pl.loop(0, n_far)
            def _(f):
                da_t = dot_t(wt[part_of(f, 2 * hw), :], dy_own[...]).astype(BF)
                q_t = dot_t(dyb[ring_origin(2 * near + 1 + f)], hb[chip, part_of(core, tok), :])
                for head in range(4):
                    part = slice(hd * head, hd * head + hd)
                    at = tok * head
                    bmat_far[f, 0:hd, at:at + tok] = eighth(jnp.concatenate(turned(q_t[part], cos_t, sin_t), axis=0))
                    bmat_far[f, hd:hw, cols_q + at:cols_q + at + tok] = da_t[part]

        @once(k == 1)
        def _(_):
            for head in range(4):
                opposite_send(head).start()

        place = part_of(b, pair)
        cos_t = trig[b, 0:quarter, :]
        sin_t = trig[b, quarter:2 * quarter, :]
        flat = dot_t(wi[...], hb[b])
        for head in range(2):
            q_rot = eighth(jnp.concatenate(turned(flat[hd * head:hd * head + hd], cos_t, sin_t), axis=0))
            for t in range(2):
                lane = pair * t + tok * head
                qt[b, :, lane:lane + tok] = q_rot[:, tok * t:tok * t + tok]
        kv_rot = keys_values(flat[hw:2 * hw], cos_t, sin_t)
        kvt[:, place] = kv_rot
        kv[place, :] = kv_rot.T

        @pl.when(k % 2 == 0)
        def _():
            ring_service(h_ring, parts * k + 2)

        ring_service(h_ring, parts * k + parts - 1)

        @once(k == 5)
        def _(_):
            for item in own_sends(*y_ring):
                item.start()

        @pl.when(b <= chip)
        def _():
            flat_far = dot_t(wt[far_first:far_first + n_far * hw, :], hb[b])
            for f in range(n_far):
                far_rot = keys_values(flat_far[hw * f:hw * f + hw], cos_t, sin_t)
                kvt_far[f, :, place] = far_rot
                kv_far[f, place, :] = far_rot.T

            @pl.loop(0, n_far)
            def _(f):
                both = dot(kv_far[f, place, :], bmat_far[f])
                s = jnp.where(seen_far | (k > 0), both[:, 0:cols_q], -1e30)
                old = stat_far[f, 0]
                new = jnp.maximum(old, col_max(s))
                p = jnp.exp(s - new)
                keep = jnp.exp(old - new)
                stat_far[f, 0] = new
                stat_far[f, 1] = stat_far[f, 1] * keep + col_sum(p)
                stat_far[f, 2] = stat_far[f, 2] * keep + col_sum(p * both[:, cols_q:2 * cols_q])

    groups = [slice(tile * g, tile * g + tile) for g in range(cols_q // tile)]

    def first_part(b, seen):
        def both_of(rows):
            both = dot(kv[rows, :], bmat[...])
            return both[:, 0:cols_q], both[:, cols_q:2 * cols_q]

        rows = part_of(b, pair)
        s, d_p = both_of(rows)
        s = jnp.where(seen, s, -1e30)
        top = col_max(s)
        p = jnp.exp(s - top)
        sbuf[rows, :] = p
        dpbuf[rows, :] = d_p
        mbuf[b] = top

        def step(c, state, chunks=1):
            old, total, weighted = state
            rows = part_of(c, chunks * pair)
            s, d_p = both_of(rows)
            new = jnp.maximum(old, col_max(s))
            p = jnp.exp(s - new)
            sbuf[rows, :] = p
            dpbuf[rows, :] = d_p
            for i in range(chunks):
                mbuf[chunks * c + i] = new
            keep = jnp.exp(old - new)
            return new, total * keep + col_sum(p), weighted * keep + col_sum(p * d_p)

        state = (top, col_sum(p), col_sum(p * d_p))
        state = lax.fori_loop(0, b // 2, functools.partial(step, chunks=2), state)
        top, total, weighted = lax.fori_loop(2 * (b // 2), b, step, state)
        inv = 1.0 / total
        return top, inv, weighted * inv

    def second_part(b, stats):
        top, inv, row_dot = stats
        adq[...] = jnp.zeros_like(adq)

        def step(c, carry):
            rows = part_of(c, pair)
            factor = jnp.exp(mbuf[c] - top) * inv
            d_k = d_v = None
            for at in groups:
                p = sbuf[rows, at] * factor[:, at]
                p_b = p.astype(BF)
                ds_b = (p * (dpbuf[rows, at] - row_dot[:, at])).astype(BF)
                adq[0:hd, at] += dot(kvt[0:hd, rows], ds_b)
                adq[hd:hw, at] += dot(kvt[hd:hw, rows], p_b)
                more_k = dot_t(bmat[0:hd, at], ds_b)
                more_v = dot_t(bmat[hd:hw, cols_q + at.start:cols_q + at.stop], p_b)
                d_k = more_k if d_k is None else d_k + more_k
                d_v = more_v if d_v is None else d_v + more_v
            dkvt[0:hd, rows] += d_k
            dkvt[hd:hw, rows] += d_v
            return carry

        lax.fori_loop(0, b + 1, step, 0)


    def send_rows(slot):
        cols = part_of(slot, tok)
        return [
            remote(dq_all.at[:, cols], dt_rv.at[own_rows], q_s.at[slot], q_r.at[me], slot),
            remote(at_all.at[:, cols], at_rv.at[own_rows], a_s.at[slot], a_r.at[me], slot),
        ]

    last = 6 * parts

    def serve(event):
        @pl.when(event < last)
        def _():
            ring_event(y_ring, event)

    @pl.loop(0, n_chip)
    def _(j):
        k = j - 1

        @pl.when(k == 0)
        def _():
            for turn in range(2):
                ring_event(y_ring, k + turn)

        @pl.when((k % 2 == 1) & (k > 0))
        def _():
            for turn in range(2, parts):
                serve(parts * k + turn)

        b = jnp.where(j == 0, opposite, ring_origin(jnp.maximum(k, 0)))

        @once(j == 0)
        def _(_):
            for item in weight_loads:
                item.start()

        @pl.loop(0, jnp.where(j == n_chip - 1, 2 + 4 * near, 0))
        def _(early):
            slot = 2 * ring_origin(early // 2) + early % 2

            @pl.when(slot != me)
            def _():
                for item in send_rows(slot):
                    item.start()

        bmat[0:hd, 0:cols_q] = qt[b]

        @once(j == 0)
        def _(_):
            for i in range(4):
                remote(da_rv.at[i], da_rv.at[i], d_s.at[0], d_r.at[i], mate).wait_recv()
                bmat[hd:hw, cols_q + tok * i:cols_q + tok * i + tok] = da_rv[i]

        @once(j > 0)
        def _(_):
            ring_mate(y_ring, k, b)
            da_t = dot_t(woi[...], dyb[b]).astype(BF)
            for t in range(2):
                for head in range(2):
                    at = cols_q + pair * t + tok * head
                    bmat[hd:hw, at:at + tok] = da_t[hd * head:hd * head + hd, tok * t:tok * t + tok]

        stats = first_part(b, row <= (lane // pair) * tok + lane % tok)
        for turn in range(2):
            serve(jnp.where(k < 0, last, parts * k + 2 + 2 * (k % 2)) + turn)
        second_part(b, stats)
        for t in range(2):
            slot = 2 * b + t
            lanes = [slice(pair * t + tok * head, pair * t + tok * head + tok) for head in range(2)]
            a_t = jnp.concatenate([adq[hd:hw, at] for at in lanes], axis=0).astype(BF)
            cos_t = trig[b, 0:quarter, tok * t:tok * t + tok]
            sin_t = trig[b, quarter:2 * quarter, tok * t:tok * t + tok]
            dq_t = jnp.concatenate([piece for at in lanes for piece in turned(adq[0:hd, at] * scale, cos_t, -sin_t)], axis=0).astype(BF)
            at_all[:, part_of(slot, tok)] = a_t
            dq_all[:, part_of(slot, tok)] = dq_t

            @pl.when(slot == me)
            def _():
                at_rv[own_rows, :] = a_t
                dt_rv[own_rows, :] = dq_t

        @pl.when((k % 2 == 0) & (k >= 0))
        def _():
            for turn in range(2):
                serve(parts * j + turn)

    far = [ring_origin(k) for k in range(n_chip - 1, 0, -1)]
    targets = [2 * c + p for c in far for p in range(2)] + [mate]
    near_targets = targets[-1 - 4 * near:]
    swap = remote(dkvt.at[part_of(1 - core, hd)], kv_rv, x_s, x_r, mate)
    swap.start()
    w_sends = [remote(dwt.at[pl.ds(0, hw), part_of(t, tok)], gw_hbm.at[own_rows], w_s.at[t], w_r.at[me], t) for t in targets]

    def columns(rows_all, buf, cols):
        acc = jnp.zeros((rows_all.shape[0], tile), F32)
        for s in range(n_chip):
            acc += dot(rows_all[:, pair * s:pair * s + pair], buf[s, :, cols])
        return acc

    def q_columns(i):
        cols = part_of(far[i] if i < n_chip - 1 else chip, pair)
        dwt[0:hw, cols] = columns(dq_all, hb, cols)
        for item in w_sends[max(2 * i - 2, 0):2 * i]:
            item.start()

    for i in range(FIRST + 1):
        q_columns(i)

    swap.wait_recv()
    mine = part_of(core, hd)
    g_rows = pl.ds(pl.multiple_of(q_rows + core * kv_w + chip * hd, hd), hd)
    for t in range(n_chip):
        cols = slice(pair * t, pair * t + pair)
        g = dkvt[mine, cols] + kv_rv[:, cols]
        cos_t = jnp.where(core == 0, trig[t, 0:quarter, :], 1.0)
        sin_t = jnp.where(core == 0, trig[t, quarter:2 * quarter, :], 0.0)
        g_b = jnp.concatenate(turned(g, cos_t, -sin_t), axis=0).astype(BF)
        kv_mine[2 * t] = g_b[:, 0:tok]
        kv_mine[2 * t + 1] = g_b[:, tok:pair]
        kv_row[:, cols] = g_b
    dt_rv[g_rows, :] = kv_mine[me]
    kv_sends = [remote(kv_mine.at[t], dt_rv.at[g_rows], kv_s.at[t], kv_r.at[me], t) for t in targets]
    for item in kv_sends:
        item.start()
    for i in range(FIRST + 1, n_chip):
        q_columns(i)
    w_sends[-1].start()
    w_own = local(dwt.at[pl.ds(0, hw), part_of(me, tok)], gw_hbm.at[own_rows], loc_sem.at[0])
    w_own.start()
    for t in range(width // tile):
        cols = slice(tile * t, tile * t + tile)
        dwt[hw:hw + hd, cols] = columns(kv_row, hb, cols)
    wk_own = local(dwt.at[pl.ds(hw, hd), part_of(me, tok)], gw_hbm.at[g_rows], loc_sem.at[1])
    wk_own.start()
    wk_sends = [remote(dwt.at[pl.ds(hw, hd), part_of(t, tok)], gw_hbm.at[g_rows], wk_s.at[t], wk_r.at[me], t) for t in targets]
    for item in wk_sends[0:HELD]:
        item.start()

    @pl.loop(last, 7 * parts)
    def _(event):
        ring_event(y_ring, event)

    ring_mate(y_ring, n_chip - 1, opposite)
    for t in range(width // tile):
        cols = slice(tile * t, tile * t + tile)
        dwo[:, cols] = columns(at_all, dyb, cols)
    store_wo = local(dwo, gwo_hbm, out_sem.at[0])
    store_wo.start()
    finish_ring(y_ring)
    wo_loads = [local(wo_hbm.at[pl.ds(pair * t, pair)], dyb.at[t], wo_sem.at[t]) for t in range(n_chip)]
    for item in wo_loads:
        item.start()

    @pl.loop(0, n_far)
    def _(f):
        c_far = ring_origin(2 * near + 1 + f)
        cos_t = trig[chip, 0:quarter, part_of(core, tok)]
        sin_t = trig[chip, quarter:2 * quarter, part_of(core, tok)]
        top = stat_far[f, 0]
        inv = 1.0 / stat_far[f, 1]
        row_dot = stat_far[f, 2] * inv

        def add_chunk(c, diagonal, chunks=1):
            rows = part_of(c, chunks * pair)
            for at in groups:
                keys = kv_far[f, rows, :]
                s = dot(keys, bmat_far[f, :, at])
                d_p = dot(keys, bmat_far[f, :, cols_q + at.start:cols_q + at.stop])
                if diagonal:
                    s = jnp.where(seen_far[:, at], s, -1e30)
                p = jnp.exp(s - top[:, at]) * inv[:, at]
                p_b = p.astype(BF)
                ds_b = (p * (d_p - row_dot[:, at])).astype(BF)
                d_q = dot(kvt_far[f, 0:hd, rows], ds_b)
                d_a = dot(kvt_far[f, hd:hw, rows], p_b)
                adq[0:hd, at] = d_q if diagonal else adq[0:hd, at] + d_q
                adq[hd:hw, at] = d_a if diagonal else adq[hd:hw, at] + d_a

        add_chunk(chip, True)

        @pl.loop(0, chip // 2)
        def _(c):
            add_chunk(c, False, 2)

        @pl.when(chip % 2 == 1)
        def _():
            add_chunk(chip - 1, False)

        for head in range(4):
            at = slice(tok * head, tok * head + tok)
            place = pl.ds(pl.multiple_of(c_far * 2 * hw + hd * head, hd), hd)
            at_rv[place, :] = adq[hd:hw, at].astype(BF)
            dt_rv[place, :] = jnp.concatenate(turned(adq[0:hd, at] * scale, cos_t, -sin_t), axis=0).astype(BF)

    for t in near_targets:
        remote(at_all.at[:, pl.ds(0, tok)], at_rv.at[part_of(t, hw)], a_s.at[t], a_r.at[t], t).wait_recv()
    for item in wo_loads:
        item.wait()
    for t in range(q_rows // tok):
        a_nat[:, tok * t:tok * t + tok] = at_rv[tok * t:tok * t + tok, :].T
    for t in range(width // tile):
        cols = slice(tile * t, tile * t + tile)
        prod = jnp.zeros((tok, tile), F32)
        for s in range(n_chip):
            prod += dot(a_nat[:, pair * s:pair * s + pair], dyb[s, :, cols])
        out_v[:, cols] = (x_v[:, cols].astype(F32) + prod).astype(BF)
    store_out = local(out_v, out_hbm, out_sem.at[1])
    store_out.start()

    for item in weight_loads:
        item.wait()

    def kv_place(t):
        return pl.ds(pl.multiple_of(q_rows + (t % 2) * kv_w + (t // 2) * hd, hd), hd)

    for t in near_targets:
        remote(dq_all.at[:, pl.ds(0, tok)], dt_rv.at[part_of(t, hw)], q_s.at[t], q_r.at[t], t).wait_recv()
    for t in targets:
        remote(kv_mine.at[0], dt_rv.at[kv_place(t)], kv_s.at[t], kv_r.at[t], t).wait_recv()
    swap.wait_send()
    for t in range(n_rows // tok):
        d_nat[:, tok * t:tok * t + tok] = dt_rv[tok * t:tok * t + tok, :].T

    mean = stat[0, :, 0:1]
    inv_std = stat[1, :, 0:1]
    dh = dkvt
    for t in range(width // tile):
        cols = slice(tile * t, tile * t + tile)
        acc = jnp.zeros((tok, tile), F32)
        for s in range(n_rows // tile):
            acc += dot(d_nat[:, tile * s:tile * s + tile], wt[tile * s:tile * s + tile, cols])
        dh[:, cols] = acc
        gg_st[0, :, cols] = col_sum(acc * ((x_v[:, cols].astype(F32) - mean) * inv_std))
        gg_st[1, :, cols] = col_sum(acc)
    g_swap = remote(gg_st.at[1 - core], gg_mx, g_s.at[n_chip], g_r.at[n_chip], mate)
    g_swap.start()
    g_swap.wait_recv()
    gg_my[...] = jnp.where(core == 0, gg_st[0], gg_st[1]) + gg_mx[...]
    gg_rv[chip] = gg_my[...]
    g_sends = [remote(gg_my, gg_rv.at[chip], g_s.at[c], g_r.at[chip], 2 * c + core) for c in far]
    for item in g_sends + wk_sends[HELD:]:
        item.start()

    grad_hat = dh[...] * gain_one
    x_hat = (x_v[...].astype(F32) - mean) * inv_std
    mean_one = row_mean(grad_hat)
    mean_two = row_mean(grad_hat * x_hat)
    store_out.wait()
    out_v[...] = (dy_own[...].astype(F32) + inv_std * (grad_hat - mean_one - x_hat * mean_two)).astype(BF)
    store_gx = local(out_v, gx_hbm, out_sem.at[2])
    store_gx.start()

    for c in far:
        remote(gg_my, gg_rv.at[c], g_s.at[c], g_r.at[c], 2 * c + core).wait_recv()
    sums = gg_rv[0]
    for c in range(1, n_chip):
        sums = sums + gg_rv[c]
    gg_out[core] = sums
    g_swap_out = remote(gg_out.at[core], gg_out.at[core], g_s.at[n_chip + 1], g_r.at[n_chip + 1], mate)
    g_swap_out.start()
    remote(gg_out.at[core], gg_out.at[1 - core], g_s.at[n_chip + 1], g_r.at[n_chip + 1], mate).wait_recv()
    store_gg = local(gg_out, gg_hbm, out_sem.at[3])
    store_gg.start()

    finish_ring(h_ring)
    for item in pos_sends + [g_swap, g_swap_out] + [opposite_send(head) for head in range(4)]:
        item.wait_send()
    for t in near_targets:
        remote(at_all.at[:, pl.ds(0, tok)], at_rv.at[pl.ds(0, hw)], a_s.at[t], a_r.at[t], t).wait_send()
        remote(dq_all.at[:, pl.ds(0, tok)], dt_rv.at[pl.ds(0, hw)], q_s.at[t], q_r.at[t], t).wait_send()
    for item in kv_sends + w_sends + g_sends + wk_sends:
        item.wait_send()
    for t in targets:
        remote(dwt.at[pl.ds(0, hw), part_of(t, tok)], gw_hbm.at[part_of(t, hw)], w_s.at[t], w_r.at[t], t).wait_recv()
        remote(dwt.at[pl.ds(hw, hd), part_of(t, tok)], gw_hbm.at[kv_place(t)], wk_s.at[t], wk_r.at[t], t).wait_recv()
    for item in (w_own, wk_own, store_wo, store_gx, store_gg):
        item.wait()


def settle_kernel(q_rows, kv_w, out_i, gx_i, gw_i, gwo_i, gg_i, out_o, gx_o, gq_o, gk_o, gv_o, gwo_o, gain_o, bias_o, b_act, b_q, b_kv, b_o, b_gg, sem_in, sem_out, sem_gg):
    half_q = q_rows // 2
    half_o = gwo_i.shape[0] // 2
    moves = [(out_i, b_act.at[0], out_o), (gx_i, b_act.at[1], gx_o)]
    for t in range(2):
        moves.append((gw_i.at[pl.ds(half_q * t, half_q)], b_q.at[t], gq_o.at[pl.ds(half_q * t, half_q)]))
        moves.append((gwo_i.at[pl.ds(half_o * t, half_o)], b_o.at[t], gwo_o.at[pl.ds(half_o * t, half_o)]))
    moves.append((gw_i.at[pl.ds(q_rows, kv_w)], b_kv.at[0], gk_o))
    moves.append((gw_i.at[pl.ds(q_rows + kv_w, kv_w)], b_kv.at[1], gv_o))
    loads = [pltpu.make_async_copy(src, mid, sem_in.at[i]) for i, (src, mid, _) in enumerate(moves)]
    stores = [pltpu.make_async_copy(mid, dst, sem_out.at[i]) for i, (_, mid, dst) in enumerate(moves)]
    load_gg = pltpu.make_async_copy(gg_i, b_gg, sem_gg)
    load_gg.start()
    for item in loads:
        item.start()
    for load, store in zip(loads, stores):
        load.wait()
        store.start()
    load_gg.wait()
    gain_o[...] = b_gg[0, 0]
    bias_o[...] = b_gg[1, 0]
    for item in stores:
        item.wait()


def solution(mesh):
    n_dev = mesh.shape['cp']

    def device_step(x_act, d_out, positions, ln_gain, ln_bias, w_query, w_key, w_value, w_out):
        tok, width = x_act.shape[1], x_act.shape[2]
        q_heads, hd = w_query.shape[1], w_query.shape[2]
        kv_heads = w_key.shape[1]
        q_w, kv_w = q_heads * hd, kv_heads * hd
        n_rows = q_w + 2 * kv_w
        seq = n_dev * tok
        hw = 2 * hd

        def flat_weight(w):
            return jnp.transpose(w, (1, 2, 0)).reshape(-1, width)

        hbm = pl.BlockSpec(memory_space=pltpu.HBM)
        vmem = pl.BlockSpec(memory_space=pltpu.VMEM)
        dma = pltpu.SemaphoreType.DMA
        n_chip = n_dev // 2
        n_far = n_chip - 1 - 2 * NEAR
        pair = 2 * tok
        scratch = [
            pltpu.VMEM((n_chip, pair, width), BF),
            pltpu.VMEM((n_chip, pair, width), BF),
            pltpu.VMEM((n_rows, width), BF),
            pltpu.VMEM((2 * hw, width), BF),
            pltpu.VMEM((hw, width), BF),
            pltpu.VMEM((n_dev, 1, tok), jnp.int32),
            pltpu.VMEM((n_chip, hd // 2, pair), F32),
            pltpu.VMEM((n_chip, hd, 2 * pair), BF),
            pltpu.VMEM((hw, seq), BF),
            pltpu.VMEM((seq, hw), BF),
            pltpu.VMEM((n_far, hw, seq), BF),
            pltpu.VMEM((n_far, seq, hw), BF),
            pltpu.VMEM((n_far, hw, 4 * pair), BF),
            pltpu.VMEM((n_far, 3, 1, 2 * pair), F32),
            pltpu.VMEM((hw, 4 * pair), BF),
            pltpu.VMEM((4, hd, tok), BF),
            pltpu.VMEM((seq, 2 * pair), F32),
            pltpu.VMEM((seq, 2 * pair), F32),
            pltpu.VMEM((n_chip, 1, 2 * pair), F32),
            pltpu.VMEM((hw, 2 * pair), F32),
            pltpu.VMEM((hw, seq), F32),
            pltpu.VMEM((hd, seq), F32),
            pltpu.VMEM((n_dev, hd, tok), BF),
            pltpu.VMEM((hd, seq), BF),
            pltpu.VMEM((hw, width), F32),
            pltpu.VMEM((hw + hd, width), F32),
            pltpu.VMEM((hw, seq), BF),
            pltpu.VMEM((hw, seq), BF),
            pltpu.VMEM((q_w, tok), BF),
            pltpu.VMEM((n_rows, tok), BF),
            pltpu.VMEM((tok, q_w), BF),
            pltpu.VMEM((tok, n_rows), BF),
            pltpu.VMEM((tok, width), BF),
            pltpu.VMEM((tok, width), BF),
            pltpu.VMEM((2, 1, width), F32),
            pltpu.VMEM((2, tok, 128), F32),
            pltpu.VMEM((tok, width), BF),
            pltpu.VMEM((2, 1, width), F32),
            pltpu.VMEM((1, width), F32),
            pltpu.VMEM((1, width), F32),
            pltpu.VMEM((n_chip, 1, width), F32),
            pltpu.VMEM((2, 1, width), F32),
            dma((10,)), dma((4 * n_far,)), dma((n_chip,)), dma((3,)), dma((4,)), dma((2,)),
        ] + [dma((9 * PARTS,)), dma((7 * PARTS,)), dma((8 * PARTS,)), dma((8 * PARTS,))] * 2 + [dma((4,))] * 2 + [dma((n_dev,))] * 6 + [dma] * 2 + [dma((n_dev,))] * 8
        out, gx, gw, gwo, gg = pl.pallas_call(
            functools.partial(block_kernel, n_dev, hd, kv_w, NEAR, PARTS),
            out_shape=(
                jax.ShapeDtypeStruct((tok, width), BF),
                jax.ShapeDtypeStruct((tok, width), BF),
                jax.ShapeDtypeStruct((n_rows, tok), F32),
                jax.ShapeDtypeStruct((hw, width), F32),
                jax.ShapeDtypeStruct((2, 1, width), F32),
            ),
            in_specs=[hbm] * 9,
            out_specs=(hbm,) * 5,
            scratch_shapes=scratch,
            compiler_params=pltpu.CompilerParams(collective_id=0, has_side_effects=True, vmem_limit_bytes=67043328),
            name='attn_block',
        )(
            x_act.reshape(tok, width), d_out.reshape(tok, width), positions.reshape(1, tok),
            ln_gain.reshape(1, width), ln_bias.reshape(1, width),
            flat_weight(w_query), flat_weight(w_key), flat_weight(w_value), w_out,
        )

        out, gx, gq, gk, gv, gwo, gain, bias = pl.pallas_call(
            functools.partial(settle_kernel, q_w, kv_w),
            out_shape=(
                jax.ShapeDtypeStruct((tok, width), BF),
                jax.ShapeDtypeStruct((tok, width), BF),
                jax.ShapeDtypeStruct((q_w, tok), F32),
                jax.ShapeDtypeStruct((kv_w, tok), F32),
                jax.ShapeDtypeStruct((kv_w, tok), F32),
                jax.ShapeDtypeStruct((hw, width), F32),
                jax.ShapeDtypeStruct((width,), F32),
                jax.ShapeDtypeStruct((width,), F32),
            ),
            in_specs=[hbm] * 5,
            out_specs=(hbm,) * 6 + (vmem,) * 2,
            scratch_shapes=[
                pltpu.VMEM((2, tok, width), BF),
                pltpu.VMEM((2, q_w // 2, tok), F32),
                pltpu.VMEM((2, kv_w, tok), F32),
                pltpu.VMEM((2, hw // 2, width), F32),
                pltpu.VMEM((2, 1, width), F32),
                dma((8,)), dma((8,)), dma,
            ],
            name='settle',
        )(out, gx, gw, gwo, gg)

        def rows_out(block, heads):
            return jnp.transpose(block.reshape(heads, hd, tok), (2, 0, 1))

        return (
            out.reshape(1, tok, width), gx.reshape(1, tok, width),
            rows_out(gq, q_heads), rows_out(gk, kv_heads), rows_out(gv, kv_heads),
            gwo, gain, bias,
        )

    return jax.shard_map(device_step, mesh=mesh, in_specs=(P('dp', 'cp', None), P('dp', 'cp', None), P('dp', 'cp'), P(None), P(None), P(None, None, None), P(None, None, None), P(None, None, None), P(None, None)), out_specs=(P('dp', 'cp', None), P('dp', 'cp', None), P(('dp', 'cp'), None, None), P(('dp', 'cp'), None, None), P(('dp', 'cp'), None, None), P(('dp', 'cp'), None), P('dp'), P('dp')), check_vma=False)
```

```python
import functools
import math

import jax
import jax.numpy as jnp
from jax import lax
from jax.experimental import pallas as pl
from jax.experimental.pallas import tpu as pltpu
from jax.sharding import PartitionSpec as P

EPS = 1e-5
ROPE_BASE = 10000.0
MESH = pl.DeviceIdType.MESH
BF = jnp.bfloat16
F32 = jnp.float32
NEAR = 1
PARTS = 4
FIRST = 1
HELD = 4


def dot(lhs, rhs):
    return jnp.dot(lhs, rhs, preferred_element_type=F32)


def col_sum(val):
    return jnp.sum(val, axis=0, keepdims=True)


def col_max(val):
    return jnp.max(val, axis=0, keepdims=True)


def row_mean(val):
    return jnp.mean(val, axis=-1, keepdims=True)


def dot_t(lhs, rhs):
    return lax.dot_general(lhs, rhs, (((1,), (1,)), ((), ())), preferred_element_type=F32)


def block_kernel(
    n_dev, hd, kv_w, near, parts,
    x_hbm, dy_hbm, pos_hbm, gain_hbm, bias_hbm, wq_hbm, wk_hbm, wv_hbm, wo_hbm,
    out_hbm, gx_hbm, gw_hbm, gwo_hbm, gg_hbm,
    hb, dyb, wt, wi, woi, w_far, pos_all, trig,
    qt, kvt, kv, kvt_far, kv_far, bmat_far, stat_far, bmat, da_rv, sbuf, dpbuf, mbuf, adq, dkvt, kv_rv, kv_mine, kv_row,
    dwo, dwt, at_all, dq_all, at_rv, dt_rv, a_nat, d_nat, x_v, dy_own, gb_v, stat, out_v, gg_st, gg_mx, gg_my, gg_rv, gg_out,
    in_sem, far_sem, wo_sem, w_sem, out_sem, loc_sem,
    hzs, hzr, hds, hdr, yzs, yzr, yds, ydr,
    d_s, d_r, pos_s, pos_r, a_s, a_r, q_s, q_r, x_s, x_r, kv_s, kv_r, w_s, w_r, wk_s, wk_r, g_s, g_r,
):
    tok, width = x_v.shape
    n_chip = n_dev // 2
    pair = 2 * tok
    me = lax.axis_index('cp')
    chip = me // 2
    core = me % 2
    right = 2 * ((chip + 1) % n_chip) + core
    left = 2 * ((chip + n_chip - 1) % n_chip) + core
    mate = 2 * chip + 1 - core
    q_rows = wq_hbm.shape[0]
    n_rows = q_rows + 2 * kv_w
    hw = 2 * hd
    quarter = hd // 4
    tile = 256
    scale = hd ** -0.5
    cols_q = 2 * pair
    n_far = n_chip - 1 - 2 * near

    def remote(src, dst, send, recv, target):
        return pltpu.make_async_remote_copy(src_ref=src, dst_ref=dst, send_sem=send, recv_sem=recv, device_id={'cp': target}, device_id_type=MESH)

    def local(src, dst, sem):
        return pltpu.make_async_copy(src, dst, sem)

    def part_of(i, size):
        return pl.ds(pl.multiple_of(i * size, size), size)

    def once(cond):
        return pl.loop(0, jnp.where(cond, 1, 0))

    def ring_steps(k):
        step = (k + 1) // 2
        return step, k % 2

    def ring_origin(k):
        step, ahead = ring_steps(k)
        return jnp.where(ahead == 1, chip + n_chip - step, chip + step) % n_chip

    own = (chip, part_of(core, tok))
    first_loads = [
        local(x_hbm, x_v, in_sem.at[0]),
        local(gain_hbm, gb_v.at[0], in_sem.at[1]),
        local(bias_hbm, gb_v.at[1], in_sem.at[2]),
        local(pos_hbm, pos_all.at[me], in_sem.at[3]),
    ]
    for item in first_loads:
        item.start()
    barrier = pltpu.get_barrier_semaphore()
    for step in range(1, n_dev):
        pl.semaphore_signal(barrier, inc=1, device_id={'cp': (me + step) % n_dev}, device_id_type=MESH)
    own_rows = part_of(me, hw)
    kv_rows = part_of(chip, hd)
    loads = [
        local(wq_hbm.at[own_rows], wi.at[pl.ds(0, hw)], in_sem.at[4]),
        local(wk_hbm.at[kv_rows], wi.at[pl.ds(hw, hd)], in_sem.at[5]),
        local(wv_hbm.at[kv_rows], wi.at[pl.ds(hw + hd, hd)], in_sem.at[6]),
        local(wo_hbm.at[own_rows], woi, in_sem.at[7]),
        local(dy_hbm, dyb.at[own], in_sem.at[8]),
        local(dy_hbm, dy_own, in_sem.at[9]),
    ]
    far_loads = []
    for f in range(n_far):
        far_rows = part_of(ring_origin(2 * near + 1 + f), hd)
        loads.append(local(wk_hbm.at[far_rows], w_far.at[pl.ds(hw * f, hd)], far_sem.at[2 * f]))
        loads.append(local(wv_hbm.at[far_rows], w_far.at[pl.ds(hw * f + hd, hd)], far_sem.at[2 * f + 1]))
        far_wo = part_of(ring_origin(2 * near + 1 + f), 2 * hw)
        far_loads.append(local(wo_hbm.at[far_wo], wt.at[pl.ds(2 * hw * f, 2 * hw)], far_sem.at[2 * n_far + f]))
        far_loads.append(local(wq_hbm.at[far_wo], wt.at[pl.ds(2 * hw * (n_far + f), 2 * hw)], far_sem.at[3 * n_far + f]))
    for item in loads + far_loads:
        item.start()

    for item in first_loads:
        item.wait()
    gain_one = 1.0 + gb_v[0]
    block = 16

    @pl.loop(0, tok // block)
    def _(i):
        rows = part_of(i, block)
        x_f = x_v[rows, :].astype(F32)
        mean = row_mean(x_f)
        centered = x_f - mean
        inv_std = lax.rsqrt(row_mean(centered * centered) + EPS)
        hb[chip, part_of(core * (tok // block) + i, block), :] = (centered * inv_std * gain_one + gb_v[1]).astype(BF)
        stat[0, rows, :] = jnp.broadcast_to(mean, (block, 128))
        stat[1, rows, :] = jnp.broadcast_to(inv_std, (block, 128))

    pl.semaphore_wait(barrier, n_dev - 1)

    def chunk(buf, origin, parity, part):
        return buf.at[origin, part_of(parts * parity + part, tok // parts)]

    turns = 2 * parts

    def own_sends(buf, zs, zr, ds, dr):
        copies = []
        for part in range(parts):
            piece = chunk(buf, chip, core, part)
            copies.append(remote(piece, piece, zs.at[2 * part], zr.at[2 * part], right))
            copies.append(remote(piece, piece, zs.at[2 * part + 1], zr.at[2 * part + 1], left))
            copies.append(remote(piece, piece, ds.at[7 * parts + part], dr.at[7 * parts + part], mate))
        return copies

    def event_place(event):
        step = event // turns + 1
        turn = event % turns
        direction = turn % 2
        part = jnp.where(step < 4, turn // 2, turn // 2 + direction * (parts // 2))
        origin = jnp.where(direction == 0, chip + n_chip - step, chip + step) % n_chip
        return step, direction, part, origin

    def last_event(part, direction):
        return 6 * parts + 2 * (part - direction * (parts // 2)) + direction

    def ring_event(ring, event):
        buf, zs, zr, ds, dr = ring
        step, direction, part, origin = event_place(event)
        piece = chunk(buf, origin, core, part)
        remote(piece, piece, zs.at[0], zr.at[event], right).wait_recv()
        onward = jnp.where(step < 3, event + turns, last_event(part, direction))

        @pl.when((step < 3) | ((step == 3) & ((part >= parts // 2) == (direction == 1))))
        def _():
            remote(piece, piece, zs.at[event + turns], zr.at[onward], jnp.where(direction == 0, right, left)).start()

        remote(piece, piece, ds.at[event], dr.at[event], mate).start()

    def ring_service(ring, event):
        @pl.when(event < 7 * parts)
        def _():
            ring_event(ring, event)

    def ring_mate(ring, k, origin):
        buf, zs, zr, ds, dr = ring
        step, ahead = ring_steps(k)
        for part in range(parts):
            event = jnp.where(k == 0, 7 * parts + part, jnp.where(step < 4, turns * (step - 1) + 2 * part + 1 - ahead, last_event(part, part // (parts // 2))))
            piece = chunk(buf, origin, 1 - core, part)
            remote(piece, piece, ds.at[0], dr.at[event], mate).wait_recv()

    def finish_ring(ring):
        buf, zs, zr, ds, dr = ring
        for item in own_sends(*ring):
            item.wait_send()

        @pl.loop(0, 7 * parts)
        def _(event):
            step, direction, part, origin = event_place(event)
            piece = chunk(buf, origin, core, part)

            @pl.when((step < 3) | ((step == 3) & ((part >= parts // 2) == (direction == 1))))
            def _():
                remote(piece, piece, zs.at[event + turns], zr.at[event], right).wait_send()

            remote(piece, piece, ds.at[event], dr.at[event], mate).wait_send()

    h_ring = (hb, hzs, hzr, hds, hdr)
    y_ring = (dyb, yzs, yzr, yds, ydr)
    for item in own_sends(*h_ring):
        item.start()
    pos_sends = [remote(pos_all.at[me], pos_all.at[me], pos_s.at[step], pos_r.at[me], (me + step) % n_dev) for step in range(1, n_dev)]
    for item in pos_sends:
        item.start()
    weight_loads = [
        local(wq_hbm, wt.at[pl.ds(0, q_rows)], w_sem.at[0]),
        local(wk_hbm, wt.at[pl.ds(q_rows, kv_w)], w_sem.at[1]),
        local(wv_hbm, wt.at[pl.ds(q_rows + kv_w, kv_w)], w_sem.at[2]),
    ]
    dkvt[...] = jnp.zeros_like(dkvt)
    bmat[...] = jnp.zeros_like(bmat)
    bmat_far[...] = jnp.zeros_like(bmat_far)
    for f in range(n_far):
        stat_far[f, 0] = jnp.full((1, cols_q), -3e38, F32)
        stat_far[f, 1] = jnp.zeros((1, cols_q), F32)
        stat_far[f, 2] = jnp.zeros((1, cols_q), F32)

    freq = jnp.exp(lax.broadcasted_iota(jnp.int32, (quarter, tok), 0).astype(F32) * (-2.0 * math.log(ROPE_BASE) / (hd // 2)))

    def make_trig(b):
        for t in range(2):
            slot = 2 * b + t

            @pl.when(slot != me)
            def _():
                remote(pos_all.at[slot], pos_all.at[slot], pos_s.at[0], pos_r.at[slot], me).wait_recv()

            angle = pos_all[slot].astype(F32) * freq
            trig[b, 0:quarter, tok * t:tok * t + tok] = jnp.cos(angle)
            trig[b, quarter:2 * quarter, tok * t:tok * t + tok] = jnp.sin(angle)

    def turned(val, cos_t, sin_t):
        u = val[0:quarter]
        w = val[quarter:2 * quarter]
        return [u * cos_t - w * sin_t, w * cos_t + u * sin_t, val[2 * quarter:hd]]

    def eighth(val):
        return val.astype(BF) * jnp.asarray(scale, BF)

    def keys_values(val, cos_t, sin_t):
        return jnp.concatenate(turned(val[0:hd], cos_t, sin_t) + [val[hd:hw]], axis=0).astype(BF)

    lane = lax.broadcasted_iota(jnp.int32, (pair, cols_q), 1)
    row = lax.broadcasted_iota(jnp.int32, (pair, cols_q), 0)
    seen_far = row <= core * tok + lane % tok

    opposite = ring_origin(n_chip - 1)

    def opposite_send(head):
        block = bmat_far.at[n_far - 1, pl.ds(hd, hd), pl.ds(cols_q + tok * head, tok)]
        return remote(block, da_rv.at[2 * core + head % 2], d_s.at[head], d_r.at[2 * core + head % 2], 2 * opposite + head // 2)

    @pl.loop(0, n_chip)
    def _(k):
        for turn in range(2):
            ring_service(h_ring, parts * k + turn)

        @pl.when(k % 2 == 1)
        def _():
            ring_service(h_ring, parts * k + 2)


        @once(k == 0)
        def _(_):
            for item in loads:
                item.wait()

        b = ring_origin(k)
        ring_mate(h_ring, k, b)
        make_trig(b)

        @once(k == 0)
        def _(_):
            for item in far_loads:
                item.wait()
            cos_t = trig[chip, 0:quarter, part_of(core, tok)]
            sin_t = trig[chip, quarter:2 * quarter, part_of(core, tok)]

            @pl.loop(0, n_far)
            def _(f):
                da_t = dot_t(wt[part_of(f, 2 * hw), :], dy_own[...]).astype(BF)
                q_t = dot_t(wt[part_of(n_far + f, 2 * hw), :], hb[chip, part_of(core, tok), :])
                for head in range(4):
                    part = slice(hd * head, hd * head + hd)
                    at = tok * head
                    bmat_far[f, 0:hd, at:at + tok] = eighth(jnp.concatenate(turned(q_t[part], cos_t, sin_t), axis=0))
                    bmat_far[f, hd:hw, cols_q + at:cols_q + at + tok] = da_t[part]

            for item in weight_loads:
                item.start()

        @once(k == 1)
        def _(_):
            for head in range(4):
                opposite_send(head).start()

        place = part_of(b, pair)
        cos_t = trig[b, 0:quarter, :]
        sin_t = trig[b, quarter:2 * quarter, :]
        flat = dot_t(wi[...], hb[b])
        for head in range(2):
            q_rot = eighth(jnp.concatenate(turned(flat[hd * head:hd * head + hd], cos_t, sin_t), axis=0))
            for t in range(2):
                lane = pair * t + tok * head
                qt[b, :, lane:lane + tok] = q_rot[:, tok * t:tok * t + tok]
        kv_rot = keys_values(flat[hw:2 * hw], cos_t, sin_t)
        kvt[:, place] = kv_rot
        kv[place, :] = kv_rot.T

        @pl.when(k % 2 == 0)
        def _():
            ring_service(h_ring, parts * k + 2)

        ring_service(h_ring, parts * k + parts - 1)

        @once(k == 5)
        def _(_):
            for item in own_sends(*y_ring):
                item.start()

        @pl.when(b <= chip)
        def _():
            flat_far = dot_t(w_far[...], hb[b])
            for f in range(n_far):
                far_rot = keys_values(flat_far[hw * f:hw * f + hw], cos_t, sin_t)
                kvt_far[f, :, place] = far_rot
                kv_far[f, place, :] = far_rot.T

            @pl.loop(0, n_far)
            def _(f):
                both = dot(kv_far[f, place, :], bmat_far[f])
                s = jnp.where(seen_far | (k > 0), both[:, 0:cols_q], -1e30)
                old = stat_far[f, 0]
                new = jnp.maximum(old, col_max(s))
                p = jnp.exp(s - new)
                keep = jnp.exp(old - new)
                stat_far[f, 0] = new
                stat_far[f, 1] = stat_far[f, 1] * keep + col_sum(p)
                stat_far[f, 2] = stat_far[f, 2] * keep + col_sum(p * both[:, cols_q:2 * cols_q])

    groups = [slice(tile * g, tile * g + tile) for g in range(cols_q // tile)]

    def first_part(b, seen):
        def both_of(rows):
            both = dot(kv[rows, :], bmat[...])
            return both[:, 0:cols_q], both[:, cols_q:2 * cols_q]

        rows = part_of(b, pair)
        s, d_p = both_of(rows)
        s = jnp.where(seen, s, -1e30)
        top = col_max(s)
        p = jnp.exp(s - top)
        sbuf[rows, :] = p
        dpbuf[rows, :] = d_p
        mbuf[b] = top

        def step(c, state, chunks=1):
            old, total, weighted = state
            rows = part_of(c, chunks * pair)
            s, d_p = both_of(rows)
            new = jnp.maximum(old, col_max(s))
            p = jnp.exp(s - new)
            sbuf[rows, :] = p
            dpbuf[rows, :] = d_p
            for i in range(chunks):
                mbuf[chunks * c + i] = new
            keep = jnp.exp(old - new)
            return new, total * keep + col_sum(p), weighted * keep + col_sum(p * d_p)

        state = (top, col_sum(p), col_sum(p * d_p))
        state = lax.fori_loop(0, b // 2, functools.partial(step, chunks=2), state)
        top, total, weighted = lax.fori_loop(2 * (b // 2), b, step, state)
        inv = 1.0 / total
        return top, inv, weighted * inv

    def second_part(b, stats):
        top, inv, row_dot = stats
        adq[...] = jnp.zeros_like(adq)

        def step(c, carry):
            rows = part_of(c, pair)
            factor = jnp.exp(mbuf[c] - top) * inv
            d_k = d_v = None
            for at in groups:
                p = sbuf[rows, at] * factor[:, at]
                p_b = p.astype(BF)
                ds_b = (p * (dpbuf[rows, at] - row_dot[:, at])).astype(BF)
                adq[0:hd, at] += dot(kvt[0:hd, rows], ds_b)
                adq[hd:hw, at] += dot(kvt[hd:hw, rows], p_b)
                more_k = dot_t(bmat[0:hd, at], ds_b)
                more_v = dot_t(bmat[hd:hw, cols_q + at.start:cols_q + at.stop], p_b)
                d_k = more_k if d_k is None else d_k + more_k
                d_v = more_v if d_v is None else d_v + more_v
            dkvt[0:hd, rows] += d_k
            dkvt[hd:hw, rows] += d_v
            return carry

        lax.fori_loop(0, b + 1, step, 0)


    def send_rows(slot):
        cols = part_of(slot, tok)
        return [
            remote(dq_all.at[:, cols], dt_rv.at[own_rows], q_s.at[slot], q_r.at[me], slot),
            remote(at_all.at[:, cols], at_rv.at[own_rows], a_s.at[slot], a_r.at[me], slot),
        ]

    last = 6 * parts

    def serve(event):
        @pl.when(event < last)
        def _():
            ring_event(y_ring, event)

    @pl.loop(0, n_chip)
    def _(j):
        k = j - 1

        @pl.when(k == 0)
        def _():
            for turn in range(2):
                ring_event(y_ring, k + turn)

        @pl.when((k % 2 == 1) & (k > 0))
        def _():
            for turn in range(2, parts):
                serve(parts * k + turn)

        b = jnp.where(j == 0, opposite, ring_origin(jnp.maximum(k, 0)))

        @once(k == 1)
        def _(_):
            for item in weight_loads:
                item.wait()

        @pl.loop(0, jnp.where(j == n_chip - 1, 2 + 4 * near, 0))
        def _(early):
            slot = 2 * ring_origin(early // 2) + early % 2

            @pl.when(slot != me)
            def _():
                for item in send_rows(slot):
                    item.start()

        bmat[0:hd, 0:cols_q] = qt[b]

        @once(j == 0)
        def _(_):
            for i in range(4):
                remote(da_rv.at[i], da_rv.at[i], d_s.at[0], d_r.at[i], mate).wait_recv()
                bmat[hd:hw, cols_q + tok * i:cols_q + tok * i + tok] = da_rv[i]

        @once(j > 0)
        def _(_):
            ring_mate(y_ring, k, b)
            da_t = dot_t(woi[...], dyb[b]).astype(BF)
            for t in range(2):
                for head in range(2):
                    at = cols_q + pair * t + tok * head
                    bmat[hd:hw, at:at + tok] = da_t[hd * head:hd * head + hd, tok * t:tok * t + tok]

        stats = first_part(b, row <= (lane // pair) * tok + lane % tok)
        for turn in range(2):
            serve(jnp.where(k < 0, last, parts * k + 2 + 2 * (k % 2)) + turn)
        second_part(b, stats)
        for t in range(2):
            slot = 2 * b + t
            lanes = [slice(pair * t + tok * head, pair * t + tok * head + tok) for head in range(2)]
            a_t = jnp.concatenate([adq[hd:hw, at] for at in lanes], axis=0).astype(BF)
            cos_t = trig[b, 0:quarter, tok * t:tok * t + tok]
            sin_t = trig[b, quarter:2 * quarter, tok * t:tok * t + tok]
            dq_t = jnp.concatenate([piece for at in lanes for piece in turned(adq[0:hd, at] * scale, cos_t, -sin_t)], axis=0).astype(BF)
            at_all[:, part_of(slot, tok)] = a_t
            dq_all[:, part_of(slot, tok)] = dq_t

            @pl.when(slot == me)
            def _():
                at_rv[own_rows, :] = a_t
                dt_rv[own_rows, :] = dq_t

        @pl.when((k % 2 == 0) & (k >= 0))
        def _():
            for turn in range(2):
                serve(parts * j + turn)

    far = [ring_origin(k) for k in range(n_chip - 1, 0, -1)]
    targets = [2 * c + p for c in far for p in range(2)] + [mate]
    near_targets = targets[-1 - 4 * near:]
    swap = remote(dkvt.at[part_of(1 - core, hd)], kv_rv, x_s, x_r, mate)
    swap.start()
    w_sends = [remote(dwt.at[pl.ds(0, hw), part_of(t, tok)], gw_hbm.at[own_rows], w_s.at[t], w_r.at[me], t) for t in targets]

    def columns(rows_all, buf, cols):
        acc = jnp.zeros((rows_all.shape[0], tile), F32)
        for s in range(n_chip):
            acc += dot(rows_all[:, pair * s:pair * s + pair], buf[s, :, cols])
        return acc

    def q_columns(i):
        cols = part_of(far[i] if i < n_chip - 1 else chip, pair)
        dwt[0:hw, cols] = columns(dq_all, hb, cols)
        for item in w_sends[max(2 * i - 2, 0):2 * i]:
            item.start()

    for i in range(FIRST + 1):
        q_columns(i)

    swap.wait_recv()
    mine = part_of(core, hd)
    g_rows = pl.ds(pl.multiple_of(q_rows + core * kv_w + chip * hd, hd), hd)
    for t in range(n_chip):
        cols = slice(pair * t, pair * t + pair)
        g = dkvt[mine, cols] + kv_rv[:, cols]
        cos_t = jnp.where(core == 0, trig[t, 0:quarter, :], 1.0)
        sin_t = jnp.where(core == 0, trig[t, quarter:2 * quarter, :], 0.0)
        g_b = jnp.concatenate(turned(g, cos_t, -sin_t), axis=0).astype(BF)
        kv_mine[2 * t] = g_b[:, 0:tok]
        kv_mine[2 * t + 1] = g_b[:, tok:pair]
        kv_row[:, cols] = g_b
    dt_rv[g_rows, :] = kv_mine[me]
    kv_sends = [remote(kv_mine.at[t], dt_rv.at[g_rows], kv_s.at[t], kv_r.at[me], t) for t in targets]
    for item in kv_sends:
        item.start()
    for i in range(FIRST + 1, n_chip):
        q_columns(i)
    w_sends[-1].start()
    w_own = local(dwt.at[pl.ds(0, hw), part_of(me, tok)], gw_hbm.at[own_rows], loc_sem.at[0])
    w_own.start()
    for t in range(width // tile):
        cols = slice(tile * t, tile * t + tile)
        dwt[hw:hw + hd, cols] = columns(kv_row, hb, cols)
    wk_own = local(dwt.at[pl.ds(hw, hd), part_of(me, tok)], gw_hbm.at[g_rows], loc_sem.at[1])
    wk_own.start()
    wk_sends = [remote(dwt.at[pl.ds(hw, hd), part_of(t, tok)], gw_hbm.at[g_rows], wk_s.at[t], wk_r.at[me], t) for t in targets]
    for item in wk_sends[0:HELD]:
        item.start()

    @pl.loop(last, 7 * parts)
    def _(event):
        ring_event(y_ring, event)

    ring_mate(y_ring, n_chip - 1, opposite)
    for t in range(width // tile):
        cols = slice(tile * t, tile * t + tile)
        dwo[:, cols] = columns(at_all, dyb, cols)
    store_wo = local(dwo, gwo_hbm, out_sem.at[0])
    store_wo.start()
    finish_ring(y_ring)
    wo_loads = [local(wo_hbm.at[pl.ds(pair * t, pair)], dyb.at[t], wo_sem.at[t]) for t in range(n_chip)]
    for item in wo_loads:
        item.start()

    @pl.loop(0, n_far)
    def _(f):
        c_far = ring_origin(2 * near + 1 + f)
        cos_t = trig[chip, 0:quarter, part_of(core, tok)]
        sin_t = trig[chip, quarter:2 * quarter, part_of(core, tok)]
        top = stat_far[f, 0]
        inv = 1.0 / stat_far[f, 1]
        row_dot = stat_far[f, 2] * inv

        def add_chunk(c, diagonal, chunks=1):
            rows = part_of(c, chunks * pair)
            for at in groups:
                keys = kv_far[f, rows, :]
                s = dot(keys, bmat_far[f, :, at])
                d_p = dot(keys, bmat_far[f, :, cols_q + at.start:cols_q + at.stop])
                if diagonal:
                    s = jnp.where(seen_far[:, at], s, -1e30)
                p = jnp.exp(s - top[:, at]) * inv[:, at]
                p_b = p.astype(BF)
                ds_b = (p * (d_p - row_dot[:, at])).astype(BF)
                d_q = dot(kvt_far[f, 0:hd, rows], ds_b)
                d_a = dot(kvt_far[f, hd:hw, rows], p_b)
                adq[0:hd, at] = d_q if diagonal else adq[0:hd, at] + d_q
                adq[hd:hw, at] = d_a if diagonal else adq[hd:hw, at] + d_a

        add_chunk(chip, True)

        @pl.loop(0, chip // 2)
        def _(c):
            add_chunk(c, False, 2)

        @pl.when(chip % 2 == 1)
        def _():
            add_chunk(chip - 1, False)

        for head in range(4):
            at = slice(tok * head, tok * head + tok)
            place = pl.ds(pl.multiple_of(c_far * 2 * hw + hd * head, hd), hd)
            at_rv[place, :] = adq[hd:hw, at].astype(BF)
            dt_rv[place, :] = jnp.concatenate(turned(adq[0:hd, at] * scale, cos_t, -sin_t), axis=0).astype(BF)

    for t in near_targets:
        remote(at_all.at[:, pl.ds(0, tok)], at_rv.at[part_of(t, hw)], a_s.at[t], a_r.at[t], t).wait_recv()
    for item in wo_loads:
        item.wait()
    for t in range(q_rows // tok):
        a_nat[:, tok * t:tok * t + tok] = at_rv[tok * t:tok * t + tok, :].T
    for t in range(width // tile):
        cols = slice(tile * t, tile * t + tile)
        prod = jnp.zeros((tok, tile), F32)
        for s in range(n_chip):
            prod += dot(a_nat[:, pair * s:pair * s + pair], dyb[s, :, cols])
        out_v[:, cols] = (x_v[:, cols].astype(F32) + prod).astype(BF)
    store_out = local(out_v, out_hbm, out_sem.at[1])
    store_out.start()

    def kv_place(t):
        return pl.ds(pl.multiple_of(q_rows + (t % 2) * kv_w + (t // 2) * hd, hd), hd)

    for t in near_targets:
        remote(dq_all.at[:, pl.ds(0, tok)], dt_rv.at[part_of(t, hw)], q_s.at[t], q_r.at[t], t).wait_recv()
    for t in targets:
        remote(kv_mine.at[0], dt_rv.at[kv_place(t)], kv_s.at[t], kv_r.at[t], t).wait_recv()
    swap.wait_send()
    for t in range(n_rows // tok):
        d_nat[:, tok * t:tok * t + tok] = dt_rv[tok * t:tok * t + tok, :].T

    mean = stat[0, :, 0:1]
    inv_std = stat[1, :, 0:1]
    dh = dkvt
    for t in range(width // tile):
        cols = slice(tile * t, tile * t + tile)
        acc = jnp.zeros((tok, tile), F32)
        for s in range(n_rows // tile):
            acc += dot(d_nat[:, tile * s:tile * s + tile], wt[tile * s:tile * s + tile, cols])
        dh[:, cols] = acc
        gg_st[0, :, cols] = col_sum(acc * ((x_v[:, cols].astype(F32) - mean) * inv_std))
        gg_st[1, :, cols] = col_sum(acc)
    g_swap = remote(gg_st.at[1 - core], gg_mx, g_s.at[n_chip], g_r.at[n_chip], mate)
    g_swap.start()
    g_swap.wait_recv()
    gg_my[...] = jnp.where(core == 0, gg_st[0], gg_st[1]) + gg_mx[...]
    gg_rv[chip] = gg_my[...]
    g_sends = [remote(gg_my, gg_rv.at[chip], g_s.at[c], g_r.at[chip], 2 * c + core) for c in far]
    for item in g_sends + wk_sends[HELD:]:
        item.start()

    grad_hat = dh[...] * gain_one
    x_hat = (x_v[...].astype(F32) - mean) * inv_std
    mean_one = row_mean(grad_hat)
    mean_two = row_mean(grad_hat * x_hat)
    store_out.wait()
    out_v[...] = (dy_own[...].astype(F32) + inv_std * (grad_hat - mean_one - x_hat * mean_two)).astype(BF)
    store_gx = local(out_v, gx_hbm, out_sem.at[2])
    store_gx.start()

    for c in far:
        remote(gg_my, gg_rv.at[c], g_s.at[c], g_r.at[c], 2 * c + core).wait_recv()
    sums = gg_rv[0]
    for c in range(1, n_chip):
        sums = sums + gg_rv[c]
    gg_out[core] = sums
    g_swap_out = remote(gg_out.at[core], gg_out.at[core], g_s.at[n_chip + 1], g_r.at[n_chip + 1], mate)
    g_swap_out.start()
    remote(gg_out.at[core], gg_out.at[1 - core], g_s.at[n_chip + 1], g_r.at[n_chip + 1], mate).wait_recv()
    store_gg = local(gg_out, gg_hbm, out_sem.at[3])
    store_gg.start()

    finish_ring(h_ring)
    for item in pos_sends + [g_swap, g_swap_out] + [opposite_send(head) for head in range(4)]:
        item.wait_send()
    for t in near_targets:
        remote(at_all.at[:, pl.ds(0, tok)], at_rv.at[pl.ds(0, hw)], a_s.at[t], a_r.at[t], t).wait_send()
        remote(dq_all.at[:, pl.ds(0, tok)], dt_rv.at[pl.ds(0, hw)], q_s.at[t], q_r.at[t], t).wait_send()
    for item in kv_sends + w_sends + g_sends + wk_sends:
        item.wait_send()
    for t in targets:
        remote(dwt.at[pl.ds(0, hw), part_of(t, tok)], gw_hbm.at[part_of(t, hw)], w_s.at[t], w_r.at[t], t).wait_recv()
        remote(dwt.at[pl.ds(hw, hd), part_of(t, tok)], gw_hbm.at[kv_place(t)], wk_s.at[t], wk_r.at[t], t).wait_recv()
    for item in (w_own, wk_own, store_wo, store_gx, store_gg):
        item.wait()


def settle_kernel(q_rows, kv_w, out_i, gx_i, gw_i, gwo_i, gg_i, out_o, gx_o, gq_o, gk_o, gv_o, gwo_o, gain_o, bias_o, b_act, b_q, b_kv, b_o, b_gg, sem_in, sem_out, sem_gg):
    half_q = q_rows // 2
    half_o = gwo_i.shape[0] // 2
    moves = [(out_i, b_act.at[0], out_o), (gx_i, b_act.at[1], gx_o)]
    for t in range(2):
        moves.append((gw_i.at[pl.ds(half_q * t, half_q)], b_q.at[t], gq_o.at[pl.ds(half_q * t, half_q)]))
        moves.append((gwo_i.at[pl.ds(half_o * t, half_o)], b_o.at[t], gwo_o.at[pl.ds(half_o * t, half_o)]))
    moves.append((gw_i.at[pl.ds(q_rows, kv_w)], b_kv.at[0], gk_o))
    moves.append((gw_i.at[pl.ds(q_rows + kv_w, kv_w)], b_kv.at[1], gv_o))
    loads = [pltpu.make_async_copy(src, mid, sem_in.at[i]) for i, (src, mid, _) in enumerate(moves)]
    stores = [pltpu.make_async_copy(mid, dst, sem_out.at[i]) for i, (_, mid, dst) in enumerate(moves)]
    load_gg = pltpu.make_async_copy(gg_i, b_gg, sem_gg)
    load_gg.start()
    for item in loads:
        item.start()
    for load, store in zip(loads, stores):
        load.wait()
        store.start()
    load_gg.wait()
    gain_o[...] = b_gg[0, 0]
    bias_o[...] = b_gg[1, 0]
    for item in stores:
        item.wait()


def solution(mesh):
    n_dev = mesh.shape['cp']

    def device_step(x_act, d_out, positions, ln_gain, ln_bias, w_query, w_key, w_value, w_out):
        tok, width = x_act.shape[1], x_act.shape[2]
        q_heads, hd = w_query.shape[1], w_query.shape[2]
        kv_heads = w_key.shape[1]
        q_w, kv_w = q_heads * hd, kv_heads * hd
        n_rows = q_w + 2 * kv_w
        seq = n_dev * tok
        hw = 2 * hd

        def flat_weight(w):
            return jnp.transpose(w, (1, 2, 0)).reshape(-1, width)

        hbm = pl.BlockSpec(memory_space=pltpu.HBM)
        vmem = pl.BlockSpec(memory_space=pltpu.VMEM)
        dma = pltpu.SemaphoreType.DMA
        n_chip = n_dev // 2
        n_far = n_chip - 1 - 2 * NEAR
        pair = 2 * tok
        scratch = [
            pltpu.VMEM((n_chip, pair, width), BF),
            pltpu.VMEM((n_chip, pair, width), BF),
            pltpu.VMEM((n_rows, width), BF),
            pltpu.VMEM((2 * hw, width), BF),
            pltpu.VMEM((hw, width), BF),
            pltpu.VMEM((n_far * hw, width), BF),
            pltpu.VMEM((n_dev, 1, tok), jnp.int32),
            pltpu.VMEM((n_chip, hd // 2, pair), F32),
            pltpu.VMEM((n_chip, hd, 2 * pair), BF),
            pltpu.VMEM((hw, seq), BF),
            pltpu.VMEM((seq, hw), BF),
            pltpu.VMEM((n_far, hw, seq), BF),
            pltpu.VMEM((n_far, seq, hw), BF),
            pltpu.VMEM((n_far, hw, 4 * pair), BF),
            pltpu.VMEM((n_far, 3, 1, 2 * pair), F32),
            pltpu.VMEM((hw, 4 * pair), BF),
            pltpu.VMEM((4, hd, tok), BF),
            pltpu.VMEM((seq, 2 * pair), F32),
            pltpu.VMEM((seq, 2 * pair), F32),
            pltpu.VMEM((n_chip, 1, 2 * pair), F32),
            pltpu.VMEM((hw, 2 * pair), F32),
            pltpu.VMEM((hw, seq), F32),
            pltpu.VMEM((hd, seq), F32),
            pltpu.VMEM((n_dev, hd, tok), BF),
            pltpu.VMEM((hd, seq), BF),
            pltpu.VMEM((hw, width), F32),
            pltpu.VMEM((hw + hd, width), F32),
            pltpu.VMEM((hw, seq), BF),
            pltpu.VMEM((hw, seq), BF),
            pltpu.VMEM((q_w, tok), BF),
            pltpu.VMEM((n_rows, tok), BF),
            pltpu.VMEM((tok, q_w), BF),
            pltpu.VMEM((tok, n_rows), BF),
            pltpu.VMEM((tok, width), BF),
            pltpu.VMEM((tok, width), BF),
            pltpu.VMEM((2, 1, width), F32),
            pltpu.VMEM((2, tok, 128), F32),
            pltpu.VMEM((tok, width), BF),
            pltpu.VMEM((2, 1, width), F32),
            pltpu.VMEM((1, width), F32),
            pltpu.VMEM((1, width), F32),
            pltpu.VMEM((n_chip, 1, width), F32),
            pltpu.VMEM((2, 1, width), F32),
            dma((10,)), dma((4 * n_far,)), dma((n_chip,)), dma((3,)), dma((4,)), dma((2,)),
        ] + [dma((9 * PARTS,)), dma((7 * PARTS,)), dma((8 * PARTS,)), dma((8 * PARTS,))] * 2 + [dma((4,))] * 2 + [dma((n_dev,))] * 6 + [dma] * 2 + [dma((n_dev,))] * 8
        out, gx, gw, gwo, gg = pl.pallas_call(
            functools.partial(block_kernel, n_dev, hd, kv_w, NEAR, PARTS),
            out_shape=(
                jax.ShapeDtypeStruct((tok, width), BF),
                jax.ShapeDtypeStruct((tok, width), BF),
                jax.ShapeDtypeStruct((n_rows, tok), F32),
                jax.ShapeDtypeStruct((hw, width), F32),
                jax.ShapeDtypeStruct((2, 1, width), F32),
            ),
            in_specs=[hbm] * 9,
            out_specs=(hbm,) * 5,
            scratch_shapes=scratch,
            compiler_params=pltpu.CompilerParams(collective_id=0, has_side_effects=True, vmem_limit_bytes=67043328),
            name='attn_block',
        )(
            x_act.reshape(tok, width), d_out.reshape(tok, width), positions.reshape(1, tok),
            ln_gain.reshape(1, width), ln_bias.reshape(1, width),
            flat_weight(w_query), flat_weight(w_key), flat_weight(w_value), w_out,
        )

        out, gx, gq, gk, gv, gwo, gain, bias = pl.pallas_call(
            functools.partial(settle_kernel, q_w, kv_w),
            out_shape=(
                jax.ShapeDtypeStruct((tok, width), BF),
                jax.ShapeDtypeStruct((tok, width), BF),
                jax.ShapeDtypeStruct((q_w, tok), F32),
                jax.ShapeDtypeStruct((kv_w, tok), F32),
                jax.ShapeDtypeStruct((kv_w, tok), F32),
                jax.ShapeDtypeStruct((hw, width), F32),
                jax.ShapeDtypeStruct((width,), F32),
                jax.ShapeDtypeStruct((width,), F32),
            ),
            in_specs=[hbm] * 5,
            out_specs=(hbm,) * 6 + (vmem,) * 2,
            scratch_shapes=[
                pltpu.VMEM((2, tok, width), BF),
                pltpu.VMEM((2, q_w // 2, tok), F32),
                pltpu.VMEM((2, kv_w, tok), F32),
                pltpu.VMEM((2, hw // 2, width), F32),
                pltpu.VMEM((2, 1, width), F32),
                dma((8,)), dma((8,)), dma,
            ],
            name='settle',
        )(out, gx, gw, gwo, gg)

        def rows_out(block, heads):
            return jnp.transpose(block.reshape(heads, hd, tok), (2, 0, 1))

        return (
            out.reshape(1, tok, width), gx.reshape(1, tok, width),
            rows_out(gq, q_heads), rows_out(gk, kv_heads), rows_out(gv, kv_heads),
            gwo, gain, bias,
        )

    return jax.shard_map(device_step, mesh=mesh, in_specs=(P('dp', 'cp', None), P('dp', 'cp', None), P('dp', 'cp'), P(None), P(None), P(None, None, None), P(None, None, None), P(None, None, None), P(None, None)), out_specs=(P('dp', 'cp', None), P('dp', 'cp', None), P(('dp', 'cp'), None, None), P(('dp', 'cp'), None, None), P(('dp', 'cp'), None, None), P(('dp', 'cp'), None), P('dp'), P('dp')), check_vma=False)
```

```python
import functools
import math

import jax
import jax.numpy as jnp
from jax import lax
from jax.experimental import pallas as pl
from jax.experimental.pallas import tpu as pltpu
from jax.sharding import PartitionSpec as P

EPS = 1e-5
ROPE_BASE = 10000.0
MESH = pl.DeviceIdType.MESH
BF = jnp.bfloat16
F32 = jnp.float32
NEAR = 1
PARTS = 4
FIRST = 1
HELD = 4


def dot(lhs, rhs):
    return jnp.dot(lhs, rhs, preferred_element_type=F32)


def col_sum(val):
    return jnp.sum(val, axis=0, keepdims=True)


def col_max(val):
    return jnp.max(val, axis=0, keepdims=True)


def row_mean(val):
    return jnp.mean(val, axis=-1, keepdims=True)


def dot_t(lhs, rhs):
    return lax.dot_general(lhs, rhs, (((1,), (1,)), ((), ())), preferred_element_type=F32)


def block_kernel(
    n_dev, hd, kv_w, near, parts,
    x_hbm, dy_hbm, pos_hbm, gain_hbm, bias_hbm, wq_hbm, wk_hbm, wv_hbm, wo_hbm,
    out_hbm, gx_hbm, gw_hbm, gwo_hbm, gg_hbm,
    hb, dyb, wt, wi, woi, w_far, pos_all, trig,
    qt, kvt, kv, kvt_far, kv_far, bmat_far, stat_far, bmat, da_rv, sbuf, dpbuf, mbuf, adq, dkvt, kv_rv, kv_mine, kv_row,
    dwo, dwt, at_all, dq_all, at_rv, dt_rv, a_nat, d_nat, x_v, dy_own, gb_v, stat, out_v, gg_st, gg_mx, gg_my, gg_rv, gg_out,
    in_sem, far_sem, wo_sem, w_sem, out_sem, loc_sem,
    hzs, hzr, hds, hdr, yzs, yzr, yds, ydr,
    d_s, d_r, pos_s, pos_r, a_s, a_r, q_s, q_r, x_s, x_r, kv_s, kv_r, w_s, w_r, wk_s, wk_r, g_s, g_r,
):
    tok, width = x_v.shape
    n_chip = n_dev // 2
    pair = 2 * tok
    me = lax.axis_index('cp')
    chip = me // 2
    core = me % 2
    right = 2 * ((chip + 1) % n_chip) + core
    left = 2 * ((chip + n_chip - 1) % n_chip) + core
    mate = 2 * chip + 1 - core
    q_rows = wq_hbm.shape[0]
    n_rows = q_rows + 2 * kv_w
    hw = 2 * hd
    quarter = hd // 4
    tile = 256
    scale = hd ** -0.5
    cols_q = 2 * pair
    n_far = n_chip - 1 - 2 * near

    def remote(src, dst, send, recv, target):
        return pltpu.make_async_remote_copy(src_ref=src, dst_ref=dst, send_sem=send, recv_sem=recv, device_id={'cp': target}, device_id_type=MESH)

    def local(src, dst, sem):
        return pltpu.make_async_copy(src, dst, sem)

    def part_of(i, size):
        return pl.ds(pl.multiple_of(i * size, size), size)

    def once(cond):
        return pl.loop(0, jnp.where(cond, 1, 0))

    def ring_steps(k):
        step = (k + 1) // 2
        return step, k % 2

    def ring_origin(k):
        step, ahead = ring_steps(k)
        return jnp.where(ahead == 1, chip + n_chip - step, chip + step) % n_chip

    own = (chip, part_of(core, tok))
    first_loads = [
        local(x_hbm, x_v, in_sem.at[0]),
        local(gain_hbm, gb_v.at[0], in_sem.at[1]),
        local(bias_hbm, gb_v.at[1], in_sem.at[2]),
        local(pos_hbm, pos_all.at[me], in_sem.at[3]),
    ]
    for item in first_loads:
        item.start()
    barrier = pltpu.get_barrier_semaphore()
    for step in range(1, n_dev):
        pl.semaphore_signal(barrier, inc=1, device_id={'cp': (me + step) % n_dev}, device_id_type=MESH)
    own_rows = part_of(me, hw)
    kv_rows = part_of(chip, hd)
    loads = [
        local(wq_hbm.at[own_rows], wi.at[pl.ds(0, hw)], in_sem.at[4]),
        local(wk_hbm.at[kv_rows], wi.at[pl.ds(hw, hd)], in_sem.at[5]),
        local(wv_hbm.at[kv_rows], wi.at[pl.ds(hw + hd, hd)], in_sem.at[6]),
        local(wo_hbm.at[own_rows], woi, in_sem.at[7]),
        local(dy_hbm, dyb.at[own], in_sem.at[8]),
        local(dy_hbm, dy_own, in_sem.at[9]),
    ]
    far_loads = []
    for f in range(n_far):
        far_rows = part_of(ring_origin(2 * near + 1 + f), hd)
        loads.append(local(wk_hbm.at[far_rows], w_far.at[pl.ds(hw * f, hd)], far_sem.at[2 * f]))
        loads.append(local(wv_hbm.at[far_rows], w_far.at[pl.ds(hw * f + hd, hd)], far_sem.at[2 * f + 1]))
        far_wo = part_of(ring_origin(2 * near + 1 + f), 2 * hw)
        far_loads.append(local(wo_hbm.at[far_wo], wt.at[pl.ds(2 * hw * f, 2 * hw)], far_sem.at[2 * n_far + f]))
        far_loads.append(local(wq_hbm.at[far_wo], wt.at[pl.ds(2 * hw * (n_far + f), 2 * hw)], far_sem.at[3 * n_far + f]))
    for item in loads + far_loads:
        item.start()

    for item in first_loads:
        item.wait()
    gain_one = 1.0 + gb_v[0]
    block = 16

    @pl.loop(0, tok // block)
    def _(i):
        rows = part_of(i, block)
        x_f = x_v[rows, :].astype(F32)
        mean = row_mean(x_f)
        centered = x_f - mean
        inv_std = lax.rsqrt(row_mean(centered * centered) + EPS)
        hb[chip, part_of(core * (tok // block) + i, block), :] = (centered * inv_std * gain_one + gb_v[1]).astype(BF)
        stat[0, rows, :] = jnp.broadcast_to(mean, (block, 128))
        stat[1, rows, :] = jnp.broadcast_to(inv_std, (block, 128))

    pl.semaphore_wait(barrier, n_dev - 1)

    def chunk(buf, origin, parity, part):
        return buf.at[origin, part_of(parts * parity + part, tok // parts)]

    turns = 2 * parts

    def own_sends(buf, zs, zr, ds, dr):
        copies = []
        for part in range(parts):
            piece = chunk(buf, chip, core, part)
            copies.append(remote(piece, piece, zs.at[2 * part], zr.at[2 * part], right))
            copies.append(remote(piece, piece, zs.at[2 * part + 1], zr.at[2 * part + 1], left))
            copies.append(remote(piece, piece, ds.at[7 * parts + part], dr.at[7 * parts + part], mate))
        return copies

    def event_place(event):
        step = event // turns + 1
        turn = event % turns
        direction = turn % 2
        part = jnp.where(step < 4, turn // 2, turn // 2 + direction * (parts // 2))
        origin = jnp.where(direction == 0, chip + n_chip - step, chip + step) % n_chip
        return step, direction, part, origin

    def last_event(part, direction):
        return 6 * parts + 2 * (part - direction * (parts // 2)) + direction

    def ring_event(ring, event):
        buf, zs, zr, ds, dr = ring
        step, direction, part, origin = event_place(event)
        piece = chunk(buf, origin, core, part)
        remote(piece, piece, zs.at[0], zr.at[event], right).wait_recv()
        onward = jnp.where(step < 3, event + turns, last_event(part, direction))

        @pl.when((step < 3) | ((step == 3) & ((part >= parts // 2) == (direction == 1))))
        def _():
            remote(piece, piece, zs.at[event + turns], zr.at[onward], jnp.where(direction == 0, right, left)).start()

        remote(piece, piece, ds.at[event], dr.at[event], mate).start()

    def ring_service(ring, event):
        @pl.when(event < 7 * parts)
        def _():
            ring_event(ring, event)

    def ring_mate(ring, k, origin):
        buf, zs, zr, ds, dr = ring
        step, ahead = ring_steps(k)
        for part in range(parts):
            event = jnp.where(k == 0, 7 * parts + part, jnp.where(step < 4, turns * (step - 1) + 2 * part + 1 - ahead, last_event(part, part // (parts // 2))))
            piece = chunk(buf, origin, 1 - core, part)
            remote(piece, piece, ds.at[0], dr.at[event], mate).wait_recv()

    def finish_ring(ring):
        buf, zs, zr, ds, dr = ring
        for item in own_sends(*ring):
            item.wait_send()

        @pl.loop(0, 7 * parts)
        def _(event):
            step, direction, part, origin = event_place(event)
            piece = chunk(buf, origin, core, part)

            @pl.when((step < 3) | ((step == 3) & ((part >= parts // 2) == (direction == 1))))
            def _():
                remote(piece, piece, zs.at[event + turns], zr.at[event], right).wait_send()

            remote(piece, piece, ds.at[event], dr.at[event], mate).wait_send()

    h_ring = (hb, hzs, hzr, hds, hdr)
    y_ring = (dyb, yzs, yzr, yds, ydr)
    for item in own_sends(*h_ring):
        item.start()
    pos_sends = [remote(pos_all.at[me], pos_all.at[me], pos_s.at[step], pos_r.at[me], (me + step) % n_dev) for step in range(1, n_dev)]
    for item in pos_sends:
        item.start()
    weight_loads = [
        local(wq_hbm, wt.at[pl.ds(0, q_rows)], w_sem.at[0]),
        local(wk_hbm, wt.at[pl.ds(q_rows, kv_w)], w_sem.at[1]),
        local(wv_hbm, wt.at[pl.ds(q_rows + kv_w, kv_w)], w_sem.at[2]),
    ]
    dkvt[...] = jnp.zeros_like(dkvt)
    bmat[...] = jnp.zeros_like(bmat)
    bmat_far[...] = jnp.zeros_like(bmat_far)
    for f in range(n_far):
        stat_far[f, 0] = jnp.full((1, cols_q), -3e38, F32)
        stat_far[f, 1] = jnp.zeros((1, cols_q), F32)
        stat_far[f, 2] = jnp.zeros((1, cols_q), F32)

    freq = jnp.exp(lax.broadcasted_iota(jnp.int32, (quarter, tok), 0).astype(F32) * (-2.0 * math.log(ROPE_BASE) / (hd // 2)))

    def make_trig(b):
        for t in range(2):
            slot = 2 * b + t

            @pl.when(slot != me)
            def _():
                remote(pos_all.at[slot], pos_all.at[slot], pos_s.at[0], pos_r.at[slot], me).wait_recv()

            angle = pos_all[slot].astype(F32) * freq
            trig[b, 0:quarter, tok * t:tok * t + tok] = jnp.cos(angle)
            trig[b, quarter:2 * quarter, tok * t:tok * t + tok] = jnp.sin(angle)

    def turned(val, cos_t, sin_t):
        u = val[0:quarter]
        w = val[quarter:2 * quarter]
        return [u * cos_t - w * sin_t, w * cos_t + u * sin_t, val[2 * quarter:hd]]

    def eighth(val):
        return val.astype(BF) * jnp.asarray(scale, BF)

    def keys_values(val, cos_t, sin_t):
        return jnp.concatenate(turned(val[0:hd], cos_t, sin_t) + [val[hd:hw]], axis=0).astype(BF)

    lane = lax.broadcasted_iota(jnp.int32, (pair, cols_q), 1)
    row = lax.broadcasted_iota(jnp.int32, (pair, cols_q), 0)
    seen_far = row <= core * tok + lane % tok

    opposite = ring_origin(n_chip - 1)

    def opposite_send(head):
        block = bmat_far.at[n_far - 1, pl.ds(hd, hd), pl.ds(cols_q + tok * head, tok)]
        return remote(block, da_rv.at[2 * core + head % 2], d_s.at[head], d_r.at[2 * core + head % 2], 2 * opposite + head // 2)

    @pl.loop(0, n_chip)
    def _(k):
        for turn in range(parts):
            ring_service(h_ring, parts * k + turn)

        @once(k == 5)
        def _(_):
            for item in [opposite_send(head) for head in range(4)] + own_sends(*y_ring):
                item.start()

        @once(k == 0)
        def _(_):
            for item in loads:
                item.wait()

        b = ring_origin(k)
        ring_mate(h_ring, k, b)
        make_trig(b)

        @once(k == 0)
        def _(_):
            for item in far_loads:
                item.wait()
            cos_t = trig[chip, 0:quarter, part_of(core, tok)]
            sin_t = trig[chip, quarter:2 * quarter, part_of(core, tok)]

            @pl.loop(0, n_far)
            def _(f):
                da_t = dot_t(wt[part_of(f, 2 * hw), :], dy_own[...]).astype(BF)
                q_t = dot_t(wt[part_of(n_far + f, 2 * hw), :], hb[chip, part_of(core, tok), :])
                for head in range(4):
                    part = slice(hd * head, hd * head + hd)
                    at = tok * head
                    bmat_far[f, 0:hd, at:at + tok] = eighth(jnp.concatenate(turned(q_t[part], cos_t, sin_t), axis=0))
                    bmat_far[f, hd:hw, cols_q + at:cols_q + at + tok] = da_t[part]

            for item in weight_loads:
                item.start()

        place = part_of(b, pair)
        cos_t = trig[b, 0:quarter, :]
        sin_t = trig[b, quarter:2 * quarter, :]
        flat = dot_t(wi[...], hb[b])
        for head in range(2):
            q_rot = eighth(jnp.concatenate(turned(flat[hd * head:hd * head + hd], cos_t, sin_t), axis=0))
            for t in range(2):
                lane = pair * t + tok * head
                qt[b, :, lane:lane + tok] = q_rot[:, tok * t:tok * t + tok]
        kv_rot = keys_values(flat[hw:2 * hw], cos_t, sin_t)
        kvt[:, place] = kv_rot
        kv[place, :] = kv_rot.T

        @pl.when(b <= chip)
        def _():
            flat_far = dot_t(w_far[...], hb[b])
            for f in range(n_far):
                far_rot = keys_values(flat_far[hw * f:hw * f + hw], cos_t, sin_t)
                kvt_far[f, :, place] = far_rot
                kv_far[f, place, :] = far_rot.T

            @pl.loop(0, n_far)
            def _(f):
                both = dot(kv_far[f, place, :], bmat_far[f])
                s = jnp.where(seen_far | (k > 0), both[:, 0:cols_q], -1e30)
                old = stat_far[f, 0]
                new = jnp.maximum(old, col_max(s))
                p = jnp.exp(s - new)
                keep = jnp.exp(old - new)
                stat_far[f, 0] = new
                stat_far[f, 1] = stat_far[f, 1] * keep + col_sum(p)
                stat_far[f, 2] = stat_far[f, 2] * keep + col_sum(p * both[:, cols_q:2 * cols_q])

    groups = [slice(tile * g, tile * g + tile) for g in range(cols_q // tile)]

    def first_part(b, seen):
        def both_of(rows):
            both = dot(kv[rows, :], bmat[...])
            return both[:, 0:cols_q], both[:, cols_q:2 * cols_q]

        rows = part_of(b, pair)
        s, d_p = both_of(rows)
        s = jnp.where(seen, s, -1e30)
        top = col_max(s)
        p = jnp.exp(s - top)
        sbuf[rows, :] = p
        dpbuf[rows, :] = d_p
        mbuf[b] = top

        def step(c, state, chunks=1):
            old, total, weighted = state
            rows = part_of(c, chunks * pair)
            s, d_p = both_of(rows)
            new = jnp.maximum(old, col_max(s))
            p = jnp.exp(s - new)
            sbuf[rows, :] = p
            dpbuf[rows, :] = d_p
            for i in range(chunks):
                mbuf[chunks * c + i] = new
            keep = jnp.exp(old - new)
            return new, total * keep + col_sum(p), weighted * keep + col_sum(p * d_p)

        state = (top, col_sum(p), col_sum(p * d_p))
        state = lax.fori_loop(0, b // 2, functools.partial(step, chunks=2), state)
        top, total, weighted = lax.fori_loop(2 * (b // 2), b, step, state)
        inv = 1.0 / total
        return top, inv, weighted * inv

    def second_part(b, stats):
        top, inv, row_dot = stats
        adq[...] = jnp.zeros_like(adq)

        def step(c, carry):
            rows = part_of(c, pair)
            factor = jnp.exp(mbuf[c] - top) * inv
            d_k = d_v = None
            for at in groups:
                p = sbuf[rows, at] * factor[:, at]
                p_b = p.astype(BF)
                ds_b = (p * (dpbuf[rows, at] - row_dot[:, at])).astype(BF)
                adq[0:hd, at] += dot(kvt[0:hd, rows], ds_b)
                adq[hd:hw, at] += dot(kvt[hd:hw, rows], p_b)
                more_k = dot_t(bmat[0:hd, at], ds_b)
                more_v = dot_t(bmat[hd:hw, cols_q + at.start:cols_q + at.stop], p_b)
                d_k = more_k if d_k is None else d_k + more_k
                d_v = more_v if d_v is None else d_v + more_v
            dkvt[0:hd, rows] += d_k
            dkvt[hd:hw, rows] += d_v
            return carry

        lax.fori_loop(0, b + 1, step, 0)


    def send_rows(slot):
        cols = part_of(slot, tok)
        return [
            remote(dq_all.at[:, cols], dt_rv.at[own_rows], q_s.at[slot], q_r.at[me], slot),
            remote(at_all.at[:, cols], at_rv.at[own_rows], a_s.at[slot], a_r.at[me], slot),
        ]

    last = 6 * parts

    def serve(event):
        @pl.when(event < last)
        def _():
            ring_event(y_ring, event)

    @pl.loop(0, n_chip)
    def _(j):
        k = j - 1

        @pl.when(k == 0)
        def _():
            for turn in range(2):
                ring_event(y_ring, k + turn)

        @pl.when((k % 2 == 1) & (k > 0))
        def _():
            for turn in range(2, parts):
                serve(parts * k + turn)

        b = jnp.where(j == 0, opposite, ring_origin(jnp.maximum(k, 0)))

        @once(k == 1)
        def _(_):
            for item in weight_loads:
                item.wait()

        @pl.loop(0, jnp.where(j == n_chip - 1, 2 + 4 * near, 0))
        def _(early):
            slot = 2 * ring_origin(early // 2) + early % 2

            @pl.when(slot != me)
            def _():
                for item in send_rows(slot):
                    item.start()

        bmat[0:hd, 0:cols_q] = qt[b]

        @once(j == 0)
        def _(_):
            for i in range(4):
                remote(da_rv.at[i], da_rv.at[i], d_s.at[0], d_r.at[i], mate).wait_recv()
                bmat[hd:hw, cols_q + tok * i:cols_q + tok * i + tok] = da_rv[i]

        @once(j > 0)
        def _(_):
            ring_mate(y_ring, k, b)
            da_t = dot_t(woi[...], dyb[b]).astype(BF)
            for t in range(2):
                for head in range(2):
                    at = cols_q + pair * t + tok * head
                    bmat[hd:hw, at:at + tok] = da_t[hd * head:hd * head + hd, tok * t:tok * t + tok]

        stats = first_part(b, row <= (lane // pair) * tok + lane % tok)
        for turn in range(2):
            serve(jnp.where(k < 0, last, parts * k + 2 + 2 * (k % 2)) + turn)
        second_part(b, stats)
        for t in range(2):
            slot = 2 * b + t
            lanes = [slice(pair * t + tok * head, pair * t + tok * head + tok) for head in range(2)]
            a_t = jnp.concatenate([adq[hd:hw, at] for at in lanes], axis=0).astype(BF)
            cos_t = trig[b, 0:quarter, tok * t:tok * t + tok]
            sin_t = trig[b, quarter:2 * quarter, tok * t:tok * t + tok]
            dq_t = jnp.concatenate([piece for at in lanes for piece in turned(adq[0:hd, at] * scale, cos_t, -sin_t)], axis=0).astype(BF)
            at_all[:, part_of(slot, tok)] = a_t
            dq_all[:, part_of(slot, tok)] = dq_t

            @pl.when(slot == me)
            def _():
                at_rv[own_rows, :] = a_t
                dt_rv[own_rows, :] = dq_t

        @pl.when((k % 2 == 0) & (k >= 0))
        def _():
            for turn in range(2):
                serve(parts * j + turn)

    far = [ring_origin(k) for k in range(n_chip - 1, 0, -1)]
    targets = [2 * c + p for c in far for p in range(2)] + [mate]
    near_targets = targets[-1 - 4 * near:]
    swap = remote(dkvt.at[part_of(1 - core, hd)], kv_rv, x_s, x_r, mate)
    swap.start()
    w_sends = [remote(dwt.at[pl.ds(0, hw), part_of(t, tok)], gw_hbm.at[own_rows], w_s.at[t], w_r.at[me], t) for t in targets]

    def columns(rows_all, buf, cols):
        acc = jnp.zeros((rows_all.shape[0], tile), F32)
        for s in range(n_chip):
            acc += dot(rows_all[:, pair * s:pair * s + pair], buf[s, :, cols])
        return acc

    def q_columns(i):
        cols = part_of(far[i] if i < n_chip - 1 else chip, pair)
        dwt[0:hw, cols] = columns(dq_all, hb, cols)
        for item in w_sends[max(2 * i - 2, 0):2 * i]:
            item.start()

    for i in range(FIRST + 1):
        q_columns(i)

    swap.wait_recv()
    mine = part_of(core, hd)
    g_rows = pl.ds(pl.multiple_of(q_rows + core * kv_w + chip * hd, hd), hd)
    for t in range(n_chip):
        cols = slice(pair * t, pair * t + pair)
        g = dkvt[mine, cols] + kv_rv[:, cols]
        cos_t = jnp.where(core == 0, trig[t, 0:quarter, :], 1.0)
        sin_t = jnp.where(core == 0, trig[t, quarter:2 * quarter, :], 0.0)
        g_b = jnp.concatenate(turned(g, cos_t, -sin_t), axis=0).astype(BF)
        kv_mine[2 * t] = g_b[:, 0:tok]
        kv_mine[2 * t + 1] = g_b[:, tok:pair]
        kv_row[:, cols] = g_b
    dt_rv[g_rows, :] = kv_mine[me]
    kv_sends = [remote(kv_mine.at[t], dt_rv.at[g_rows], kv_s.at[t], kv_r.at[me], t) for t in targets]
    for item in kv_sends:
        item.start()
    for i in range(FIRST + 1, n_chip):
        q_columns(i)
    w_sends[-1].start()
    w_own = local(dwt.at[pl.ds(0, hw), part_of(me, tok)], gw_hbm.at[own_rows], loc_sem.at[0])
    w_own.start()
    for t in range(width // tile):
        cols = slice(tile * t, tile * t + tile)
        dwt[hw:hw + hd, cols] = columns(kv_row, hb, cols)
    wk_own = local(dwt.at[pl.ds(hw, hd), part_of(me, tok)], gw_hbm.at[g_rows], loc_sem.at[1])
    wk_own.start()
    wk_sends = [remote(dwt.at[pl.ds(hw, hd), part_of(t, tok)], gw_hbm.at[g_rows], wk_s.at[t], wk_r.at[me], t) for t in targets]
    for item in wk_sends[0:HELD]:
        item.start()

    @pl.loop(last, 7 * parts)
    def _(event):
        ring_event(y_ring, event)

    ring_mate(y_ring, n_chip - 1, opposite)
    for t in range(width // tile):
        cols = slice(tile * t, tile * t + tile)
        dwo[:, cols] = columns(at_all, dyb, cols)
    store_wo = local(dwo, gwo_hbm, out_sem.at[0])
    store_wo.start()
    finish_ring(y_ring)
    wo_loads = [local(wo_hbm.at[pl.ds(pair * t, pair)], dyb.at[t], wo_sem.at[t]) for t in range(n_chip)]
    for item in wo_loads:
        item.start()

    @pl.loop(0, n_far)
    def _(f):
        c_far = ring_origin(2 * near + 1 + f)
        cos_t = trig[chip, 0:quarter, part_of(core, tok)]
        sin_t = trig[chip, quarter:2 * quarter, part_of(core, tok)]
        top = stat_far[f, 0]
        inv = 1.0 / stat_far[f, 1]
        row_dot = stat_far[f, 2] * inv

        def add_chunk(c, diagonal, chunks=1):
            rows = part_of(c, chunks * pair)
            for at in groups:
                keys = kv_far[f, rows, :]
                s = dot(keys, bmat_far[f, :, at])
                d_p = dot(keys, bmat_far[f, :, cols_q + at.start:cols_q + at.stop])
                if diagonal:
                    s = jnp.where(seen_far[:, at], s, -1e30)
                p = jnp.exp(s - top[:, at]) * inv[:, at]
                p_b = p.astype(BF)
                ds_b = (p * (d_p - row_dot[:, at])).astype(BF)
                d_q = dot(kvt_far[f, 0:hd, rows], ds_b)
                d_a = dot(kvt_far[f, hd:hw, rows], p_b)
                adq[0:hd, at] = d_q if diagonal else adq[0:hd, at] + d_q
                adq[hd:hw, at] = d_a if diagonal else adq[hd:hw, at] + d_a

        add_chunk(chip, True)

        @pl.loop(0, chip // 2)
        def _(c):
            add_chunk(c, False, 2)

        @pl.when(chip % 2 == 1)
        def _():
            add_chunk(chip - 1, False)

        for head in range(4):
            at = slice(tok * head, tok * head + tok)
            place = pl.ds(pl.multiple_of(c_far * 2 * hw + hd * head, hd), hd)
            at_rv[place, :] = adq[hd:hw, at].astype(BF)
            dt_rv[place, :] = jnp.concatenate(turned(adq[0:hd, at] * scale, cos_t, -sin_t), axis=0).astype(BF)

    for t in near_targets:
        remote(at_all.at[:, pl.ds(0, tok)], at_rv.at[part_of(t, hw)], a_s.at[t], a_r.at[t], t).wait_recv()
    for item in wo_loads:
        item.wait()
    for t in range(q_rows // tok):
        a_nat[:, tok * t:tok * t + tok] = at_rv[tok * t:tok * t + tok, :].T
    for t in range(width // tile):
        cols = slice(tile * t, tile * t + tile)
        prod = jnp.zeros((tok, tile), F32)
        for s in range(n_chip):
            prod += dot(a_nat[:, pair * s:pair * s + pair], dyb[s, :, cols])
        out_v[:, cols] = (x_v[:, cols].astype(F32) + prod).astype(BF)
    store_out = local(out_v, out_hbm, out_sem.at[1])
    store_out.start()

    def kv_place(t):
        return pl.ds(pl.multiple_of(q_rows + (t % 2) * kv_w + (t // 2) * hd, hd), hd)

    for t in near_targets:
        remote(dq_all.at[:, pl.ds(0, tok)], dt_rv.at[part_of(t, hw)], q_s.at[t], q_r.at[t], t).wait_recv()
    for t in targets:
        remote(kv_mine.at[0], dt_rv.at[kv_place(t)], kv_s.at[t], kv_r.at[t], t).wait_recv()
    swap.wait_send()
    for t in range(n_rows // tok):
        d_nat[:, tok * t:tok * t + tok] = dt_rv[tok * t:tok * t + tok, :].T

    mean = stat[0, :, 0:1]
    inv_std = stat[1, :, 0:1]
    dh = dkvt
    for t in range(width // tile):
        cols = slice(tile * t, tile * t + tile)
        acc = jnp.zeros((tok, tile), F32)
        for s in range(n_rows // tile):
            acc += dot(d_nat[:, tile * s:tile * s + tile], wt[tile * s:tile * s + tile, cols])
        dh[:, cols] = acc
        gg_st[0, :, cols] = col_sum(acc * ((x_v[:, cols].astype(F32) - mean) * inv_std))
        gg_st[1, :, cols] = col_sum(acc)
    g_swap = remote(gg_st.at[1 - core], gg_mx, g_s.at[n_chip], g_r.at[n_chip], mate)
    g_swap.start()
    g_swap.wait_recv()
    gg_my[...] = jnp.where(core == 0, gg_st[0], gg_st[1]) + gg_mx[...]
    gg_rv[chip] = gg_my[...]
    g_sends = [remote(gg_my, gg_rv.at[chip], g_s.at[c], g_r.at[chip], 2 * c + core) for c in far]
    for item in g_sends + wk_sends[HELD:]:
        item.start()

    grad_hat = dh[...] * gain_one
    x_hat = (x_v[...].astype(F32) - mean) * inv_std
    mean_one = row_mean(grad_hat)
    mean_two = row_mean(grad_hat * x_hat)
    store_out.wait()
    out_v[...] = (dy_own[...].astype(F32) + inv_std * (grad_hat - mean_one - x_hat * mean_two)).astype(BF)
    store_gx = local(out_v, gx_hbm, out_sem.at[2])
    store_gx.start()

    for c in far:
        remote(gg_my, gg_rv.at[c], g_s.at[c], g_r.at[c], 2 * c + core).wait_recv()
    sums = gg_rv[0]
    for c in range(1, n_chip):
        sums = sums + gg_rv[c]
    gg_out[core] = sums
    g_swap_out = remote(gg_out.at[core], gg_out.at[core], g_s.at[n_chip + 1], g_r.at[n_chip + 1], mate)
    g_swap_out.start()
    remote(gg_out.at[core], gg_out.at[1 - core], g_s.at[n_chip + 1], g_r.at[n_chip + 1], mate).wait_recv()
    store_gg = local(gg_out, gg_hbm, out_sem.at[3])
    store_gg.start()

    finish_ring(h_ring)
    for item in pos_sends + [g_swap, g_swap_out] + [opposite_send(head) for head in range(4)]:
        item.wait_send()
    for t in near_targets:
        remote(at_all.at[:, pl.ds(0, tok)], at_rv.at[pl.ds(0, hw)], a_s.at[t], a_r.at[t], t).wait_send()
        remote(dq_all.at[:, pl.ds(0, tok)], dt_rv.at[pl.ds(0, hw)], q_s.at[t], q_r.at[t], t).wait_send()
    for item in kv_sends + w_sends + g_sends + wk_sends:
        item.wait_send()
    for t in targets:
        remote(dwt.at[pl.ds(0, hw), part_of(t, tok)], gw_hbm.at[part_of(t, hw)], w_s.at[t], w_r.at[t], t).wait_recv()
        remote(dwt.at[pl.ds(hw, hd), part_of(t, tok)], gw_hbm.at[kv_place(t)], wk_s.at[t], wk_r.at[t], t).wait_recv()
    for item in (w_own, wk_own, store_wo, store_gx, store_gg):
        item.wait()


def settle_kernel(q_rows, kv_w, out_i, gx_i, gw_i, gwo_i, gg_i, out_o, gx_o, gq_o, gk_o, gv_o, gwo_o, gain_o, bias_o, b_act, b_q, b_kv, b_o, b_gg, sem_in, sem_out, sem_gg):
    half_q = q_rows // 2
    half_o = gwo_i.shape[0] // 2
    moves = [(out_i, b_act.at[0], out_o), (gx_i, b_act.at[1], gx_o)]
    for t in range(2):
        moves.append((gw_i.at[pl.ds(half_q * t, half_q)], b_q.at[t], gq_o.at[pl.ds(half_q * t, half_q)]))
        moves.append((gwo_i.at[pl.ds(half_o * t, half_o)], b_o.at[t], gwo_o.at[pl.ds(half_o * t, half_o)]))
    moves.append((gw_i.at[pl.ds(q_rows, kv_w)], b_kv.at[0], gk_o))
    moves.append((gw_i.at[pl.ds(q_rows + kv_w, kv_w)], b_kv.at[1], gv_o))
    loads = [pltpu.make_async_copy(src, mid, sem_in.at[i]) for i, (src, mid, _) in enumerate(moves)]
    stores = [pltpu.make_async_copy(mid, dst, sem_out.at[i]) for i, (_, mid, dst) in enumerate(moves)]
    load_gg = pltpu.make_async_copy(gg_i, b_gg, sem_gg)
    load_gg.start()
    for item in loads:
        item.start()
    for load, store in zip(loads, stores):
        load.wait()
        store.start()
    load_gg.wait()
    gain_o[...] = b_gg[0, 0]
    bias_o[...] = b_gg[1, 0]
    for item in stores:
        item.wait()


def solution(mesh):
    n_dev = mesh.shape['cp']

    def device_step(x_act, d_out, positions, ln_gain, ln_bias, w_query, w_key, w_value, w_out):
        tok, width = x_act.shape[1], x_act.shape[2]
        q_heads, hd = w_query.shape[1], w_query.shape[2]
        kv_heads = w_key.shape[1]
        q_w, kv_w = q_heads * hd, kv_heads * hd
        n_rows = q_w + 2 * kv_w
        seq = n_dev * tok
        hw = 2 * hd

        def flat_weight(w):
            return jnp.transpose(w, (1, 2, 0)).reshape(-1, width)

        hbm = pl.BlockSpec(memory_space=pltpu.HBM)
        vmem = pl.BlockSpec(memory_space=pltpu.VMEM)
        dma = pltpu.SemaphoreType.DMA
        n_chip = n_dev // 2
        n_far = n_chip - 1 - 2 * NEAR
        pair = 2 * tok
        scratch = [
            pltpu.VMEM((n_chip, pair, width), BF),
            pltpu.VMEM((n_chip, pair, width), BF),
            pltpu.VMEM((n_rows, width), BF),
            pltpu.VMEM((2 * hw, width), BF),
            pltpu.VMEM((hw, width), BF),
            pltpu.VMEM((n_far * hw, width), BF),
            pltpu.VMEM((n_dev, 1, tok), jnp.int32),
            pltpu.VMEM((n_chip, hd // 2, pair), F32),
            pltpu.VMEM((n_chip, hd, 2 * pair), BF),
            pltpu.VMEM((hw, seq), BF),
            pltpu.VMEM((seq, hw), BF),
            pltpu.VMEM((n_far, hw, seq), BF),
            pltpu.VMEM((n_far, seq, hw), BF),
            pltpu.VMEM((n_far, hw, 4 * pair), BF),
            pltpu.VMEM((n_far, 3, 1, 2 * pair), F32),
            pltpu.VMEM((hw, 4 * pair), BF),
            pltpu.VMEM((4, hd, tok), BF),
            pltpu.VMEM((seq, 2 * pair), F32),
            pltpu.VMEM((seq, 2 * pair), F32),
            pltpu.VMEM((n_chip, 1, 2 * pair), F32),
            pltpu.VMEM((hw, 2 * pair), F32),
            pltpu.VMEM((hw, seq), F32),
            pltpu.VMEM((hd, seq), F32),
            pltpu.VMEM((n_dev, hd, tok), BF),
            pltpu.VMEM((hd, seq), BF),
            pltpu.VMEM((hw, width), F32),
            pltpu.VMEM((hw + hd, width), F32),
            pltpu.VMEM((hw, seq), BF),
            pltpu.VMEM((hw, seq), BF),
            pltpu.VMEM((q_w, tok), BF),
            pltpu.VMEM((n_rows, tok), BF),
            pltpu.VMEM((tok, q_w), BF),
            pltpu.VMEM((tok, n_rows), BF),
            pltpu.VMEM((tok, width), BF),
            pltpu.VMEM((tok, width), BF),
            pltpu.VMEM((2, 1, width), F32),
            pltpu.VMEM((2, tok, 128), F32),
            pltpu.VMEM((tok, width), BF),
            pltpu.VMEM((2, 1, width), F32),
            pltpu.VMEM((1, width), F32),
            pltpu.VMEM((1, width), F32),
            pltpu.VMEM((n_chip, 1, width), F32),
            pltpu.VMEM((2, 1, width), F32),
            dma((10,)), dma((4 * n_far,)), dma((n_chip,)), dma((3,)), dma((4,)), dma((2,)),
        ] + [dma((9 * PARTS,)), dma((7 * PARTS,)), dma((8 * PARTS,)), dma((8 * PARTS,))] * 2 + [dma((4,))] * 2 + [dma((n_dev,))] * 6 + [dma] * 2 + [dma((n_dev,))] * 8
        out, gx, gw, gwo, gg = pl.pallas_call(
            functools.partial(block_kernel, n_dev, hd, kv_w, NEAR, PARTS),
            out_shape=(
                jax.ShapeDtypeStruct((tok, width), BF),
                jax.ShapeDtypeStruct((tok, width), BF),
                jax.ShapeDtypeStruct((n_rows, tok), F32),
                jax.ShapeDtypeStruct((hw, width), F32),
                jax.ShapeDtypeStruct((2, 1, width), F32),
            ),
            in_specs=[hbm] * 9,
            out_specs=(hbm,) * 5,
            scratch_shapes=scratch,
            compiler_params=pltpu.CompilerParams(collective_id=0, has_side_effects=True, vmem_limit_bytes=67043328),
            name='attn_block',
        )(
            x_act.reshape(tok, width), d_out.reshape(tok, width), positions.reshape(1, tok),
            ln_gain.reshape(1, width), ln_bias.reshape(1, width),
            flat_weight(w_query), flat_weight(w_key), flat_weight(w_value), w_out,
        )

        out, gx, gq, gk, gv, gwo, gain, bias = pl.pallas_call(
            functools.partial(settle_kernel, q_w, kv_w),
            out_shape=(
                jax.ShapeDtypeStruct((tok, width), BF),
                jax.ShapeDtypeStruct((tok, width), BF),
                jax.ShapeDtypeStruct((q_w, tok), F32),
                jax.ShapeDtypeStruct((kv_w, tok), F32),
                jax.ShapeDtypeStruct((kv_w, tok), F32),
                jax.ShapeDtypeStruct((hw, width), F32),
                jax.ShapeDtypeStruct((width,), F32),
                jax.ShapeDtypeStruct((width,), F32),
            ),
            in_specs=[hbm] * 5,
            out_specs=(hbm,) * 6 + (vmem,) * 2,
            scratch_shapes=[
                pltpu.VMEM((2, tok, width), BF),
                pltpu.VMEM((2, q_w // 2, tok), F32),
                pltpu.VMEM((2, kv_w, tok), F32),
                pltpu.VMEM((2, hw // 2, width), F32),
                pltpu.VMEM((2, 1, width), F32),
                dma((8,)), dma((8,)), dma,
            ],
            name='settle',
        )(out, gx, gw, gwo, gg)

        def rows_out(block, heads):
            return jnp.transpose(block.reshape(heads, hd, tok), (2, 0, 1))

        return (
            out.reshape(1, tok, width), gx.reshape(1, tok, width),
            rows_out(gq, q_heads), rows_out(gk, kv_heads), rows_out(gv, kv_heads),
            gwo, gain, bias,
        )

    return jax.shard_map(device_step, mesh=mesh, in_specs=(P('dp', 'cp', None), P('dp', 'cp', None), P('dp', 'cp'), P(None), P(None), P(None, None, None), P(None, None, None), P(None, None, None), P(None, None)), out_specs=(P('dp', 'cp', None), P('dp', 'cp', None), P(('dp', 'cp'), None, None), P(('dp', 'cp'), None, None), P(('dp', 'cp'), None, None), P(('dp', 'cp'), None), P('dp'), P('dp')), check_vma=False)
```

```python
import functools
import math

import jax
import jax.numpy as jnp
from jax import lax
from jax.experimental import pallas as pl
from jax.experimental.pallas import tpu as pltpu
from jax.sharding import PartitionSpec as P

EPS = 1e-5
ROPE_BASE = 10000.0
MESH = pl.DeviceIdType.MESH
BF = jnp.bfloat16
F32 = jnp.float32
NEAR = 1
PARTS = 4
FIRST = 2
HELD = 4


def dot(lhs, rhs):
    return jnp.dot(lhs, rhs, preferred_element_type=F32)


def col_sum(val):
    return jnp.sum(val, axis=0, keepdims=True)


def col_max(val):
    return jnp.max(val, axis=0, keepdims=True)


def row_mean(val):
    return jnp.mean(val, axis=-1, keepdims=True)


def dot_t(lhs, rhs):
    return lax.dot_general(lhs, rhs, (((1,), (1,)), ((), ())), preferred_element_type=F32)


def block_kernel(
    n_dev, hd, kv_w, near, parts,
    x_hbm, dy_hbm, pos_hbm, gain_hbm, bias_hbm, wq_hbm, wk_hbm, wv_hbm, wo_hbm,
    out_hbm, gx_hbm, gw_hbm, gwo_hbm, gg_hbm,
    hb, dyb, wt, wi, woi, w_far, pos_all, trig,
    qt, kvt, kv, kvt_far, kv_far, bmat_far, stat_far, bmat, da_rv, sbuf, dpbuf, mbuf, adq, dkvt, kv_rv, kv_mine, kv_row,
    dwo, dwt, at_all, dq_all, at_rv, dt_rv, a_nat, d_nat, x_v, dy_own, gb_v, stat, out_v, gg_st, gg_mx, gg_my, gg_rv, gg_out,
    in_sem, far_sem, wo_sem, w_sem, out_sem, loc_sem,
    hzs, hzr, hds, hdr, yzs, yzr, yds, ydr,
    d_s, d_r, pos_s, pos_r, a_s, a_r, q_s, q_r, x_s, x_r, kv_s, kv_r, w_s, w_r, wk_s, wk_r, g_s, g_r,
):
    tok, width = x_v.shape
    n_chip = n_dev // 2
    pair = 2 * tok
    me = lax.axis_index('cp')
    chip = me // 2
    core = me % 2
    right = 2 * ((chip + 1) % n_chip) + core
    left = 2 * ((chip + n_chip - 1) % n_chip) + core
    mate = 2 * chip + 1 - core
    q_rows = wq_hbm.shape[0]
    n_rows = q_rows + 2 * kv_w
    hw = 2 * hd
    quarter = hd // 4
    tile = 256
    scale = hd ** -0.5
    cols_q = 2 * pair
    n_far = n_chip - 1 - 2 * near

    def remote(src, dst, send, recv, target):
        return pltpu.make_async_remote_copy(src_ref=src, dst_ref=dst, send_sem=send, recv_sem=recv, device_id={'cp': target}, device_id_type=MESH)

    def local(src, dst, sem):
        return pltpu.make_async_copy(src, dst, sem)

    def part_of(i, size):
        return pl.ds(pl.multiple_of(i * size, size), size)

    def once(cond):
        return pl.loop(0, jnp.where(cond, 1, 0))

    def ring_steps(k):
        step = (k + 1) // 2
        return step, k % 2

    def ring_origin(k):
        step, ahead = ring_steps(k)
        return jnp.where(ahead == 1, chip + n_chip - step, chip + step) % n_chip

    own = (chip, part_of(core, tok))
    first_loads = [
        local(x_hbm, x_v, in_sem.at[0]),
        local(gain_hbm, gb_v.at[0], in_sem.at[1]),
        local(bias_hbm, gb_v.at[1], in_sem.at[2]),
        local(pos_hbm, pos_all.at[me], in_sem.at[3]),
    ]
    for item in first_loads:
        item.start()
    barrier = pltpu.get_barrier_semaphore()
    for step in range(1, n_dev):
        pl.semaphore_signal(barrier, inc=1, device_id={'cp': (me + step) % n_dev}, device_id_type=MESH)
    own_rows = part_of(me, hw)
    kv_rows = part_of(chip, hd)
    loads = [
        local(wq_hbm.at[own_rows], wi.at[pl.ds(0, hw)], in_sem.at[4]),
        local(wk_hbm.at[kv_rows], wi.at[pl.ds(hw, hd)], in_sem.at[5]),
        local(wv_hbm.at[kv_rows], wi.at[pl.ds(hw + hd, hd)], in_sem.at[6]),
        local(wo_hbm.at[own_rows], woi, in_sem.at[7]),
        local(dy_hbm, dyb.at[own], in_sem.at[8]),
        local(dy_hbm, dy_own, in_sem.at[9]),
    ]
    far_loads = []
    for f in range(n_far):
        far_rows = part_of(ring_origin(2 * near + 1 + f), hd)
        loads.append(local(wk_hbm.at[far_rows], w_far.at[pl.ds(hw * f, hd)], far_sem.at[2 * f]))
        loads.append(local(wv_hbm.at[far_rows], w_far.at[pl.ds(hw * f + hd, hd)], far_sem.at[2 * f + 1]))
        far_wo = part_of(ring_origin(2 * near + 1 + f), 2 * hw)
        far_loads.append(local(wo_hbm.at[far_wo], wt.at[pl.ds(2 * hw * f, 2 * hw)], far_sem.at[2 * n_far + f]))
        far_loads.append(local(wq_hbm.at[far_wo], wt.at[pl.ds(2 * hw * (n_far + f), 2 * hw)], far_sem.at[3 * n_far + f]))
    for item in loads + far_loads:
        item.start()

    for item in first_loads:
        item.wait()
    gain_one = 1.0 + gb_v[0]
    block = 16

    @pl.loop(0, tok // block)
    def _(i):
        rows = part_of(i, block)
        x_f = x_v[rows, :].astype(F32)
        mean = row_mean(x_f)
        centered = x_f - mean
        inv_std = lax.rsqrt(row_mean(centered * centered) + EPS)
        hb[chip, part_of(core * (tok // block) + i, block), :] = (centered * inv_std * gain_one + gb_v[1]).astype(BF)
        stat[0, rows, :] = jnp.broadcast_to(mean, (block, 128))
        stat[1, rows, :] = jnp.broadcast_to(inv_std, (block, 128))

    pl.semaphore_wait(barrier, n_dev - 1)

    def chunk(buf, origin, parity, part):
        return buf.at[origin, part_of(parts * parity + part, tok // parts)]

    turns = 2 * parts

    def own_sends(buf, zs, zr, ds, dr):
        copies = []
        for part in range(parts):
            piece = chunk(buf, chip, core, part)
            copies.append(remote(piece, piece, zs.at[2 * part], zr.at[2 * part], right))
            copies.append(remote(piece, piece, zs.at[2 * part + 1], zr.at[2 * part + 1], left))
            copies.append(remote(piece, piece, ds.at[7 * parts + part], dr.at[7 * parts + part], mate))
        return copies

    def event_place(event):
        step = event // turns + 1
        turn = event % turns
        direction = turn % 2
        part = jnp.where(step < 4, turn // 2, turn // 2 + direction * (parts // 2))
        origin = jnp.where(direction == 0, chip + n_chip - step, chip + step) % n_chip
        return step, direction, part, origin

    def last_event(part, direction):
        return 6 * parts + 2 * (part - direction * (parts // 2)) + direction

    def ring_event(ring, event):
        buf, zs, zr, ds, dr = ring
        step, direction, part, origin = event_place(event)
        piece = chunk(buf, origin, core, part)
        remote(piece, piece, zs.at[0], zr.at[event], right).wait_recv()
        onward = jnp.where(step < 3, event + turns, last_event(part, direction))

        @pl.when((step < 3) | ((step == 3) & ((part >= parts // 2) == (direction == 1))))
        def _():
            remote(piece, piece, zs.at[event + turns], zr.at[onward], jnp.where(direction == 0, right, left)).start()

        remote(piece, piece, ds.at[event], dr.at[event], mate).start()

    def ring_service(ring, event):
        @pl.when(event < 7 * parts)
        def _():
            ring_event(ring, event)

    def ring_mate(ring, k, origin):
        buf, zs, zr, ds, dr = ring
        step, ahead = ring_steps(k)
        for part in range(parts):
            event = jnp.where(k == 0, 7 * parts + part, jnp.where(step < 4, turns * (step - 1) + 2 * part + 1 - ahead, last_event(part, part // (parts // 2))))
            piece = chunk(buf, origin, 1 - core, part)
            remote(piece, piece, ds.at[0], dr.at[event], mate).wait_recv()

    def finish_ring(ring):
        buf, zs, zr, ds, dr = ring
        for item in own_sends(*ring):
            item.wait_send()

        @pl.loop(0, 7 * parts)
        def _(event):
            step, direction, part, origin = event_place(event)
            piece = chunk(buf, origin, core, part)

            @pl.when((step < 3) | ((step == 3) & ((part >= parts // 2) == (direction == 1))))
            def _():
                remote(piece, piece, zs.at[event + turns], zr.at[event], right).wait_send()

            remote(piece, piece, ds.at[event], dr.at[event], mate).wait_send()

    h_ring = (hb, hzs, hzr, hds, hdr)
    y_ring = (dyb, yzs, yzr, yds, ydr)
    for item in own_sends(*h_ring):
        item.start()
    pos_sends = [remote(pos_all.at[me], pos_all.at[me], pos_s.at[step], pos_r.at[me], (me + step) % n_dev) for step in range(1, n_dev)]
    for item in pos_sends:
        item.start()
    weight_loads = [
        local(wq_hbm, wt.at[pl.ds(0, q_rows)], w_sem.at[0]),
        local(wk_hbm, wt.at[pl.ds(q_rows, kv_w)], w_sem.at[1]),
        local(wv_hbm, wt.at[pl.ds(q_rows + kv_w, kv_w)], w_sem.at[2]),
    ]
    dkvt[...] = jnp.zeros_like(dkvt)
    bmat[...] = jnp.zeros_like(bmat)
    bmat_far[...] = jnp.zeros_like(bmat_far)
    for f in range(n_far):
        stat_far[f, 0] = jnp.full((1, cols_q), -3e38, F32)
        stat_far[f, 1] = jnp.zeros((1, cols_q), F32)
        stat_far[f, 2] = jnp.zeros((1, cols_q), F32)

    freq = jnp.exp(lax.broadcasted_iota(jnp.int32, (quarter, tok), 0).astype(F32) * (-2.0 * math.log(ROPE_BASE) / (hd // 2)))

    def make_trig(b):
        for t in range(2):
            slot = 2 * b + t

            @pl.when(slot != me)
            def _():
                remote(pos_all.at[slot], pos_all.at[slot], pos_s.at[0], pos_r.at[slot], me).wait_recv()

            angle = pos_all[slot].astype(F32) * freq
            trig[b, 0:quarter, tok * t:tok * t + tok] = jnp.cos(angle)
            trig[b, quarter:2 * quarter, tok * t:tok * t + tok] = jnp.sin(angle)

    def turned(val, cos_t, sin_t):
        u = val[0:quarter]
        w = val[quarter:2 * quarter]
        return [u * cos_t - w * sin_t, w * cos_t + u * sin_t, val[2 * quarter:hd]]

    def eighth(val):
        return val.astype(BF) * jnp.asarray(scale, BF)

    def keys_values(val, cos_t, sin_t):
        return jnp.concatenate(turned(val[0:hd], cos_t, sin_t) + [val[hd:hw]], axis=0).astype(BF)

    lane = lax.broadcasted_iota(jnp.int32, (pair, cols_q), 1)
    row = lax.broadcasted_iota(jnp.int32, (pair, cols_q), 0)
    seen_far = row <= core * tok + lane % tok

    opposite = ring_origin(n_chip - 1)

    def opposite_send(head):
        block = bmat_far.at[n_far - 1, pl.ds(hd, hd), pl.ds(cols_q + tok * head, tok)]
        return remote(block, da_rv.at[2 * core + head % 2], d_s.at[head], d_r.at[2 * core + head % 2], 2 * opposite + head // 2)

    @pl.loop(0, n_chip)
    def _(k):
        for turn in range(parts):
            ring_service(h_ring, parts * k + turn)

        @once(k == 5)
        def _(_):
            for item in [opposite_send(head) for head in range(4)] + own_sends(*y_ring):
                item.start()

        @once(k == 0)
        def _(_):
            for item in loads:
                item.wait()

        b = ring_origin(k)
        ring_mate(h_ring, k, b)
        make_trig(b)

        @once(k == 0)
        def _(_):
            for item in far_loads:
                item.wait()
            cos_t = trig[chip, 0:quarter, part_of(core, tok)]
            sin_t = trig[chip, quarter:2 * quarter, part_of(core, tok)]

            @pl.loop(0, n_far)
            def _(f):
                da_t = dot_t(wt[part_of(f, 2 * hw), :], dy_own[...]).astype(BF)
                q_t = dot_t(wt[part_of(n_far + f, 2 * hw), :], hb[chip, part_of(core, tok), :])
                for head in range(4):
                    part = slice(hd * head, hd * head + hd)
                    at = tok * head
                    bmat_far[f, 0:hd, at:at + tok] = eighth(jnp.concatenate(turned(q_t[part], cos_t, sin_t), axis=0))
                    bmat_far[f, hd:hw, cols_q + at:cols_q + at + tok] = da_t[part]

            for item in weight_loads:
                item.start()

        place = part_of(b, pair)
        cos_t = trig[b, 0:quarter, :]
        sin_t = trig[b, quarter:2 * quarter, :]
        flat = dot_t(wi[...], hb[b])
        for head in range(2):
            q_rot = eighth(jnp.concatenate(turned(flat[hd * head:hd * head + hd], cos_t, sin_t), axis=0))
            for t in range(2):
                lane = pair * t + tok * head
                qt[b, :, lane:lane + tok] = q_rot[:, tok * t:tok * t + tok]
        kv_rot = keys_values(flat[hw:2 * hw], cos_t, sin_t)
        kvt[:, place] = kv_rot
        kv[place, :] = kv_rot.T

        @pl.when(b <= chip)
        def _():
            flat_far = dot_t(w_far[...], hb[b])
            for f in range(n_far):
                far_rot = keys_values(flat_far[hw * f:hw * f + hw], cos_t, sin_t)
                kvt_far[f, :, place] = far_rot
                kv_far[f, place, :] = far_rot.T

            @pl.loop(0, n_far)
            def _(f):
                both = dot(kv_far[f, place, :], bmat_far[f])
                s = jnp.where(seen_far | (k > 0), both[:, 0:cols_q], -1e30)
                old = stat_far[f, 0]
                new = jnp.maximum(old, col_max(s))
                p = jnp.exp(s - new)
                keep = jnp.exp(old - new)
                stat_far[f, 0] = new
                stat_far[f, 1] = stat_far[f, 1] * keep + col_sum(p)
                stat_far[f, 2] = stat_far[f, 2] * keep + col_sum(p * both[:, cols_q:2 * cols_q])

    groups = [slice(tile * g, tile * g + tile) for g in range(cols_q // tile)]

    def first_part(b, seen):
        def both_of(rows):
            both = dot(kv[rows, :], bmat[...])
            return both[:, 0:cols_q], both[:, cols_q:2 * cols_q]

        rows = part_of(b, pair)
        s, d_p = both_of(rows)
        s = jnp.where(seen, s, -1e30)
        top = col_max(s)
        p = jnp.exp(s - top)
        sbuf[rows, :] = p
        dpbuf[rows, :] = d_p
        mbuf[b] = top

        def step(c, state, chunks=1):
            old, total, weighted = state
            rows = part_of(c, chunks * pair)
            s, d_p = both_of(rows)
            new = jnp.maximum(old, col_max(s))
            p = jnp.exp(s - new)
            sbuf[rows, :] = p
            dpbuf[rows, :] = d_p
            for i in range(chunks):
                mbuf[chunks * c + i] = new
            keep = jnp.exp(old - new)
            return new, total * keep + col_sum(p), weighted * keep + col_sum(p * d_p)

        state = (top, col_sum(p), col_sum(p * d_p))
        state = lax.fori_loop(0, b // 2, functools.partial(step, chunks=2), state)
        top, total, weighted = lax.fori_loop(2 * (b // 2), b, step, state)
        inv = 1.0 / total
        return top, inv, weighted * inv

    def second_part(b, stats):
        top, inv, row_dot = stats
        adq[...] = jnp.zeros_like(adq)

        def step(c, carry):
            rows = part_of(c, pair)
            factor = jnp.exp(mbuf[c] - top) * inv
            d_k = d_v = None
            for at in groups:
                p = sbuf[rows, at] * factor[:, at]
                p_b = p.astype(BF)
                ds_b = (p * (dpbuf[rows, at] - row_dot[:, at])).astype(BF)
                adq[0:hd, at] += dot(kvt[0:hd, rows], ds_b)
                adq[hd:hw, at] += dot(kvt[hd:hw, rows], p_b)
                more_k = dot_t(bmat[0:hd, at], ds_b)
                more_v = dot_t(bmat[hd:hw, cols_q + at.start:cols_q + at.stop], p_b)
                d_k = more_k if d_k is None else d_k + more_k
                d_v = more_v if d_v is None else d_v + more_v
            dkvt[0:hd, rows] += d_k
            dkvt[hd:hw, rows] += d_v
            return carry

        lax.fori_loop(0, b + 1, step, 0)


    def send_rows(slot):
        cols = part_of(slot, tok)
        return [
            remote(dq_all.at[:, cols], dt_rv.at[own_rows], q_s.at[slot], q_r.at[me], slot),
            remote(at_all.at[:, cols], at_rv.at[own_rows], a_s.at[slot], a_r.at[me], slot),
        ]

    last = 6 * parts

    def serve(event):
        @pl.when(event < last)
        def _():
            ring_event(y_ring, event)

    @pl.loop(0, n_chip)
    def _(j):
        k = j - 1

        @pl.when(k == 0)
        def _():
            for turn in range(2):
                ring_event(y_ring, k + turn)

        @pl.when((k % 2 == 1) & (k > 0))
        def _():
            for turn in range(2, parts):
                serve(parts * k + turn)

        b = jnp.where(j == 0, opposite, ring_origin(jnp.maximum(k, 0)))

        @once(k == 1)
        def _(_):
            for item in weight_loads:
                item.wait()

        @pl.loop(0, jnp.where(j == n_chip - 1, 2 + 4 * near, 0))
        def _(early):
            slot = 2 * ring_origin(early // 2) + early % 2

            @pl.when(slot != me)
            def _():
                for item in send_rows(slot):
                    item.start()

        bmat[0:hd, 0:cols_q] = qt[b]

        @once(j == 0)
        def _(_):
            for i in range(4):
                remote(da_rv.at[i], da_rv.at[i], d_s.at[0], d_r.at[i], mate).wait_recv()
                bmat[hd:hw, cols_q + tok * i:cols_q + tok * i + tok] = da_rv[i]

        @once(j > 0)
        def _(_):
            ring_mate(y_ring, k, b)
            da_t = dot_t(woi[...], dyb[b]).astype(BF)
            for t in range(2):
                for head in range(2):
                    at = cols_q + pair * t + tok * head
                    bmat[hd:hw, at:at + tok] = da_t[hd * head:hd * head + hd, tok * t:tok * t + tok]

        stats = first_part(b, row <= (lane // pair) * tok + lane % tok)
        for turn in range(2):
            serve(jnp.where(k < 0, last, parts * k + 2 + 2 * (k % 2)) + turn)
        second_part(b, stats)
        for t in range(2):
            slot = 2 * b + t
            lanes = [slice(pair * t + tok * head, pair * t + tok * head + tok) for head in range(2)]
            a_t = jnp.concatenate([adq[hd:hw, at] for at in lanes], axis=0).astype(BF)
            cos_t = trig[b, 0:quarter, tok * t:tok * t + tok]
            sin_t = trig[b, quarter:2 * quarter, tok * t:tok * t + tok]
            dq_t = jnp.concatenate([piece for at in lanes for piece in turned(adq[0:hd, at] * scale, cos_t, -sin_t)], axis=0).astype(BF)
            at_all[:, part_of(slot, tok)] = a_t
            dq_all[:, part_of(slot, tok)] = dq_t

            @pl.when(slot == me)
            def _():
                at_rv[own_rows, :] = a_t
                dt_rv[own_rows, :] = dq_t

        @pl.when((k % 2 == 0) & (k >= 0))
        def _():
            for turn in range(2):
                serve(parts * j + turn)

    far = [ring_origin(k) for k in range(n_chip - 1, 0, -1)]
    targets = [2 * c + p for c in far for p in range(2)] + [mate]
    near_targets = targets[-1 - 4 * near:]
    swap = remote(dkvt.at[part_of(1 - core, hd)], kv_rv, x_s, x_r, mate)
    swap.start()
    w_sends = [remote(dwt.at[pl.ds(0, hw), part_of(t, tok)], gw_hbm.at[own_rows], w_s.at[t], w_r.at[me], t) for t in targets]

    def columns(rows_all, buf, cols):
        acc = jnp.zeros((rows_all.shape[0], tile), F32)
        for s in range(n_chip):
            acc += dot(rows_all[:, pair * s:pair * s + pair], buf[s, :, cols])
        return acc

    def q_columns(i):
        cols = part_of(far[i] if i < n_chip - 1 else chip, pair)
        dwt[0:hw, cols] = columns(dq_all, hb, cols)
        for item in w_sends[max(2 * i - 2, 0):2 * i]:
            item.start()

    for i in range(FIRST + 1):
        q_columns(i)

    swap.wait_recv()
    mine = part_of(core, hd)
    g_rows = pl.ds(pl.multiple_of(q_rows + core * kv_w + chip * hd, hd), hd)
    for t in range(n_chip):
        cols = slice(pair * t, pair * t + pair)
        g = dkvt[mine, cols] + kv_rv[:, cols]
        cos_t = jnp.where(core == 0, trig[t, 0:quarter, :], 1.0)
        sin_t = jnp.where(core == 0, trig[t, quarter:2 * quarter, :], 0.0)
        g_b = jnp.concatenate(turned(g, cos_t, -sin_t), axis=0).astype(BF)
        kv_mine[2 * t] = g_b[:, 0:tok]
        kv_mine[2 * t + 1] = g_b[:, tok:pair]
        kv_row[:, cols] = g_b
    dt_rv[g_rows, :] = kv_mine[me]
    kv_sends = [remote(kv_mine.at[t], dt_rv.at[g_rows], kv_s.at[t], kv_r.at[me], t) for t in targets]
    for item in kv_sends:
        item.start()
    for i in range(FIRST + 1, n_chip):
        q_columns(i)
    w_sends[-1].start()
    w_own = local(dwt.at[pl.ds(0, hw), part_of(me, tok)], gw_hbm.at[own_rows], loc_sem.at[0])
    w_own.start()
    for t in range(width // tile):
        cols = slice(tile * t, tile * t + tile)
        dwt[hw:hw + hd, cols] = columns(kv_row, hb, cols)
    wk_own = local(dwt.at[pl.ds(hw, hd), part_of(me, tok)], gw_hbm.at[g_rows], loc_sem.at[1])
    wk_own.start()
    wk_sends = [remote(dwt.at[pl.ds(hw, hd), part_of(t, tok)], gw_hbm.at[g_rows], wk_s.at[t], wk_r.at[me], t) for t in targets]
    for item in wk_sends[0:HELD]:
        item.start()

    @pl.loop(last, 7 * parts)
    def _(event):
        ring_event(y_ring, event)

    ring_mate(y_ring, n_chip - 1, opposite)
    for t in range(width // tile):
        cols = slice(tile * t, tile * t + tile)
        dwo[:, cols] = columns(at_all, dyb, cols)
    store_wo = local(dwo, gwo_hbm, out_sem.at[0])
    store_wo.start()
    finish_ring(y_ring)
    wo_loads = [local(wo_hbm.at[pl.ds(pair * t, pair)], dyb.at[t], wo_sem.at[t]) for t in range(n_chip)]
    for item in wo_loads:
        item.start()

    @pl.loop(0, n_far)
    def _(f):
        c_far = ring_origin(2 * near + 1 + f)
        cos_t = trig[chip, 0:quarter, part_of(core, tok)]
        sin_t = trig[chip, quarter:2 * quarter, part_of(core, tok)]
        top = stat_far[f, 0]
        inv = 1.0 / stat_far[f, 1]
        row_dot = stat_far[f, 2] * inv

        def add_chunk(c, diagonal, chunks=1):
            rows = part_of(c, chunks * pair)
            for at in groups:
                keys = kv_far[f, rows, :]
                s = dot(keys, bmat_far[f, :, at])
                d_p = dot(keys, bmat_far[f, :, cols_q + at.start:cols_q + at.stop])
                if diagonal:
                    s = jnp.where(seen_far[:, at], s, -1e30)
                p = jnp.exp(s - top[:, at]) * inv[:, at]
                p_b = p.astype(BF)
                ds_b = (p * (d_p - row_dot[:, at])).astype(BF)
                d_q = dot(kvt_far[f, 0:hd, rows], ds_b)
                d_a = dot(kvt_far[f, hd:hw, rows], p_b)
                adq[0:hd, at] = d_q if diagonal else adq[0:hd, at] + d_q
                adq[hd:hw, at] = d_a if diagonal else adq[hd:hw, at] + d_a

        add_chunk(chip, True)

        @pl.loop(0, chip // 2)
        def _(c):
            add_chunk(c, False, 2)

        @pl.when(chip % 2 == 1)
        def _():
            add_chunk(chip - 1, False)

        for head in range(4):
            at = slice(tok * head, tok * head + tok)
            place = pl.ds(pl.multiple_of(c_far * 2 * hw + hd * head, hd), hd)
            at_rv[place, :] = adq[hd:hw, at].astype(BF)
            dt_rv[place, :] = jnp.concatenate(turned(adq[0:hd, at] * scale, cos_t, -sin_t), axis=0).astype(BF)

    for t in near_targets:
        remote(at_all.at[:, pl.ds(0, tok)], at_rv.at[part_of(t, hw)], a_s.at[t], a_r.at[t], t).wait_recv()
    for item in wo_loads:
        item.wait()
    for t in range(q_rows // tok):
        a_nat[:, tok * t:tok * t + tok] = at_rv[tok * t:tok * t + tok, :].T
    for t in range(width // tile):
        cols = slice(tile * t, tile * t + tile)
        prod = jnp.zeros((tok, tile), F32)
        for s in range(n_chip):
            prod += dot(a_nat[:, pair * s:pair * s + pair], dyb[s, :, cols])
        out_v[:, cols] = (x_v[:, cols].astype(F32) + prod).astype(BF)
    store_out = local(out_v, out_hbm, out_sem.at[1])
    store_out.start()

    def kv_place(t):
        return pl.ds(pl.multiple_of(q_rows + (t % 2) * kv_w + (t // 2) * hd, hd), hd)

    for t in near_targets:
        remote(dq_all.at[:, pl.ds(0, tok)], dt_rv.at[part_of(t, hw)], q_s.at[t], q_r.at[t], t).wait_recv()
    for t in targets:
        remote(kv_mine.at[0], dt_rv.at[kv_place(t)], kv_s.at[t], kv_r.at[t], t).wait_recv()
    swap.wait_send()
    for t in range(n_rows // tok):
        d_nat[:, tok * t:tok * t + tok] = dt_rv[tok * t:tok * t + tok, :].T

    mean = stat[0, :, 0:1]
    inv_std = stat[1, :, 0:1]
    dh = dkvt
    for t in range(width // tile):
        cols = slice(tile * t, tile * t + tile)
        acc = jnp.zeros((tok, tile), F32)
        for s in range(n_rows // tile):
            acc += dot(d_nat[:, tile * s:tile * s + tile], wt[tile * s:tile * s + tile, cols])
        dh[:, cols] = acc
        gg_st[0, :, cols] = col_sum(acc * ((x_v[:, cols].astype(F32) - mean) * inv_std))
        gg_st[1, :, cols] = col_sum(acc)
    g_swap = remote(gg_st.at[1 - core], gg_mx, g_s.at[n_chip], g_r.at[n_chip], mate)
    g_swap.start()
    g_swap.wait_recv()
    gg_my[...] = jnp.where(core == 0, gg_st[0], gg_st[1]) + gg_mx[...]
    gg_rv[chip] = gg_my[...]
    g_sends = [remote(gg_my, gg_rv.at[chip], g_s.at[c], g_r.at[chip], 2 * c + core) for c in far]
    for item in g_sends + wk_sends[HELD:]:
        item.start()

    grad_hat = dh[...] * gain_one
    x_hat = (x_v[...].astype(F32) - mean) * inv_std
    mean_one = row_mean(grad_hat)
    mean_two = row_mean(grad_hat * x_hat)
    store_out.wait()
    out_v[...] = (dy_own[...].astype(F32) + inv_std * (grad_hat - mean_one - x_hat * mean_two)).astype(BF)
    store_gx = local(out_v, gx_hbm, out_sem.at[2])
    store_gx.start()

    for c in far:
        remote(gg_my, gg_rv.at[c], g_s.at[c], g_r.at[c], 2 * c + core).wait_recv()
    sums = gg_rv[0]
    for c in range(1, n_chip):
        sums = sums + gg_rv[c]
    gg_out[core] = sums
    g_swap_out = remote(gg_out.at[core], gg_out.at[core], g_s.at[n_chip + 1], g_r.at[n_chip + 1], mate)
    g_swap_out.start()
    remote(gg_out.at[core], gg_out.at[1 - core], g_s.at[n_chip + 1], g_r.at[n_chip + 1], mate).wait_recv()
    store_gg = local(gg_out, gg_hbm, out_sem.at[3])
    store_gg.start()

    finish_ring(h_ring)
    for item in pos_sends + [g_swap, g_swap_out] + [opposite_send(head) for head in range(4)]:
        item.wait_send()
    for t in near_targets:
        remote(at_all.at[:, pl.ds(0, tok)], at_rv.at[pl.ds(0, hw)], a_s.at[t], a_r.at[t], t).wait_send()
        remote(dq_all.at[:, pl.ds(0, tok)], dt_rv.at[pl.ds(0, hw)], q_s.at[t], q_r.at[t], t).wait_send()
    for item in kv_sends + w_sends + g_sends + wk_sends:
        item.wait_send()
    for t in targets:
        remote(dwt.at[pl.ds(0, hw), part_of(t, tok)], gw_hbm.at[part_of(t, hw)], w_s.at[t], w_r.at[t], t).wait_recv()
        remote(dwt.at[pl.ds(hw, hd), part_of(t, tok)], gw_hbm.at[kv_place(t)], wk_s.at[t], wk_r.at[t], t).wait_recv()
    for item in (w_own, wk_own, store_wo, store_gx, store_gg):
        item.wait()


def settle_kernel(q_rows, kv_w, out_i, gx_i, gw_i, gwo_i, gg_i, out_o, gx_o, gq_o, gk_o, gv_o, gwo_o, gain_o, bias_o, b_act, b_q, b_kv, b_o, b_gg, sem_in, sem_out, sem_gg):
    moves = []

    def split(src, mid, dst, pieces):
        rows = dst.shape[0] // pieces
        for i in range(pieces):
            part = pl.ds(rows * i, rows)
            moves.append((src.at[part], mid.at[part], dst.at[part]))

    split(out_i, b_act.at[0], out_o, 2)
    split(gx_i, b_act.at[1], gx_o, 2)
    split(gwo_i, b_o, gwo_o, 4)
    split(gw_i.at[pl.ds(0, q_rows)], b_q, gq_o, 4)
    split(gw_i.at[pl.ds(q_rows, kv_w)], b_kv.at[0], gk_o, 1)
    split(gw_i.at[pl.ds(q_rows + kv_w, kv_w)], b_kv.at[1], gv_o, 1)
    loads = [pltpu.make_async_copy(src, mid, sem_in.at[i]) for i, (src, mid, _) in enumerate(moves)]
    stores = [pltpu.make_async_copy(mid, dst, sem_out.at[i]) for i, (_, mid, dst) in enumerate(moves)]
    load_gg = pltpu.make_async_copy(gg_i, b_gg, sem_gg)
    load_gg.start()
    for item in loads:
        item.start()
    for load, store in zip(loads, stores):
        load.wait()
        store.start()
    load_gg.wait()
    gain_o[...] = b_gg[0, 0]
    bias_o[...] = b_gg[1, 0]
    for item in stores:
        item.wait()


def solution(mesh):
    n_dev = mesh.shape['cp']

    def device_step(x_act, d_out, positions, ln_gain, ln_bias, w_query, w_key, w_value, w_out):
        tok, width = x_act.shape[1], x_act.shape[2]
        q_heads, hd = w_query.shape[1], w_query.shape[2]
        kv_heads = w_key.shape[1]
        q_w, kv_w = q_heads * hd, kv_heads * hd
        n_rows = q_w + 2 * kv_w
        seq = n_dev * tok
        hw = 2 * hd

        def flat_weight(w):
            return jnp.transpose(w, (1, 2, 0)).reshape(-1, width)

        hbm = pl.BlockSpec(memory_space=pltpu.HBM)
        vmem = pl.BlockSpec(memory_space=pltpu.VMEM)
        dma = pltpu.SemaphoreType.DMA
        n_chip = n_dev // 2
        n_far = n_chip - 1 - 2 * NEAR
        pair = 2 * tok
        scratch = [
            pltpu.VMEM((n_chip, pair, width), BF),
            pltpu.VMEM((n_chip, pair, width), BF),
            pltpu.VMEM((n_rows, width), BF),
            pltpu.VMEM((2 * hw, width), BF),
            pltpu.VMEM((hw, width), BF),
            pltpu.VMEM((n_far * hw, width), BF),
            pltpu.VMEM((n_dev, 1, tok), jnp.int32),
            pltpu.VMEM((n_chip, hd // 2, pair), F32),
            pltpu.VMEM((n_chip, hd, 2 * pair), BF),
            pltpu.VMEM((hw, seq), BF),
            pltpu.VMEM((seq, hw), BF),
            pltpu.VMEM((n_far, hw, seq), BF),
            pltpu.VMEM((n_far, seq, hw), BF),
            pltpu.VMEM((n_far, hw, 4 * pair), BF),
            pltpu.VMEM((n_far, 3, 1, 2 * pair), F32),
            pltpu.VMEM((hw, 4 * pair), BF),
            pltpu.VMEM((4, hd, tok), BF),
            pltpu.VMEM((seq, 2 * pair), F32),
            pltpu.VMEM((seq, 2 * pair), F32),
            pltpu.VMEM((n_chip, 1, 2 * pair), F32),
            pltpu.VMEM((hw, 2 * pair), F32),
            pltpu.VMEM((hw, seq), F32),
            pltpu.VMEM((hd, seq), F32),
            pltpu.VMEM((n_dev, hd, tok), BF),
            pltpu.VMEM((hd, seq), BF),
            pltpu.VMEM((hw, width), F32),
            pltpu.VMEM((hw + hd, width), F32),
            pltpu.VMEM((hw, seq), BF),
            pltpu.VMEM((hw, seq), BF),
            pltpu.VMEM((q_w, tok), BF),
            pltpu.VMEM((n_rows, tok), BF),
            pltpu.VMEM((tok, q_w), BF),
            pltpu.VMEM((tok, n_rows), BF),
            pltpu.VMEM((tok, width), BF),
            pltpu.VMEM((tok, width), BF),
            pltpu.VMEM((2, 1, width), F32),
            pltpu.VMEM((2, tok, 128), F32),
            pltpu.VMEM((tok, width), BF),
            pltpu.VMEM((2, 1, width), F32),
            pltpu.VMEM((1, width), F32),
            pltpu.VMEM((1, width), F32),
            pltpu.VMEM((n_chip, 1, width), F32),
            pltpu.VMEM((2, 1, width), F32),
            dma((10,)), dma((4 * n_far,)), dma((n_chip,)), dma((3,)), dma((4,)), dma((2,)),
        ] + [dma((9 * PARTS,)), dma((7 * PARTS,)), dma((8 * PARTS,)), dma((8 * PARTS,))] * 2 + [dma((4,))] * 2 + [dma((n_dev,))] * 6 + [dma] * 2 + [dma((n_dev,))] * 8
        out, gx, gw, gwo, gg = pl.pallas_call(
            functools.partial(block_kernel, n_dev, hd, kv_w, NEAR, PARTS),
            out_shape=(
                jax.ShapeDtypeStruct((tok, width), BF),
                jax.ShapeDtypeStruct((tok, width), BF),
                jax.ShapeDtypeStruct((n_rows, tok), F32),
                jax.ShapeDtypeStruct((hw, width), F32),
                jax.ShapeDtypeStruct((2, 1, width), F32),
            ),
            in_specs=[hbm] * 9,
            out_specs=(hbm,) * 5,
            scratch_shapes=scratch,
            compiler_params=pltpu.CompilerParams(collective_id=0, has_side_effects=True, vmem_limit_bytes=67043328),
            name='attn_block',
        )(
            x_act.reshape(tok, width), d_out.reshape(tok, width), positions.reshape(1, tok),
            ln_gain.reshape(1, width), ln_bias.reshape(1, width),
            flat_weight(w_query), flat_weight(w_key), flat_weight(w_value), w_out,
        )

        out, gx, gq, gk, gv, gwo, gain, bias = pl.pallas_call(
            functools.partial(settle_kernel, q_w, kv_w),
            out_shape=(
                jax.ShapeDtypeStruct((tok, width), BF),
                jax.ShapeDtypeStruct((tok, width), BF),
                jax.ShapeDtypeStruct((q_w, tok), F32),
                jax.ShapeDtypeStruct((kv_w, tok), F32),
                jax.ShapeDtypeStruct((kv_w, tok), F32),
                jax.ShapeDtypeStruct((hw, width), F32),
                jax.ShapeDtypeStruct((width,), F32),
                jax.ShapeDtypeStruct((width,), F32),
            ),
            in_specs=[hbm] * 5,
            out_specs=(hbm,) * 6 + (vmem,) * 2,
            scratch_shapes=[
                pltpu.VMEM((2, tok, width), BF),
                pltpu.VMEM((q_w, tok), F32),
                pltpu.VMEM((2, kv_w, tok), F32),
                pltpu.VMEM((hw, width), F32),
                pltpu.VMEM((2, 1, width), F32),
                dma((14,)), dma((14,)), dma,
            ],
            name='settle',
        )(out, gx, gw, gwo, gg)

        def rows_out(block, heads):
            return jnp.transpose(block.reshape(heads, hd, tok), (2, 0, 1))

        return (
            out.reshape(1, tok, width), gx.reshape(1, tok, width),
            rows_out(gq, q_heads), rows_out(gk, kv_heads), rows_out(gv, kv_heads),
            gwo, gain, bias,
        )

    return jax.shard_map(device_step, mesh=mesh, in_specs=(P('dp', 'cp', None), P('dp', 'cp', None), P('dp', 'cp'), P(None), P(None), P(None, None, None), P(None, None, None), P(None, None, None), P(None, None)), out_specs=(P('dp', 'cp', None), P('dp', 'cp', None), P(('dp', 'cp'), None, None), P(('dp', 'cp'), None, None), P(('dp', 'cp'), None, None), P(('dp', 'cp'), None), P('dp'), P('dp')), check_vma=False)
```

```python
import functools
import math

import jax
import jax.numpy as jnp
from jax import lax
from jax.experimental import pallas as pl
from jax.experimental.pallas import tpu as pltpu
from jax.sharding import PartitionSpec as P

EPS = 1e-5
ROPE_BASE = 10000.0
MESH = pl.DeviceIdType.MESH
BF = jnp.bfloat16
F32 = jnp.float32
NEAR = 1
PARTS = 4
FIRST = 0
HELD = 4


def dot(lhs, rhs):
    return jnp.dot(lhs, rhs, preferred_element_type=F32)


def col_sum(val):
    return jnp.sum(val, axis=0, keepdims=True)


def col_max(val):
    return jnp.max(val, axis=0, keepdims=True)


def row_mean(val):
    return jnp.mean(val, axis=-1, keepdims=True)


def dot_t(lhs, rhs):
    return lax.dot_general(lhs, rhs, (((1,), (1,)), ((), ())), preferred_element_type=F32)


def block_kernel(
    n_dev, hd, kv_w, near, parts,
    x_hbm, dy_hbm, pos_hbm, gain_hbm, bias_hbm, wq_hbm, wk_hbm, wv_hbm, wo_hbm,
    out_hbm, gx_hbm, gw_hbm, gwo_hbm, gg_hbm,
    hb, dyb, wt, wi, woi, w_far, pos_all, trig,
    qt, kvt, kv, kvt_far, kv_far, bmat_far, stat_far, bmat, da_rv, sbuf, dpbuf, mbuf, adq, dkvt, kv_rv, kv_mine, kv_row,
    dwo, dwt, at_all, dq_all, at_rv, dt_rv, a_nat, d_nat, x_v, dy_own, gb_v, stat, out_v, gg_st, gg_mx, gg_my, gg_rv, gg_out,
    in_sem, far_sem, wo_sem, w_sem, out_sem, loc_sem,
    hzs, hzr, hds, hdr, yzs, yzr, yds, ydr,
    d_s, d_r, pos_s, pos_r, a_s, a_r, q_s, q_r, x_s, x_r, kv_s, kv_r, w_s, w_r, wk_s, wk_r, g_s, g_r,
):
    tok, width = x_v.shape
    n_chip = n_dev // 2
    pair = 2 * tok
    me = lax.axis_index('cp')
    chip = me // 2
    core = me % 2
    right = 2 * ((chip + 1) % n_chip) + core
    left = 2 * ((chip + n_chip - 1) % n_chip) + core
    mate = 2 * chip + 1 - core
    q_rows = wq_hbm.shape[0]
    n_rows = q_rows + 2 * kv_w
    hw = 2 * hd
    quarter = hd // 4
    tile = 256
    scale = hd ** -0.5
    cols_q = 2 * pair
    n_far = n_chip - 1 - 2 * near

    def remote(src, dst, send, recv, target):
        return pltpu.make_async_remote_copy(src_ref=src, dst_ref=dst, send_sem=send, recv_sem=recv, device_id={'cp': target}, device_id_type=MESH)

    def local(src, dst, sem):
        return pltpu.make_async_copy(src, dst, sem)

    def part_of(i, size):
        return pl.ds(pl.multiple_of(i * size, size), size)

    def once(cond):
        return pl.loop(0, jnp.where(cond, 1, 0))

    def ring_steps(k):
        step = (k + 1) // 2
        return step, k % 2

    def ring_origin(k):
        step, ahead = ring_steps(k)
        return jnp.where(ahead == 1, chip + n_chip - step, chip + step) % n_chip

    own = (chip, part_of(core, tok))
    first_loads = [
        local(x_hbm, x_v, in_sem.at[0]),
        local(gain_hbm, gb_v.at[0], in_sem.at[1]),
        local(bias_hbm, gb_v.at[1], in_sem.at[2]),
        local(pos_hbm, pos_all.at[me], in_sem.at[3]),
    ]
    for item in first_loads:
        item.start()
    barrier = pltpu.get_barrier_semaphore()
    for step in range(1, n_dev):
        pl.semaphore_signal(barrier, inc=1, device_id={'cp': (me + step) % n_dev}, device_id_type=MESH)
    own_rows = part_of(me, hw)
    kv_rows = part_of(chip, hd)
    loads = [
        local(wq_hbm.at[own_rows], wi.at[pl.ds(0, hw)], in_sem.at[4]),
        local(wk_hbm.at[kv_rows], wi.at[pl.ds(hw, hd)], in_sem.at[5]),
        local(wv_hbm.at[kv_rows], wi.at[pl.ds(hw + hd, hd)], in_sem.at[6]),
        local(wo_hbm.at[own_rows], woi, in_sem.at[7]),
        local(dy_hbm, dyb.at[own], in_sem.at[8]),
        local(dy_hbm, dy_own, in_sem.at[9]),
    ]
    far_loads = []
    for f in range(n_far):
        far_rows = part_of(ring_origin(2 * near + 1 + f), hd)
        loads.append(local(wk_hbm.at[far_rows], w_far.at[pl.ds(hw * f, hd)], far_sem.at[2 * f]))
        loads.append(local(wv_hbm.at[far_rows], w_far.at[pl.ds(hw * f + hd, hd)], far_sem.at[2 * f + 1]))
        far_wo = part_of(ring_origin(2 * near + 1 + f), 2 * hw)
        far_loads.append(local(wo_hbm.at[far_wo], wt.at[pl.ds(2 * hw * f, 2 * hw)], far_sem.at[2 * n_far + f]))
        far_loads.append(local(wq_hbm.at[far_wo], wt.at[pl.ds(2 * hw * (n_far + f), 2 * hw)], far_sem.at[3 * n_far + f]))
    for item in loads + far_loads:
        item.start()

    for item in first_loads:
        item.wait()
    gain_one = 1.0 + gb_v[0]
    block = 16

    @pl.loop(0, tok // block)
    def _(i):
        rows = part_of(i, block)
        x_f = x_v[rows, :].astype(F32)
        mean = row_mean(x_f)
        centered = x_f - mean
        inv_std = lax.rsqrt(row_mean(centered * centered) + EPS)
        hb[chip, part_of(core * (tok // block) + i, block), :] = (centered * inv_std * gain_one + gb_v[1]).astype(BF)
        stat[0, rows, :] = jnp.broadcast_to(mean, (block, 128))
        stat[1, rows, :] = jnp.broadcast_to(inv_std, (block, 128))

    pl.semaphore_wait(barrier, n_dev - 1)

    def chunk(buf, origin, parity, part):
        return buf.at[origin, part_of(parts * parity + part, tok // parts)]

    turns = 2 * parts

    def own_sends(buf, zs, zr, ds, dr):
        copies = []
        for part in range(parts):
            piece = chunk(buf, chip, core, part)
            copies.append(remote(piece, piece, zs.at[2 * part], zr.at[2 * part], right))
            copies.append(remote(piece, piece, zs.at[2 * part + 1], zr.at[2 * part + 1], left))
            copies.append(remote(piece, piece, ds.at[7 * parts + part], dr.at[7 * parts + part], mate))
        return copies

    def event_place(event):
        step = event // turns + 1
        turn = event % turns
        direction = turn % 2
        part = jnp.where(step < 4, turn // 2, turn // 2 + direction * (parts // 2))
        origin = jnp.where(direction == 0, chip + n_chip - step, chip + step) % n_chip
        return step, direction, part, origin

    def last_event(part, direction):
        return 6 * parts + 2 * (part - direction * (parts // 2)) + direction

    def ring_event(ring, event):
        buf, zs, zr, ds, dr = ring
        step, direction, part, origin = event_place(event)
        piece = chunk(buf, origin, core, part)
        remote(piece, piece, zs.at[0], zr.at[event], right).wait_recv()
        onward = jnp.where(step < 3, event + turns, last_event(part, direction))

        @pl.when((step < 3) | ((step == 3) & ((part >= parts // 2) == (direction == 1))))
        def _():
            remote(piece, piece, zs.at[event + turns], zr.at[onward], jnp.where(direction == 0, right, left)).start()

        remote(piece, piece, ds.at[event], dr.at[event], mate).start()

    def ring_service(ring, event):
        @pl.when(event < 7 * parts)
        def _():
            ring_event(ring, event)

    def ring_mate(ring, k, origin):
        buf, zs, zr, ds, dr = ring
        step, ahead = ring_steps(k)
        for part in range(parts):
            event = jnp.where(k == 0, 7 * parts + part, jnp.where(step < 4, turns * (step - 1) + 2 * part + 1 - ahead, last_event(part, part // (parts // 2))))
            piece = chunk(buf, origin, 1 - core, part)
            remote(piece, piece, ds.at[0], dr.at[event], mate).wait_recv()

    def finish_ring(ring):
        buf, zs, zr, ds, dr = ring
        for item in own_sends(*ring):
            item.wait_send()

        @pl.loop(0, 7 * parts)
        def _(event):
            step, direction, part, origin = event_place(event)
            piece = chunk(buf, origin, core, part)

            @pl.when((step < 3) | ((step == 3) & ((part >= parts // 2) == (direction == 1))))
            def _():
                remote(piece, piece, zs.at[event + turns], zr.at[event], right).wait_send()

            remote(piece, piece, ds.at[event], dr.at[event], mate).wait_send()

    h_ring = (hb, hzs, hzr, hds, hdr)
    y_ring = (dyb, yzs, yzr, yds, ydr)
    for item in own_sends(*h_ring):
        item.start()
    pos_sends = [remote(pos_all.at[me], pos_all.at[me], pos_s.at[step], pos_r.at[me], (me + step) % n_dev) for step in range(1, n_dev)]
    for item in pos_sends:
        item.start()
    weight_loads = [
        local(wq_hbm, wt.at[pl.ds(0, q_rows)], w_sem.at[0]),
        local(wk_hbm, wt.at[pl.ds(q_rows, kv_w)], w_sem.at[1]),
        local(wv_hbm, wt.at[pl.ds(q_rows + kv_w, kv_w)], w_sem.at[2]),
    ]
    dkvt[...] = jnp.zeros_like(dkvt)
    bmat[...] = jnp.zeros_like(bmat)
    bmat_far[...] = jnp.zeros_like(bmat_far)
    for f in range(n_far):
        stat_far[f, 0] = jnp.full((1, cols_q), -3e38, F32)
        stat_far[f, 1] = jnp.zeros((1, cols_q), F32)
        stat_far[f, 2] = jnp.zeros((1, cols_q), F32)

    freq = jnp.exp(lax.broadcasted_iota(jnp.int32, (quarter, tok), 0).astype(F32) * (-2.0 * math.log(ROPE_BASE) / (hd // 2)))

    def make_trig(b):
        for t in range(2):
            slot = 2 * b + t

            @pl.when(slot != me)
            def _():
                remote(pos_all.at[slot], pos_all.at[slot], pos_s.at[0], pos_r.at[slot], me).wait_recv()

            angle = pos_all[slot].astype(F32) * freq
            trig[b, 0:quarter, tok * t:tok * t + tok] = jnp.cos(angle)
            trig[b, quarter:2 * quarter, tok * t:tok * t + tok] = jnp.sin(angle)

    def turned(val, cos_t, sin_t):
        u = val[0:quarter]
        w = val[quarter:2 * quarter]
        return [u * cos_t - w * sin_t, w * cos_t + u * sin_t, val[2 * quarter:hd]]

    def eighth(val):
        return val.astype(BF) * jnp.asarray(scale, BF)

    def keys_values(val, cos_t, sin_t):
        return jnp.concatenate(turned(val[0:hd], cos_t, sin_t) + [val[hd:hw]], axis=0).astype(BF)

    lane = lax.broadcasted_iota(jnp.int32, (pair, cols_q), 1)
    row = lax.broadcasted_iota(jnp.int32, (pair, cols_q), 0)
    seen_far = row <= core * tok + lane % tok

    opposite = ring_origin(n_chip - 1)

    def opposite_send(head):
        block = bmat_far.at[n_far - 1, pl.ds(hd, hd), pl.ds(cols_q + tok * head, tok)]
        return remote(block, da_rv.at[2 * core + head % 2], d_s.at[head], d_r.at[2 * core + head % 2], 2 * opposite + head // 2)

    @pl.loop(0, n_chip)
    def _(k):
        for turn in range(parts):
            ring_service(h_ring, parts * k + turn)

        @once(k == 5)
        def _(_):
            for item in [opposite_send(head) for head in range(4)] + own_sends(*y_ring):
                item.start()

        @once(k == 0)
        def _(_):
            for item in loads:
                item.wait()

        b = ring_origin(k)
        ring_mate(h_ring, k, b)
        make_trig(b)

        @once(k == 0)
        def _(_):
            for item in far_loads:
                item.wait()
            cos_t = trig[chip, 0:quarter, part_of(core, tok)]
            sin_t = trig[chip, quarter:2 * quarter, part_of(core, tok)]

            @pl.loop(0, n_far)
            def _(f):
                da_t = dot_t(wt[part_of(f, 2 * hw), :], dy_own[...]).astype(BF)
                q_t = dot_t(wt[part_of(n_far + f, 2 * hw), :], hb[chip, part_of(core, tok), :])
                for head in range(4):
                    part = slice(hd * head, hd * head + hd)
                    at = tok * head
                    bmat_far[f, 0:hd, at:at + tok] = eighth(jnp.concatenate(turned(q_t[part], cos_t, sin_t), axis=0))
                    bmat_far[f, hd:hw, cols_q + at:cols_q + at + tok] = da_t[part]

            for item in weight_loads:
                item.start()

        place = part_of(b, pair)
        cos_t = trig[b, 0:quarter, :]
        sin_t = trig[b, quarter:2 * quarter, :]
        flat = dot_t(wi[...], hb[b])
        for head in range(2):
            q_rot = eighth(jnp.concatenate(turned(flat[hd * head:hd * head + hd], cos_t, sin_t), axis=0))
            for t in range(2):
                lane = pair * t + tok * head
                qt[b, :, lane:lane + tok] = q_rot[:, tok * t:tok * t + tok]
        kv_rot = keys_values(flat[hw:2 * hw], cos_t, sin_t)
        kvt[:, place] = kv_rot
        kv[place, :] = kv_rot.T

        @pl.when(b <= chip)
        def _():
            flat_far = dot_t(w_far[...], hb[b])
            for f in range(n_far):
                far_rot = keys_values(flat_far[hw * f:hw * f + hw], cos_t, sin_t)
                kvt_far[f, :, place] = far_rot
                kv_far[f, place, :] = far_rot.T

            @pl.loop(0, n_far)
            def _(f):
                both = dot(kv_far[f, place, :], bmat_far[f])
                s = jnp.where(seen_far | (k > 0), both[:, 0:cols_q], -1e30)
                old = stat_far[f, 0]
                new = jnp.maximum(old, col_max(s))
                p = jnp.exp(s - new)
                keep = jnp.exp(old - new)
                stat_far[f, 0] = new
                stat_far[f, 1] = stat_far[f, 1] * keep + col_sum(p)
                stat_far[f, 2] = stat_far[f, 2] * keep + col_sum(p * both[:, cols_q:2 * cols_q])

    groups = [slice(tile * g, tile * g + tile) for g in range(cols_q // tile)]

    def first_part(b, seen):
        def both_of(rows):
            both = dot(kv[rows, :], bmat[...])
            return both[:, 0:cols_q], both[:, cols_q:2 * cols_q]

        rows = part_of(b, pair)
        s, d_p = both_of(rows)
        s = jnp.where(seen, s, -1e30)
        top = col_max(s)
        p = jnp.exp(s - top)
        sbuf[rows, :] = p
        dpbuf[rows, :] = d_p
        mbuf[b] = top

        def step(c, state, chunks=1):
            old, total, weighted = state
            rows = part_of(c, chunks * pair)
            s, d_p = both_of(rows)
            new = jnp.maximum(old, col_max(s))
            p = jnp.exp(s - new)
            sbuf[rows, :] = p
            dpbuf[rows, :] = d_p
            for i in range(chunks):
                mbuf[chunks * c + i] = new
            keep = jnp.exp(old - new)
            return new, total * keep + col_sum(p), weighted * keep + col_sum(p * d_p)

        state = (top, col_sum(p), col_sum(p * d_p))
        state = lax.fori_loop(0, b // 2, functools.partial(step, chunks=2), state)
        top, total, weighted = lax.fori_loop(2 * (b // 2), b, step, state)
        inv = 1.0 / total
        return top, inv, weighted * inv

    def second_part(b, stats):
        top, inv, row_dot = stats
        adq[...] = jnp.zeros_like(adq)

        def step(c, carry):
            rows = part_of(c, pair)
            factor = jnp.exp(mbuf[c] - top) * inv
            d_k = d_v = None
            for at in groups:
                p = sbuf[rows, at] * factor[:, at]
                p_b = p.astype(BF)
                ds_b = (p * (dpbuf[rows, at] - row_dot[:, at])).astype(BF)
                adq[0:hd, at] += dot(kvt[0:hd, rows], ds_b)
                adq[hd:hw, at] += dot(kvt[hd:hw, rows], p_b)
                more_k = dot_t(bmat[0:hd, at], ds_b)
                more_v = dot_t(bmat[hd:hw, cols_q + at.start:cols_q + at.stop], p_b)
                d_k = more_k if d_k is None else d_k + more_k
                d_v = more_v if d_v is None else d_v + more_v
            dkvt[0:hd, rows] += d_k
            dkvt[hd:hw, rows] += d_v
            return carry

        lax.fori_loop(0, b + 1, step, 0)


    def send_rows(slot):
        cols = part_of(slot, tok)
        return [
            remote(dq_all.at[:, cols], dt_rv.at[own_rows], q_s.at[slot], q_r.at[me], slot),
            remote(at_all.at[:, cols], at_rv.at[own_rows], a_s.at[slot], a_r.at[me], slot),
        ]

    last = 6 * parts

    def serve(event):
        @pl.when(event < last)
        def _():
            ring_event(y_ring, event)

    @pl.loop(0, n_chip)
    def _(j):
        k = j - 1

        @pl.when(k == 0)
        def _():
            for turn in range(2):
                ring_event(y_ring, k + turn)

        @pl.when((k % 2 == 1) & (k > 0))
        def _():
            for turn in range(2, parts):
                serve(parts * k + turn)

        b = jnp.where(j == 0, opposite, ring_origin(jnp.maximum(k, 0)))

        @once(k == 1)
        def _(_):
            for item in weight_loads:
                item.wait()

        @pl.loop(0, jnp.where(j == n_chip - 1, 2 + 4 * near, 0))
        def _(early):
            slot = 2 * ring_origin(early // 2) + early % 2

            @pl.when(slot != me)
            def _():
                for item in send_rows(slot):
                    item.start()

        bmat[0:hd, 0:cols_q] = qt[b]

        @once(j == 0)
        def _(_):
            for i in range(4):
                remote(da_rv.at[i], da_rv.at[i], d_s.at[0], d_r.at[i], mate).wait_recv()
                bmat[hd:hw, cols_q + tok * i:cols_q + tok * i + tok] = da_rv[i]

        @once(j > 0)
        def _(_):
            ring_mate(y_ring, k, b)
            da_t = dot_t(woi[...], dyb[b]).astype(BF)
            for t in range(2):
                for head in range(2):
                    at = cols_q + pair * t + tok * head
                    bmat[hd:hw, at:at + tok] = da_t[hd * head:hd * head + hd, tok * t:tok * t + tok]

        stats = first_part(b, row <= (lane // pair) * tok + lane % tok)
        for turn in range(2):
            serve(jnp.where(k < 0, last, parts * k + 2 + 2 * (k % 2)) + turn)
        second_part(b, stats)
        for t in range(2):
            slot = 2 * b + t
            lanes = [slice(pair * t + tok * head, pair * t + tok * head + tok) for head in range(2)]
            a_t = jnp.concatenate([adq[hd:hw, at] for at in lanes], axis=0).astype(BF)
            cos_t = trig[b, 0:quarter, tok * t:tok * t + tok]
            sin_t = trig[b, quarter:2 * quarter, tok * t:tok * t + tok]
            dq_t = jnp.concatenate([piece for at in lanes for piece in turned(adq[0:hd, at] * scale, cos_t, -sin_t)], axis=0).astype(BF)
            at_all[:, part_of(slot, tok)] = a_t
            dq_all[:, part_of(slot, tok)] = dq_t

            @pl.when(slot == me)
            def _():
                at_rv[own_rows, :] = a_t
                dt_rv[own_rows, :] = dq_t

        @pl.when((k % 2 == 0) & (k >= 0))
        def _():
            for turn in range(2):
                serve(parts * j + turn)

    far = [ring_origin(k) for k in range(n_chip - 1, 0, -1)]
    targets = [2 * c + p for c in far for p in range(2)] + [mate]
    near_targets = targets[-1 - 4 * near:]
    swap = remote(dkvt.at[part_of(1 - core, hd)], kv_rv, x_s, x_r, mate)
    swap.start()
    w_sends = [remote(dwt.at[pl.ds(0, hw), part_of(t, tok)], gw_hbm.at[own_rows], w_s.at[t], w_r.at[me], t) for t in targets]

    def columns(rows_all, buf, cols):
        acc = jnp.zeros((rows_all.shape[0], tile), F32)
        for s in range(n_chip):
            acc += dot(rows_all[:, pair * s:pair * s + pair], buf[s, :, cols])
        return acc

    def q_columns(i):
        cols = part_of(far[i] if i < n_chip - 1 else chip, pair)
        dwt[0:hw, cols] = columns(dq_all, hb, cols)
        for item in w_sends[max(2 * i - 2, 0):2 * i]:
            item.start()

    for i in range(FIRST + 1):
        q_columns(i)

    swap.wait_recv()
    mine = part_of(core, hd)
    g_rows = pl.ds(pl.multiple_of(q_rows + core * kv_w + chip * hd, hd), hd)
    for t in range(n_chip):
        cols = slice(pair * t, pair * t + pair)
        g = dkvt[mine, cols] + kv_rv[:, cols]
        cos_t = jnp.where(core == 0, trig[t, 0:quarter, :], 1.0)
        sin_t = jnp.where(core == 0, trig[t, quarter:2 * quarter, :], 0.0)
        g_b = jnp.concatenate(turned(g, cos_t, -sin_t), axis=0).astype(BF)
        kv_mine[2 * t] = g_b[:, 0:tok]
        kv_mine[2 * t + 1] = g_b[:, tok:pair]
        kv_row[:, cols] = g_b
    dt_rv[g_rows, :] = kv_mine[me]
    kv_sends = [remote(kv_mine.at[t], dt_rv.at[g_rows], kv_s.at[t], kv_r.at[me], t) for t in targets]
    for item in kv_sends:
        item.start()
    for i in range(FIRST + 1, n_chip):
        q_columns(i)
    w_sends[-1].start()
    w_own = local(dwt.at[pl.ds(0, hw), part_of(me, tok)], gw_hbm.at[own_rows], loc_sem.at[0])
    w_own.start()
    for t in range(width // tile):
        cols = slice(tile * t, tile * t + tile)
        dwt[hw:hw + hd, cols] = columns(kv_row, hb, cols)
    wk_own = local(dwt.at[pl.ds(hw, hd), part_of(me, tok)], gw_hbm.at[g_rows], loc_sem.at[1])
    wk_own.start()
    wk_sends = [remote(dwt.at[pl.ds(hw, hd), part_of(t, tok)], gw_hbm.at[g_rows], wk_s.at[t], wk_r.at[me], t) for t in targets]
    for item in wk_sends[0:HELD]:
        item.start()

    @pl.loop(last, 7 * parts)
    def _(event):
        ring_event(y_ring, event)

    ring_mate(y_ring, n_chip - 1, opposite)
    for t in range(width // tile):
        cols = slice(tile * t, tile * t + tile)
        dwo[:, cols] = columns(at_all, dyb, cols)
    store_wo = local(dwo, gwo_hbm, out_sem.at[0])
    store_wo.start()
    finish_ring(y_ring)
    wo_loads = [local(wo_hbm.at[pl.ds(pair * t, pair)], dyb.at[t], wo_sem.at[t]) for t in range(n_chip)]
    for item in wo_loads:
        item.start()

    @pl.loop(0, n_far)
    def _(f):
        c_far = ring_origin(2 * near + 1 + f)
        cos_t = trig[chip, 0:quarter, part_of(core, tok)]
        sin_t = trig[chip, quarter:2 * quarter, part_of(core, tok)]
        top = stat_far[f, 0]
        inv = 1.0 / stat_far[f, 1]
        row_dot = stat_far[f, 2] * inv

        def add_chunk(c, diagonal, chunks=1):
            rows = part_of(c, chunks * pair)
            for at in groups:
                keys = kv_far[f, rows, :]
                s = dot(keys, bmat_far[f, :, at])
                d_p = dot(keys, bmat_far[f, :, cols_q + at.start:cols_q + at.stop])
                if diagonal:
                    s = jnp.where(seen_far[:, at], s, -1e30)
                p = jnp.exp(s - top[:, at]) * inv[:, at]
                p_b = p.astype(BF)
                ds_b = (p * (d_p - row_dot[:, at])).astype(BF)
                d_q = dot(kvt_far[f, 0:hd, rows], ds_b)
                d_a = dot(kvt_far[f, hd:hw, rows], p_b)
                adq[0:hd, at] = d_q if diagonal else adq[0:hd, at] + d_q
                adq[hd:hw, at] = d_a if diagonal else adq[hd:hw, at] + d_a

        add_chunk(chip, True)

        @pl.loop(0, chip // 2)
        def _(c):
            add_chunk(c, False, 2)

        @pl.when(chip % 2 == 1)
        def _():
            add_chunk(chip - 1, False)

        for head in range(4):
            at = slice(tok * head, tok * head + tok)
            place = pl.ds(pl.multiple_of(c_far * 2 * hw + hd * head, hd), hd)
            at_rv[place, :] = adq[hd:hw, at].astype(BF)
            dt_rv[place, :] = jnp.concatenate(turned(adq[0:hd, at] * scale, cos_t, -sin_t), axis=0).astype(BF)

    for t in near_targets:
        remote(at_all.at[:, pl.ds(0, tok)], at_rv.at[part_of(t, hw)], a_s.at[t], a_r.at[t], t).wait_recv()
    for item in wo_loads:
        item.wait()
    for t in range(q_rows // tok):
        a_nat[:, tok * t:tok * t + tok] = at_rv[tok * t:tok * t + tok, :].T
    for t in range(width // tile):
        cols = slice(tile * t, tile * t + tile)
        prod = jnp.zeros((tok, tile), F32)
        for s in range(n_chip):
            prod += dot(a_nat[:, pair * s:pair * s + pair], dyb[s, :, cols])
        out_v[:, cols] = (x_v[:, cols].astype(F32) + prod).astype(BF)
    store_out = local(out_v, out_hbm, out_sem.at[1])
    store_out.start()

    def kv_place(t):
        return pl.ds(pl.multiple_of(q_rows + (t % 2) * kv_w + (t // 2) * hd, hd), hd)

    for t in near_targets:
        remote(dq_all.at[:, pl.ds(0, tok)], dt_rv.at[part_of(t, hw)], q_s.at[t], q_r.at[t], t).wait_recv()
    for t in targets:
        remote(kv_mine.at[0], dt_rv.at[kv_place(t)], kv_s.at[t], kv_r.at[t], t).wait_recv()
    swap.wait_send()
    for t in range(n_rows // tok):
        d_nat[:, tok * t:tok * t + tok] = dt_rv[tok * t:tok * t + tok, :].T

    mean = stat[0, :, 0:1]
    inv_std = stat[1, :, 0:1]
    dh = dkvt
    for t in range(width // tile):
        cols = slice(tile * t, tile * t + tile)
        acc = jnp.zeros((tok, tile), F32)
        for s in range(n_rows // tile):
            acc += dot(d_nat[:, tile * s:tile * s + tile], wt[tile * s:tile * s + tile, cols])
        dh[:, cols] = acc
        gg_st[0, :, cols] = col_sum(acc * ((x_v[:, cols].astype(F32) - mean) * inv_std))
        gg_st[1, :, cols] = col_sum(acc)
    g_swap = remote(gg_st.at[1 - core], gg_mx, g_s.at[n_chip], g_r.at[n_chip], mate)
    g_swap.start()
    g_swap.wait_recv()
    gg_my[...] = jnp.where(core == 0, gg_st[0], gg_st[1]) + gg_mx[...]
    gg_rv[chip] = gg_my[...]
    g_sends = [remote(gg_my, gg_rv.at[chip], g_s.at[c], g_r.at[chip], 2 * c + core) for c in far]
    for item in g_sends + wk_sends[HELD:]:
        item.start()

    grad_hat = dh[...] * gain_one
    x_hat = (x_v[...].astype(F32) - mean) * inv_std
    mean_one = row_mean(grad_hat)
    mean_two = row_mean(grad_hat * x_hat)
    store_out.wait()
    out_v[...] = (dy_own[...].astype(F32) + inv_std * (grad_hat - mean_one - x_hat * mean_two)).astype(BF)
    store_gx = local(out_v, gx_hbm, out_sem.at[2])
    store_gx.start()

    for c in far:
        remote(gg_my, gg_rv.at[c], g_s.at[c], g_r.at[c], 2 * c + core).wait_recv()
    sums = gg_rv[0]
    for c in range(1, n_chip):
        sums = sums + gg_rv[c]
    gg_out[core] = sums
    g_swap_out = remote(gg_out.at[core], gg_out.at[core], g_s.at[n_chip + 1], g_r.at[n_chip + 1], mate)
    g_swap_out.start()
    remote(gg_out.at[core], gg_out.at[1 - core], g_s.at[n_chip + 1], g_r.at[n_chip + 1], mate).wait_recv()
    store_gg = local(gg_out, gg_hbm, out_sem.at[3])
    store_gg.start()

    finish_ring(h_ring)
    for item in pos_sends + [g_swap, g_swap_out] + [opposite_send(head) for head in range(4)]:
        item.wait_send()
    for t in near_targets:
        remote(at_all.at[:, pl.ds(0, tok)], at_rv.at[pl.ds(0, hw)], a_s.at[t], a_r.at[t], t).wait_send()
        remote(dq_all.at[:, pl.ds(0, tok)], dt_rv.at[pl.ds(0, hw)], q_s.at[t], q_r.at[t], t).wait_send()
    for item in kv_sends + w_sends + g_sends + wk_sends:
        item.wait_send()
    for t in targets:
        remote(dwt.at[pl.ds(0, hw), part_of(t, tok)], gw_hbm.at[part_of(t, hw)], w_s.at[t], w_r.at[t], t).wait_recv()
        remote(dwt.at[pl.ds(hw, hd), part_of(t, tok)], gw_hbm.at[kv_place(t)], wk_s.at[t], wk_r.at[t], t).wait_recv()
    for item in (w_own, wk_own, store_wo, store_gx, store_gg):
        item.wait()


def settle_kernel(q_rows, kv_w, out_i, gx_i, gw_i, gwo_i, gg_i, out_o, gx_o, gq_o, gk_o, gv_o, gwo_o, gain_o, bias_o, b_out, b_gx, b_w, b_o, b_gg, sem_in, sem_out):
    pairs = [(gg_i, b_gg), (gw_i, b_w), (gwo_i, b_o), (out_i, b_out), (gx_i, b_gx)]
    loads = [pltpu.make_async_copy(src, dst, sem_in.at[i]) for i, (src, dst) in enumerate(pairs)]
    for item in loads:
        item.start()
    k_row, v_row = q_rows, q_rows + kv_w
    moves = [
        (1, b_w.at[pl.ds(0, q_rows)], gq_o), (1, b_w.at[pl.ds(k_row, kv_w)], gk_o), (1, b_w.at[pl.ds(v_row, kv_w)], gv_o),
        (2, b_o, gwo_o), (3, b_out, out_o), (4, b_gx, gx_o),
    ]
    stores = []
    waited = set()
    for i, (which, src, dst) in enumerate(moves):
        if which not in waited:
            loads[which].wait()
            waited.add(which)
        stores.append(pltpu.make_async_copy(src, dst, sem_out.at[i]))
        stores[i].start()
    loads[0].wait()
    gain_o[...] = b_gg[0, 0]
    bias_o[...] = b_gg[1, 0]
    for item in stores:
        item.wait()


def solution(mesh):
    n_dev = mesh.shape['cp']

    def device_step(x_act, d_out, positions, ln_gain, ln_bias, w_query, w_key, w_value, w_out):
        tok, width = x_act.shape[1], x_act.shape[2]
        q_heads, hd = w_query.shape[1], w_query.shape[2]
        kv_heads = w_key.shape[1]
        q_w, kv_w = q_heads * hd, kv_heads * hd
        n_rows = q_w + 2 * kv_w
        seq = n_dev * tok
        hw = 2 * hd

        def flat_weight(w):
            return jnp.transpose(w, (1, 2, 0)).reshape(-1, width)

        hbm = pl.BlockSpec(memory_space=pltpu.HBM)
        vmem = pl.BlockSpec(memory_space=pltpu.VMEM)
        dma = pltpu.SemaphoreType.DMA
        n_chip = n_dev // 2
        n_far = n_chip - 1 - 2 * NEAR
        pair = 2 * tok
        scratch = [
            pltpu.VMEM((n_chip, pair, width), BF),
            pltpu.VMEM((n_chip, pair, width), BF),
            pltpu.VMEM((n_rows, width), BF),
            pltpu.VMEM((2 * hw, width), BF),
            pltpu.VMEM((hw, width), BF),
            pltpu.VMEM((n_far * hw, width), BF),
            pltpu.VMEM((n_dev, 1, tok), jnp.int32),
            pltpu.VMEM((n_chip, hd // 2, pair), F32),
            pltpu.VMEM((n_chip, hd, 2 * pair), BF),
            pltpu.VMEM((hw, seq), BF),
            pltpu.VMEM((seq, hw), BF),
            pltpu.VMEM((n_far, hw, seq), BF),
            pltpu.VMEM((n_far, seq, hw), BF),
            pltpu.VMEM((n_far, hw, 4 * pair), BF),
            pltpu.VMEM((n_far, 3, 1, 2 * pair), F32),
            pltpu.VMEM((hw, 4 * pair), BF),
            pltpu.VMEM((4, hd, tok), BF),
            pltpu.VMEM((seq, 2 * pair), F32),
            pltpu.VMEM((seq, 2 * pair), F32),
            pltpu.VMEM((n_chip, 1, 2 * pair), F32),
            pltpu.VMEM((hw, 2 * pair), F32),
            pltpu.VMEM((hw, seq), F32),
            pltpu.VMEM((hd, seq), F32),
            pltpu.VMEM((n_dev, hd, tok), BF),
            pltpu.VMEM((hd, seq), BF),
            pltpu.VMEM((hw, width), F32),
            pltpu.VMEM((hw + hd, width), F32),
            pltpu.VMEM((hw, seq), BF),
            pltpu.VMEM((hw, seq), BF),
            pltpu.VMEM((q_w, tok), BF),
            pltpu.VMEM((n_rows, tok), BF),
            pltpu.VMEM((tok, q_w), BF),
            pltpu.VMEM((tok, n_rows), BF),
            pltpu.VMEM((tok, width), BF),
            pltpu.VMEM((tok, width), BF),
            pltpu.VMEM((2, 1, width), F32),
            pltpu.VMEM((2, tok, 128), F32),
            pltpu.VMEM((tok, width), BF),
            pltpu.VMEM((2, 1, width), F32),
            pltpu.VMEM((1, width), F32),
            pltpu.VMEM((1, width), F32),
            pltpu.VMEM((n_chip, 1, width), F32),
            pltpu.VMEM((2, 1, width), F32),
            dma((10,)), dma((4 * n_far,)), dma((n_chip,)), dma((3,)), dma((4,)), dma((2,)),
        ] + [dma((9 * PARTS,)), dma((7 * PARTS,)), dma((8 * PARTS,)), dma((8 * PARTS,))] * 2 + [dma((4,))] * 2 + [dma((n_dev,))] * 6 + [dma] * 2 + [dma((n_dev,))] * 8
        out, gx, gw, gwo, gg = pl.pallas_call(
            functools.partial(block_kernel, n_dev, hd, kv_w, NEAR, PARTS),
            out_shape=(
                jax.ShapeDtypeStruct((tok, width), BF),
                jax.ShapeDtypeStruct((tok, width), BF),
                jax.ShapeDtypeStruct((n_rows, tok), F32),
                jax.ShapeDtypeStruct((hw, width), F32),
                jax.ShapeDtypeStruct((2, 1, width), F32),
            ),
            in_specs=[hbm] * 9,
            out_specs=(hbm,) * 5,
            scratch_shapes=scratch,
            compiler_params=pltpu.CompilerParams(collective_id=0, has_side_effects=True, vmem_limit_bytes=67043328),
            name='attn_block',
        )(
            x_act.reshape(tok, width), d_out.reshape(tok, width), positions.reshape(1, tok),
            ln_gain.reshape(1, width), ln_bias.reshape(1, width),
            flat_weight(w_query), flat_weight(w_key), flat_weight(w_value), w_out,
        )

        out, gx, gq, gk, gv, gwo, gain, bias = pl.pallas_call(
            functools.partial(settle_kernel, q_w, kv_w),
            out_shape=(
                jax.ShapeDtypeStruct((tok, width), BF),
                jax.ShapeDtypeStruct((tok, width), BF),
                jax.ShapeDtypeStruct((q_w, tok), F32),
                jax.ShapeDtypeStruct((kv_w, tok), F32),
                jax.ShapeDtypeStruct((kv_w, tok), F32),
                jax.ShapeDtypeStruct((hw, width), F32),
                jax.ShapeDtypeStruct((width,), F32),
                jax.ShapeDtypeStruct((width,), F32),
            ),
            in_specs=[hbm] * 5,
            out_specs=(hbm,) * 6 + (vmem,) * 2,
            scratch_shapes=[
                pltpu.VMEM((tok, width), BF),
                pltpu.VMEM((tok, width), BF),
                pltpu.VMEM((n_rows, tok), F32),
                pltpu.VMEM((hw, width), F32),
                pltpu.VMEM((2, 1, width), F32),
                dma((5,)), dma((6,)),
            ],
            name='settle',
        )(out, gx, gw, gwo, gg)

        def rows_out(block, heads):
            return jnp.transpose(block.reshape(heads, hd, tok), (2, 0, 1))

        return (
            out.reshape(1, tok, width), gx.reshape(1, tok, width),
            rows_out(gq, q_heads), rows_out(gk, kv_heads), rows_out(gv, kv_heads),
            gwo, gain, bias,
        )

    return jax.shard_map(device_step, mesh=mesh, in_specs=(P('dp', 'cp', None), P('dp', 'cp', None), P('dp', 'cp'), P(None), P(None), P(None, None, None), P(None, None, None), P(None, None, None), P(None, None)), out_specs=(P('dp', 'cp', None), P('dp', 'cp', None), P(('dp', 'cp'), None, None), P(('dp', 'cp'), None, None), P(('dp', 'cp'), None, None), P(('dp', 'cp'), None), P('dp'), P('dp')), check_vma=False)
```

```python
import functools
import math

import jax
import jax.numpy as jnp
from jax import lax
from jax.experimental import pallas as pl
from jax.experimental.pallas import tpu as pltpu
from jax.sharding import PartitionSpec as P

EPS = 1e-5
ROPE_BASE = 10000.0
MESH = pl.DeviceIdType.MESH
BF = jnp.bfloat16
F32 = jnp.float32
NEAR = 1
PARTS = 4
FIRST = 1
HELD = 8


def dot(lhs, rhs):
    return jnp.dot(lhs, rhs, preferred_element_type=F32)


def col_sum(val):
    return jnp.sum(val, axis=0, keepdims=True)


def col_max(val):
    return jnp.max(val, axis=0, keepdims=True)


def row_mean(val):
    return jnp.mean(val, axis=-1, keepdims=True)


def dot_t(lhs, rhs):
    return lax.dot_general(lhs, rhs, (((1,), (1,)), ((), ())), preferred_element_type=F32)


def block_kernel(
    n_dev, hd, kv_w, near, parts,
    x_hbm, dy_hbm, pos_hbm, gain_hbm, bias_hbm, wq_hbm, wk_hbm, wv_hbm, wo_hbm,
    out_hbm, gx_hbm, gw_hbm, gwo_hbm, gg_hbm,
    hb, dyb, wt, wi, woi, w_far, pos_all, trig,
    qt, kvt, kv, kvt_far, kv_far, bmat_far, stat_far, bmat, da_rv, sbuf, dpbuf, mbuf, adq, dkvt, kv_rv, kv_mine, kv_row,
    dwo, dwt, at_all, dq_all, at_rv, dt_rv, a_nat, d_nat, x_v, dy_own, gb_v, stat, out_v, gg_st, gg_mx, gg_my, gg_rv, gg_out,
    in_sem, far_sem, wo_sem, w_sem, out_sem, loc_sem,
    hzs, hzr, hds, hdr, yzs, yzr, yds, ydr,
    d_s, d_r, pos_s, pos_r, a_s, a_r, q_s, q_r, x_s, x_r, kv_s, kv_r, w_s, w_r, wk_s, wk_r, g_s, g_r,
):
    tok, width = x_v.shape
    n_chip = n_dev // 2
    pair = 2 * tok
    me = lax.axis_index('cp')
    chip = me // 2
    core = me % 2
    right = 2 * ((chip + 1) % n_chip) + core
    left = 2 * ((chip + n_chip - 1) % n_chip) + core
    mate = 2 * chip + 1 - core
    q_rows = wq_hbm.shape[0]
    n_rows = q_rows + 2 * kv_w
    hw = 2 * hd
    quarter = hd // 4
    tile = 256
    scale = hd ** -0.5
    cols_q = 2 * pair
    n_far = n_chip - 1 - 2 * near

    def remote(src, dst, send, recv, target):
        return pltpu.make_async_remote_copy(src_ref=src, dst_ref=dst, send_sem=send, recv_sem=recv, device_id={'cp': target}, device_id_type=MESH)

    def local(src, dst, sem):
        return pltpu.make_async_copy(src, dst, sem)

    def part_of(i, size):
        return pl.ds(pl.multiple_of(i * size, size), size)

    def once(cond):
        return pl.loop(0, jnp.where(cond, 1, 0))

    def ring_steps(k):
        step = (k + 1) // 2
        return step, k % 2

    def ring_origin(k):
        step, ahead = ring_steps(k)
        return jnp.where(ahead == 1, chip + n_chip - step, chip + step) % n_chip

    own = (chip, part_of(core, tok))
    first_loads = [
        local(x_hbm, x_v, in_sem.at[0]),
        local(gain_hbm, gb_v.at[0], in_sem.at[1]),
        local(bias_hbm, gb_v.at[1], in_sem.at[2]),
        local(pos_hbm, pos_all.at[me], in_sem.at[3]),
    ]
    for item in first_loads:
        item.start()
    barrier = pltpu.get_barrier_semaphore()
    for step in range(1, n_dev):
        pl.semaphore_signal(barrier, inc=1, device_id={'cp': (me + step) % n_dev}, device_id_type=MESH)
    own_rows = part_of(me, hw)
    kv_rows = part_of(chip, hd)
    loads = [
        local(wq_hbm.at[own_rows], wi.at[pl.ds(0, hw)], in_sem.at[4]),
        local(wk_hbm.at[kv_rows], wi.at[pl.ds(hw, hd)], in_sem.at[5]),
        local(wv_hbm.at[kv_rows], wi.at[pl.ds(hw + hd, hd)], in_sem.at[6]),
        local(wo_hbm.at[own_rows], woi, in_sem.at[7]),
        local(dy_hbm, dyb.at[own], in_sem.at[8]),
        local(dy_hbm, dy_own, in_sem.at[9]),
    ]
    far_loads = []
    for f in range(n_far):
        far_rows = part_of(ring_origin(2 * near + 1 + f), hd)
        loads.append(local(wk_hbm.at[far_rows], w_far.at[pl.ds(hw * f, hd)], far_sem.at[2 * f]))
        loads.append(local(wv_hbm.at[far_rows], w_far.at[pl.ds(hw * f + hd, hd)], far_sem.at[2 * f + 1]))
        far_wo = part_of(ring_origin(2 * near + 1 + f), 2 * hw)
        far_loads.append(local(wo_hbm.at[far_wo], wt.at[pl.ds(2 * hw * f, 2 * hw)], far_sem.at[2 * n_far + f]))
        far_loads.append(local(wq_hbm.at[far_wo], wt.at[pl.ds(2 * hw * (n_far + f), 2 * hw)], far_sem.at[3 * n_far + f]))
    for item in loads + far_loads:
        item.start()

    for item in first_loads:
        item.wait()
    gain_one = 1.0 + gb_v[0]
    block = 16

    @pl.loop(0, tok // block)
    def _(i):
        rows = part_of(i, block)
        x_f = x_v[rows, :].astype(F32)
        mean = row_mean(x_f)
        centered = x_f - mean
        inv_std = lax.rsqrt(row_mean(centered * centered) + EPS)
        hb[chip, part_of(core * (tok // block) + i, block), :] = (centered * inv_std * gain_one + gb_v[1]).astype(BF)
        stat[0, rows, :] = jnp.broadcast_to(mean, (block, 128))
        stat[1, rows, :] = jnp.broadcast_to(inv_std, (block, 128))

    pl.semaphore_wait(barrier, n_dev - 1)

    def chunk(buf, origin, parity, part):
        return buf.at[origin, part_of(parts * parity + part, tok // parts)]

    turns = 2 * parts

    def own_sends(buf, zs, zr, ds, dr):
        copies = []
        for part in range(parts):
            piece = chunk(buf, chip, core, part)
            copies.append(remote(piece, piece, zs.at[2 * part], zr.at[2 * part], right))
            copies.append(remote(piece, piece, zs.at[2 * part + 1], zr.at[2 * part + 1], left))
            copies.append(remote(piece, piece, ds.at[7 * parts + part], dr.at[7 * parts + part], mate))
        return copies

    def event_place(event):
        step = event // turns + 1
        turn = event % turns
        direction = turn % 2
        part = jnp.where(step < 4, turn // 2, turn // 2 + direction * (parts // 2))
        origin = jnp.where(direction == 0, chip + n_chip - step, chip + step) % n_chip
        return step, direction, part, origin

    def last_event(part, direction):
        return 6 * parts + 2 * (part - direction * (parts // 2)) + direction

    def ring_event(ring, event):
        buf, zs, zr, ds, dr = ring
        step, direction, part, origin = event_place(event)
        piece = chunk(buf, origin, core, part)
        remote(piece, piece, zs.at[0], zr.at[event], right).wait_recv()
        onward = jnp.where(step < 3, event + turns, last_event(part, direction))

        @pl.when((step < 3) | ((step == 3) & ((part >= parts // 2) == (direction == 1))))
        def _():
            remote(piece, piece, zs.at[event + turns], zr.at[onward], jnp.where(direction == 0, right, left)).start()

        remote(piece, piece, ds.at[event], dr.at[event], mate).start()

    def ring_service(ring, event):
        @pl.when(event < 7 * parts)
        def _():
            ring_event(ring, event)

    def ring_mate(ring, k, origin):
        buf, zs, zr, ds, dr = ring
        step, ahead = ring_steps(k)
        for part in range(parts):
            event = jnp.where(k == 0, 7 * parts + part, jnp.where(step < 4, turns * (step - 1) + 2 * part + 1 - ahead, last_event(part, part // (parts // 2))))
            piece = chunk(buf, origin, 1 - core, part)
            remote(piece, piece, ds.at[0], dr.at[event], mate).wait_recv()

    def finish_ring(ring):
        buf, zs, zr, ds, dr = ring
        for item in own_sends(*ring):
            item.wait_send()

        @pl.loop(0, 7 * parts)
        def _(event):
            step, direction, part, origin = event_place(event)
            piece = chunk(buf, origin, core, part)

            @pl.when((step < 3) | ((step == 3) & ((part >= parts // 2) == (direction == 1))))
            def _():
                remote(piece, piece, zs.at[event + turns], zr.at[event], right).wait_send()

            remote(piece, piece, ds.at[event], dr.at[event], mate).wait_send()

    h_ring = (hb, hzs, hzr, hds, hdr)
    y_ring = (dyb, yzs, yzr, yds, ydr)
    for item in own_sends(*h_ring):
        item.start()
    pos_sends = [remote(pos_all.at[me], pos_all.at[me], pos_s.at[step], pos_r.at[me], (me + step) % n_dev) for step in range(1, n_dev)]
    for item in pos_sends:
        item.start()
    weight_loads = [
        local(wq_hbm, wt.at[pl.ds(0, q_rows)], w_sem.at[0]),
        local(wk_hbm, wt.at[pl.ds(q_rows, kv_w)], w_sem.at[1]),
        local(wv_hbm, wt.at[pl.ds(q_rows + kv_w, kv_w)], w_sem.at[2]),
    ]
    dkvt[...] = jnp.zeros_like(dkvt)
    bmat[...] = jnp.zeros_like(bmat)
    bmat_far[...] = jnp.zeros_like(bmat_far)
    for f in range(n_far):
        stat_far[f, 0] = jnp.full((1, cols_q), -3e38, F32)
        stat_far[f, 1] = jnp.zeros((1, cols_q), F32)
        stat_far[f, 2] = jnp.zeros((1, cols_q), F32)

    freq = jnp.exp(lax.broadcasted_iota(jnp.int32, (quarter, tok), 0).astype(F32) * (-2.0 * math.log(ROPE_BASE) / (hd // 2)))

    def make_trig(b):
        for t in range(2):
            slot = 2 * b + t

            @pl.when(slot != me)
            def _():
                remote(pos_all.at[slot], pos_all.at[slot], pos_s.at[0], pos_r.at[slot], me).wait_recv()

            angle = pos_all[slot].astype(F32) * freq
            trig[b, 0:quarter, tok * t:tok * t + tok] = jnp.cos(angle)
            trig[b, quarter:2 * quarter, tok * t:tok * t + tok] = jnp.sin(angle)

    def turned(val, cos_t, sin_t):
        u = val[0:quarter]
        w = val[quarter:2 * quarter]
        return [u * cos_t - w * sin_t, w * cos_t + u * sin_t, val[2 * quarter:hd]]

    def eighth(val):
        return val.astype(BF) * jnp.asarray(scale, BF)

    def keys_values(val, cos_t, sin_t):
        return jnp.concatenate(turned(val[0:hd], cos_t, sin_t) + [val[hd:hw]], axis=0).astype(BF)

    lane = lax.broadcasted_iota(jnp.int32, (pair, cols_q), 1)
    row = lax.broadcasted_iota(jnp.int32, (pair, cols_q), 0)
    seen_far = row <= core * tok + lane % tok

    opposite = ring_origin(n_chip - 1)

    def opposite_send(head):
        block = bmat_far.at[n_far - 1, pl.ds(hd, hd), pl.ds(cols_q + tok * head, tok)]
        return remote(block, da_rv.at[2 * core + head % 2], d_s.at[head], d_r.at[2 * core + head % 2], 2 * opposite + head // 2)

    @pl.loop(0, n_chip)
    def _(k):
        for turn in range(parts):
            ring_service(h_ring, parts * k + turn)

        @once(k == 5)
        def _(_):
            for item in [opposite_send(head) for head in range(4)] + own_sends(*y_ring):
                item.start()

        @once(k == 0)
        def _(_):
            for item in loads:
                item.wait()

        b = ring_origin(k)
        ring_mate(h_ring, k, b)
        make_trig(b)

        @once(k == 0)
        def _(_):
            for item in far_loads:
                item.wait()
            cos_t = trig[chip, 0:quarter, part_of(core, tok)]
            sin_t = trig[chip, quarter:2 * quarter, part_of(core, tok)]

            @pl.loop(0, n_far)
            def _(f):
                da_t = dot_t(wt[part_of(f, 2 * hw), :], dy_own[...]).astype(BF)
                q_t = dot_t(wt[part_of(n_far + f, 2 * hw), :], hb[chip, part_of(core, tok), :])
                for head in range(4):
                    part = slice(hd * head, hd * head + hd)
                    at = tok * head
                    bmat_far[f, 0:hd, at:at + tok] = eighth(jnp.concatenate(turned(q_t[part], cos_t, sin_t), axis=0))
                    bmat_far[f, hd:hw, cols_q + at:cols_q + at + tok] = da_t[part]

            for item in weight_loads:
                item.start()

        place = part_of(b, pair)
        cos_t = trig[b, 0:quarter, :]
        sin_t = trig[b, quarter:2 * quarter, :]
        flat = dot_t(wi[...], hb[b])
        for head in range(2):
            q_rot = eighth(jnp.concatenate(turned(flat[hd * head:hd * head + hd], cos_t, sin_t), axis=0))
            for t in range(2):
                lane = pair * t + tok * head
                qt[b, :, lane:lane + tok] = q_rot[:, tok * t:tok * t + tok]
        kv_rot = keys_values(flat[hw:2 * hw], cos_t, sin_t)
        kvt[:, place] = kv_rot
        kv[place, :] = kv_rot.T

        @pl.when(b <= chip)
        def _():
            flat_far = dot_t(w_far[...], hb[b])
            for f in range(n_far):
                far_rot = keys_values(flat_far[hw * f:hw * f + hw], cos_t, sin_t)
                kvt_far[f, :, place] = far_rot
                kv_far[f, place, :] = far_rot.T

            @pl.loop(0, n_far)
            def _(f):
                both = dot(kv_far[f, place, :], bmat_far[f])
                s = jnp.where(seen_far | (k > 0), both[:, 0:cols_q], -1e30)
                old = stat_far[f, 0]
                new = jnp.maximum(old, col_max(s))
                p = jnp.exp(s - new)
                keep = jnp.exp(old - new)
                stat_far[f, 0] = new
                stat_far[f, 1] = stat_far[f, 1] * keep + col_sum(p)
                stat_far[f, 2] = stat_far[f, 2] * keep + col_sum(p * both[:, cols_q:2 * cols_q])

    groups = [slice(tile * g, tile * g + tile) for g in range(cols_q // tile)]

    def first_part(b, seen):
        def both_of(rows):
            both = dot(kv[rows, :], bmat[...])
            return both[:, 0:cols_q], both[:, cols_q:2 * cols_q]

        rows = part_of(b, pair)
        s, d_p = both_of(rows)
        s = jnp.where(seen, s, -1e30)
        top = col_max(s)
        p = jnp.exp(s - top)
        sbuf[rows, :] = p
        dpbuf[rows, :] = d_p
        mbuf[b] = top

        def step(c, state, chunks=1):
            old, total, weighted = state
            rows = part_of(c, chunks * pair)
            s, d_p = both_of(rows)
            new = jnp.maximum(old, col_max(s))
            p = jnp.exp(s - new)
            sbuf[rows, :] = p
            dpbuf[rows, :] = d_p
            for i in range(chunks):
                mbuf[chunks * c + i] = new
            keep = jnp.exp(old - new)
            return new, total * keep + col_sum(p), weighted * keep + col_sum(p * d_p)

        state = (top, col_sum(p), col_sum(p * d_p))
        state = lax.fori_loop(0, b // 2, functools.partial(step, chunks=2), state)
        top, total, weighted = lax.fori_loop(2 * (b // 2), b, step, state)
        inv = 1.0 / total
        return top, inv, weighted * inv

    def second_part(b, stats):
        top, inv, row_dot = stats
        adq[...] = jnp.zeros_like(adq)

        def step(c, carry):
            rows = part_of(c, pair)
            factor = jnp.exp(mbuf[c] - top) * inv
            d_k = d_v = None
            for at in groups:
                p = sbuf[rows, at] * factor[:, at]
                p_b = p.astype(BF)
                ds_b = (p * (dpbuf[rows, at] - row_dot[:, at])).astype(BF)
                adq[0:hd, at] += dot(kvt[0:hd, rows], ds_b)
                adq[hd:hw, at] += dot(kvt[hd:hw, rows], p_b)
                more_k = dot_t(bmat[0:hd, at], ds_b)
                more_v = dot_t(bmat[hd:hw, cols_q + at.start:cols_q + at.stop], p_b)
                d_k = more_k if d_k is None else d_k + more_k
                d_v = more_v if d_v is None else d_v + more_v
            dkvt[0:hd, rows] += d_k
            dkvt[hd:hw, rows] += d_v
            return carry

        lax.fori_loop(0, b + 1, step, 0)


    def send_rows(slot):
        cols = part_of(slot, tok)
        return [
            remote(dq_all.at[:, cols], dt_rv.at[own_rows], q_s.at[slot], q_r.at[me], slot),
            remote(at_all.at[:, cols], at_rv.at[own_rows], a_s.at[slot], a_r.at[me], slot),
        ]

    last = 6 * parts

    def serve(event):
        @pl.when(event < last)
        def _():
            ring_event(y_ring, event)

    @pl.loop(0, n_chip)
    def _(j):
        k = j - 1

        @pl.when(k == 0)
        def _():
            for turn in range(2):
                ring_event(y_ring, k + turn)

        @pl.when((k % 2 == 1) & (k > 0))
        def _():
            for turn in range(2, parts):
                serve(parts * k + turn)

        b = jnp.where(j == 0, opposite, ring_origin(jnp.maximum(k, 0)))

        @once(k == 1)
        def _(_):
            for item in weight_loads:
                item.wait()

        @pl.loop(0, jnp.where(j == n_chip - 1, 2 + 4 * near, 0))
        def _(early):
            slot = 2 * ring_origin(early // 2) + early % 2

            @pl.when(slot != me)
            def _():
                for item in send_rows(slot):
                    item.start()

        bmat[0:hd, 0:cols_q] = qt[b]

        @once(j == 0)
        def _(_):
            for i in range(4):
                remote(da_rv.at[i], da_rv.at[i], d_s.at[0], d_r.at[i], mate).wait_recv()
                bmat[hd:hw, cols_q + tok * i:cols_q + tok * i + tok] = da_rv[i]

        @once(j > 0)
        def _(_):
            ring_mate(y_ring, k, b)
            da_t = dot_t(woi[...], dyb[b]).astype(BF)
            for t in range(2):
                for head in range(2):
                    at = cols_q + pair * t + tok * head
                    bmat[hd:hw, at:at + tok] = da_t[hd * head:hd * head + hd, tok * t:tok * t + tok]

        stats = first_part(b, row <= (lane // pair) * tok + lane % tok)
        for turn in range(2):
            serve(jnp.where(k < 0, last, parts * k + 2 + 2 * (k % 2)) + turn)
        second_part(b, stats)
        for t in range(2):
            slot = 2 * b + t
            lanes = [slice(pair * t + tok * head, pair * t + tok * head + tok) for head in range(2)]
            a_t = jnp.concatenate([adq[hd:hw, at] for at in lanes], axis=0).astype(BF)
            cos_t = trig[b, 0:quarter, tok * t:tok * t + tok]
            sin_t = trig[b, quarter:2 * quarter, tok * t:tok * t + tok]
            dq_t = jnp.concatenate([piece for at in lanes for piece in turned(adq[0:hd, at] * scale, cos_t, -sin_t)], axis=0).astype(BF)
            at_all[:, part_of(slot, tok)] = a_t
            dq_all[:, part_of(slot, tok)] = dq_t

            @pl.when(slot == me)
            def _():
                at_rv[own_rows, :] = a_t
                dt_rv[own_rows, :] = dq_t

        @pl.when((k % 2 == 0) & (k >= 0))
        def _():
            for turn in range(2):
                serve(parts * j + turn)

    far = [ring_origin(k) for k in range(n_chip - 1, 0, -1)]
    targets = [2 * c + p for c in far for p in range(2)] + [mate]
    near_targets = targets[-1 - 4 * near:]
    swap = remote(dkvt.at[part_of(1 - core, hd)], kv_rv, x_s, x_r, mate)
    swap.start()
    w_sends = [remote(dwt.at[pl.ds(0, hw), part_of(t, tok)], gw_hbm.at[own_rows], w_s.at[t], w_r.at[me], t) for t in targets]

    def columns(rows_all, buf, cols):
        acc = jnp.zeros((rows_all.shape[0], tile), F32)
        for s in range(n_chip):
            acc += dot(rows_all[:, pair * s:pair * s + pair], buf[s, :, cols])
        return acc

    def q_columns(i):
        cols = part_of(far[i] if i < n_chip - 1 else chip, pair)
        dwt[0:hw, cols] = columns(dq_all, hb, cols)
        for item in w_sends[max(2 * i - 2, 0):2 * i]:
            item.start()

    for i in range(FIRST + 1):
        q_columns(i)

    swap.wait_recv()
    mine = part_of(core, hd)
    g_rows = pl.ds(pl.multiple_of(q_rows + core * kv_w + chip * hd, hd), hd)
    for t in range(n_chip):
        cols = slice(pair * t, pair * t + pair)
        g = dkvt[mine, cols] + kv_rv[:, cols]
        cos_t = jnp.where(core == 0, trig[t, 0:quarter, :], 1.0)
        sin_t = jnp.where(core == 0, trig[t, quarter:2 * quarter, :], 0.0)
        g_b = jnp.concatenate(turned(g, cos_t, -sin_t), axis=0).astype(BF)
        kv_mine[2 * t] = g_b[:, 0:tok]
        kv_mine[2 * t + 1] = g_b[:, tok:pair]
        kv_row[:, cols] = g_b
    dt_rv[g_rows, :] = kv_mine[me]
    kv_sends = [remote(kv_mine.at[t], dt_rv.at[g_rows], kv_s.at[t], kv_r.at[me], t) for t in targets]
    for item in kv_sends:
        item.start()
    for i in range(FIRST + 1, n_chip):
        q_columns(i)
    w_sends[-1].start()
    w_own = local(dwt.at[pl.ds(0, hw), part_of(me, tok)], gw_hbm.at[own_rows], loc_sem.at[0])
    w_own.start()
    for t in range(width // tile):
        cols = slice(tile * t, tile * t + tile)
        dwt[hw:hw + hd, cols] = columns(kv_row, hb, cols)
    wk_own = local(dwt.at[pl.ds(hw, hd), part_of(me, tok)], gw_hbm.at[g_rows], loc_sem.at[1])
    wk_own.start()
    wk_sends = [remote(dwt.at[pl.ds(hw, hd), part_of(t, tok)], gw_hbm.at[g_rows], wk_s.at[t], wk_r.at[me], t) for t in targets]
    for item in wk_sends[0:HELD]:
        item.start()

    @pl.loop(last, 7 * parts)
    def _(event):
        ring_event(y_ring, event)

    ring_mate(y_ring, n_chip - 1, opposite)
    for t in range(width // tile):
        cols = slice(tile * t, tile * t + tile)
        dwo[:, cols] = columns(at_all, dyb, cols)
    store_wo = local(dwo, gwo_hbm, out_sem.at[0])
    store_wo.start()
    finish_ring(y_ring)
    wo_loads = [local(wo_hbm.at[pl.ds(pair * t, pair)], dyb.at[t], wo_sem.at[t]) for t in range(n_chip)]
    for item in wo_loads:
        item.start()

    @pl.loop(0, n_far)
    def _(f):
        c_far = ring_origin(2 * near + 1 + f)
        cos_t = trig[chip, 0:quarter, part_of(core, tok)]
        sin_t = trig[chip, quarter:2 * quarter, part_of(core, tok)]
        top = stat_far[f, 0]
        inv = 1.0 / stat_far[f, 1]
        row_dot = stat_far[f, 2] * inv

        def add_chunk(c, diagonal, chunks=1):
            rows = part_of(c, chunks * pair)
            for at in groups:
                keys = kv_far[f, rows, :]
                s = dot(keys, bmat_far[f, :, at])
                d_p = dot(keys, bmat_far[f, :, cols_q + at.start:cols_q + at.stop])
                if diagonal:
                    s = jnp.where(seen_far[:, at], s, -1e30)
                p = jnp.exp(s - top[:, at]) * inv[:, at]
                p_b = p.astype(BF)
                ds_b = (p * (d_p - row_dot[:, at])).astype(BF)
                d_q = dot(kvt_far[f, 0:hd, rows], ds_b)
                d_a = dot(kvt_far[f, hd:hw, rows], p_b)
                adq[0:hd, at] = d_q if diagonal else adq[0:hd, at] + d_q
                adq[hd:hw, at] = d_a if diagonal else adq[hd:hw, at] + d_a

        add_chunk(chip, True)

        @pl.loop(0, chip // 2)
        def _(c):
            add_chunk(c, False, 2)

        @pl.when(chip % 2 == 1)
        def _():
            add_chunk(chip - 1, False)

        for head in range(4):
            at = slice(tok * head, tok * head + tok)
            place = pl.ds(pl.multiple_of(c_far * 2 * hw + hd * head, hd), hd)
            at_rv[place, :] = adq[hd:hw, at].astype(BF)
            dt_rv[place, :] = jnp.concatenate(turned(adq[0:hd, at] * scale, cos_t, -sin_t), axis=0).astype(BF)

    for t in near_targets:
        remote(at_all.at[:, pl.ds(0, tok)], at_rv.at[part_of(t, hw)], a_s.at[t], a_r.at[t], t).wait_recv()
    for item in wo_loads:
        item.wait()
    for t in range(q_rows // tok):
        a_nat[:, tok * t:tok * t + tok] = at_rv[tok * t:tok * t + tok, :].T
    for t in range(width // tile):
        cols = slice(tile * t, tile * t + tile)
        prod = jnp.zeros((tok, tile), F32)
        for s in range(n_chip):
            prod += dot(a_nat[:, pair * s:pair * s + pair], dyb[s, :, cols])
        out_v[:, cols] = (x_v[:, cols].astype(F32) + prod).astype(BF)
    store_out = local(out_v, out_hbm, out_sem.at[1])
    store_out.start()

    def kv_place(t):
        return pl.ds(pl.multiple_of(q_rows + (t % 2) * kv_w + (t // 2) * hd, hd), hd)

    for t in near_targets:
        remote(dq_all.at[:, pl.ds(0, tok)], dt_rv.at[part_of(t, hw)], q_s.at[t], q_r.at[t], t).wait_recv()
    for t in targets:
        remote(kv_mine.at[0], dt_rv.at[kv_place(t)], kv_s.at[t], kv_r.at[t], t).wait_recv()
    swap.wait_send()
    for t in range(n_rows // tok):
        d_nat[:, tok * t:tok * t + tok] = dt_rv[tok * t:tok * t + tok, :].T

    mean = stat[0, :, 0:1]
    inv_std = stat[1, :, 0:1]
    dh = dkvt
    for t in range(width // tile):
        cols = slice(tile * t, tile * t + tile)
        acc = jnp.zeros((tok, tile), F32)
        for s in range(n_rows // tile):
            acc += dot(d_nat[:, tile * s:tile * s + tile], wt[tile * s:tile * s + tile, cols])
        dh[:, cols] = acc
        gg_st[0, :, cols] = col_sum(acc * ((x_v[:, cols].astype(F32) - mean) * inv_std))
        gg_st[1, :, cols] = col_sum(acc)
    g_swap = remote(gg_st.at[1 - core], gg_mx, g_s.at[n_chip], g_r.at[n_chip], mate)
    g_swap.start()
    g_swap.wait_recv()
    gg_my[...] = jnp.where(core == 0, gg_st[0], gg_st[1]) + gg_mx[...]
    gg_rv[chip] = gg_my[...]
    g_sends = [remote(gg_my, gg_rv.at[chip], g_s.at[c], g_r.at[chip], 2 * c + core) for c in far]
    for item in g_sends + wk_sends[HELD:]:
        item.start()

    grad_hat = dh[...] * gain_one
    x_hat = (x_v[...].astype(F32) - mean) * inv_std
    mean_one = row_mean(grad_hat)
    mean_two = row_mean(grad_hat * x_hat)
    store_out.wait()
    out_v[...] = (dy_own[...].astype(F32) + inv_std * (grad_hat - mean_one - x_hat * mean_two)).astype(BF)
    store_gx = local(out_v, gx_hbm, out_sem.at[2])
    store_gx.start()

    for c in far:
        remote(gg_my, gg_rv.at[c], g_s.at[c], g_r.at[c], 2 * c + core).wait_recv()
    sums = gg_rv[0]
    for c in range(1, n_chip):
        sums = sums + gg_rv[c]
    gg_out[core] = sums
    g_swap_out = remote(gg_out.at[core], gg_out.at[core], g_s.at[n_chip + 1], g_r.at[n_chip + 1], mate)
    g_swap_out.start()
    remote(gg_out.at[core], gg_out.at[1 - core], g_s.at[n_chip + 1], g_r.at[n_chip + 1], mate).wait_recv()
    store_gg = local(gg_out, gg_hbm, out_sem.at[3])
    store_gg.start()

    finish_ring(h_ring)
    for item in pos_sends + [g_swap, g_swap_out] + [opposite_send(head) for head in range(4)]:
        item.wait_send()
    for t in near_targets:
        remote(at_all.at[:, pl.ds(0, tok)], at_rv.at[pl.ds(0, hw)], a_s.at[t], a_r.at[t], t).wait_send()
        remote(dq_all.at[:, pl.ds(0, tok)], dt_rv.at[pl.ds(0, hw)], q_s.at[t], q_r.at[t], t).wait_send()
    for item in kv_sends + w_sends + g_sends + wk_sends:
        item.wait_send()
    for t in targets:
        remote(dwt.at[pl.ds(0, hw), part_of(t, tok)], gw_hbm.at[part_of(t, hw)], w_s.at[t], w_r.at[t], t).wait_recv()
        remote(dwt.at[pl.ds(hw, hd), part_of(t, tok)], gw_hbm.at[kv_place(t)], wk_s.at[t], wk_r.at[t], t).wait_recv()
    for item in (w_own, wk_own, store_wo, store_gx, store_gg):
        item.wait()


def settle_kernel(q_rows, kv_w, out_i, gx_i, gw_i, gwo_i, gg_i, out_o, gx_o, gq_o, gk_o, gv_o, gwo_o, gain_o, bias_o, b_act, b_q, b_kv, b_o, b_gg, sem_in, sem_out, sem_gg):
    half_q = q_rows // 2
    half_o = gwo_i.shape[0] // 2
    moves = [(out_i, b_act.at[0], out_o), (gx_i, b_act.at[1], gx_o)]
    for t in range(2):
        moves.append((gw_i.at[pl.ds(half_q * t, half_q)], b_q.at[t], gq_o.at[pl.ds(half_q * t, half_q)]))
        moves.append((gwo_i.at[pl.ds(half_o * t, half_o)], b_o.at[t], gwo_o.at[pl.ds(half_o * t, half_o)]))
    moves.append((gw_i.at[pl.ds(q_rows, kv_w)], b_kv.at[0], gk_o))
    moves.append((gw_i.at[pl.ds(q_rows + kv_w, kv_w)], b_kv.at[1], gv_o))
    loads = [pltpu.make_async_copy(src, mid, sem_in.at[i]) for i, (src, mid, _) in enumerate(moves)]
    stores = [pltpu.make_async_copy(mid, dst, sem_out.at[i]) for i, (_, mid, dst) in enumerate(moves)]
    load_gg = pltpu.make_async_copy(gg_i, b_gg, sem_gg)
    load_gg.start()
    for item in loads:
        item.start()
    for load, store in zip(loads, stores):
        load.wait()
        store.start()
    load_gg.wait()
    gain_o[...] = b_gg[0, 0]
    bias_o[...] = b_gg[1, 0]
    for item in stores:
        item.wait()


def solution(mesh):
    n_dev = mesh.shape['cp']

    def device_step(x_act, d_out, positions, ln_gain, ln_bias, w_query, w_key, w_value, w_out):
        tok, width = x_act.shape[1], x_act.shape[2]
        q_heads, hd = w_query.shape[1], w_query.shape[2]
        kv_heads = w_key.shape[1]
        q_w, kv_w = q_heads * hd, kv_heads * hd
        n_rows = q_w + 2 * kv_w
        seq = n_dev * tok
        hw = 2 * hd

        def flat_weight(w):
            return jnp.transpose(w, (1, 2, 0)).reshape(-1, width)

        hbm = pl.BlockSpec(memory_space=pltpu.HBM)
        vmem = pl.BlockSpec(memory_space=pltpu.VMEM)
        dma = pltpu.SemaphoreType.DMA
        n_chip = n_dev // 2
        n_far = n_chip - 1 - 2 * NEAR
        pair = 2 * tok
        scratch = [
            pltpu.VMEM((n_chip, pair, width), BF),
            pltpu.VMEM((n_chip, pair, width), BF),
            pltpu.VMEM((n_rows, width), BF),
            pltpu.VMEM((2 * hw, width), BF),
            pltpu.VMEM((hw, width), BF),
            pltpu.VMEM((n_far * hw, width), BF),
            pltpu.VMEM((n_dev, 1, tok), jnp.int32),
            pltpu.VMEM((n_chip, hd // 2, pair), F32),
            pltpu.VMEM((n_chip, hd, 2 * pair), BF),
            pltpu.VMEM((hw, seq), BF),
            pltpu.VMEM((seq, hw), BF),
            pltpu.VMEM((n_far, hw, seq), BF),
            pltpu.VMEM((n_far, seq, hw), BF),
            pltpu.VMEM((n_far, hw, 4 * pair), BF),
            pltpu.VMEM((n_far, 3, 1, 2 * pair), F32),
            pltpu.VMEM((hw, 4 * pair), BF),
            pltpu.VMEM((4, hd, tok), BF),
            pltpu.VMEM((seq, 2 * pair), F32),
            pltpu.VMEM((seq, 2 * pair), F32),
            pltpu.VMEM((n_chip, 1, 2 * pair), F32),
            pltpu.VMEM((hw, 2 * pair), F32),
            pltpu.VMEM((hw, seq), F32),
            pltpu.VMEM((hd, seq), F32),
            pltpu.VMEM((n_dev, hd, tok), BF),
            pltpu.VMEM((hd, seq), BF),
            pltpu.VMEM((hw, width), F32),
            pltpu.VMEM((hw + hd, width), F32),
            pltpu.VMEM((hw, seq), BF),
            pltpu.VMEM((hw, seq), BF),
            pltpu.VMEM((q_w, tok), BF),
            pltpu.VMEM((n_rows, tok), BF),
            pltpu.VMEM((tok, q_w), BF),
            pltpu.VMEM((tok, n_rows), BF),
            pltpu.VMEM((tok, width), BF),
            pltpu.VMEM((tok, width), BF),
            pltpu.VMEM((2, 1, width), F32),
            pltpu.VMEM((2, tok, 128), F32),
            pltpu.VMEM((tok, width), BF),
            pltpu.VMEM((2, 1, width), F32),
            pltpu.VMEM((1, width), F32),
            pltpu.VMEM((1, width), F32),
            pltpu.VMEM((n_chip, 1, width), F32),
            pltpu.VMEM((2, 1, width), F32),
            dma((10,)), dma((4 * n_far,)), dma((n_chip,)), dma((3,)), dma((4,)), dma((2,)),
        ] + [dma((9 * PARTS,)), dma((7 * PARTS,)), dma((8 * PARTS,)), dma((8 * PARTS,))] * 2 + [dma((4,))] * 2 + [dma((n_dev,))] * 6 + [dma] * 2 + [dma((n_dev,))] * 8
        out, gx, gw, gwo, gg = pl.pallas_call(
            functools.partial(block_kernel, n_dev, hd, kv_w, NEAR, PARTS),
            out_shape=(
                jax.ShapeDtypeStruct((tok, width), BF),
                jax.ShapeDtypeStruct((tok, width), BF),
                jax.ShapeDtypeStruct((n_rows, tok), F32),
                jax.ShapeDtypeStruct((hw, width), F32),
                jax.ShapeDtypeStruct((2, 1, width), F32),
            ),
            in_specs=[hbm] * 9,
            out_specs=(hbm,) * 5,
            scratch_shapes=scratch,
            compiler_params=pltpu.CompilerParams(collective_id=0, has_side_effects=True, vmem_limit_bytes=67043328),
            name='attn_block',
        )(
            x_act.reshape(tok, width), d_out.reshape(tok, width), positions.reshape(1, tok),
            ln_gain.reshape(1, width), ln_bias.reshape(1, width),
            flat_weight(w_query), flat_weight(w_key), flat_weight(w_value), w_out,
        )

        out, gx, gq, gk, gv, gwo, gain, bias = pl.pallas_call(
            functools.partial(settle_kernel, q_w, kv_w),
            out_shape=(
                jax.ShapeDtypeStruct((tok, width), BF),
                jax.ShapeDtypeStruct((tok, width), BF),
                jax.ShapeDtypeStruct((q_w, tok), F32),
                jax.ShapeDtypeStruct((kv_w, tok), F32),
                jax.ShapeDtypeStruct((kv_w, tok), F32),
                jax.ShapeDtypeStruct((hw, width), F32),
                jax.ShapeDtypeStruct((width,), F32),
                jax.ShapeDtypeStruct((width,), F32),
            ),
            in_specs=[hbm] * 5,
            out_specs=(hbm,) * 6 + (vmem,) * 2,
            scratch_shapes=[
                pltpu.VMEM((2, tok, width), BF),
                pltpu.VMEM((2, q_w // 2, tok), F32),
                pltpu.VMEM((2, kv_w, tok), F32),
                pltpu.VMEM((2, hw // 2, width), F32),
                pltpu.VMEM((2, 1, width), F32),
                dma((8,)), dma((8,)), dma,
            ],
            name='settle',
        )(out, gx, gw, gwo, gg)

        def rows_out(block, heads):
            return jnp.transpose(block.reshape(heads, hd, tok), (2, 0, 1))

        return (
            out.reshape(1, tok, width), gx.reshape(1, tok, width),
            rows_out(gq, q_heads), rows_out(gk, kv_heads), rows_out(gv, kv_heads),
            gwo, gain, bias,
        )

    return jax.shard_map(device_step, mesh=mesh, in_specs=(P('dp', 'cp', None), P('dp', 'cp', None), P('dp', 'cp'), P(None), P(None), P(None, None, None), P(None, None, None), P(None, None, None), P(None, None)), out_specs=(P('dp', 'cp', None), P('dp', 'cp', None), P(('dp', 'cp'), None, None), P(('dp', 'cp'), None, None), P(('dp', 'cp'), None, None), P(('dp', 'cp'), None), P('dp'), P('dp')), check_vma=False)
```
